32 devices in a mesh: vp: 4 (over z), dp: 8 (over y, x, core).
Axes of the slice: x: 2, y: 2, z: 4, core: 2. Of those that a mesh axis runs over, the one named last changes fastest.
Arguments:
- hidden: bfloat16 [128, 512, 1024], P('dp')
- mask_pos: int32 [128, 77], P('dp')
- labels: int32 [128, 77], P('dp')
- w_trans: bfloat16 [1024, 1024], replicated
- b_trans: float32 [1024], replicated
- ln_gain: float32 [1024], replicated
- ln_bias: float32 [1024], replicated
- emb_table: bfloat16 [50304, 1024], P('vp')
- b_vocab: float32 [50304], P('vp')
Outputs:
- output 1: float32 [], replicated
- output 2: bfloat16 [128, 512, 1024], P('dp')
- output 3: float32 [1024, 1024], replicated
- output 4: float32 [1024], replicated
- output 5: float32 [1024], replicated
- output 6: float32 [1024], replicated
- output 7: float32 [50304, 1024], P('vp')
- output 8: float32 [50304], P('vp')
All inputs are finite; a program needn't handle non-finite values.
Results may differ from the reference program's by a relative error of at most 0.0106996.
Values sent between devices are 32-bit elements.
A program may use at most 1 GiB of HBM per device.

```python
import jax
import jax.numpy as jnp
from jax import lax

HIDDEN = 1024
VOCAB_PAD = 50304
VOCAB_REAL = 50265
SEQ_LEN = 512
N_MASKS = 77
BATCH_ALL = 128
SHARDS = 4
LOG_VOCAB = (VOCAB_REAL - 1).bit_length()
LN_EPS = 1e-5
PAD_BIAS = -1.0e9


def head_norm(pre_act, ln_gain, ln_bias):
    gelu_out = jax.nn.gelu(pre_act, approximate=False)
    row_mean = jnp.mean(gelu_out, axis=-1, keepdims=True)
    centered = gelu_out - row_mean
    row_var = jnp.mean(centered * centered, axis=-1, keepdims=True)
    return centered * lax.rsqrt(row_var + LN_EPS) * ln_gain + ln_bias


def setup_inputs(seed: int = 0) -> dict:
    sub_keys = jax.random.split(jax.random.key(seed), 12)
    hidden = jax.random.normal(sub_keys[0], (BATCH_ALL, SEQ_LEN, HIDDEN), jnp.float32).astype(jnp.bfloat16)

    def draw_row(row_key):
        return jax.random.permutation(row_key, SEQ_LEN)[:N_MASKS]

    mask_pos = jax.vmap(draw_row)(jax.random.split(sub_keys[1], BATCH_ALL)).astype(jnp.int32)
    label_exp = jax.random.randint(sub_keys[2], (BATCH_ALL, N_MASKS), 0, LOG_VOCAB + 1)
    label_top = jnp.minimum(jnp.left_shift(jnp.ones_like(label_exp), label_exp), VOCAB_REAL)
    labels = jax.random.randint(sub_keys[3], (BATCH_ALL, N_MASKS), 0, label_top)
    labels = labels.at[0, 0].set(VOCAB_REAL - 1).astype(jnp.int32)
    w_trans = (jax.random.normal(sub_keys[4], (HIDDEN, HIDDEN), jnp.float32) * HIDDEN ** -0.5).astype(jnp.bfloat16)
    b_trans = 0.5 * jax.random.normal(sub_keys[5], (HIDDEN,), jnp.float32)
    ln_gain = 1.0 + 0.3 * jax.random.normal(sub_keys[6], (HIDDEN,), jnp.float32)
    ln_bias = 0.3 * jax.random.normal(sub_keys[7], (HIDDEN,), jnp.float32)
    emb_table = (jax.random.normal(sub_keys[8], (VOCAB_PAD, HIDDEN), jnp.float32) * HIDDEN ** -0.5).astype(jnp.bfloat16)
    bias_slope = jax.random.uniform(sub_keys[9], (), jnp.float32, 0.3, 0.6)
    bias_noise = jax.random.normal(sub_keys[10], (VOCAB_PAD,), jnp.float32)
    vocab_ids = jnp.arange(VOCAB_PAD)
    b_vocab = 0.5 * bias_noise - bias_slope * jnp.log1p(vocab_ids.astype(jnp.float32))
    b_vocab = jnp.where(vocab_ids < VOCAB_REAL, b_vocab, PAD_BIAS).astype(jnp.float32)
    return {"hidden": hidden, "mask_pos": mask_pos, "labels": labels, "w_trans": w_trans, "b_trans": b_trans, "ln_gain": ln_gain, "ln_bias": ln_bias, "emb_table": emb_table, "b_vocab": b_vocab}


def reference(hidden, mask_pos, labels, w_trans, b_trans, ln_gain, ln_bias, emb_table, b_vocab):
    n_rows = hidden.shape[0]
    n_tokens = n_rows * N_MASKS
    shard_rows = VOCAB_PAD // SHARDS
    masked_h = jnp.take_along_axis(hidden, mask_pos[:, :, None], axis=1).reshape(n_tokens, HIDDEN)
    pre_act = jnp.dot(masked_h, w_trans, preferred_element_type=jnp.float32) + b_trans
    u_norm, head_vjp = jax.vjp(head_norm, pre_act, ln_gain, ln_bias)
    u_bf16 = u_norm.astype(jnp.bfloat16)
    flat_labels = labels.reshape(n_tokens)
    emb_blocks = emb_table.reshape(SHARDS, shard_rows, HIDDEN)
    bias_blocks = b_vocab.reshape(SHARDS, shard_rows)
    row_starts = jnp.arange(SHARDS) * shard_rows
    row_ids = jnp.arange(shard_rows)

    def block_logits(emb_block, bias_block):
        return jnp.dot(u_bf16, emb_block.T, preferred_element_type=jnp.float32) + bias_block

    def block_stats(block):
        emb_block, bias_block, row_start = block
        logits = block_logits(emb_block, bias_block)
        local_max = jnp.max(logits, axis=1)
        local_sum = jnp.sum(jnp.exp(logits - local_max[:, None]), axis=1)
        is_label = (flat_labels - row_start)[:, None] == row_ids[None, :]
        label_logit = jnp.sum(jnp.where(is_label, logits, 0.0), axis=1)
        return local_max, local_sum, label_logit

    block_max, block_sum, block_label = lax.map(block_stats, (emb_blocks, bias_blocks, row_starts))
    global_max = jnp.max(block_max, axis=0)
    log_norm = global_max + jnp.log(jnp.sum(block_sum * jnp.exp(block_max - global_max), axis=0))
    mlm_loss = jnp.mean(log_norm - jnp.sum(block_label, axis=0))

    def block_grads(block):
        emb_block, bias_block, row_start = block
        logits = block_logits(emb_block, bias_block)
        is_label = (flat_labels - row_start)[:, None] == row_ids[None, :]
        d_logits = (jnp.exp(logits - log_norm[:, None]) - is_label.astype(jnp.float32)) / n_tokens
        d_logits_bf = d_logits.astype(jnp.bfloat16)
        d_emb_block = jnp.dot(d_logits_bf.T, u_bf16, preferred_element_type=jnp.float32)
        du_part = jnp.dot(d_logits_bf, emb_block, preferred_element_type=jnp.float32).astype(jnp.bfloat16)
        return d_emb_block, jnp.sum(d_logits, axis=0), du_part

    d_emb_blocks, d_bias_blocks, du_parts = lax.map(block_grads, (emb_blocks, bias_blocks, row_starts))
    d_unorm = jnp.sum(du_parts.astype(jnp.float32), axis=0)
    d_pre, d_ln_gain, d_ln_bias = head_vjp(d_unorm)
    d_pre_bf = d_pre.astype(jnp.bfloat16)
    d_w_trans = jnp.dot(masked_h.T, d_pre_bf, preferred_element_type=jnp.float32)
    d_b_trans = jnp.sum(d_pre, axis=0)
    d_masked = jnp.dot(d_pre_bf, w_trans.T, preferred_element_type=jnp.float32).astype(jnp.bfloat16)
    row_index = jnp.arange(n_rows)[:, None]
    d_hidden = jnp.zeros_like(hidden).at[row_index, mask_pos].set(d_masked.reshape(n_rows, N_MASKS, HIDDEN))
    return (mlm_loss, d_hidden, d_w_trans, d_b_trans, d_ln_gain, d_ln_bias, d_emb_blocks.reshape(VOCAB_PAD, HIDDEN), d_bias_blocks.reshape(VOCAB_PAD))
```

```python
import functools

import jax
import jax.numpy as jnp
from jax import lax
from jax.experimental import pallas as pl
from jax.experimental.pallas import tpu as pltpu
from jax.sharding import PartitionSpec as P

F32, BF16, I32 = jnp.float32, jnp.bfloat16, jnp.int32
NT = (((1,), (1,)), ((), ()))
NN = (((1,), (0,)), ((), ()))
VB = 1024
SUB = 256
VMEM_LIMIT = 60 << 20
CH = 16


def row_cuts(rows, parts=4):
    cuts = [16 * (rows // 16 * k // parts) for k in range(parts)] + [rows]
    return list(zip(cuts[:-1], cuts[1:]))


def dot(a, b, dims):
    return lax.dot_general(a, b, dims, preferred_element_type=F32)


def stats_kernel(n_vocab, u_ref, emb_ref, b_ref, lab_ref, logits_ref, m_ref, s_ref, l_ref, m_sc, s_sc, l_sc):
    i, n_blocks = pl.program_id(0), pl.num_programs(0)
    lane = lax.broadcasted_iota(I32, (1, 128), 1)

    @pl.when(i == 0)
    def _():
        m_sc[...] = jnp.full_like(m_sc, -jnp.inf)
        s_sc[...] = jnp.zeros_like(s_sc)
        l_sc[...] = jnp.zeros_like(l_sc)

    def run(width):
        wide = -(-width // 128) * 128
        for r0, r1 in row_cuts(u_ref.shape[0]):
            tile = dot(u_ref[r0:r1, :], emb_ref[:wide, :], NT) + b_ref[:, :wide]
            if wide > width:
                tile = jnp.where(lax.broadcasted_iota(I32, (1, wide), 1) < width, tile, -jnp.inf)
            logits_ref[r0:r1, :wide] = tile
            for q in range(r0, r1, CH):
                rs = slice(q, min(q + CH, r1))
                parts = [logits_ref[rs, k:k + 128] for k in range(0, wide, 128)]
                m_old = m_sc[rs, :]
                m_new = functools.reduce(jnp.maximum, parts, m_old)
                s_new = s_sc[rs, :] * jnp.exp(m_old - m_new)
                l_new = l_sc[rs, :]
                lab = lab_ref[rs, :] - i * VB
                for k, part in enumerate(parts):
                    s_new += jnp.exp(part - m_new)
                    l_new = jnp.where(lab == lane + k * 128, part, l_new)
                m_sc[rs, :], s_sc[rs, :], l_sc[rs, :] = m_new, s_new, l_new

    tail = n_vocab % VB
    if tail:
        pl.when(i < n_blocks - 1)(functools.partial(run, VB))
        pl.when(i == n_blocks - 1)(functools.partial(run, tail))
    else:
        run(VB)

    @pl.when(i == n_blocks - 1)
    def _():
        m_all = jnp.max(m_sc[...], axis=1, keepdims=True)
        m_ref[...] = m_all
        s_ref[...] = jnp.sum(s_sc[...] * jnp.exp(m_sc[...] - m_all), axis=1, keepdims=True)
        l_ref[...] = jnp.sum(l_sc[...], axis=1, keepdims=True)


def stats(u, emb, bias, lab):
    t, e = u.shape
    v = emb.shape[0]
    n = pl.cdiv(v, VB)
    col = jax.ShapeDtypeStruct((t, 1), F32)
    whole = lambda *s: pl.BlockSpec(s, lambda i: (0,) * len(s))
    return pl.pallas_call(
        functools.partial(stats_kernel, v),
        grid=(n,),
        in_specs=[whole(t, e), pl.BlockSpec((VB, e), lambda i: (i, 0)), pl.BlockSpec((1, VB), lambda i: (0, i)), whole(t, 128)],
        out_specs=[pl.BlockSpec((t, VB), lambda i: (0, i)), whole(t, 1), whole(t, 1), whole(t, 1)],
        out_shape=[jax.ShapeDtypeStruct((t, v), F32), col, col, col],
        scratch_shapes=[pltpu.VMEM((t, 128), F32)] * 3,
        compiler_params=pltpu.CompilerParams(dimension_semantics=("arbitrary",), vmem_limit_bytes=VMEM_LIMIT),
        cost_estimate=pl.CostEstimate(flops=2 * t * v * e, bytes_accessed=t * v * 4 + v * e * 2, transcendentals=t * v),
        name="stats",
    )(u, emb, bias, lab)


def du_kernel(n_vocab, scale, logits_ref, emb_ref, lse_ref, lab_ref, du_ref, db_ref, g_sc, db_sc):
    i, n_blocks = pl.program_id(0), pl.num_programs(0)
    t = logits_ref.shape[0]
    lane = lax.broadcasted_iota(I32, (1, 128), 1)

    @pl.when(i == 0)
    def _():
        du_ref[...] = jnp.zeros_like(du_ref)

    def run(width):
        wide = -(-width // 128) * 128
        emb = emb_ref[:wide, :]
        if wide > width:
            emb = jnp.where(lax.broadcasted_iota(I32, (wide, 1), 0) < width, emb, jnp.zeros_like(emb))
        for r0, r1 in row_cuts(t):
            sums = [None] * (wide // 128)
            for q in range(r0, r1, 16):
                rs = slice(q, q + 16)
                lse = lse_ref[rs, :]
                lab = lab_ref[rs, :] - i * VB
                for k in range(wide // 128):
                    c = k * 128
                    g = jnp.exp(logits_ref[rs, c:c + 128] - lse)
                    g -= jnp.where(lab == lane + c, scale, 0.0)
                    if c + 128 > width:
                        g = jnp.where(lane < width - c, g, 0.0)
                    part = g[:8] + g[8:]
                    sums[k] = part if sums[k] is None else sums[k] + part
                    g_sc[rs, c:c + 128] = g.astype(BF16)
            for k in range(wide // 128):
                cs = slice(k * 128, (k + 1) * 128)
                db_sc[:, cs] = sums[k] if r0 == 0 else db_sc[:, cs] + sums[k]
            du_ref[r0:r1, :] += dot(g_sc[r0:r1, :wide], emb, NN)
        db_ref[:, :wide] = jnp.sum(db_sc[:, :wide], axis=0, keepdims=True)

    tail = n_vocab % VB
    if tail:
        pl.when(i < n_blocks - 1)(functools.partial(run, VB))
        pl.when(i == n_blocks - 1)(functools.partial(run, tail))
    else:
        run(VB)

    @pl.when(i == n_blocks - 1)
    def _():
        du_ref[...] = du_ref[...].astype(BF16).astype(F32)


def du_pass(scale, logits, emb, lse, lab):
    t, v = logits.shape
    e = emb.shape[1]
    n = pl.cdiv(v, VB)
    whole = lambda *s: pl.BlockSpec(s, lambda i: (0,) * len(s))
    return pl.pallas_call(
        functools.partial(du_kernel, v, scale),
        grid=(n,),
        in_specs=[pl.BlockSpec((t, VB), lambda i: (0, i)), pl.BlockSpec((VB, e), lambda i: (i, 0)), whole(t, 128), whole(t, 128)],
        out_specs=[whole(t, e), pl.BlockSpec((1, VB), lambda i: (0, i))],
        out_shape=[jax.ShapeDtypeStruct((t, e), F32), jax.ShapeDtypeStruct((1, v), F32)],
        scratch_shapes=[pltpu.VMEM((t, VB), BF16), pltpu.VMEM((8, VB), F32)],
        compiler_params=pltpu.CompilerParams(dimension_semantics=("arbitrary",), vmem_limit_bytes=VMEM_LIMIT),
        cost_estimate=pl.CostEstimate(flops=2 * t * v * e, bytes_accessed=t * v * 4 + v * e * 2, transcendentals=t * v),
        name="du_pass",
    )(logits, emb, lse, lab)


TB = 1408


def rows_kernel(n_tok, scale, m, n_pieces, first, pos, emb_hbm, u_ref, bias_ref, lse_ref, lab_ref, *rest):
    rest = list(rest)
    if not first:
        rest.pop(0)
    pieces = [rest.pop(0) for _ in range(n_pieces)]
    out_ref, big_ref, emb_sc, g_sc, hold, sem, in_sem, out_sem = rest
    i, n_blocks = pl.program_id(0), pl.num_programs(0)
    row = lambda j: pl.multiple_of(pos[j], 8)
    sizes = [p.shape[0] for p in pieces]
    loads = [pltpu.make_async_copy(p, hold.at[j, :n, :], in_sem.at[j]) for j, (p, n) in enumerate(zip(pieces, sizes))]
    stores = [pltpu.make_async_copy(hold.at[j, :n, :], big_ref.at[pl.ds(row(3 + j), n), :], out_sem.at[j]) for j, n in enumerate(sizes)]

    @pl.when(i == 0)
    def _():
        cp = pltpu.make_async_copy(emb_hbm.at[pl.ds(row(0), m), :], emb_sc, sem)
        cp.start()
        for c in loads:
            c.start()
        out_ref[...] = jnp.zeros_like(out_ref)
        cp.wait()

    @pl.when(i == 2)
    def _():
        for a, b in zip(loads, stores):
            a.wait()
            b.start()

    mm = m // 16 * 8
    u = u_ref[...]
    for r0, r1 in ((0, mm), (mm, m)):
        rs = slice(r0, r1)
        part = dot(emb_sc[rs, :], u, NT)
        hit = lab_ref[...] == lax.broadcasted_iota(I32, (r1 - r0, 1), 0) + (pos[1] + r0)
        g = jnp.exp(part + bias_ref[rs, :] - lse_ref[...]) - jnp.where(hit, scale, 0.0)
        g_sc[rs, :] = g.astype(BF16)
        out_ref[rs, :] += dot(g_sc[rs, :], u, NN)

    @pl.when(i == n_blocks - 1)
    def _():
        own = pltpu.make_async_copy(out_ref, big_ref.at[pl.ds(row(2), m), :], sem)
        own.start()
        for b in stores:
            b.wait()
        own.wait()


def rows_pass(scale, v_rows, m, pos, emb, u, bias, lse, lab, big, pieces):
    t, e = u.shape
    first = big is None
    extra = ([] if first else [big]) + pieces
    any_spec = pl.BlockSpec(memory_space=pl.ANY)
    n_hold = max(1, len(pieces))
    gs = pltpu.PrefetchScalarGridSpec(
        num_scalar_prefetch=1,
        grid=(t // TB,),
        in_specs=[
            any_spec,
            pl.BlockSpec((TB, e), lambda i, s: (i, 0)),
            pl.BlockSpec((m, 1), lambda i, s: (0, 0)),
            pl.BlockSpec((1, TB), lambda i, s: (0, i)),
            pl.BlockSpec((1, TB), lambda i, s: (0, i)),
        ] + [any_spec] * len(extra),
        out_specs=[pl.BlockSpec((m, e), lambda i, s: (0, 0)), any_spec],
        scratch_shapes=[
            pltpu.VMEM((m, e), BF16),
            pltpu.VMEM((m, TB), BF16),
            pltpu.VMEM((n_hold, max([p.shape[0] for p in pieces] + [8]), e), F32),
            pltpu.SemaphoreType.DMA,
            pltpu.SemaphoreType.DMA((n_hold,)),
            pltpu.SemaphoreType.DMA((n_hold,)),
        ],
    )
    return pl.pallas_call(
        functools.partial(rows_kernel, t, scale, m, len(pieces), first),
        grid_spec=gs,
        out_shape=[jax.ShapeDtypeStruct((m, e), F32), jax.ShapeDtypeStruct((v_rows, e), F32)],
        input_output_aliases={} if first else {6: 1},
        compiler_params=pltpu.CompilerParams(dimension_semantics=("arbitrary",), vmem_limit_bytes=VMEM_LIMIT),
        cost_estimate=pl.CostEstimate(flops=4 * t * m * e, bytes_accessed=t * e * 2 + m * e * 6, transcendentals=t * m),
        name="rows_pass",
    )(pos, emb, u, bias, lse, lab, *extra)


def put_kernel(n, pos, *refs):
    pieces, out_ref, hold, in_sem, out_sem = refs[1:1 + n], *refs[1 + n:]
    loads, stores = [], []
    for j, p in enumerate(pieces):
        slot = hold.at[j, :p.shape[0], :]
        loads.append(pltpu.make_async_copy(p, slot, in_sem.at[j]))
        stores.append(pltpu.make_async_copy(slot, out_ref.at[pl.ds(pl.multiple_of(pos[j], 8), p.shape[0]), :], out_sem.at[j]))
    for a in loads:
        a.start()
    for a, b in zip(loads, stores):
        a.wait()
        b.start()
    for b in stores:
        b.wait()


def put_rows(pos, big, pieces):
    n, e = len(pieces), big.shape[1]
    any_spec = pl.BlockSpec(memory_space=pl.ANY)
    return pl.pallas_call(
        functools.partial(put_kernel, n),
        in_specs=[pl.BlockSpec(memory_space=pltpu.SMEM)] + [any_spec] * (n + 1),
        out_specs=any_spec,
        out_shape=jax.ShapeDtypeStruct(big.shape, big.dtype),
        scratch_shapes=[
            pltpu.VMEM((n, max(p.shape[0] for p in pieces), e), F32),
            pltpu.SemaphoreType.DMA((n,)),
            pltpu.SemaphoreType.DMA((n,)),
        ],
        input_output_aliases={1: 0},
        compiler_params=pltpu.CompilerParams(vmem_limit_bytes=VMEM_LIMIT),
        cost_estimate=pl.CostEstimate(flops=0, bytes_accessed=sum(p.size for p in pieces) * 8, transcendentals=0),
        name="put_rows",
    )(pos, big, *pieces)


def narrow_kernel(first, pos, *refs):
    piece, out_ref, wide, thin, in_sem, sem = refs if first else refs[1:]
    load = pltpu.make_async_copy(piece, wide, in_sem)
    load.start()
    load.wait()
    thin[...] = wide[...].astype(BF16)
    store = pltpu.make_async_copy(thin, out_ref.at[pl.ds(pl.multiple_of(pos[0], 16), thin.shape[0]), :], sem)
    store.start()
    store.wait()


def narrow_into(pos, n_tok, big, piece):
    m, e = piece.shape
    first = big is None
    any_spec = pl.BlockSpec(memory_space=pl.ANY)
    return pl.pallas_call(
        functools.partial(narrow_kernel, first),
        in_specs=[pl.BlockSpec(memory_space=pltpu.SMEM)] + [any_spec] * (1 if first else 2),
        out_specs=any_spec,
        out_shape=jax.ShapeDtypeStruct((n_tok, e), BF16),
        scratch_shapes=[pltpu.VMEM((m, e), F32), pltpu.VMEM((m, e), BF16), pltpu.SemaphoreType.DMA, pltpu.SemaphoreType.DMA],
        input_output_aliases={} if first else {1: 0},
        compiler_params=pltpu.CompilerParams(vmem_limit_bytes=VMEM_LIMIT),
        cost_estimate=pl.CostEstimate(flops=m * e, bytes_accessed=m * e * 6, transcendentals=0),
        name="narrow_into",
    )(*([pos, piece] if first else [pos, big, piece]))


LN_EPS = 1e-5


def head_norm(pre_act, ln_gain, ln_bias):
    gelu_out = jax.nn.gelu(pre_act, approximate=False)
    row_mean = jnp.mean(gelu_out, axis=-1, keepdims=True)
    centered = gelu_out - row_mean
    row_var = jnp.mean(centered * centered, axis=-1, keepdims=True)
    return centered * lax.rsqrt(row_var + LN_EPS) * ln_gain + ln_bias


CORE, X, Y = 1, 2, 4


def solution(mesh):
    n_groups = mesh.shape["dp"]

    def swap(a, bit):
        return lax.ppermute(a, "dp", [(d, d ^ bit) for d in range(n_groups)])

    def hop(a):
        return lax.ppermute(a, "dp", [(d, d ^ (Y if d & CORE else X)) for d in range(n_groups)])

    def local_step(hidden, mask_pos, labels, w_trans, b_trans, ln_gain, ln_bias, emb_table, b_vocab):
        n_rows, seq_len, width = hidden.shape
        n_masks = mask_pos.shape[1]
        shard_rows = emb_table.shape[0]
        n_loc = n_rows * n_masks
        n_tokens = n_loc * n_groups
        dp = lax.axis_index("dp")
        row_start = lax.axis_index("vp") * shard_rows

        pos_onehot = (mask_pos[:, :, None] == jnp.arange(seq_len)[None, None, :]).astype(BF16)
        masked_h = jnp.einsum("clt,cte->cle", pos_onehot, hidden, preferred_element_type=F32).astype(BF16).reshape(n_loc, width)
        pre_act = dot(masked_h, w_trans, NN) + b_trans
        u_norm, head_vjp = jax.vjp(head_norm, pre_act, ln_gain, ln_bias)
        u_wide = lax.reduce_precision(u_norm, 8, 7)
        u_bf16 = u_norm.astype(BF16)
        flat_labels = labels.reshape(n_loc)
        lab_local = flat_labels - row_start
        lab_local = jnp.where((lab_local >= 0) & (lab_local < shard_rows), lab_local, -1)
        lab_local = jnp.broadcast_to(lab_local[:, None], (n_loc, 128))

        cut = n_loc // 32 * 16
        x_lo, x_hi = swap(u_wide[:cut], X), swap(u_wide[cut:], X)
        y_hi, y_lo = swap(u_wide[cut:], Y), swap(u_wide[:cut], Y)
        c_all = swap(u_wide, CORE)
        logits, local_max, local_sum, label_logit = stats(u_bf16, emb_table, b_vocab[None, :], lab_local)
        (x_lo, y_hi), _ = lax.optimization_barrier(((x_lo, y_hi), local_max))
        d_lo, d_hi = swap(x_lo, Y), swap(y_hi, X)
        tok_stats = lax.all_gather(jnp.concatenate([local_max, local_sum, label_logit], axis=1), "vp")
        all_max, all_sum, all_label = tok_stats[:, :, 0], tok_stats[:, :, 1], tok_stats[:, :, 2]
        global_max = jnp.max(all_max, axis=0)
        log_norm = global_max + jnp.log(jnp.sum(all_sum * jnp.exp(all_max - global_max), axis=0))
        loss_part = jnp.sum(log_norm - jnp.sum(all_label, axis=0))
        lse = log_norm + jnp.log(jnp.float32(n_tokens))
        scale = 1.0 / n_tokens

        du_part, db_part = du_pass(scale, logits, emb_table, jnp.broadcast_to(lse[:, None], (n_loc, 128)), lab_local)
        d_unorm = lax.psum(du_part, "vp")

        token_info = lax.all_gather(jnp.stack([lse, flat_labels.astype(F32)]), "dp")
        lse_all = token_info[:, 0].reshape(1, n_tokens)
        lab_all = token_info[:, 1].astype(I32).reshape(1, n_tokens)

        u_all = None
        (u_wide, x_lo, x_hi, y_lo, y_hi, d_lo, d_hi), _ = lax.optimization_barrier(((u_wide, x_lo, x_hi, y_lo, y_hi, d_lo, d_hi), du_part))
        cx_lo, cx_hi, cy_lo, cy_hi = swap(x_lo, CORE), swap(x_hi, CORE), swap(y_lo, CORE), swap(y_hi, CORE)
        cd_lo, cd_hi = swap(d_lo, CORE), swap(d_hi, CORE)
        for bits, off, piece in (
            (0, 0, u_wide), (CORE, 0, c_all), (X, 0, x_lo), (Y, cut, y_hi), (CORE | X, 0, cx_lo), (CORE | Y, cut, cy_hi),
            (X, cut, x_hi), (Y, 0, y_lo), (CORE | X, cut, cx_hi), (CORE | Y, 0, cy_lo),
            (X | Y, 0, d_lo), (X | Y, cut, d_hi), (CORE | X | Y, 0, cd_lo), (CORE | X | Y, cut, cd_hi),
        ):
            u_all = narrow_into(((dp ^ bits) * n_loc + off)[None], n_tokens, u_all, piece)

        core, mine = dp & 1, (dp >> 1 ^ dp >> 2) & 1
        half, quarter = shard_rows // 2, shard_rows // 4
        block = -(-quarter // 6 // 16) * 16
        spans = [(s, min(s + block, quarter)) for s in range(0, quarter, block)]
        my_start = mine * half + core * quarter
        twin_start = mine * half + (1 - core) * quarter
        far_start = (1 - mine) * half + core * quarter
        far_twin_start = (1 - mine) * half + (1 - core) * quarter
        bias_col = lax.dynamic_slice(b_vocab, (my_start,), (quarter,))[:, None]

        big, waiting = None, []
        lag = 3
        arrived = []
        for k, (s0, s1) in enumerate(spans):
            ready = arrived[k - lag] if k >= lag else []
            pos = jnp.stack([my_start + s0, row_start + my_start + s0, my_start + s0] + [p for p, _ in ready])
            chunk, big = rows_pass(scale, shard_rows, s1 - s0, pos, emb_table, u_all, bias_col[s0:s1], lse_all, lab_all, big, [a for _, a in ready])
            twin, far = swap(chunk, CORE), hop(chunk)
            far_twin = swap(far, CORE)
            arrived.append([(twin_start + s0, twin), (far_start + s0, far), (far_twin_start + s0, far_twin)])
        for ready in arrived[-lag:]:
            big = put_rows(jnp.stack([p for p, _ in ready]), big, [a for _, a in ready])

        d_pre, d_ln_gain, d_ln_bias = head_vjp(d_unorm)
        d_pre_bf = d_pre.astype(BF16)
        d_w_trans = lax.psum(lax.dot_general(masked_h, d_pre_bf, (((0,), (0,)), ((), ())), preferred_element_type=F32), "dp")
        small = lax.psum(
            (jnp.stack([jnp.sum(d_pre, axis=0), d_ln_gain, d_ln_bias]), db_part, loss_part), "dp"
        )
        d_masked = dot(d_pre_bf, w_trans, NT).astype(BF16).reshape(n_rows, n_masks, width)
        d_hidden = jnp.einsum("clt,cle->cte", pos_onehot, d_masked, preferred_element_type=F32).astype(BF16)
        vec, db, loss = small
        return loss / n_tokens, d_hidden, d_w_trans, vec[0], vec[1], vec[2], big, db.reshape(shard_rows)

    in_specs = (P("dp", None, None), P("dp", None), P("dp", None), P(None, None), P(None), P(None), P(None), P("vp", None), P("vp"))
    out_specs = (P(), P("dp", None, None), P(None, None), P(None), P(None), P(None), P("vp", None), P("vp"))
    return jax.shard_map(local_step, mesh=mesh, in_specs=in_specs, out_specs=out_specs, check_vma=False)
```

```python
import functools

import jax
import jax.numpy as jnp
from jax import lax
from jax.experimental import pallas as pl
from jax.experimental.pallas import tpu as pltpu
from jax.sharding import PartitionSpec as P


F32, BF16, I32 = jnp.float32, jnp.bfloat16, jnp.int32
NT = (((1,), (1,)), ((), ()))
NN = (((1,), (0,)), ((), ()))
VB = 1024
VMEM_LIMIT = 60 << 20
COVER = 100
CH = 16


def row_cuts(rows, parts=4):
    cuts = [16 * (rows // 16 * k // parts) for k in range(parts)] + [rows]
    return list(zip(cuts[:-1], cuts[1:]))


def dot(a, b, dims):
    return lax.dot_general(a, b, dims, preferred_element_type=F32)


def stats_kernel(n_vocab, u_ref, emb_ref, b_ref, lab_ref, logits_ref, stat_ref, m_sc, s_sc, l_sc):
    i, n_blocks = pl.program_id(0), pl.num_programs(0)
    lane = lax.broadcasted_iota(I32, (1, 128), 1)

    @pl.when(i == 0)
    def _():
        m_sc[...] = jnp.full_like(m_sc, -jnp.inf)
        s_sc[...] = jnp.zeros_like(s_sc)
        l_sc[...] = jnp.zeros_like(l_sc)

    def run(width):
        wide = -(-width // 128) * 128
        for r0, r1 in row_cuts(u_ref.shape[0]):
            tile = dot(u_ref[r0:r1, :], emb_ref[:wide, :], NT) + b_ref[:, :wide]
            if wide > width:
                tile = jnp.where(lax.broadcasted_iota(I32, (1, wide), 1) < width, tile, -jnp.inf)
            logits_ref[r0:r1, :wide] = tile
            for q in range(r0, r1, CH):
                rs = slice(q, min(q + CH, r1))
                parts = [logits_ref[rs, k:k + 128] for k in range(0, wide, 128)]
                m_old = m_sc[rs, :]
                m_new = functools.reduce(jnp.maximum, parts, m_old)
                s_new = s_sc[rs, :] * jnp.exp(m_old - m_new)
                l_new = l_sc[rs, :]
                lab = lab_ref[rs, :] - i * VB
                for k, part in enumerate(parts):
                    s_new += jnp.exp(part - m_new)
                    l_new = jnp.where(lab == lane + k * 128, part, l_new)
                m_sc[rs, :], s_sc[rs, :], l_sc[rs, :] = m_new, s_new, l_new

    tail = n_vocab % VB
    if tail:
        pl.when(i < n_blocks - 1)(functools.partial(run, VB))
        pl.when(i == n_blocks - 1)(functools.partial(run, tail))
    else:
        run(VB)

    @pl.when(i == n_blocks - 1)
    def _():
        m_t, s_t, l_t = m_sc[...].T, s_sc[...].T, l_sc[...].T
        m_all = jnp.max(m_t, axis=0, keepdims=True)
        stat_ref[0:1, :] = m_all
        stat_ref[1:2, :] = jnp.sum(s_t * jnp.exp(m_t - m_all), axis=0, keepdims=True)
        stat_ref[2:3, :] = jnp.sum(l_t, axis=0, keepdims=True)
        stat_ref[3:8, :] = jnp.zeros_like(stat_ref[3:8, :])


def stats(u, emb, bias, lab):
    t, e = u.shape
    v = emb.shape[0]
    n = pl.cdiv(v, VB)
    whole = lambda *s: pl.BlockSpec(s, lambda i: (0,) * len(s))
    return pl.pallas_call(
        functools.partial(stats_kernel, v),
        grid=(n,),
        in_specs=[whole(t, e), pl.BlockSpec((VB, e), lambda i: (i, 0)), pl.BlockSpec((1, VB), lambda i: (0, i)), whole(t, 128)],
        out_specs=[pl.BlockSpec((t, VB), lambda i: (0, i)), whole(8, t)],
        out_shape=[jax.ShapeDtypeStruct((t, v), F32), jax.ShapeDtypeStruct((8, t), F32)],
        scratch_shapes=[pltpu.VMEM((t, 128), F32)] * 3,
        compiler_params=pltpu.CompilerParams(dimension_semantics=("arbitrary",), vmem_limit_bytes=VMEM_LIMIT),
        cost_estimate=pl.CostEstimate(flops=(2 * t * v * e) // COVER, bytes_accessed=t * v * 4 + v * e * 2, transcendentals=t * v),
        name="stats",
    )(u, emb, bias, lab)


def du_kernel(n_vocab, scale, logits_ref, emb_ref, lse_ref, lab_ref, du_ref, db_ref, g_sc, db_sc):
    i, n_blocks = pl.program_id(0), pl.num_programs(0)
    t = logits_ref.shape[0]
    lane = lax.broadcasted_iota(I32, (1, 128), 1)

    @pl.when(i == 0)
    def _():
        du_ref[...] = jnp.zeros_like(du_ref)

    def run(width):
        wide = -(-width // 128) * 128
        emb = emb_ref[:wide, :]
        if wide > width:
            emb = jnp.where(lax.broadcasted_iota(I32, (wide, 1), 0) < width, emb, jnp.zeros_like(emb))
        for r0, r1 in row_cuts(t):
            sums = [None] * (wide // 128)
            for q in range(r0, r1, 16):
                rs = slice(q, q + 16)
                lse = lse_ref[rs, :]
                lab = lab_ref[rs, :] - i * VB
                for k in range(wide // 128):
                    c = k * 128
                    g = jnp.exp(logits_ref[rs, c:c + 128] - lse)
                    g -= jnp.where(lab == lane + c, scale, 0.0)
                    if c + 128 > width:
                        g = jnp.where(lane < width - c, g, 0.0)
                    part = g[:8] + g[8:]
                    sums[k] = part if sums[k] is None else sums[k] + part
                    g_sc[rs, c:c + 128] = g.astype(BF16)
            for k in range(wide // 128):
                cs = slice(k * 128, (k + 1) * 128)
                db_sc[:, cs] = sums[k] if r0 == 0 else db_sc[:, cs] + sums[k]
            du_ref[r0:r1, :] += dot(g_sc[r0:r1, :wide], emb, NN)
        db_ref[:, :wide] = jnp.sum(db_sc[:, :wide], axis=0, keepdims=True)

    tail = n_vocab % VB
    if tail:
        pl.when(i < n_blocks - 1)(functools.partial(run, VB))
        pl.when(i == n_blocks - 1)(functools.partial(run, tail))
    else:
        run(VB)

    @pl.when(i == n_blocks - 1)
    def _():
        du_ref[...] = du_ref[...].astype(BF16).astype(F32)


def du_pass(scale, padded, logits, emb, lse, lab):
    t, v = logits.shape
    e = emb.shape[1]
    n = pl.cdiv(v, VB)
    whole = lambda *s: pl.BlockSpec(s, lambda i: (0,) * len(s))
    return pl.pallas_call(
        functools.partial(du_kernel, v, scale),
        grid=(n,),
        in_specs=[pl.BlockSpec((t, VB), lambda i: (0, i)), pl.BlockSpec((VB, e), lambda i: (i, 0)), whole(t, 128), whole(t, 128)],
        out_specs=[whole(padded, e), pl.BlockSpec((1, VB), lambda i: (0, i))],
        out_shape=[jax.ShapeDtypeStruct((padded, e), F32), jax.ShapeDtypeStruct((1, v), F32)],
        scratch_shapes=[pltpu.VMEM((t, VB), BF16), pltpu.VMEM((8, VB), F32)],
        compiler_params=pltpu.CompilerParams(dimension_semantics=("arbitrary",), vmem_limit_bytes=VMEM_LIMIT),
        cost_estimate=pl.CostEstimate(flops=(2 * t * v * e) // COVER, bytes_accessed=t * v * 4 + v * e * 2, transcendentals=t * v),
        name="du_pass",
    )(logits, emb, lse, lab)


LN_EPS = 1e-5
CORE, X, Y = 1, 2, 4
CHIPS = (0, X, Y, X | Y)
ANY = pl.BlockSpec(memory_space=pl.ANY)
VMEM = pl.BlockSpec(memory_space=pltpu.VMEM)
SMEM = pl.BlockSpec(memory_space=pltpu.SMEM)
DMA = pltpu.SemaphoreType.DMA


def gelu_norm(a):
    cdf = 0.5 * (1.0 + lax.erf(a * (0.5 ** 0.5)))
    g = a * cdf
    centered = g - jnp.mean(g, axis=1, keepdims=True)
    rstd = lax.rsqrt(jnp.mean(centered * centered, axis=1, keepdims=True) + LN_EPS)
    return cdf, centered * rstd, rstd


def head_kernel(n_masks, cut, hid, pos_ref, w_ref, b_ref, gain_ref, bias_ref, z_out, pre_out, u_out, lo_out, hi_out,
                hbuf, zf, zb, pre_v, ub, uf, in_sem, out_sem):
    n_seq, seq_len = hid.shape[0], hid.shape[1]
    n_loc, padded = n_seq * n_masks, zb.shape[0]
    loads = [pltpu.make_async_copy(hid.at[b], hbuf.at[b], in_sem.at[b]) for b in range(n_seq)]
    for c in loads:
        c.start()
    lane = lax.broadcasted_iota(I32, (1, 128), 1)
    zb[n_loc:, :] = jnp.zeros((padded - n_loc, zb.shape[1]), BF16)
    pre_v[n_loc:, :] = jnp.zeros((padded - n_loc, zb.shape[1]), F32)
    cuts = [0, cut // 32 * 16, cut, cut + (n_loc - cut) // 32 * 16, n_loc]
    done, stores = 0, []

    def send(src, dst, r0, r1, base):
        c = pltpu.make_async_copy(src.at[r0:r1, :], dst.at[r0 - base:r1 - base, :], out_sem.at[len(stores)])
        c.start()
        stores.append(c)

    for b in range(n_seq):
        loads[b].wait()
        hot = jnp.concatenate([jnp.where(pos_ref[b] == lane + j, 1.0, 0.0).astype(BF16) for j in range(0, seq_len, 128)], axis=1)
        zf[b * n_masks:(b + 1) * n_masks, :] = dot(hot, hbuf[b], NN)[:n_masks, :]
        while done < 4 and cuts[done + 1] <= (b + 1) * n_masks:
            r0, r1 = cuts[done], cuts[done + 1]
            z = zf[r0:r1, :].astype(BF16)
            zb[r0:r1, :] = z
            a = dot(z, w_ref[...], NN) + b_ref[...]
            pre_v[r0:r1, :] = a
            _, normed, _ = gelu_norm(a)
            u = (normed * gain_ref[...] + bias_ref[...]).astype(BF16)
            ub[r0:r1, :] = u
            uf[r0:r1, :] = u.astype(F32)
            done += 1
            end = padded if done == 4 else r1
            send(uf, hi_out if r0 >= cut else lo_out, r0, r1, cut if r0 >= cut else 0)
            send(ub, u_out, r0, r1, 0)
            send(zb, z_out, r0, end, 0)
            send(pre_v, pre_out, r0, end, 0)
    for c in stores:
        c.wait()


def head_pass(n_masks, padded, cut, hidden, pos, w, b, gain, bias):
    n_seq, seq_len, e = hidden.shape
    n_loc = n_seq * n_masks
    sds = jax.ShapeDtypeStruct
    return pl.pallas_call(
        functools.partial(head_kernel, n_masks, cut),
        in_specs=[ANY] + [VMEM] * 5,
        out_specs=[ANY] * 5,
        out_shape=[sds((padded, e), BF16), sds((padded, e), F32), sds((n_loc, e), BF16), sds((cut, e), F32), sds((n_loc - cut, e), F32)],
        scratch_shapes=[
            pltpu.VMEM((n_seq, seq_len, e), BF16), pltpu.VMEM((n_loc, e), F32), pltpu.VMEM((padded, e), BF16), pltpu.VMEM((padded, e), F32),
            pltpu.VMEM((n_loc, e), BF16), pltpu.VMEM((n_loc, e), F32), DMA((n_seq,)), DMA((16,)),
        ],
        compiler_params=pltpu.CompilerParams(vmem_limit_bytes=VMEM_LIMIT),
        cost_estimate=pl.CostEstimate(flops=(4 * n_loc * e * e) // COVER, bytes_accessed=hidden.size * 2 + n_loc * e * 16, transcendentals=n_loc * e),
        name="head",
    )(hidden, pos, w, b, gain, bias)


def rows_kernel(mode, scale, m, cut, n_loc, chips, n_put, first, pos, emb_hbm, bias_ref, lse_ref, lab_ref, *rest):
    rest = list(rest)
    take = lambda n: [rest.pop(0) for _ in range(n)]
    src = [[take(2), take(2)] for _ in chips]
    if not first and mode != "first":
        take(1)
    puts = take(n_put)
    parts = take(2) if mode == "last" else []
    if mode == "first":
        own_ref, side_ref = take(2)
    else:
        out_ref, big_ref = take(2)
    buf, ub, emb_sc, g_sc, acc, hold, sem, tok_sem, in_sem, out_sem = rest
    i, n_blocks = pl.program_id(0), pl.num_programs(0)
    row = lambda j: pl.multiple_of(pos[j], 8)
    core = pos[2]

    def fetch(step, slot):
        for g, chip in enumerate(src):
            for rel, (lo, hi) in enumerate(chip):
                @pl.when(step == 2 * g + (core ^ rel))
                def _():
                    pltpu.make_async_copy(lo, buf.at[slot, :cut, :], tok_sem.at[slot, 0]).start()
                    pltpu.make_async_copy(hi, buf.at[slot, cut:n_loc, :], tok_sem.at[slot, 1]).start()

    loads = [pltpu.make_async_copy(p, hold.at[j, :p.shape[0], :], in_sem.at[j]) for j, p in enumerate(puts)]
    stores = [pltpu.make_async_copy(hold.at[j, :p.shape[0], :], big_ref.at[pl.ds(row(3 + j), p.shape[0]), :], out_sem.at[j])
              for j, p in enumerate(puts)]

    @pl.when(i == 0)
    def _():
        fetch(0, 0)
        cp = pltpu.make_async_copy(emb_hbm.at[pl.ds(row(0), m), :], emb_sc, sem)
        cp.start()
        acc[...] = jnp.zeros_like(acc)
        ub[n_loc:, :] = jnp.zeros((ub.shape[0] - n_loc, ub.shape[1]), BF16)
        cp.wait()

    slot = lax.rem(i, 2)
    lo, hi = src[0][0]
    pltpu.make_async_copy(lo, buf.at[slot, :cut, :], tok_sem.at[slot, 0]).wait()
    pltpu.make_async_copy(hi, buf.at[slot, cut:n_loc, :], tok_sem.at[slot, 1]).wait()
    fetch(i + 1, 1 - slot)

    @pl.when(i == 1)
    def _():
        for c in loads:
            c.start()

    @pl.when(i == 4)
    def _():
        for a, b in zip(loads, stores):
            a.wait()
            b.start()

    ub[:n_loc, :] = buf[slot].astype(BF16)
    u = ub[...]
    g_id = lax.div(i, 2)
    rel = chips[0] + 2 * g_id + (lax.rem(i, 2) ^ core)
    lse, lab = lse_ref[rel], lab_ref[rel]
    mid = -(-m // 32) * 16
    for r0, r1 in ((0, mid), (mid, m)):
        part = dot(emb_sc[r0:r1, :], u, NT)
        hit = lab == lax.broadcasted_iota(I32, (r1 - r0, 1), 0) + (pos[1] + r0)
        g = jnp.exp(part + bias_ref[r0:r1, :] - lse) - jnp.where(hit, scale, 0.0)
        g_sc[r0:r1, :] = g.astype(BF16)
        acc[g_id, r0:r1, :] += dot(g_sc[r0:r1, :], u, NN)

    @pl.when(i == n_blocks - 1)
    def _():
        if mode == "first":
            own_ref[...] = acc[0]
            side_ref[...] = acc[1] + acc[2]
        else:
            if mode == "whole":
                out_ref[...] = (acc[0] + acc[3]) + (acc[1] + acc[2])
            else:
                out_ref[...] = (parts[0][...] + acc[0]) + parts[1][...]
            own = pltpu.make_async_copy(out_ref, big_ref.at[pl.ds(row(0), m), :], sem)
            own.start()
            for b in stores:
                b.wait()
            own.wait()


def rows_pass(mode, scale, v_rows, m, cut, pos, emb, bias, lse, lab, tokens, big=None, puts=(), parts=()):
    e = emb.shape[1]
    n_loc = tokens[0][0].shape[0] + tokens[0][1].shape[0]
    padded = lse.shape[-1]
    chips = {"whole": CHIPS, "first": CHIPS[:3], "last": CHIPS[3:]}[mode]
    src = [half for c in chips for rel in (0, CORE) for half in tokens[c | rel]]
    has_big = big is not None and mode != "first"
    extra = src + ([big] if has_big else []) + list(puts)
    n_put = max(1, len(puts))
    sds = jax.ShapeDtypeStruct
    block = lambda *s: pl.BlockSpec(s, lambda i, p: (0,) * len(s))
    if mode == "first":
        out_specs, out_shape = [block(m, e)] * 2, [sds((m, e), F32)] * 2
    else:
        out_specs, out_shape = [block(m, e), ANY], [sds((m, e), F32), sds((v_rows, e), F32)]
    gs = pltpu.PrefetchScalarGridSpec(
        num_scalar_prefetch=1,
        grid=(2 * len(chips),),
        in_specs=[ANY, block(m, 1), block(*lse.shape), block(*lab.shape)] + [ANY] * len(extra) + [block(m, e)] * len(parts),
        out_specs=out_specs,
        scratch_shapes=[
            pltpu.VMEM((2, n_loc, e), F32), pltpu.VMEM((padded, e), BF16), pltpu.VMEM((m, e), BF16), pltpu.VMEM((m, padded), BF16),
            pltpu.VMEM((len(chips), m, e), F32), pltpu.VMEM((n_put, max([p.shape[0] for p in puts] + [8]), e), F32),
            DMA, DMA((2, 2)), DMA((n_put,)), DMA((n_put,)),
        ],
    )
    t = n_loc * 2 * len(chips)
    return pl.pallas_call(
        functools.partial(rows_kernel, mode, scale, m, cut, n_loc, chips, len(puts), not has_big),
        grid_spec=gs,
        out_shape=out_shape,
        input_output_aliases={5 + len(src): 1} if has_big else {},
        compiler_params=pltpu.CompilerParams(dimension_semantics=("arbitrary",), vmem_limit_bytes=VMEM_LIMIT),
        cost_estimate=pl.CostEstimate(flops=(4 * t * m * e) // COVER, bytes_accessed=t * e * 4 + m * e * 6, transcendentals=t * m),
    )(pos, emb, bias, lse, lab, *extra, *parts)


def put_kernel(n, pos, *refs):
    pieces, (out_ref, hold, in_sem, out_sem) = refs[1:1 + n], refs[1 + n:]
    loads, stores = [], []
    for j, p in enumerate(pieces):
        slot = hold.at[j, :p.shape[0], :]
        loads.append(pltpu.make_async_copy(p, slot, in_sem.at[j]))
        stores.append(pltpu.make_async_copy(slot, out_ref.at[pl.ds(pl.multiple_of(pos[j], 8), p.shape[0]), :], out_sem.at[j]))
    for a in loads:
        a.start()
    for a, b in zip(loads, stores):
        a.wait()
        b.start()
    for b in stores:
        b.wait()


def put_rows(pos, big, pieces):
    n, e = len(pieces), big.shape[1]
    return pl.pallas_call(
        functools.partial(put_kernel, n),
        in_specs=[SMEM] + [ANY] * (n + 1),
        out_specs=ANY,
        out_shape=jax.ShapeDtypeStruct(big.shape, big.dtype),
        scratch_shapes=[pltpu.VMEM((n, max(p.shape[0] for p in pieces), e), F32), DMA((n,)), DMA((n,))],
        input_output_aliases={1: 0},
        compiler_params=pltpu.CompilerParams(vmem_limit_bytes=VMEM_LIMIT),
        cost_estimate=pl.CostEstimate(flops=(sum(p.size for p in pieces)) // COVER, bytes_accessed=sum(p.size for p in pieces) * 8, transcendentals=0),
        name="put_rows",
    )(pos, big, *pieces)


def back_kernel(d_rows, db_rows, vp, pre_ref, z_ref, du_ref, w_ref, gain_ref, loss_ref, db_ref, dz_ref, pack_ref):
    a, du = pre_ref[...], du_ref[...]
    cdf, normed, rstd = gelu_norm(a)
    dn = du * gain_ref[...]
    dg = rstd * (dn - jnp.mean(dn, axis=1, keepdims=True) - normed * jnp.mean(dn * normed, axis=1, keepdims=True))
    da = dg * (cdf + a * (jnp.exp(-0.5 * a * a) * 0.3989422804014327))
    dab = da.astype(BF16)
    dz_ref[...] = dot(dab, w_ref[...], NT).astype(BF16).astype(F32)
    pack_ref[:d_rows, :] = lax.dot_general(z_ref[...], dab, (((0,), (0,)), ((), ())), preferred_element_type=F32)
    pack_ref[d_rows:, :] = jnp.zeros((pack_ref.shape[0] - d_rows, pack_ref.shape[1]), F32)
    for j, x in enumerate((da, du * normed, du)):
        pack_ref[d_rows + j:d_rows + j + 1, :] = jnp.sum(x, axis=0, keepdims=True)
    pack_ref[d_rows + 3:d_rows + 4, :] = loss_ref[...]
    pack_ref[pl.ds(pl.multiple_of(d_rows + 8 + db_rows * vp[0], 8), db_rows), :] = db_ref[...]


def back_pass(n_shards, vp, pre, z, du, w, gain, loss, db):
    rows, e = du.shape
    db_rows = db.shape[0]
    n_pack = e + 8 + n_shards * db_rows
    block = lambda *s: pl.BlockSpec(s, lambda i, p: (0,) * len(s))
    share = pl.BlockSpec((rows, e), lambda i, p: (p[0], 0))
    gs = pltpu.PrefetchScalarGridSpec(
        num_scalar_prefetch=1,
        grid=(1,),
        in_specs=[share, share, block(rows, e), block(e, e), block(1, e), block(1, e), block(db_rows, e)],
        out_specs=[block(rows, e), block(n_pack, e)],
    )
    return pl.pallas_call(
        functools.partial(back_kernel, e, db_rows),
        grid_spec=gs,
        out_shape=[jax.ShapeDtypeStruct((rows, e), F32), jax.ShapeDtypeStruct((n_pack, e), F32)],
        compiler_params=pltpu.CompilerParams(dimension_semantics=("arbitrary",), vmem_limit_bytes=VMEM_LIMIT),
        cost_estimate=pl.CostEstimate(flops=(4 * rows * e * e) // COVER, bytes_accessed=rows * e * 16 + e * e * 6, transcendentals=rows * e * 2),
        name="back",
    )(vp, pre, z, du, w, gain, loss, db)


def spread_kernel(n_masks, vp, pos_ref, *refs):
    pieces, (out_ref, dz, obuf, in_sem, out_sem) = refs[:4], refs[4:]
    share = pieces[0].shape[0]
    loads = [pltpu.make_async_copy(p, dz.at[pl.ds(pl.multiple_of((vp[0] ^ k) * share, 8), share), :], in_sem.at[k]) for k, p in enumerate(pieces)]
    for c in loads:
        c.start()
    for c in loads:
        c.wait()
    n_seq, seq_len, _ = out_ref.shape
    place = lax.broadcasted_iota(I32, (seq_len, 1), 0)
    slots = pos_ref.shape[2]
    stores = []
    for b in range(n_seq):
        if b >= 4:
            stores[b - 4].wait()
        hot = jnp.where(place == pos_ref[b], 1.0, 0.0).astype(BF16)
        rows = dz[b * n_masks:b * n_masks + slots, :].astype(BF16)
        obuf[b % 4] = dot(hot, rows, NN).astype(BF16)
        c = pltpu.make_async_copy(obuf.at[b % 4], out_ref.at[b], out_sem.at[b])
        c.start()
        stores.append(c)
    for c in stores[-4:]:
        c.wait()


def spread_pass(n_masks, shape, vp, pos, pieces):
    share, e = pieces[0].shape
    return pl.pallas_call(
        functools.partial(spread_kernel, n_masks),
        in_specs=[SMEM, VMEM] + [ANY] * 4,
        out_specs=ANY,
        out_shape=jax.ShapeDtypeStruct(shape, BF16),
        scratch_shapes=[pltpu.VMEM((4 * share, e), F32), pltpu.VMEM((4,) + shape[1:], BF16), DMA((4,)), DMA((shape[0],))],
        compiler_params=pltpu.CompilerParams(vmem_limit_bytes=VMEM_LIMIT),
        cost_estimate=pl.CostEstimate(flops=(2 * shape[0] * shape[1] * 128 * e) // COVER, bytes_accessed=shape[0] * shape[1] * e * 2, transcendentals=0),
        name="spread",
    )(vp, pos, *pieces)


def after(x, *deps):
    return lax.optimization_barrier((x, deps))[0]


def solution(mesh):
    n_groups, n_shards = mesh.shape["dp"], mesh.shape["vp"]

    def swap(a, bit):
        return lax.ppermute(a, "dp", [(d, d ^ bit) for d in range(n_groups)])

    def swap_vp(a, bit):
        return lax.ppermute(a, "vp", [(d, d ^ bit) for d in range(n_shards)])

    def hop(a):
        return lax.ppermute(a, "dp", [(d, d ^ (Y if d & CORE else X)) for d in range(n_groups)])

    def local_step(hidden, mask_pos, labels, w_trans, b_trans, ln_gain, ln_bias, emb_table, b_vocab):
        n_rows, _, width = hidden.shape
        n_masks = mask_pos.shape[1]
        shard_rows = emb_table.shape[0]
        n_loc = n_rows * n_masks
        n_tokens = n_loc * n_groups
        padded = -(-n_loc // 256) * 256
        slots = -(-n_masks // 16) * 16
        cut = n_loc // 32 * 16
        dp, vp = lax.axis_index("dp"), lax.axis_index("vp")
        row_start = vp * shard_rows
        scale = 1.0 / n_tokens

        pos_pad = jnp.pad(mask_pos, ((0, 0), (0, slots - n_masks)), constant_values=-1)
        z, pre, u, u_lo, u_hi = head_pass(
            n_masks, padded, cut, hidden, jnp.broadcast_to(pos_pad[:, :, None], (n_rows, slots, 128)),
            w_trans, b_trans[None], ln_gain[None], ln_bias[None])

        x_lo, y_hi = swap(u_lo, X), swap(u_hi, Y)
        x_hi, y_lo = swap(u_hi, X), swap(u_lo, Y)
        c_lo, c_hi = swap(u_lo, CORE), swap(u_hi, CORE)

        flat_labels = labels.reshape(n_loc)
        lab_local = flat_labels - row_start
        lab_local = jnp.where((lab_local >= 0) & (lab_local < shard_rows), lab_local, -1)
        lab_local = jnp.broadcast_to(lab_local[:, None], (n_loc, 128))
        logits, stat = stats(u, emb_table, b_vocab[None], lab_local)
        all_stats = [stat] + [swap_vp(stat, b) for b in range(1, n_shards)]
        order = lambda f: f(f(all_stats[0], all_stats[1]), f(all_stats[2], all_stats[3]))
        global_max = order(lambda a, b: jnp.maximum(a, b))[0]
        log_norm = global_max + jnp.log(sum(s[1] * jnp.exp(s[0] - global_max) for s in all_stats))
        loss_part = jnp.where(vp == 0, jnp.sum(log_norm - sum(s[2] for s in all_stats)), 0.0)
        lse = log_norm + jnp.log(jnp.float32(n_tokens))
        x_lo, y_hi = after((x_lo, y_hi), lse)
        d_lo, d_hi = swap(x_lo, Y), swap(y_hi, X)
        info = jnp.stack([lse, flat_labels.astype(F32)])
        info = [info] + [swap(info, b) for b in range(1, n_groups)]

        du_part, db_part = du_pass(scale, padded, logits, emb_table, jnp.broadcast_to(lse[:, None], (n_loc, 128)), lab_local)
        du_share = lax.psum_scatter(du_part, "vp", scatter_dimension=0, tiled=True)

        info = jnp.stack(after(info, du_part))
        fill = ((0, 0), (0, padded - n_loc))
        lse_all = jnp.pad(info[:, 0], fill, constant_values=jnp.inf)[:, None]
        lab_all = jnp.pad(info[:, 1].astype(I32), fill, constant_values=-1)[:, None]
        x_lo, x_hi, y_lo, y_hi = after((x_lo, x_hi, y_lo, y_hi), du_part)
        tokens = {
            0: (u_lo, u_hi), CORE: (c_lo, c_hi), X: (x_lo, x_hi), Y: (y_lo, y_hi),
            X | CORE: (swap(x_lo, CORE), swap(x_hi, CORE)), Y | CORE: (swap(y_lo, CORE), swap(y_hi, CORE)),
        }

        core, mine = dp & 1, (dp >> 1 ^ dp >> 2) & 1
        half, quarter = shard_rows // 2, shard_rows // 4
        my_start = mine * half + core * quarter
        twin_start = mine * half + (1 - core) * quarter
        far_start = (1 - mine) * half + core * quarter
        far_twin_start = (1 - mine) * half + (1 - core) * quarter
        bias_col = lax.dynamic_slice(b_vocab, (my_start,), (quarter,))[:, None]
        weights = (640, 608, 576, 528, 448, 344)
        ends = [0]
        for w in weights[:-1]:
            ends.append(ends[-1] + max(16, quarter * w // sum(weights) // 16 * 16))
        spans = list(zip(ends, ends[1:] + [quarter]))

        def rows(mode, k, **kw):
            s0, s1 = spans[k]
            puts = kw.pop("ready", [])
            pos = jnp.stack([my_start + s0, row_start + my_start + s0, core] + [p for p, _ in puts])
            pos = after(pos, *kw.pop("wait", ()))
            return rows_pass(mode, scale, shard_rows, s1 - s0, cut, pos, emb_table, bias_col[s0:s1], lse_all, lab_all, tokens,
                             puts=[a for _, a in puts], **kw)

        early = 2
        parts = []
        for k in range(early):
            parts.append(rows("first", k))
        d_lo, d_hi = after((d_lo, d_hi), *parts)
        tokens[X | Y] = (d_lo, d_hi)
        tokens[X | Y | CORE] = (swap(d_lo, CORE), swap(d_hi, CORE))

        big, arrived, sent, waits = None, [], [], {}
        lag = 4
        for k, (s0, s1) in enumerate(spans):
            ready = []
            if k >= lag:
                ready = arrived[k - lag]
            if k < early:
                chunk, big = rows("last", k, parts=parts[k], big=big)
            else:
                chunk, big = rows("whole", k, big=big, ready=ready, wait=waits.pop(k, ()))
            twin, far = swap(chunk, CORE), hop(chunk)
            sent.append(far)
            arrived.append([(twin_start + s0, twin)])
            for j in {1: (), 2: (0, 1)}.get(k, (k - 1,) if k else ()):
                prev = after(sent[j], chunk)
                passed = swap(prev, CORE)
                arrived[j] += [(far_start + spans[j][0], prev), (far_twin_start + spans[j][0], passed)]
            if k == 2:
                du_share = after(du_share, chunk)
                loss_row = jnp.pad(loss_part[None, None], ((0, 0), (0, width - 1)))
                db_rows = -(-shard_rows // width // 8) * 8
                db_mat = jnp.pad(db_part[0], (0, db_rows * width - shard_rows)).reshape(db_rows, width)
                dz, pack = back_pass(n_shards, vp[None], pre, z, du_share, w_trans, ln_gain[None], loss_row, db_mat)
                waits[k + 1] = (dz,)
                pack = lax.psum(pack, ("vp", "dp"))
                dz = [dz] + [swap_vp(dz, b) for b in range(1, n_shards)]
        far = sent[-1]
        s0 = spans[-1][0]
        arrived[-1] += [(far_start + s0, far), (far_twin_start + s0, swap(far, CORE))]
        dz = after(dz, chunk)
        d_hidden = spread_pass(n_masks, hidden.shape, vp[None], pos_pad[:, None], dz)
        for ready in (arrived[2] + arrived[3], arrived[4], arrived[5]):
            big = put_rows(jnp.stack([p for p, _ in ready]), big, [a for _, a in ready])

        vec = pack[width:width + 4]
        db = lax.dynamic_slice(pack, (width + 8 + db_rows * vp, 0), (db_rows, width)).reshape(-1)[:shard_rows]
        return vec[3, 0] / n_tokens, d_hidden, pack[:width], vec[0], vec[1], vec[2], big, db

    in_specs = (P("dp", None, None), P("dp", None), P("dp", None), P(None, None), P(None), P(None), P(None), P("vp", None), P("vp"))
    out_specs = (P(), P("dp", None, None), P(None, None), P(None), P(None), P(None), P("vp", None), P("vp"))
    return jax.shard_map(local_step, mesh=mesh, in_specs=in_specs, out_specs=out_specs, check_vma=False)
```

```python
import functools

import jax
import jax.numpy as jnp
from jax import lax
from jax.experimental import pallas as pl
from jax.experimental.pallas import tpu as pltpu
from jax.sharding import PartitionSpec as P


F32, BF16, I32 = jnp.float32, jnp.bfloat16, jnp.int32
NT = (((1,), (1,)), ((), ()))
NN = (((1,), (0,)), ((), ()))
VB = 1024
VMEM_LIMIT = 60 << 20
COVER = 100
CH = 16


def row_cuts(rows, parts=4):
    cuts = [16 * (rows // 16 * k // parts) for k in range(parts)] + [rows]
    return list(zip(cuts[:-1], cuts[1:]))


def dot(a, b, dims):
    return lax.dot_general(a, b, dims, preferred_element_type=F32)


def stats_kernel(n_vocab, u_ref, emb_ref, b_ref, lab_ref, logits_ref, stat_ref, m_sc, s_sc, l_sc):
    i, n_blocks = pl.program_id(0), pl.num_programs(0)
    lane = lax.broadcasted_iota(I32, (1, 128), 1)

    @pl.when(i == 0)
    def _():
        m_sc[...] = jnp.full_like(m_sc, -jnp.inf)
        s_sc[...] = jnp.zeros_like(s_sc)
        l_sc[...] = jnp.zeros_like(l_sc)

    def run(width):
        wide = -(-width // 128) * 128
        for r0, r1 in row_cuts(u_ref.shape[0]):
            tile = dot(u_ref[r0:r1, :], emb_ref[:wide, :], NT) + b_ref[:, :wide]
            if wide > width:
                tile = jnp.where(lax.broadcasted_iota(I32, (1, wide), 1) < width, tile, -jnp.inf)
            logits_ref[r0:r1, :wide] = tile
            for q in range(r0, r1, CH):
                rs = slice(q, min(q + CH, r1))
                parts = [logits_ref[rs, k:k + 128] for k in range(0, wide, 128)]
                m_old = m_sc[rs, :]
                m_new = functools.reduce(jnp.maximum, parts, m_old)
                s_new = s_sc[rs, :] * jnp.exp(m_old - m_new)
                l_new = l_sc[rs, :]
                lab = lab_ref[rs, :] - i * VB
                for k, part in enumerate(parts):
                    s_new += jnp.exp(part - m_new)
                    l_new = jnp.where(lab == lane + k * 128, part, l_new)
                m_sc[rs, :], s_sc[rs, :], l_sc[rs, :] = m_new, s_new, l_new

    tail = n_vocab % VB
    if tail:
        pl.when(i < n_blocks - 1)(functools.partial(run, VB))
        pl.when(i == n_blocks - 1)(functools.partial(run, tail))
    else:
        run(VB)

    @pl.when(i == n_blocks - 1)
    def _():
        m_t, s_t, l_t = m_sc[...].T, s_sc[...].T, l_sc[...].T
        m_all = jnp.max(m_t, axis=0, keepdims=True)
        stat_ref[0:1, :] = m_all
        stat_ref[1:2, :] = jnp.sum(s_t * jnp.exp(m_t - m_all), axis=0, keepdims=True)
        stat_ref[2:3, :] = jnp.sum(l_t, axis=0, keepdims=True)
        stat_ref[3:8, :] = jnp.zeros_like(stat_ref[3:8, :])


def stats(u, emb, bias, lab):
    t, e = u.shape
    v = emb.shape[0]
    n = pl.cdiv(v, VB)
    whole = lambda *s: pl.BlockSpec(s, lambda i: (0,) * len(s))
    return pl.pallas_call(
        functools.partial(stats_kernel, v),
        grid=(n,),
        in_specs=[whole(t, e), pl.BlockSpec((VB, e), lambda i: (i, 0)), pl.BlockSpec((1, VB), lambda i: (0, i)), whole(t, 128)],
        out_specs=[pl.BlockSpec((t, VB), lambda i: (0, i)), whole(8, t)],
        out_shape=[jax.ShapeDtypeStruct((t, v), F32), jax.ShapeDtypeStruct((8, t), F32)],
        scratch_shapes=[pltpu.VMEM((t, 128), F32)] * 3,
        compiler_params=pltpu.CompilerParams(dimension_semantics=("arbitrary",), vmem_limit_bytes=VMEM_LIMIT),
        cost_estimate=pl.CostEstimate(flops=(2 * t * v * e) // COVER, bytes_accessed=t * v * 4 + v * e * 2, transcendentals=t * v),
        name="stats",
    )(u, emb, bias, lab)


def du_kernel(n_vocab, scale, logits_ref, emb_ref, lse_ref, lab_ref, out_ref, db_ref, du_ref, g_sc, db_sc):
    i, n_blocks = pl.program_id(0), pl.num_programs(0)
    t = logits_ref.shape[0]
    lane = lax.broadcasted_iota(I32, (1, 128), 1)

    @pl.when(i == 0)
    def _():
        du_ref[...] = jnp.zeros_like(du_ref)

    def run(width):
        wide = -(-width // 128) * 128
        emb = emb_ref[:wide, :]
        if wide > width:
            emb = jnp.where(lax.broadcasted_iota(I32, (wide, 1), 0) < width, emb, jnp.zeros_like(emb))
        for r0, r1 in row_cuts(t):
            sums = [None] * (wide // 128)
            for q in range(r0, r1, 16):
                rs = slice(q, q + 16)
                lse = lse_ref[rs, :]
                lab = lab_ref[rs, :] - i * VB
                for k in range(wide // 128):
                    c = k * 128
                    g = jnp.exp(logits_ref[rs, c:c + 128] - lse)
                    g -= jnp.where(lab == lane + c, scale, 0.0)
                    if c + 128 > width:
                        g = jnp.where(lane < width - c, g, 0.0)
                    part = g[:8] + g[8:]
                    sums[k] = part if sums[k] is None else sums[k] + part
                    g_sc[rs, c:c + 128] = g.astype(BF16)
            for k in range(wide // 128):
                cs = slice(k * 128, (k + 1) * 128)
                db_sc[:, cs] = sums[k] if r0 == 0 else db_sc[:, cs] + sums[k]
            du_ref[r0:r1, :] += dot(g_sc[r0:r1, :wide], emb, NN)
        db_ref[:, :wide] = jnp.sum(db_sc[:, :wide], axis=0, keepdims=True)

    tail = n_vocab % VB
    if tail:
        pl.when(i < n_blocks - 1)(functools.partial(run, VB))
        pl.when(i == n_blocks - 1)(functools.partial(run, tail))
    else:
        run(VB)

    @pl.when(i == n_blocks - 1)
    def _():
        parts, _, cols = out_ref.shape
        for q in range(parts):
            out_ref[q] = du_ref[:, q * cols:(q + 1) * cols].astype(BF16).astype(F32)


def du_pass(scale, parts, logits, emb, lse, lab):
    t, v = logits.shape
    e = emb.shape[1]
    n = pl.cdiv(v, VB)
    whole = lambda *s: pl.BlockSpec(s, lambda i: (0,) * len(s))
    return pl.pallas_call(
        functools.partial(du_kernel, v, scale),
        grid=(n,),
        in_specs=[pl.BlockSpec((t, VB), lambda i: (0, i)), pl.BlockSpec((VB, e), lambda i: (i, 0)), whole(t, 128), whole(t, 128)],
        out_specs=[whole(parts, t, e // parts), pl.BlockSpec((1, VB), lambda i: (0, i))],
        out_shape=[jax.ShapeDtypeStruct((parts, t, e // parts), F32), jax.ShapeDtypeStruct((1, v), F32)],
        scratch_shapes=[pltpu.VMEM((t, e), F32), pltpu.VMEM((t, VB), BF16), pltpu.VMEM((8, VB), F32)],
        compiler_params=pltpu.CompilerParams(dimension_semantics=("arbitrary",), vmem_limit_bytes=VMEM_LIMIT),
        cost_estimate=pl.CostEstimate(flops=(2 * t * v * e) // COVER, bytes_accessed=t * v * 4 + v * e * 2, transcendentals=t * v),
        name="du_pass",
    )(logits, emb, lse, lab)


LN_EPS = 1e-5
CORE, X, Y = 1, 2, 4
ANY = pl.BlockSpec(memory_space=pl.ANY)
VMEM = pl.BlockSpec(memory_space=pltpu.VMEM)
SMEM = pl.BlockSpec(memory_space=pltpu.SMEM)
DMA = pltpu.SemaphoreType.DMA


def gelu_norm(a):
    cdf = 0.5 * (1.0 + lax.erf(a * (0.5 ** 0.5)))
    g = a * cdf
    centered = g - jnp.mean(g, axis=1, keepdims=True)
    rstd = lax.rsqrt(jnp.mean(centered * centered, axis=1, keepdims=True) + LN_EPS)
    return cdf, centered * rstd, rstd


def head_kernel(n_masks, cut, hid, pos_ref, w_ref, b_ref, gain_ref, bias_ref, z_out, pre_out, norm_out, rstd_out, u_out, lo_out, hi_out,
                hbuf, zf, zb, pre_v, norm_v, rstd_v, ub, uf, in_sem, out_sem):
    n_seq, seq_len = hid.shape[0], hid.shape[1]
    n_loc = n_seq * n_masks
    loads = [pltpu.make_async_copy(hid.at[b], hbuf.at[b], in_sem.at[b]) for b in range(n_seq)]
    for c in loads:
        c.start()
    lane = lax.broadcasted_iota(I32, (1, 128), 1)
    cuts = [0, cut // 32 * 16, cut, cut + (n_loc - cut) // 32 * 16, n_loc]
    done, stores = 0, []

    def send(src, dst, r0, r1, base=0):
        c = pltpu.make_async_copy(src.at[r0:r1, :], dst.at[r0 - base:r1 - base, :], out_sem.at[len(stores)])
        c.start()
        stores.append(c)

    for b in range(n_seq):
        loads[b].wait()
        hot = jnp.concatenate([jnp.where(pos_ref[b] == lane + j, 1.0, 0.0).astype(BF16) for j in range(0, seq_len, 128)], axis=1)
        zf[b * n_masks:(b + 1) * n_masks, :] = dot(hot, hbuf[b], NN)[:n_masks, :]
        while done < 4 and cuts[done + 1] <= (b + 1) * n_masks:
            r0, r1 = cuts[done], cuts[done + 1]
            z = zf[r0:r1, :].astype(BF16)
            zb[r0:r1, :] = z
            a = dot(z, w_ref[...], NN) + b_ref[...]
            pre_v[r0:r1, :] = a
            _, normed, rstd = gelu_norm(a)
            norm_v[r0:r1, :] = normed
            rstd_v[r0:r1, :] = jnp.broadcast_to(rstd, (r1 - r0, 128))
            u = (normed * gain_ref[...] + bias_ref[...]).astype(BF16)
            ub[r0:r1, :] = u
            uf[r0:r1, :] = u.astype(F32)
            done += 1
            send(uf, hi_out if r0 >= cut else lo_out, r0, r1, cut if r0 >= cut else 0)
            for src, dst in ((ub, u_out), (zb, z_out), (pre_v, pre_out), (norm_v, norm_out), (rstd_v, rstd_out)):
                send(src, dst, r0, r1)
    for c in stores:
        c.wait()


def head_pass(n_masks, cut, hidden, pos, w, b, gain, bias):
    n_seq, seq_len, e = hidden.shape
    n = n_seq * n_masks
    kinds = [((n, e), BF16), ((n, e), F32), ((n, e), F32), ((n, 128), F32), ((n, e), BF16), ((cut, e), F32), ((n - cut, e), F32)]
    return pl.pallas_call(
        functools.partial(head_kernel, n_masks, cut),
        in_specs=[ANY] + [VMEM] * 5,
        out_specs=[ANY] * len(kinds),
        out_shape=[jax.ShapeDtypeStruct(*k) for k in kinds],
        scratch_shapes=[pltpu.VMEM((n_seq, seq_len, e), BF16), pltpu.VMEM((n, e), F32)]
        + [pltpu.VMEM(*k) for k in kinds[:5]] + [pltpu.VMEM((n, e), F32), DMA((n_seq,)), DMA((24,))],
        compiler_params=pltpu.CompilerParams(vmem_limit_bytes=VMEM_LIMIT),
        cost_estimate=pl.CostEstimate(flops=(4 * n * e * e) // COVER, bytes_accessed=hidden.size * 2 + n * e * 20, transcendentals=n * e),
        name="head",
    )(hidden, pos, w, b, gain, bias)


def narrow_kernel(first, offs, pos, *refs):
    refs = list(refs)
    n = len(offs)
    if not first:
        refs.pop(0)
    pieces, (out_ref, wide, thin, pad, in_sem, out_sem, sem) = refs[:n], refs[n:]
    loads, stores = [], []
    for j, p in enumerate(pieces):
        m = p.shape[0]
        loads.append(pltpu.make_async_copy(p, wide.at[j, :m, :], in_sem.at[j]))
        row = pl.multiple_of(pos[j], 16)
        stores.append(pltpu.make_async_copy(thin.at[j, :m, :], out_ref.at[pl.ds(row, m), :], out_sem.at[j]))
    for c in loads:
        c.start()
    if first:
        pad[...] = jnp.zeros_like(pad)
        c = pltpu.make_async_copy(pad, out_ref.at[out_ref.shape[0] - pad.shape[0]:, :], sem)
        c.start()
        c.wait()
    for j, p in enumerate(pieces):
        m = p.shape[0]
        loads[j].wait()
        thin[j, :m, :] = wide[j, :m, :].astype(BF16)
        stores[j].start()
    for c in stores:
        c.wait()


def narrow_into(big, n_tok, rows, pieces):
    first = big is None
    n, e = len(pieces), pieces[0].shape[1]
    m = max(p.shape[0] for p in pieces)
    padded = -(-n_tok // TB) * TB
    size = sum(p.size for p in pieces)
    return pl.pallas_call(
        functools.partial(narrow_kernel, first, [p.shape[0] for p in pieces]),
        in_specs=[SMEM] + [ANY] * (n + (not first)),
        out_specs=ANY,
        out_shape=jax.ShapeDtypeStruct((padded, e), BF16),
        scratch_shapes=[pltpu.VMEM((n, m, e), F32), pltpu.VMEM((n, m, e), BF16), pltpu.VMEM((padded - n_tok, e), BF16), DMA((n,)), DMA((n,)), DMA],
        input_output_aliases={} if first else {1: 0},
        compiler_params=pltpu.CompilerParams(vmem_limit_bytes=VMEM_LIMIT),
        cost_estimate=pl.CostEstimate(flops=(size) // COVER, bytes_accessed=size * 6, transcendentals=0),
        name="narrow",
    )(jnp.stack(rows), *([] if first else [big]), *pieces)


TB = 768


def rows_kernel(scale, m, n_put, has_big, pos, emb_hbm, u_hbm, bias_ref, lse_ref, lab_ref, *refs):
    refs = list(refs)
    if has_big:
        refs.pop(0)
    puts, (out_hbm, big_ref, u_all, emb_sc, g_sc, acc, hold, sem, tok_sem, in_sem, out_sem) = refs[:n_put], refs[n_put:]
    n_blocks = lse_ref.shape[0]
    row = lambda j: pl.multiple_of(pos[j], 8)
    blocks = [pltpu.make_async_copy(u_hbm.at[j * TB:(j + 1) * TB, :], u_all.at[j * TB:(j + 1) * TB, :], tok_sem.at[j]) for j in range(n_blocks)]
    loads = [pltpu.make_async_copy(p, hold.at[j, :p.shape[0], :], in_sem.at[j]) for j, p in enumerate(puts)]
    stores = [pltpu.make_async_copy(hold.at[j, :p.shape[0], :], big_ref.at[pl.ds(row(2 + j), p.shape[0]), :], out_sem.at[j])
              for j, p in enumerate(puts)]
    emb_copy = pltpu.make_async_copy(emb_hbm.at[pl.ds(row(0), m), :], emb_sc, sem)
    emb_copy.start()
    for c in blocks + loads:
        c.start()
    acc[...] = jnp.zeros_like(acc)
    emb_copy.wait()
    parts = max(1, round(m / 256))
    cuts = [-(-m * k // (parts * 16)) * 16 for k in range(parts)] + [m]
    cuts = list(zip(cuts[:-1], cuts[1:]))

    @pl.loop(0, n_blocks)
    def _(i):
        at = pl.ds(pl.multiple_of(i * TB, TB), TB)
        pltpu.make_async_copy(u_hbm.at[at, :], u_all.at[at, :], tok_sem.at[i]).wait()
        for j, (a, b) in enumerate(zip(loads, stores)):
            @pl.when(i == 3 + j)
            def _():
                a.wait()
                b.start()

        def weights(r0, r1):
            part = dot(emb_sc[r0:r1, :], u_all[at, :], NT)
            hit = lab_ref[i] == lax.broadcasted_iota(I32, (r1 - r0, 1), 0) + (pos[1] + r0)
            g = jnp.exp(part + bias_ref[r0:r1, :] - lse_ref[i]) - jnp.where(hit, scale, 0.0)
            g_sc[r0:r1, :] = g.astype(BF16)

        weights(*cuts[0])
        for k, (r0, r1) in enumerate(cuts):
            if k + 1 < len(cuts):
                weights(*cuts[k + 1])
            acc[r0:r1, :] += dot(g_sc[r0:r1, :], u_all[at, :], NN)

    own = pltpu.make_async_copy(acc, out_hbm, sem)
    own.start()
    for b in stores:
        b.wait()
    own.wait()


def rows_pass(scale, v_rows, m, pos, emb, u, bias, lse, lab, big, puts):
    t, e = u.shape
    n, n_put = t // TB, max(1, len(puts))
    sds = jax.ShapeDtypeStruct
    has_big = big is not None
    extra = ([big] if has_big else []) + list(puts)
    return pl.pallas_call(
        functools.partial(rows_kernel, scale, m, len(puts), has_big),
        in_specs=[SMEM, ANY, ANY, VMEM, VMEM, VMEM] + [ANY] * len(extra),
        out_specs=[ANY, ANY],
        out_shape=[sds((m, e), F32), sds((v_rows, e), F32)],
        scratch_shapes=[
            pltpu.VMEM((t, e), BF16), pltpu.VMEM((m, e), BF16), pltpu.VMEM((m, TB), BF16), pltpu.VMEM((m, e), F32),
            pltpu.VMEM((n_put, max([p.shape[0] for p in puts] + [8]), e), F32), DMA, DMA((n,)), DMA((n_put,)), DMA((n_put,)),
        ],
        input_output_aliases={6: 1} if has_big else {},
        compiler_params=pltpu.CompilerParams(vmem_limit_bytes=VMEM_LIMIT),
        cost_estimate=pl.CostEstimate(flops=(4 * t * m * e) // COVER, bytes_accessed=t * e * 2 + m * e * 6, transcendentals=t * m),
        name="rows",
    )(pos, emb, u, bias, lse, lab, *extra)


def put_kernel(n, pos, *refs):
    pieces, (out_ref, hold, in_sem, out_sem) = refs[1:1 + n], refs[1 + n:]
    loads, stores = [], []
    for j, p in enumerate(pieces):
        slot = hold.at[j, :p.shape[0], :]
        loads.append(pltpu.make_async_copy(p, slot, in_sem.at[j]))
        stores.append(pltpu.make_async_copy(slot, out_ref.at[pl.ds(pl.multiple_of(pos[j], 8), p.shape[0]), :], out_sem.at[j]))
    for a in loads:
        a.start()
    for a, b in zip(loads, stores):
        a.wait()
        b.start()
    for b in stores:
        b.wait()


def put_rows(pos, big, pieces):
    n, e = len(pieces), big.shape[1]
    return pl.pallas_call(
        functools.partial(put_kernel, n),
        in_specs=[SMEM] + [ANY] * (n + 1),
        out_specs=ANY,
        out_shape=jax.ShapeDtypeStruct(big.shape, big.dtype),
        scratch_shapes=[pltpu.VMEM((n, max(p.shape[0] for p in pieces), e), F32), DMA((n,)), DMA((n,))],
        input_output_aliases={1: 0},
        compiler_params=pltpu.CompilerParams(vmem_limit_bytes=VMEM_LIMIT),
        cost_estimate=pl.CostEstimate(flops=(sum(p.size for p in pieces)) // COVER, bytes_accessed=sum(p.size for p in pieces) * 8, transcendentals=0),
        name="put_rows",
    )(pos, big, *pieces)


def sums_kernel(du_ref, norm_ref, gain_ref, out_ref):
    cols = du_ref.shape[2]
    total = [jnp.zeros((du_ref.shape[1], 128), F32)] * 2
    for q in range(du_ref.shape[0]):
        for c in range(0, cols, 128):
            at = slice(q * cols + c, q * cols + c + 128)
            dn = du_ref[q, :, c:c + 128] * gain_ref[:, at]
            total = [total[0] + dn, total[1] + dn * norm_ref[:, at]]
    out_ref[2:, :] = jnp.zeros_like(out_ref[2:, :])
    for j, x in enumerate(total):
        out_ref[j:j + 1, :] = jnp.sum(x.T, axis=0, keepdims=True)


def sums_pass(du, normed, gain):
    n, e = normed.shape
    return pl.pallas_call(
        sums_kernel,
        in_specs=[VMEM] * 3,
        out_specs=VMEM,
        out_shape=jax.ShapeDtypeStruct((8, n), F32),
        compiler_params=pltpu.CompilerParams(vmem_limit_bytes=VMEM_LIMIT),
        cost_estimate=pl.CostEstimate(flops=(4 * n * e) // COVER, bytes_accessed=n * e * 8, transcendentals=0),
        name="sums",
    )(du, normed, gain)


def back_kernel(vp, pre_ref, norm_ref, rstd_ref, z_ref, du_ref, m1_ref, m2_ref, gain_ref, loss_ref, db_ref, dab_ref, pack_ref):
    e, cols = z_ref.shape[1], du_ref.shape[1]
    for c in range(0, cols, 128):
        cs = slice(c, c + 128)
        a, du, normed = pre_ref[:, cs], du_ref[:, cs], norm_ref[:, cs]
        cdf = 0.5 * (1.0 + lax.erf(a * (0.5 ** 0.5)))
        dg = rstd_ref[...] * (du * gain_ref[:, cs] - m1_ref[...] - normed * m2_ref[...])
        da = dg * (cdf + a * (jnp.exp(-0.5 * a * a) * 0.3989422804014327))
        dab_ref[:, cs] = da.astype(BF16).astype(F32)
        for j, x in enumerate((da, du * normed, du)):
            pack_ref[e + j:e + j + 1, cs] = jnp.sum(x, axis=0, keepdims=True)
    pack_ref[:e, :] = lax.dot_general(z_ref[...], dab_ref[...].astype(BF16), (((0,), (0,)), ((), ())), preferred_element_type=F32)
    pack_ref[e + 3:e + 4, :] = loss_ref[...]
    pack_ref[e + 4:e + 8, :] = jnp.zeros_like(pack_ref[e + 4:e + 8, :])
    pack_ref[e + 8:, :] = db_ref[...]


def back_pass(vp, pre, normed, rstd, z, du, m1, m2, gain, loss, db):
    n, cols = du.shape
    e = z.shape[1]
    n_pack = e + 8 + db.shape[0]
    block = lambda *s: pl.BlockSpec(s, lambda i, p: (0,) * len(s))
    share = lambda r: pl.BlockSpec((r, cols), lambda i, p: (0, p[0]))
    gs = pltpu.PrefetchScalarGridSpec(
        num_scalar_prefetch=1,
        grid=(1,),
        in_specs=[share(n), share(n), block(n, 128), block(n, e), block(n, cols), block(n, 128), block(n, 128), share(1), block(1, cols), block(*db.shape)],
        out_specs=[block(n, cols), block(n_pack, cols)],
    )
    return pl.pallas_call(
        back_kernel,
        grid_spec=gs,
        out_shape=[jax.ShapeDtypeStruct((n, cols), F32), jax.ShapeDtypeStruct((n_pack, cols), F32)],
        compiler_params=pltpu.CompilerParams(dimension_semantics=("arbitrary",), vmem_limit_bytes=VMEM_LIMIT),
        cost_estimate=pl.CostEstimate(flops=(2 * n * e * cols) // COVER, bytes_accessed=n * (cols * 16 + e * 2 + 1536), transcendentals=n * cols * 2),
        name="back",
    )(vp, pre, normed, rstd, z, du, m1, m2, gain, loss, db)


def spread_kernel(n_masks, vp, pos_ref, w_ref, *refs):
    pieces, (out_ref, dab, dz, obuf, in_sem, out_sem) = refs[:4], refs[4:]
    n, cols = pieces[0].shape
    loads = [pltpu.make_async_copy(p, dab.at[:, pl.ds(pl.multiple_of((vp[0] ^ k) * cols, cols), cols)], in_sem.at[k]) for k, p in enumerate(pieces)]
    for c in loads:
        c.start()
    dz[n:, :] = jnp.zeros((dz.shape[0] - n, dz.shape[1]), F32)
    n_seq, seq_len, _ = out_ref.shape
    place = lax.broadcasted_iota(I32, (seq_len, 1), 0)
    slots = pos_ref.shape[2]
    for c in loads:
        c.wait()
    stores, done = [], 0
    for b in range(n_seq):
        while done < min(n, b * n_masks + slots):
            r1 = min(n, done + 304)
            dz[done:r1, :] = dot(dab[done:r1, :].astype(BF16), w_ref[...], NT).astype(BF16).astype(F32)
            done = r1
        if b >= 4:
            stores[b - 4].wait()
        hot = jnp.where(place == pos_ref[b], 1.0, 0.0).astype(BF16)
        obuf[b % 4] = dot(hot, dz[b * n_masks:b * n_masks + slots, :].astype(BF16), NN).astype(BF16)
        c = pltpu.make_async_copy(obuf.at[b % 4], out_ref.at[b], out_sem.at[b])
        c.start()
        stores.append(c)
    for c in stores[-4:]:
        c.wait()


def spread_pass(n_masks, shape, vp, pos, w, pieces):
    n, cols = pieces[0].shape
    e = w.shape[0]
    return pl.pallas_call(
        functools.partial(spread_kernel, n_masks),
        in_specs=[SMEM, VMEM, VMEM] + [ANY] * 4,
        out_specs=ANY,
        out_shape=jax.ShapeDtypeStruct(shape, BF16),
        scratch_shapes=[pltpu.VMEM((n, 4 * cols), F32), pltpu.VMEM((n + 16, e), F32), pltpu.VMEM((4,) + shape[1:], BF16), DMA((4,)), DMA((shape[0],))],
        compiler_params=pltpu.CompilerParams(vmem_limit_bytes=VMEM_LIMIT),
        cost_estimate=pl.CostEstimate(flops=(2 * shape[0] * shape[1] * 128 * e) // COVER, bytes_accessed=shape[0] * shape[1] * e * 2, transcendentals=0),
        name="spread",
    )(vp, pos, w, *pieces)


def order_sum(xs):
    return (xs[0] + xs[1]) + (xs[2] + xs[3])


def after(x, *deps):
    return lax.optimization_barrier((x, deps))[0]


def solution(mesh):
    n_groups, n_shards = mesh.shape["dp"], mesh.shape["vp"]

    def swap(a, bit):
        return lax.ppermute(a, "dp", [(d, d ^ bit) for d in range(n_groups)])

    def swap_vp(a, bit):
        return lax.ppermute(a, "vp", [(d, d ^ bit) for d in range(n_shards)])

    def hop(a):
        return lax.ppermute(a, "dp", [(d, d ^ (Y if d & CORE else X)) for d in range(n_groups)])

    def local_step(hidden, mask_pos, labels, w_trans, b_trans, ln_gain, ln_bias, emb_table, b_vocab):
        n_rows, _, width = hidden.shape
        n_masks = mask_pos.shape[1]
        shard_rows = emb_table.shape[0]
        n_loc = n_rows * n_masks
        n_tokens = n_loc * n_groups
        padded = -(-n_tokens // TB) * TB
        slots = -(-n_masks // 16) * 16
        cut = n_loc // 32 * 16
        cols = width // n_shards
        dp, vp = lax.axis_index("dp"), lax.axis_index("vp")
        row_start = vp * shard_rows
        scale = 1.0 / n_tokens

        pos_pad = jnp.pad(mask_pos, ((0, 0), (0, slots - n_masks)), constant_values=-1)
        z, pre, normed, rstd, u, u_lo, u_hi = head_pass(
            n_masks, cut, hidden, jnp.broadcast_to(pos_pad[:, :, None], (n_rows, slots, 128)),
            w_trans, b_trans[None], ln_gain[None], ln_bias[None])

        x_lo, y_hi = swap(u_lo, X), swap(u_hi, Y)
        x_hi, y_lo = swap(u_hi, X), swap(u_lo, Y)
        c_lo, c_hi = swap(u_lo, CORE), swap(u_hi, CORE)

        flat_labels = labels.reshape(n_loc)
        lab_local = flat_labels - row_start
        lab_local = jnp.where((lab_local >= 0) & (lab_local < shard_rows), lab_local, -1)
        lab_local = jnp.broadcast_to(lab_local[:, None], (n_loc, 128))
        logits, stat = stats(u, emb_table, b_vocab[None], lab_local)
        all_stats = [stat] + [swap_vp(stat, b) for b in range(1, n_shards)]
        global_max = functools.reduce(jnp.maximum, [s[0] for s in all_stats])
        log_norm = global_max + jnp.log(order_sum([s[1] * jnp.exp(s[0] - global_max) for s in all_stats]))
        loss_part = jnp.sum(log_norm - order_sum([s[2] for s in all_stats]))
        lse = log_norm + jnp.log(jnp.float32(n_tokens))
        x_lo, y_hi = after((x_lo, y_hi), lse)
        d_lo, d_hi = swap(x_lo, Y), swap(y_hi, X)

        du_part, db_part = du_pass(scale, n_shards, logits, emb_table, jnp.broadcast_to(lse[:, None], (n_loc, 128)), lab_local)
        du_share = lax.psum_scatter(du_part.reshape(n_shards * n_loc, cols), "vp", scatter_dimension=0, tiled=True)

        lse, x_hi, y_lo, u_lo, u_hi, c_lo, c_hi = after((lse, x_hi, y_lo, u_lo, u_hi, c_lo, c_hi), du_part)
        info = jnp.stack([lse, flat_labels.astype(F32)])
        info = jnp.stack([info] + [swap(info, b) for b in range(1, n_groups)])
        info = jnp.take(info, jnp.arange(n_groups) ^ dp, axis=0, mode="clip")
        fill = (0, padded - n_tokens)
        lse_all = jnp.pad(info[:, 0].reshape(-1), fill, constant_values=jnp.inf).reshape(-1, 1, TB)
        lab_all = jnp.pad(info[:, 1].reshape(-1).astype(I32), fill, constant_values=-1).reshape(-1, 1, TB)

        sums = sums_pass(du_part, normed, ln_gain[None])
        sums = order_sum([sums] + [swap_vp(sums, b) for b in range(1, n_shards)]) / width
        m1, m2 = (jnp.broadcast_to(sums[j][:, None], (n_loc, 128)) for j in range(2))

        at = lambda bits, off: (dp ^ bits) * n_loc + off
        halves = lambda bits, lo, hi: [(at(bits, 0), lo), (at(bits, cut), hi)]

        def narrow(big, items):
            return narrow_into(big, n_tokens, [r for r, _ in items], [a for _, a in items])

        u_all = narrow(None, halves(0, u_lo, u_hi) + halves(CORE, c_lo, c_hi))
        cx = swap(x_lo, CORE), swap(x_hi, CORE)
        cy = swap(y_lo, CORE), swap(y_hi, CORE)
        u_all = narrow(u_all, halves(X, x_lo, x_hi) + halves(Y, y_lo, y_hi) + halves(X | CORE, *cx) + halves(Y | CORE, *cy))
        d_lo, d_hi = after((d_lo, d_hi), u_all)
        u_all = narrow(u_all, halves(X | Y, d_lo, d_hi) + halves(X | Y | CORE, swap(d_lo, CORE), swap(d_hi, CORE)))

        core, mine = dp & 1, (dp >> 1 ^ dp >> 2) & 1
        half, quarter = shard_rows // 2, shard_rows // 4
        my_start = mine * half + core * quarter
        twin_start = mine * half + (1 - core) * quarter
        far_start = (1 - mine) * half + core * quarter
        far_twin_start = (1 - mine) * half + (1 - core) * quarter
        bias_col = lax.dynamic_slice(b_vocab, (my_start,), (quarter,))[:, None]
        shares = (960, 880, 768, 536)
        ends = [0]
        for w in shares[:-1]:
            ends.append(ends[-1] + max(16, quarter * w // sum(shares) // 16 * 16))
        spans = list(zip(ends, ends[1:] + [quarter]))

        def rows(k, big, puts, *wait):
            s0, s1 = spans[k]
            pos = jnp.stack([my_start + s0, row_start + my_start + s0] + [p for p, _ in puts])
            return rows_pass(scale, shard_rows, s1 - s0, after(pos, *wait), emb_table, u_all, bias_col[s0:s1], lse_all, lab_all,
                             big, [a for _, a in puts])

        def send(k, chunk):
            return (twin_start + spans[k][0], swap(chunk, CORE)), hop(chunk)

        def forward(k, far, *wait):
            far = after(far, *wait)
            return (far_start + spans[k][0], far), (far_twin_start + spans[k][0], swap(far, CORE))

        own = lambda k, chunk: (my_start + spans[k][0], chunk)
        chunk0, big = rows(0, None, [])
        twin0, far0 = send(0, chunk0)

        du_share = after(du_share, chunk0)
        loss_row = jnp.pad(loss_part[None, None], ((0, 0), (0, cols - 1)))
        db_rows = -(-shard_rows // cols // 8) * 8
        db_mat = jnp.pad(db_part[0], (0, db_rows * cols - shard_rows)).reshape(db_rows, cols)
        dab, pack = back_pass(vp[None], pre, normed, rstd, z, du_share, m1, m2, ln_gain[None], loss_row, db_mat)
        wait = dab
        pack = lax.psum(pack, "dp")
        dab = [dab] + [swap_vp(dab, b) for b in range(1, n_shards)]

        chunk1, big = rows(1, big, [own(0, chunk0)], wait)
        twin1, far1 = send(1, chunk1)
        far0, far_twin0 = forward(0, far0, chunk1)
        chunk2, big = rows(2, big, [own(1, chunk1), twin0, far0])
        twin2, far2 = send(2, chunk2)
        far1, far_twin1 = forward(1, far1, chunk2)

        pack = after(pack, chunk2)
        n_gather = width + 8
        part = lax.dynamic_slice(pack, (core * (n_gather // 2), 0), (n_gather // 2, cols))
        parts = [swap_vp(part, b) for b in range(1, n_shards)]

        chunk3, big = rows(3, big, [own(2, chunk2), twin1, far1, far_twin0])
        twin3, far3 = send(3, chunk3)
        far2, far_twin2 = forward(2, far2, chunk3)
        *dab_wait, parts = after((*dab, parts), chunk3)
        d_hidden = spread_pass(n_masks, hidden.shape, vp[None], pos_pad[:, None], w_trans, dab_wait)
        others = [swap(p, CORE) for p in parts]
        items = [own(3, chunk3), twin2, far2, far_twin1, far_twin2, twin3]
        big = put_rows(jnp.stack([p for p, _ in items]), big, [a for _, a in items])
        items = forward(3, far3)
        big = put_rows(jnp.stack([p for p, _ in items]), big, [a for _, a in items])

        gathered = [pack[:n_gather]]
        for p, o in zip(parts, others):
            gathered.append(jnp.concatenate([jnp.where(core == 0, p, o), jnp.where(core == 0, o, p)]))
        gathered = jnp.take(jnp.stack(gathered), jnp.arange(n_shards) ^ vp, axis=0, mode="clip")
        gathered = jnp.transpose(gathered, (1, 0, 2)).reshape(n_gather, width)
        db = pack[n_gather:].reshape(-1)[:shard_rows]
        return (pack[width + 3, 0] / n_tokens, d_hidden, gathered[:width], gathered[width], gathered[width + 1], gathered[width + 2], big, db)

    in_specs = (P("dp", None, None), P("dp", None), P("dp", None), P(None, None), P(None), P(None), P(None), P("vp", None), P("vp"))
    out_specs = (P(), P("dp", None, None), P(None, None), P(None), P(None), P(None), P("vp", None), P("vp"))
    return jax.shard_map(local_step, mesh=mesh, in_specs=in_specs, out_specs=out_specs, check_vma=False)
```

```python
import functools

import jax
import jax.numpy as jnp
from jax import lax
from jax.experimental import pallas as pl
from jax.experimental.pallas import tpu as pltpu
from jax.sharding import PartitionSpec as P


F32, BF16, I32 = jnp.float32, jnp.bfloat16, jnp.int32
NT = (((1,), (1,)), ((), ()))
NN = (((1,), (0,)), ((), ()))
VB = 1024
VMEM_LIMIT = 60 << 20
COVER = 100
CH = 16


def row_cuts(rows, parts=4):
    cuts = [16 * (rows // 16 * k // parts) for k in range(parts)] + [rows]
    return list(zip(cuts[:-1], cuts[1:]))


def dot(a, b, dims):
    return lax.dot_general(a, b, dims, preferred_element_type=F32)


def stats_kernel(n_vocab, u_ref, emb_ref, b_ref, lab_ref, logits_ref, stat_ref, m_sc, s_sc, l_sc):
    i, n_blocks = pl.program_id(0), pl.num_programs(0)
    lane = lax.broadcasted_iota(I32, (1, 128), 1)

    @pl.when(i == 0)
    def _():
        m_sc[...] = jnp.full_like(m_sc, -jnp.inf)
        s_sc[...] = jnp.zeros_like(s_sc)
        l_sc[...] = jnp.zeros_like(l_sc)

    def run(width):
        wide = -(-width // 128) * 128
        for r0, r1 in row_cuts(u_ref.shape[0]):
            tile = dot(u_ref[r0:r1, :], emb_ref[:wide, :], NT) + b_ref[:, :wide]
            if wide > width:
                tile = jnp.where(lax.broadcasted_iota(I32, (1, wide), 1) < width, tile, -jnp.inf)
            logits_ref[r0:r1, :wide] = tile
            for q in range(r0, r1, CH):
                rs = slice(q, min(q + CH, r1))
                parts = [logits_ref[rs, k:k + 128] for k in range(0, wide, 128)]
                m_old = m_sc[rs, :]
                m_new = functools.reduce(jnp.maximum, parts, m_old)
                s_new = s_sc[rs, :] * jnp.exp(m_old - m_new)
                l_new = l_sc[rs, :]
                lab = lab_ref[rs, :] - i * VB
                for k, part in enumerate(parts):
                    s_new += jnp.exp(part - m_new)
                    l_new = jnp.where(lab == lane + k * 128, part, l_new)
                m_sc[rs, :], s_sc[rs, :], l_sc[rs, :] = m_new, s_new, l_new

    tail = n_vocab % VB
    if tail:
        pl.when(i < n_blocks - 1)(functools.partial(run, VB))
        pl.when(i == n_blocks - 1)(functools.partial(run, tail))
    else:
        run(VB)

    @pl.when(i == n_blocks - 1)
    def _():
        m_t, s_t, l_t = m_sc[...].T, s_sc[...].T, l_sc[...].T
        m_all = jnp.max(m_t, axis=0, keepdims=True)
        stat_ref[0:1, :] = m_all
        stat_ref[1:2, :] = jnp.sum(s_t * jnp.exp(m_t - m_all), axis=0, keepdims=True)
        stat_ref[2:3, :] = jnp.sum(l_t, axis=0, keepdims=True)
        stat_ref[3:8, :] = jnp.zeros_like(stat_ref[3:8, :])


def stats(u, emb, bias, lab):
    t, e = u.shape
    v = emb.shape[0]
    n = pl.cdiv(v, VB)
    whole = lambda *s: pl.BlockSpec(s, lambda i: (0,) * len(s))
    return pl.pallas_call(
        functools.partial(stats_kernel, v),
        grid=(n,),
        in_specs=[whole(t, e), pl.BlockSpec((VB, e), lambda i: (i, 0)), pl.BlockSpec((1, VB), lambda i: (0, i)), whole(t, 128)],
        out_specs=[pl.BlockSpec((t, VB), lambda i: (0, i)), whole(8, t)],
        out_shape=[jax.ShapeDtypeStruct((t, v), F32), jax.ShapeDtypeStruct((8, t), F32)],
        scratch_shapes=[pltpu.VMEM((t, 128), F32)] * 3,
        compiler_params=pltpu.CompilerParams(dimension_semantics=("arbitrary",), vmem_limit_bytes=VMEM_LIMIT),
        cost_estimate=pl.CostEstimate(flops=(2 * t * v * e) // COVER, bytes_accessed=t * v * 4 + v * e * 2, transcendentals=t * v),
        name="stats",
    )(u, emb, bias, lab)


def du_kernel(n_vocab, scale, logits_ref, emb_ref, lse_ref, lab_ref, norm_hbm, gain_ref, out_ref, db_ref, sum_ref, du_ref, g_sc, db_sc, norm_sc, db_sc2, sem):
    i, n_blocks = pl.program_id(0), pl.num_programs(0)
    t = logits_ref.shape[0]
    lane = lax.broadcasted_iota(I32, (1, 128), 1)

    norm_copy = pltpu.make_async_copy(norm_hbm, norm_sc, sem)

    @pl.when(i == 0)
    def _():
        du_ref[...] = jnp.zeros_like(du_ref)

    @pl.when(i == 2)
    def _():
        norm_copy.start()

    def run(width):
        wide = -(-width // 128) * 128
        emb = emb_ref[:wide, :]
        if wide > width:
            emb = jnp.where(lax.broadcasted_iota(I32, (wide, 1), 0) < width, emb, jnp.zeros_like(emb))
        for r0, r1 in row_cuts(t):
            sums = [None] * (wide // 128)
            for q in range(r0, r1, 16):
                rs = slice(q, q + 16)
                lse = lse_ref[rs, :]
                lab = lab_ref[rs, :] - i * VB
                for k in range(wide // 128):
                    c = k * 128
                    g = jnp.exp(logits_ref[rs, c:c + 128] - lse)
                    g -= jnp.where(lab == lane + c, scale, 0.0)
                    if c + 128 > width:
                        g = jnp.where(lane < width - c, g, 0.0)
                    part = g[:8] + g[8:]
                    sums[k] = part if sums[k] is None else sums[k] + part
                    g_sc[rs, c:c + 128] = g.astype(BF16)
            for k in range(wide // 128):
                cs = slice(k * 128, (k + 1) * 128)
                db_sc[:, cs] = sums[k] if r0 == 0 else db_sc[:, cs] + sums[k]
            du_ref[r0:r1, :] += dot(g_sc[r0:r1, :wide], emb, NN)
        db_ref[:, :wide] = jnp.sum(db_sc[:, :wide], axis=0, keepdims=True)

    tail = n_vocab % VB
    if tail:
        pl.when(i < n_blocks - 1)(functools.partial(run, VB))
        pl.when(i == n_blocks - 1)(functools.partial(run, tail))
    else:
        run(VB)

    @pl.when(i == n_blocks - 1)
    def _():
        norm_copy.wait()
        parts, rows, cols = out_ref.shape
        for r in range(0, rows, 112):
            rs = slice(r, r + 112)
            total = [jnp.zeros((112, 128), F32)] * 2
            for c in range(0, parts * cols, 128):
                x = du_ref[rs, c:c + 128].astype(BF16).astype(F32)
                out_ref[c // cols, rs, c % cols:c % cols + 128] = x
                dn = x * gain_ref[:, c:c + 128]
                total = [total[0] + dn, total[1] + dn * norm_sc[rs, c:c + 128]]
            for j, x in enumerate(total):
                db_sc2[j, rs, :] = x
        for j in range(2):
            sum_ref[j:j + 1, :] = jnp.sum(db_sc2[j].T, axis=0, keepdims=True)
        sum_ref[2:, :] = jnp.zeros_like(sum_ref[2:, :])


def du_pass(scale, parts, logits, emb, lse, lab, normed, gain):
    t, v = logits.shape
    e = emb.shape[1]
    n = pl.cdiv(v, VB)
    whole = lambda *s: pl.BlockSpec(s, lambda i: (0,) * len(s))
    return pl.pallas_call(
        functools.partial(du_kernel, v, scale),
        grid=(n,),
        in_specs=[pl.BlockSpec((t, VB), lambda i: (0, i)), pl.BlockSpec((VB, e), lambda i: (i, 0)), whole(t, 128), whole(t, 128), pl.BlockSpec(memory_space=pl.ANY), whole(1, e)],
        out_specs=[whole(parts, t, e // parts), pl.BlockSpec((1, VB), lambda i: (0, i)), whole(8, t)],
        out_shape=[jax.ShapeDtypeStruct((parts, t, e // parts), F32), jax.ShapeDtypeStruct((1, v), F32), jax.ShapeDtypeStruct((8, t), F32)],
        scratch_shapes=[pltpu.VMEM((t, e), F32), pltpu.VMEM((t, VB), BF16), pltpu.VMEM((8, VB), F32), pltpu.VMEM((t, e), F32), pltpu.VMEM((2, t, 128), F32), pltpu.SemaphoreType.DMA],
        compiler_params=pltpu.CompilerParams(dimension_semantics=("arbitrary",), vmem_limit_bytes=VMEM_LIMIT),
        cost_estimate=pl.CostEstimate(flops=(2 * t * v * e) // COVER, bytes_accessed=t * v * 4 + v * e * 2, transcendentals=t * v),
        name="du_pass",
    )(logits, emb, lse, lab, normed, gain)


LN_EPS = 1e-5
CORE, X, Y = 1, 2, 4
ANY = pl.BlockSpec(memory_space=pl.ANY)
VMEM = pl.BlockSpec(memory_space=pltpu.VMEM)
SMEM = pl.BlockSpec(memory_space=pltpu.SMEM)
DMA = pltpu.SemaphoreType.DMA


def gelu_norm(a):
    cdf = 0.5 * (1.0 + lax.erf(a * (0.5 ** 0.5)))
    g = a * cdf
    centered = g - jnp.mean(g, axis=1, keepdims=True)
    rstd = lax.rsqrt(jnp.mean(centered * centered, axis=1, keepdims=True) + LN_EPS)
    return cdf, centered * rstd, rstd


def head_kernel(n_masks, cut, hid, pos_ref, w_ref, b_ref, gain_ref, bias_ref, z_out, pre_out, norm_out, rstd_out, u_out, lo_out, hi_out,
                hbuf, zf, zb, pre_v, norm_v, rstd_v, ub, uf, in_sem, out_sem):
    n_seq, seq_len = hid.shape[0], hid.shape[1]
    n_loc = n_seq * n_masks
    loads = [pltpu.make_async_copy(hid.at[b], hbuf.at[b], in_sem.at[b]) for b in range(n_seq)]
    for c in loads:
        c.start()
    lane = lax.broadcasted_iota(I32, (1, 128), 1)
    cuts = [0, cut // 32 * 16, cut, cut + (n_loc - cut) // 32 * 16, n_loc]
    done, stores = 0, []

    def send(src, dst, r0, r1, base=0):
        c = pltpu.make_async_copy(src.at[r0:r1, :], dst.at[r0 - base:r1 - base, :], out_sem.at[len(stores)])
        c.start()
        stores.append(c)

    for b in range(n_seq):
        loads[b].wait()
        hot = jnp.concatenate([jnp.where(pos_ref[b] == lane + j, 1.0, 0.0).astype(BF16) for j in range(0, seq_len, 128)], axis=1)
        zf[b * n_masks:(b + 1) * n_masks, :] = dot(hot, hbuf[b], NN)[:n_masks, :]
        while done < 4 and cuts[done + 1] <= (b + 1) * n_masks:
            r0, r1 = cuts[done], cuts[done + 1]
            z = zf[r0:r1, :].astype(BF16)
            zb[r0:r1, :] = z
            a = dot(z, w_ref[...], NN) + b_ref[...]
            pre_v[r0:r1, :] = a
            _, normed, rstd = gelu_norm(a)
            norm_v[r0:r1, :] = normed
            rstd_v[r0:r1, :] = jnp.broadcast_to(rstd, (r1 - r0, 128))
            u = (normed * gain_ref[...] + bias_ref[...]).astype(BF16)
            ub[r0:r1, :] = u
            uf[r0:r1, :] = u.astype(F32)
            done += 1
            send(uf, hi_out if r0 >= cut else lo_out, r0, r1, cut if r0 >= cut else 0)
            for src, dst in ((ub, u_out), (zb, z_out), (pre_v, pre_out), (norm_v, norm_out), (rstd_v, rstd_out)):
                send(src, dst, r0, r1)
    for c in stores:
        c.wait()


def head_pass(n_masks, cut, hidden, pos, w, b, gain, bias):
    n_seq, seq_len, e = hidden.shape
    n = n_seq * n_masks
    kinds = [((n, e), BF16), ((n, e), F32), ((n, e), F32), ((n, 128), F32), ((n, e), BF16), ((cut, e), F32), ((n - cut, e), F32)]
    return pl.pallas_call(
        functools.partial(head_kernel, n_masks, cut),
        in_specs=[ANY] + [VMEM] * 5,
        out_specs=[ANY] * len(kinds),
        out_shape=[jax.ShapeDtypeStruct(*k) for k in kinds],
        scratch_shapes=[pltpu.VMEM((n_seq, seq_len, e), BF16), pltpu.VMEM((n, e), F32)]
        + [pltpu.VMEM(*k) for k in kinds[:5]] + [pltpu.VMEM((n, e), F32), DMA((n_seq,)), DMA((24,))],
        compiler_params=pltpu.CompilerParams(vmem_limit_bytes=VMEM_LIMIT),
        cost_estimate=pl.CostEstimate(flops=(4 * n * e * e) // COVER, bytes_accessed=hidden.size * 2 + n * e * 20, transcendentals=n * e),
        name="head",
    )(hidden, pos, w, b, gain, bias)


BLK = 1280
ME, MINE, MINE_ID, TWIN, FAR, FAR_TWIN = range(6)


def rows_kernel(kind, scale, s0, m, cut, n_loc, sources, spots, has_big, pos, emb_hbm, bias_ref, info_ref, *refs):
    refs = list(refs)
    take = lambda n: [refs.pop(0) for _ in range(n)]
    wide = sources is not None
    if wide:
        src = {r: take(2) for r in sources}
        if kind != "own":
            take(1)
    else:
        u_hbm, = take(1)
    if has_big:
        take(1)
    parts = take({"far": 2, "rest": 1}.get(kind, 0))
    puts = take(len(spots))
    out_hbm, = take(1)
    if wide:
        u_hbm, = take(1)
    if kind in ("far", "rest", "whole"):
        big_ref, = take(1)
    if wide:
        buf, = take(1)
    ring, emb_sc, g_sc, acc, hold, sem, tok_sem, back_sem, in_sem, out_sem = refs
    me = pos[ME]
    chip = lax.div(me, 2)
    n_steps = {"own": 2, "again": 2, "side": 4, "far": 2, "rest": 6, "whole": 8}[kind]
    along_x, along_y = chip ^ 1, chip ^ 2

    def device(i):
        side = 2 * jnp.where(i < 2, jnp.minimum(along_x, along_y), jnp.maximum(along_x, along_y)) + lax.rem(i, 2)
        far = 2 * (chip ^ 3) + lax.rem(i, 2)
        if kind in ("own", "again"):
            return 2 * chip + i
        return {"side": side, "far": far, "rest": jnp.where(i < 4, side, far), "whole": i}[kind]

    depth = ring.shape[0]

    def fetch(i):
        slot = lax.rem(i, 2 if wide else depth)
        if not wide:
            pltpu.make_async_copy(u_hbm.at[device(i)], ring.at[slot], tok_sem.at[slot, 0]).start()
            return
        for r, (lo, hi) in src.items():
            @pl.when(device(i) ^ me == r)
            def _():
                pltpu.make_async_copy(lo, buf.at[slot, :cut, :], tok_sem.at[slot, 0]).start()
                pltpu.make_async_copy(hi, buf.at[slot, cut:, :], tok_sem.at[slot, 1]).start()

    row = lambda j, off: pl.multiple_of(pos[j] + off, 8)
    emb_copy = pltpu.make_async_copy(emb_hbm.at[pl.ds(row(MINE, s0), m), :], emb_sc, sem)
    emb_copy.start()
    fetch(0)
    loads, stores = [], []
    for j, (p, (base, off)) in enumerate(zip(puts, spots)):
        n = p.shape[0]
        loads.append(pltpu.make_async_copy(p, hold.at[j, :n, :], in_sem.at[j]))
        stores.append(pltpu.make_async_copy(hold.at[j, :n, :], big_ref.at[pl.ds(row(base, off), n), :], out_sem.at[j]))
    for j, p in enumerate(parts):
        loads.append(pltpu.make_async_copy(p, hold.at[len(puts) + j, :m, :], in_sem.at[len(puts) + j]))
    acc[...] = jnp.zeros_like(acc)
    if wide:
        for k in range(2):
            ring[k, n_loc:, :] = jnp.zeros((BLK - n_loc, ring.shape[2]), BF16)
    emb_copy.wait()
    n_cuts = max(1, round(m / 320))
    cuts = [-(-m * k // (n_cuts * 16)) * 16 for k in range(n_cuts)] + [m]
    cuts = list(zip(cuts[:-1], cuts[1:]))
    kept = lambda i: pltpu.make_async_copy(ring.at[lax.rem(i, 2)], u_hbm.at[device(i)], back_sem.at[lax.rem(i, 2)])

    @pl.loop(0, n_steps)
    def _(i):
        slot = lax.rem(i, 2 if wide else depth)
        if wide:
            any_lo, any_hi = next(iter(src.values()))
            pltpu.make_async_copy(any_lo, buf.at[slot, :cut, :], tok_sem.at[slot, 0]).wait()
            pltpu.make_async_copy(any_hi, buf.at[slot, cut:, :], tok_sem.at[slot, 1]).wait()

            @pl.when(i >= 2)
            def _():
                kept(i - 2).wait()
        else:
            pltpu.make_async_copy(u_hbm.at[device(i)], ring.at[slot], tok_sem.at[slot, 0]).wait()

        @pl.when(i + 1 < n_steps)
        def _():
            fetch(i + 1)

        @pl.when(i == 0)
        def _():
            for c in loads:
                c.start()

        for j, (a, b) in enumerate(zip(loads, stores)):
            @pl.when(i == min(2 + j, n_steps - 1))
            def _():
                a.wait()
                b.start()

        if wide:
            ring[slot, :n_loc, :] = buf[slot].astype(BF16)
            kept(i).start()
        group = (i >= 4).astype(I32) if kind == "rest" else 0
        rel = device(i) ^ me
        lse, lab = info_ref[rel, 0:1, :], info_ref[rel, 1:2, :]

        def weights(r0, r1):
            part = dot(emb_sc[r0:r1, :], ring[slot], NT)
            ids = lax.broadcasted_iota(I32, (r1 - r0, 1), 0) + (pos[MINE_ID] + (s0 + r0))
            g = jnp.exp(part + bias_ref[s0 + r0:s0 + r1, :] - lse) - jnp.where(lab == ids.astype(F32), scale, 0.0)
            g_sc[r0:r1, :] = g.astype(BF16)

        weights(*cuts[0])
        for k, (r0, r1) in enumerate(cuts):
            if k + 1 < len(cuts):
                weights(*cuts[k + 1])
            acc[group, r0:r1, :] += dot(g_sc[r0:r1, :], ring[slot], NN)

    for c in loads[len(puts):]:
        c.wait()
    if kind == "far":
        acc[0] = (hold[0, :m, :] + acc[0]) + hold[1, :m, :]
    if kind == "rest":
        acc[0] = (hold[len(puts), :m, :] + acc[1]) + acc[0]
    done = [pltpu.make_async_copy(acc.at[0], out_hbm, sem)]
    if kind in ("far", "rest", "whole"):
        done.append(pltpu.make_async_copy(acc.at[0], big_ref.at[pl.ds(row(MINE, s0), m), :], emb_sem(tok_sem)))
    for c in done:
        c.start()
    if wide:
        for i in range(n_steps - 2, n_steps):
            kept(i).wait()
    for c in stores + done:
        c.wait()


def emb_sem(tok_sem):
    return tok_sem.at[0, 0]


def rows_pass(kind, scale, v_rows, span, cut, pos, emb, bias, info, tokens=None, u_all=None, big=None, parts=(), puts=()):
    s0, s1 = span
    m, e = s1 - s0, emb.shape[1]
    sds = jax.ShapeDtypeStruct
    wide = kind in ("own", "side", "far")
    final = kind in ("far", "rest", "whole")
    n_dev = info.shape[0]
    args, aliases = [pos, emb, bias, info], {}
    outs = [sds((m, e), F32)]
    sources = None
    if wide:
        sources = {"own": (0, CORE), "side": (X, X | CORE, Y, Y | CORE), "far": (X | Y, X | Y | CORE)}[kind]
        args += [h for r in sources for h in tokens[r]]
        n_loc = tokens[0][0].shape[0] + tokens[0][1].shape[0]
        outs.append(sds((n_dev, BLK, e), BF16))
        if kind != "own":
            aliases[len(args)] = 1
            args.append(u_all)
    else:
        n_loc = BLK
        args.append(u_all)
    if final:
        if big is not None:
            aliases[len(args)] = len(outs)
            args.append(big)
        outs.append(sds((v_rows, e), F32))
    args += list(parts) + [a for _, a in puts]
    n_hold = max(1, len(parts) + len(puts))
    tallest = max([m] * len(parts) + [a.shape[0] for _, a in puts] + [8])
    steps = {"own": 2, "again": 2, "side": 4, "far": 2, "rest": 6, "whole": 8}[kind]
    t = steps * BLK
    scratch = [pltpu.VMEM((2, n_loc, e), F32)] if wide else []
    scratch += [
        pltpu.VMEM((2 if wide else 3, BLK, e), BF16), pltpu.VMEM((m, e), BF16), pltpu.VMEM((m, BLK), BF16),
        pltpu.VMEM((2 if kind == "rest" else 1, m, e), F32), pltpu.VMEM((n_hold, tallest, e), F32),
        DMA, DMA((3, 2)), DMA((2,)), DMA((n_hold,)), DMA((n_hold,)),
    ]
    return pl.pallas_call(
        functools.partial(rows_kernel, kind, scale, s0, m, cut, n_loc, sources, [spot for spot, _ in puts], big is not None),
        in_specs=[SMEM, ANY, VMEM, VMEM] + [ANY] * (len(args) - 4),
        out_specs=[ANY] * len(outs),
        out_shape=outs,
        scratch_shapes=scratch,
        input_output_aliases=aliases,
        compiler_params=pltpu.CompilerParams(vmem_limit_bytes=VMEM_LIMIT),
        cost_estimate=pl.CostEstimate(flops=(4 * t * m * e) // COVER, bytes_accessed=t * e * 2 + m * e * 6, transcendentals=t * m),
    )(*args)


def put_kernel(spots, pos, *refs):
    n = len(spots)
    pieces, (out_ref, hold, in_sem, out_sem) = refs[1:1 + n], refs[1 + n:]
    loads, stores = [], []
    for j, (p, (base, off)) in enumerate(zip(pieces, spots)):
        slot = hold.at[j, :p.shape[0], :]
        loads.append(pltpu.make_async_copy(p, slot, in_sem.at[j]))
        stores.append(pltpu.make_async_copy(slot, out_ref.at[pl.ds(pl.multiple_of(pos[base] + off, 8), p.shape[0]), :], out_sem.at[j]))
    for a in loads:
        a.start()
    for a, b in zip(loads, stores):
        a.wait()
        b.start()
    for b in stores:
        b.wait()


def put_rows(pos, big, puts):
    spots, pieces = [s for s, _ in puts], [a for _, a in puts]
    n, e = len(pieces), big.shape[1]
    size = sum(p.size for p in pieces)
    return pl.pallas_call(
        functools.partial(put_kernel, spots),
        in_specs=[SMEM] + [ANY] * (n + 1),
        out_specs=ANY,
        out_shape=jax.ShapeDtypeStruct(big.shape, big.dtype),
        scratch_shapes=[pltpu.VMEM((n, max(p.shape[0] for p in pieces), e), F32), DMA((n,)), DMA((n,))],
        input_output_aliases={1: 0},
        compiler_params=pltpu.CompilerParams(vmem_limit_bytes=VMEM_LIMIT),
        cost_estimate=pl.CostEstimate(flops=(size) // COVER, bytes_accessed=size * 8, transcendentals=0),
        name="put_rows",
    )(pos, big, *pieces)


def join_kernel(n_vec, idx, *refs):
    own, mine, theirs, (dw_ref, vec_ref, full, in_sem, out_sem) = refs[0], refs[1:4], refs[4:7], refs[7:]
    vp, core = idx[0], idx[1]
    half, cols = mine[0].shape
    col = lambda k: pl.ds(pl.multiple_of((vp ^ k) * cols, cols), cols)
    row = lambda c: pl.ds(pl.multiple_of(c * half, 8), half)
    loads = [pltpu.make_async_copy(own.at[:2 * half, :], full.at[:, col(0)], in_sem.at[0])]
    for k in range(3):
        loads.append(pltpu.make_async_copy(mine[k], full.at[row(core), col(k + 1)], in_sem.at[1 + k]))
        loads.append(pltpu.make_async_copy(theirs[k], full.at[row(1 - core), col(k + 1)], in_sem.at[4 + k]))
    for c in loads:
        c.start()
    for c in loads:
        c.wait()
    e = dw_ref.shape[0]
    stores = [pltpu.make_async_copy(full.at[:e, :], dw_ref, out_sem.at[0]), pltpu.make_async_copy(full.at[e:e + n_vec, :], vec_ref, out_sem.at[1])]
    for c in stores:
        c.start()
    for c in stores:
        c.wait()


def join_pass(idx, own, mine, theirs):
    half, cols = mine[0].shape
    e = 4 * cols
    return pl.pallas_call(
        functools.partial(join_kernel, 8),
        in_specs=[SMEM] + [ANY] * 7,
        out_specs=[ANY] * 2,
        out_shape=[jax.ShapeDtypeStruct((e, e), F32), jax.ShapeDtypeStruct((8, e), F32)],
        scratch_shapes=[pltpu.VMEM((2 * half, e), F32), DMA((7,)), DMA((2,))],
        compiler_params=pltpu.CompilerParams(vmem_limit_bytes=VMEM_LIMIT),
        cost_estimate=pl.CostEstimate(flops=(e * e) // COVER, bytes_accessed=e * e * 8, transcendentals=0),
        name="join",
    )(idx, own, *mine, *theirs)


def back_kernel(vp, pre_ref, norm_ref, rstd_ref, z_ref, du_ref, m1_ref, m2_ref, gain_ref, loss_ref, db_ref, dab_ref, pack_ref):
    e, cols = z_ref.shape[1], du_ref.shape[1]
    for c in range(0, cols, 128):
        cs = slice(c, c + 128)
        a, du, normed = pre_ref[:, cs], du_ref[:, cs], norm_ref[:, cs]
        cdf = 0.5 * (1.0 + lax.erf(a * (0.5 ** 0.5)))
        dg = rstd_ref[...] * (du * gain_ref[:, cs] - m1_ref[...] - normed * m2_ref[...])
        da = dg * (cdf + a * (jnp.exp(-0.5 * a * a) * 0.3989422804014327))
        dab_ref[:, cs] = da.astype(BF16).astype(F32)
        for j, x in enumerate((da, du * normed, du)):
            pack_ref[e + j:e + j + 1, cs] = jnp.sum(x, axis=0, keepdims=True)
    pack_ref[:e, :] = lax.dot_general(z_ref[...], dab_ref[...].astype(BF16), (((0,), (0,)), ((), ())), preferred_element_type=F32)
    pack_ref[e + 3:e + 4, :] = loss_ref[...]
    pack_ref[e + 4:e + 16, :] = jnp.zeros_like(pack_ref[e + 4:e + 16, :])
    pack_ref[e + 16:, :] = db_ref[...]


def back_pass(vp, pre, normed, rstd, z, du, m1, m2, gain, loss, db):
    n, cols = du.shape
    e = z.shape[1]
    n_pack = e + 16 + db.shape[0]
    block = lambda *s: pl.BlockSpec(s, lambda i, p: (0,) * len(s))
    share = lambda r: pl.BlockSpec((r, cols), lambda i, p: (0, p[0]))
    gs = pltpu.PrefetchScalarGridSpec(
        num_scalar_prefetch=1,
        grid=(1,),
        in_specs=[share(n), share(n), block(n, 128), block(n, e), block(n, cols), block(n, 128), block(n, 128), share(1), block(1, cols), block(*db.shape)],
        out_specs=[block(n, cols), block(n_pack, cols)],
    )
    return pl.pallas_call(
        back_kernel,
        grid_spec=gs,
        out_shape=[jax.ShapeDtypeStruct((n, cols), F32), jax.ShapeDtypeStruct((n_pack, cols), F32)],
        compiler_params=pltpu.CompilerParams(dimension_semantics=("arbitrary",), vmem_limit_bytes=VMEM_LIMIT),
        cost_estimate=pl.CostEstimate(flops=(2 * n * e * cols) // COVER, bytes_accessed=n * (cols * 16 + e * 2 + 1536), transcendentals=n * cols * 2),
        name="back",
    )(vp, pre, normed, rstd, z, du, m1, m2, gain, loss, db)


def spread_kernel(n_masks, vp, pos_ref, w_ref, *refs):
    pieces, (out_ref, dab, dz, obuf, in_sem, out_sem) = refs[:4], refs[4:]
    n, cols = pieces[0].shape
    loads = [pltpu.make_async_copy(p, dab.at[:, pl.ds(pl.multiple_of((vp[0] ^ k) * cols, cols), cols)], in_sem.at[k]) for k, p in enumerate(pieces)]
    for c in loads:
        c.start()
    dz[n:, :] = jnp.zeros((dz.shape[0] - n, dz.shape[1]), F32)
    n_seq, seq_len, _ = out_ref.shape
    place = lax.broadcasted_iota(I32, (seq_len, 1), 0)
    slots = pos_ref.shape[2]
    for c in loads:
        c.wait()
    stores, done = [], 0
    for b in range(n_seq):
        while done < min(n, b * n_masks + slots):
            r1 = min(n, done + 304)
            dz[done:r1, :] = dot(dab[done:r1, :].astype(BF16), w_ref[...], NT).astype(BF16).astype(F32)
            done = r1
        if b >= 4:
            stores[b - 4].wait()
        hot = jnp.where(place == pos_ref[b], 1.0, 0.0).astype(BF16)
        obuf[b % 4] = dot(hot, dz[b * n_masks:b * n_masks + slots, :].astype(BF16), NN).astype(BF16)
        c = pltpu.make_async_copy(obuf.at[b % 4], out_ref.at[b], out_sem.at[b])
        c.start()
        stores.append(c)
    for c in stores[-4:]:
        c.wait()


def spread_pass(n_masks, shape, vp, pos, w, pieces):
    n, cols = pieces[0].shape
    e = w.shape[0]
    return pl.pallas_call(
        functools.partial(spread_kernel, n_masks),
        in_specs=[SMEM, VMEM, VMEM] + [ANY] * 4,
        out_specs=ANY,
        out_shape=jax.ShapeDtypeStruct(shape, BF16),
        scratch_shapes=[pltpu.VMEM((n, 4 * cols), F32), pltpu.VMEM((n + 16, e), F32), pltpu.VMEM((4,) + shape[1:], BF16), DMA((4,)), DMA((shape[0],))],
        compiler_params=pltpu.CompilerParams(vmem_limit_bytes=VMEM_LIMIT),
        cost_estimate=pl.CostEstimate(flops=(2 * shape[0] * shape[1] * 128 * e) // COVER, bytes_accessed=shape[0] * shape[1] * e * 2, transcendentals=0),
        name="spread",
    )(vp, pos, w, *pieces)


def order_sum(xs):
    return (xs[0] + xs[1]) + (xs[2] + xs[3])


def after(x, *deps):
    return lax.optimization_barrier((x, deps))[0]


def solution(mesh):
    n_groups, n_shards = mesh.shape["dp"], mesh.shape["vp"]

    def swap(a, bit):
        return lax.ppermute(a, "dp", [(d, d ^ bit) for d in range(n_groups)])

    def swap_vp(a, bit):
        return lax.ppermute(a, "vp", [(d, d ^ bit) for d in range(n_shards)])

    def hop(a):
        return lax.ppermute(a, "dp", [(d, d ^ (Y if d & CORE else X)) for d in range(n_groups)])

    def local_step(hidden, mask_pos, labels, w_trans, b_trans, ln_gain, ln_bias, emb_table, b_vocab):
        n_rows, _, width = hidden.shape
        n_masks = mask_pos.shape[1]
        shard_rows = emb_table.shape[0]
        n_loc = n_rows * n_masks
        n_tokens = n_loc * n_groups
        slots = -(-n_masks // 16) * 16
        cut = n_loc // 32 * 16
        cols = width // n_shards
        dp, vp = lax.axis_index("dp"), lax.axis_index("vp")
        row_start = vp * shard_rows
        scale = 1.0 / n_tokens
        core, mine = dp & 1, (dp >> 1 ^ dp >> 2) & 1

        pos_pad = jnp.pad(mask_pos, ((0, 0), (0, slots - n_masks)), constant_values=-1)
        z, pre, normed, rstd, u, u_lo, u_hi = head_pass(
            n_masks, cut, hidden, jnp.broadcast_to(pos_pad[:, :, None], (n_rows, slots, 128)),
            w_trans, b_trans[None], ln_gain[None], ln_bias[None])

        x_lo, y_hi = swap(u_lo, X), swap(u_hi, Y)
        x_hi, y_lo = swap(u_hi, X), swap(u_lo, Y)
        c_lo, c_hi = swap(u_lo, CORE), swap(u_hi, CORE)

        flat_labels = labels.reshape(n_loc)
        lab_local = flat_labels - row_start
        lab_local = jnp.where((lab_local >= 0) & (lab_local < shard_rows), lab_local, -1)
        lab_local = jnp.broadcast_to(lab_local[:, None], (n_loc, 128))
        logits, stat = stats(u, emb_table, b_vocab[None], lab_local)
        x_lo, y_hi = after((x_lo, y_hi), stat)
        d_lo, d_hi = swap(x_lo, Y), swap(y_hi, X)
        cx_lo, cy_hi = swap(x_lo, CORE), swap(y_hi, CORE)
        all_stats = [stat] + [swap_vp(stat, b) for b in range(1, n_shards)]
        global_max = functools.reduce(jnp.maximum, [s[0] for s in all_stats])
        log_norm = global_max + jnp.log(order_sum([s[1] * jnp.exp(s[0] - global_max) for s in all_stats]))
        loss_part = jnp.sum(log_norm - order_sum([s[2] for s in all_stats]))
        lse = log_norm + jnp.log(jnp.float32(n_tokens))

        du_part, db_part, sums = du_pass(
            scale, n_shards, logits, emb_table, jnp.broadcast_to(lse[:, None], (n_loc, 128)), lab_local, normed, ln_gain[None])
        du_share = lax.psum_scatter(du_part.reshape(n_shards * n_loc, cols), "vp", scatter_dimension=0, tiled=True)

        lse, x_hi, y_lo = after((lse, x_hi, y_lo), du_part)
        fill = (0, BLK - n_loc)
        info = jnp.stack([jnp.pad(lse, fill, constant_values=jnp.inf), jnp.pad(flat_labels.astype(F32), fill, constant_values=-1.0)])[None]
        for bit in (CORE, X, Y):
            info = jnp.concatenate([info, swap(info, bit)])

        half, quarter = shard_rows // 2, shard_rows // 4
        start = lambda h, c: h * half + c * quarter
        pos = jnp.stack([dp, start(mine, core), row_start + start(mine, core), start(mine, 1 - core), start(1 - mine, core), start(1 - mine, 1 - core)])
        bias_col = lax.dynamic_slice(b_vocab, (start(mine, core),), (quarter,))[:, None]
        shares = (640, 896, 896, 712)
        ends = [0]
        for w in shares[:-1]:
            ends.append(ends[-1] + max(16, quarter * w // sum(shares) // 16 * 16))
        spans = list(zip(ends, ends[1:] + [quarter]))

        def rows(kind, k, *wait, **kw):
            return rows_pass(kind, scale, shard_rows, spans[k], cut, after(pos, *wait), emb_table, bias_col, info, **kw)

        def send(k, chunk):
            return ((TWIN, spans[k][0]), swap(chunk, CORE)), hop(chunk)

        def forward(k, far, *wait):
            far = after(far, *wait)
            return ((FAR, spans[k][0]), far), ((FAR_TWIN, spans[k][0]), swap(far, CORE))

        tokens = {0: (u_lo, u_hi), CORE: (c_lo, c_hi), X: (x_lo, x_hi), Y: (y_lo, y_hi)}
        own0, u_all = rows("own", 0, tokens=tokens)
        own1, = rows("again", 1, own0, u_all=u_all)
        x_hi, y_lo = after((x_hi, y_lo), own1)
        tokens[X | CORE] = cx_lo, swap(x_hi, CORE)
        tokens[Y | CORE] = swap(y_lo, CORE), cy_hi
        tokens[X], tokens[Y] = (x_lo, x_hi), (y_lo, y_hi)
        side0, u_all = rows("side", 0, tokens=tokens, u_all=u_all)
        d_lo, d_hi = after((d_lo, d_hi), side0)
        tokens[X | Y] = d_lo, d_hi
        tokens[X | Y | CORE] = swap(d_lo, CORE), swap(d_hi, CORE)
        chunk0, u_all, big = rows("far", 0, tokens=tokens, u_all=u_all, parts=(own0, side0))
        twin0, far0 = send(0, chunk0)

        du_share = after(du_share, chunk0)
        sums = [sums] + [swap_vp(sums, b) for b in range(1, n_shards)]
        sums = order_sum(sums) / width
        m1, m2 = (jnp.broadcast_to(sums[j][:, None], (n_loc, 128)) for j in range(2))
        loss_row = jnp.pad(loss_part[None, None], ((0, 0), (0, cols - 1)))
        db_rows = -(-shard_rows // cols // 8) * 8
        db_mat = jnp.pad(db_part[0], (0, db_rows * cols - shard_rows)).reshape(db_rows, cols)
        dab, pack = back_pass(vp[None], pre, normed, rstd, z, du_share, m1, m2, ln_gain[None], loss_row, db_mat)
        back_done = dab
        pack = lax.psum(pack, "dp")
        dab = [dab] + [swap_vp(dab, b) for b in range(1, n_shards)]

        chunk1, big = rows("rest", 1, back_done, u_all=u_all, big=big, parts=(own1,))
        twin1, far1 = send(1, chunk1)
        far0, far_twin0 = forward(0, far0, chunk1)

        chunk2, big = rows("whole", 2, u_all=u_all, big=big, puts=[twin0, far0])
        twin2, far2 = send(2, chunk2)
        far1, far_twin1 = forward(1, far1, chunk2)
        pack = after(pack, chunk2)
        n_half = (width + 16) // 2
        part = lax.dynamic_slice(pack, (core * n_half, 0), (n_half, cols))
        parts = [swap_vp(part, b) for b in range(1, n_shards)]

        chunk3, big = rows("whole", 3, part, u_all=u_all, big=big, puts=[far_twin0, twin1, far1])
        twin3, far3 = send(3, chunk3)
        far2, far_twin2 = forward(2, far2, chunk3)
        d_hidden = spread_pass(n_masks, hidden.shape, vp[None], pos_pad[:, None], w_trans, after(dab, chunk3))
        parts = after(parts, d_hidden)
        others = [swap(p, CORE) for p in parts]
        big = put_rows(pos, big, [far_twin1, twin2, far2, far_twin2, twin3])
        pack, parts, others = after((pack, parts, others), big)
        d_w, vec = join_pass(jnp.stack([vp, core]), pack, parts, others)
        far3 = after(far3, big)
        far3, far_twin3 = forward(3, far3)
        big = put_rows(pos, big, [far3])
        big = put_rows(pos, big, [far_twin3])

        db = pack[width + 16:].reshape(-1)[:shard_rows]
        return pack[width + 3, 0] / n_tokens, d_hidden, d_w, vec[0], vec[1], vec[2], big, db

    in_specs = (P("dp", None, None), P("dp", None), P("dp", None), P(None, None), P(None), P(None), P(None), P("vp", None), P("vp"))
    out_specs = (P(), P("dp", None, None), P(None, None), P(None), P(None), P(None), P("vp", None), P("vp"))
    return jax.shard_map(local_step, mesh=mesh, in_specs=in_specs, out_specs=out_specs, check_vma=False)
```

```python
import functools

import jax
import jax.numpy as jnp
from jax import lax
from jax.experimental import pallas as pl
from jax.experimental.pallas import tpu as pltpu
from jax.sharding import PartitionSpec as P


F32, BF16, I32 = jnp.float32, jnp.bfloat16, jnp.int32
NT = (((1,), (1,)), ((), ()))
NN = (((1,), (0,)), ((), ()))
VB = 1024
VMEM_LIMIT = 60 << 20
COVER = 100
CH = 16


def row_cuts(rows, parts=4):
    cuts = [16 * (rows // 16 * k // parts) for k in range(parts)] + [rows]
    return list(zip(cuts[:-1], cuts[1:]))


def dot(a, b, dims):
    return lax.dot_general(a, b, dims, preferred_element_type=F32)


def stats_kernel(n_vocab, u_ref, emb_ref, b_ref, lab_ref, logits_ref, stat_ref, m_sc, s_sc, l_sc):
    i, n_blocks = pl.program_id(0), pl.num_programs(0)
    lane = lax.broadcasted_iota(I32, (1, 128), 1)

    @pl.when(i == 0)
    def _():
        m_sc[...] = jnp.full_like(m_sc, -jnp.inf)
        s_sc[...] = jnp.zeros_like(s_sc)
        l_sc[...] = jnp.zeros_like(l_sc)

    def run(width):
        wide = -(-width // 128) * 128
        for r0, r1 in row_cuts(u_ref.shape[0]):
            tile = dot(u_ref[r0:r1, :], emb_ref[:wide, :], NT) + b_ref[:, :wide]
            if wide > width:
                tile = jnp.where(lax.broadcasted_iota(I32, (1, wide), 1) < width, tile, -jnp.inf)
            logits_ref[r0:r1, :wide] = tile
            for q in range(r0, r1, CH):
                rs = slice(q, min(q + CH, r1))
                parts = [logits_ref[rs, k:k + 128] for k in range(0, wide, 128)]
                m_old = m_sc[rs, :]
                m_new = functools.reduce(jnp.maximum, parts, m_old)
                s_new = s_sc[rs, :] * jnp.exp(m_old - m_new)
                l_new = l_sc[rs, :]
                lab = lab_ref[rs, :] - i * VB
                for k, part in enumerate(parts):
                    s_new += jnp.exp(part - m_new)
                    l_new = jnp.where(lab == lane + k * 128, part, l_new)
                m_sc[rs, :], s_sc[rs, :], l_sc[rs, :] = m_new, s_new, l_new

    tail = n_vocab % VB
    if tail:
        pl.when(i < n_blocks - 1)(functools.partial(run, VB))
        pl.when(i == n_blocks - 1)(functools.partial(run, tail))
    else:
        run(VB)

    @pl.when(i == n_blocks - 1)
    def _():
        m_t, s_t, l_t = m_sc[...].T, s_sc[...].T, l_sc[...].T
        m_all = jnp.max(m_t, axis=0, keepdims=True)
        stat_ref[0:1, :] = m_all
        stat_ref[1:2, :] = jnp.sum(s_t * jnp.exp(m_t - m_all), axis=0, keepdims=True)
        stat_ref[2:3, :] = jnp.sum(l_t, axis=0, keepdims=True)
        stat_ref[3:8, :] = jnp.zeros_like(stat_ref[3:8, :])


def stats(u, emb, bias, lab):
    t, e = u.shape
    v = emb.shape[0]
    n = pl.cdiv(v, VB)
    whole = lambda *s: pl.BlockSpec(s, lambda i: (0,) * len(s))
    return pl.pallas_call(
        functools.partial(stats_kernel, v),
        grid=(n,),
        in_specs=[whole(t, e), pl.BlockSpec((VB, e), lambda i: (i, 0)), pl.BlockSpec((1, VB), lambda i: (0, i)), whole(t, 128)],
        out_specs=[pl.BlockSpec((t, VB), lambda i: (0, i)), whole(8, t)],
        out_shape=[jax.ShapeDtypeStruct((t, v), F32), jax.ShapeDtypeStruct((8, t), F32)],
        scratch_shapes=[pltpu.VMEM((t, 128), F32)] * 3,
        compiler_params=pltpu.CompilerParams(dimension_semantics=("arbitrary",), vmem_limit_bytes=VMEM_LIMIT),
        cost_estimate=pl.CostEstimate(flops=(2 * t * v * e) // COVER, bytes_accessed=t * v * 4 + v * e * 2, transcendentals=t * v),
        name="stats",
    )(u, emb, bias, lab)


def du_kernel(n_vocab, scale, logits_ref, emb_ref, lse_ref, lab_ref, norm_hbm, gain_ref, out_ref, db_ref, sum_ref, du_ref, g_sc, db_sc, norm_sc, db_sc2, sem):
    i, n_blocks = pl.program_id(0), pl.num_programs(0)
    t = logits_ref.shape[0]
    lane = lax.broadcasted_iota(I32, (1, 128), 1)

    norm_copy = pltpu.make_async_copy(norm_hbm, norm_sc, sem)

    @pl.when(i == 0)
    def _():
        du_ref[...] = jnp.zeros_like(du_ref)

    @pl.when(i == 2)
    def _():
        norm_copy.start()

    def run(width):
        wide = -(-width // 128) * 128
        emb = emb_ref[:wide, :]
        if wide > width:
            emb = jnp.where(lax.broadcasted_iota(I32, (wide, 1), 0) < width, emb, jnp.zeros_like(emb))
        for r0, r1 in row_cuts(t):
            sums = [None] * (wide // 128)
            for q in range(r0, r1, 16):
                rs = slice(q, q + 16)
                lse = lse_ref[rs, :]
                lab = lab_ref[rs, :] - i * VB
                for k in range(wide // 128):
                    c = k * 128
                    g = jnp.exp(logits_ref[rs, c:c + 128] - lse)
                    g -= jnp.where(lab == lane + c, scale, 0.0)
                    if c + 128 > width:
                        g = jnp.where(lane < width - c, g, 0.0)
                    part = g[:8] + g[8:]
                    sums[k] = part if sums[k] is None else sums[k] + part
                    g_sc[rs, c:c + 128] = g.astype(BF16)
            for k in range(wide // 128):
                cs = slice(k * 128, (k + 1) * 128)
                db_sc[:, cs] = sums[k] if r0 == 0 else db_sc[:, cs] + sums[k]
            du_ref[r0:r1, :] += dot(g_sc[r0:r1, :wide], emb, NN)
        db_ref[:, :wide] = jnp.sum(db_sc[:, :wide], axis=0, keepdims=True)

    tail = n_vocab % VB
    if tail:
        pl.when(i < n_blocks - 1)(functools.partial(run, VB))
        pl.when(i == n_blocks - 1)(functools.partial(run, tail))
    else:
        run(VB)

    @pl.when(i == n_blocks - 1)
    def _():
        norm_copy.wait()
        parts, rows, cols = out_ref.shape
        for r in range(0, rows, 112):
            rs = slice(r, r + 112)
            total = [jnp.zeros((112, 128), F32)] * 2
            for c in range(0, parts * cols, 128):
                x = du_ref[rs, c:c + 128].astype(BF16).astype(F32)
                out_ref[c // cols, rs, c % cols:c % cols + 128] = x
                dn = x * gain_ref[:, c:c + 128]
                total = [total[0] + dn, total[1] + dn * norm_sc[rs, c:c + 128]]
            for j, x in enumerate(total):
                db_sc2[j, rs, :] = x
        for j in range(2):
            sum_ref[j:j + 1, :] = jnp.sum(db_sc2[j].T, axis=0, keepdims=True)
        sum_ref[2:, :] = jnp.zeros_like(sum_ref[2:, :])


def du_pass(scale, parts, logits, emb, lse, lab, normed, gain):
    t, v = logits.shape
    e = emb.shape[1]
    n = pl.cdiv(v, VB)
    whole = lambda *s: pl.BlockSpec(s, lambda i: (0,) * len(s))
    return pl.pallas_call(
        functools.partial(du_kernel, v, scale),
        grid=(n,),
        in_specs=[pl.BlockSpec((t, VB), lambda i: (0, i)), pl.BlockSpec((VB, e), lambda i: (i, 0)), whole(t, 128), whole(t, 128), pl.BlockSpec(memory_space=pl.ANY), whole(1, e)],
        out_specs=[whole(parts, t, e // parts), pl.BlockSpec((1, VB), lambda i: (0, i)), whole(8, t)],
        out_shape=[jax.ShapeDtypeStruct((parts, t, e // parts), F32), jax.ShapeDtypeStruct((1, v), F32), jax.ShapeDtypeStruct((8, t), F32)],
        scratch_shapes=[pltpu.VMEM((t, e), F32), pltpu.VMEM((t, VB), BF16), pltpu.VMEM((8, VB), F32), pltpu.VMEM((t, e), F32), pltpu.VMEM((2, t, 128), F32), pltpu.SemaphoreType.DMA],
        compiler_params=pltpu.CompilerParams(dimension_semantics=("arbitrary",), vmem_limit_bytes=VMEM_LIMIT),
        cost_estimate=pl.CostEstimate(flops=(2 * t * v * e) // COVER, bytes_accessed=t * v * 4 + v * e * 2, transcendentals=t * v),
        name="du_pass",
    )(logits, emb, lse, lab, normed, gain)


LN_EPS = 1e-5
CORE, X, Y = 1, 2, 4
ANY = pl.BlockSpec(memory_space=pl.ANY)
VMEM = pl.BlockSpec(memory_space=pltpu.VMEM)
SMEM = pl.BlockSpec(memory_space=pltpu.SMEM)
DMA = pltpu.SemaphoreType.DMA


def gelu_norm(a):
    cdf = 0.5 * (1.0 + lax.erf(a * (0.5 ** 0.5)))
    g = a * cdf
    centered = g - jnp.mean(g, axis=1, keepdims=True)
    rstd = lax.rsqrt(jnp.mean(centered * centered, axis=1, keepdims=True) + LN_EPS)
    return cdf, centered * rstd, rstd


def head_kernel(n_masks, cut, hid, pos_ref, w_ref, b_ref, gain_ref, bias_ref, z_out, pre_out, norm_out, rstd_out, u_out, lo_out, hi_out,
                hbuf, zf, zb, pre_v, norm_v, rstd_v, ub, uf, in_sem, out_sem):
    n_seq, seq_len = hid.shape[0], hid.shape[1]
    n_loc = n_seq * n_masks
    loads = [pltpu.make_async_copy(hid.at[b], hbuf.at[b], in_sem.at[b]) for b in range(n_seq)]
    for c in loads:
        c.start()
    lane = lax.broadcasted_iota(I32, (1, 128), 1)
    cuts = [0, cut // 32 * 16, cut, cut + (n_loc - cut) // 32 * 16, n_loc]
    done, stores = 0, []

    def send(src, dst, r0, r1, base=0):
        c = pltpu.make_async_copy(src.at[r0:r1, :], dst.at[r0 - base:r1 - base, :], out_sem.at[len(stores)])
        c.start()
        stores.append(c)

    for b in range(n_seq):
        loads[b].wait()
        hot = jnp.concatenate([jnp.where(pos_ref[b] == lane + j, 1.0, 0.0).astype(BF16) for j in range(0, seq_len, 128)], axis=1)
        zf[b * n_masks:(b + 1) * n_masks, :] = dot(hot, hbuf[b], NN)[:n_masks, :]
        while done < 4 and cuts[done + 1] <= (b + 1) * n_masks:
            r0, r1 = cuts[done], cuts[done + 1]
            z = zf[r0:r1, :].astype(BF16)
            zb[r0:r1, :] = z
            a = dot(z, w_ref[...], NN) + b_ref[...]
            pre_v[r0:r1, :] = a
            _, normed, rstd = gelu_norm(a)
            norm_v[r0:r1, :] = normed
            rstd_v[r0:r1, :] = jnp.broadcast_to(rstd, (r1 - r0, 128))
            u = (normed * gain_ref[...] + bias_ref[...]).astype(BF16)
            ub[r0:r1, :] = u
            uf[r0:r1, :] = u.astype(F32)
            done += 1
            send(uf, hi_out if r0 >= cut else lo_out, r0, r1, cut if r0 >= cut else 0)
            for src, dst in ((ub, u_out), (zb, z_out), (pre_v, pre_out), (norm_v, norm_out), (rstd_v, rstd_out)):
                send(src, dst, r0, r1)
    for c in stores:
        c.wait()


def head_pass(n_masks, cut, hidden, pos, w, b, gain, bias):
    n_seq, seq_len, e = hidden.shape
    n = n_seq * n_masks
    kinds = [((n, e), BF16), ((n, e), F32), ((n, e), F32), ((n, 128), F32), ((n, e), BF16), ((cut, e), F32), ((n - cut, e), F32)]
    return pl.pallas_call(
        functools.partial(head_kernel, n_masks, cut),
        in_specs=[ANY] + [VMEM] * 5,
        out_specs=[ANY] * len(kinds),
        out_shape=[jax.ShapeDtypeStruct(*k) for k in kinds],
        scratch_shapes=[pltpu.VMEM((n_seq, seq_len, e), BF16), pltpu.VMEM((n, e), F32)]
        + [pltpu.VMEM(*k) for k in kinds[:5]] + [pltpu.VMEM((n, e), F32), DMA((n_seq,)), DMA((24,))],
        compiler_params=pltpu.CompilerParams(vmem_limit_bytes=VMEM_LIMIT),
        cost_estimate=pl.CostEstimate(flops=(4 * n * e * e) // COVER, bytes_accessed=hidden.size * 2 + n * e * 20, transcendentals=n * e),
        name="head",
    )(hidden, pos, w, b, gain, bias)


BLK = 1280
STEPS = {"own": 2, "again": 2, "side": 4, "far": 2, "last": 2, "whole": 8}
ME, MINE, MINE_ID, TWIN, FAR, FAR_TWIN = range(6)


def rows_kernel(kind, scale, s0, m, cut, n_loc, sources, skips, spots, has_big, pos, emb_hbm, bias_ref, info_ref, *refs):
    refs = list(refs)
    take = lambda n: [refs.pop(0) for _ in range(n)]
    wide = sources is not None
    if wide:
        src = {r: take(2) for r in sources}
        if kind != "own":
            take(1)
    else:
        u_hbm, = take(1)
    if has_big:
        take(1)
    parts = take(len(skips))
    puts = take(len(spots))
    out_hbm, = take(1)
    if wide:
        u_hbm, = take(1)
    if kind in ("far", "last", "whole"):
        big_ref, = take(1)
    if wide:
        buf, = take(1)
    ring, emb_sc, g_sc, acc, hold, sem, tok_sem, back_sem, in_sem, out_sem = refs
    me = pos[ME]
    chip = lax.div(me, 2)
    n_steps = STEPS[kind]
    along_x, along_y = chip ^ 1, chip ^ 2

    def device(i):
        side = 2 * jnp.where(i < 2, jnp.minimum(along_x, along_y), jnp.maximum(along_x, along_y)) + lax.rem(i, 2)
        far = 2 * (chip ^ 3) + lax.rem(i, 2)
        if kind in ("own", "again"):
            return 2 * chip + i
        return {"side": side, "far": far, "last": far, "whole": i}[kind]

    depth = ring.shape[0]

    def fetch(i):
        slot = lax.rem(i, 2 if wide else depth)
        if not wide:
            pltpu.make_async_copy(u_hbm.at[device(i)], ring.at[slot], tok_sem.at[slot, 0]).start()
            return
        for r, (lo, hi) in src.items():
            @pl.when(device(i) ^ me == r)
            def _():
                pltpu.make_async_copy(lo, buf.at[slot, :cut, :], tok_sem.at[slot, 0]).start()
                pltpu.make_async_copy(hi, buf.at[slot, cut:, :], tok_sem.at[slot, 1]).start()

    row = lambda j, off: pl.multiple_of(pos[j] + off, 8)
    emb_copy = pltpu.make_async_copy(emb_hbm.at[pl.ds(row(MINE, s0), m), :], emb_sc, sem)
    emb_copy.start()
    fetch(0)
    loads, stores = [], []
    for j, (p, (base, off)) in enumerate(zip(puts, spots)):
        n = p.shape[0]
        loads.append(pltpu.make_async_copy(p, hold.at[j, :n, :], in_sem.at[j]))
        stores.append(pltpu.make_async_copy(hold.at[j, :n, :], big_ref.at[pl.ds(row(base, off), n), :], out_sem.at[j]))
    for j, (p, skip) in enumerate(zip(parts, skips)):
        loads.append(pltpu.make_async_copy(p.at[skip:skip + m, :], hold.at[len(puts) + j, :m, :], in_sem.at[len(puts) + j]))
    acc[...] = jnp.zeros_like(acc)
    if wide:
        for k in range(2):
            ring[k, n_loc:, :] = jnp.zeros((BLK - n_loc, ring.shape[2]), BF16)
    emb_copy.wait()
    n_cuts = max(1, round(m / 300))
    cuts = [-(-m * k // (n_cuts * 16)) * 16 for k in range(n_cuts)] + [m]
    cuts = list(zip(cuts[:-1], cuts[1:]))
    kept = lambda i: pltpu.make_async_copy(ring.at[lax.rem(i, 2)], u_hbm.at[device(i)], back_sem.at[lax.rem(i, 2)])

    @pl.loop(0, n_steps)
    def _(i):
        slot = lax.rem(i, 2 if wide else depth)
        if wide:
            any_lo, any_hi = next(iter(src.values()))
            pltpu.make_async_copy(any_lo, buf.at[slot, :cut, :], tok_sem.at[slot, 0]).wait()
            pltpu.make_async_copy(any_hi, buf.at[slot, cut:, :], tok_sem.at[slot, 1]).wait()

            @pl.when(i >= 2)
            def _():
                kept(i - 2).wait()
        else:
            pltpu.make_async_copy(u_hbm.at[device(i)], ring.at[slot], tok_sem.at[slot, 0]).wait()

        @pl.when(i + 1 < n_steps)
        def _():
            fetch(i + 1)

        @pl.when(i == 0)
        def _():
            for c in loads:
                c.start()

        for j, (a, b) in enumerate(zip(loads, stores)):
            @pl.when(i == min(2 + j, n_steps - 1))
            def _():
                a.wait()
                b.start()

        if wide:
            ring[slot, :n_loc, :] = buf[slot].astype(BF16)
            kept(i).start()
        rel = device(i) ^ me
        lse, lab = info_ref[rel, 0:1, :], info_ref[rel, 1:2, :]

        def weights(r0, r1):
            part = dot(emb_sc[r0:r1, :], ring[slot], NT)
            ids = lax.broadcasted_iota(I32, (r1 - r0, 1), 0) + (pos[MINE_ID] + (s0 + r0))
            g = jnp.exp(part + bias_ref[s0 + r0:s0 + r1, :] - lse) - jnp.where(lab == ids.astype(F32), scale, 0.0)
            g_sc[r0:r1, :] = g.astype(BF16)

        weights(*cuts[0])
        for k, (r0, r1) in enumerate(cuts):
            if k + 1 < len(cuts):
                weights(*cuts[k + 1])
            acc[r0:r1, :] += dot(g_sc[r0:r1, :], ring[slot], NN)

    for c in loads[len(puts):]:
        c.wait()
    if parts:
        acc[...] = (hold[len(puts), :m, :] + acc[...]) + hold[len(puts) + 1, :m, :]
    done = [pltpu.make_async_copy(acc, out_hbm, sem)]
    if kind in ("far", "last", "whole"):
        done.append(pltpu.make_async_copy(acc, big_ref.at[pl.ds(row(MINE, s0), m), :], emb_sem(tok_sem)))
    for c in done:
        c.start()
    if wide:
        for i in range(n_steps - 2, n_steps):
            kept(i).wait()
    for c in stores + done:
        c.wait()


def emb_sem(tok_sem):
    return tok_sem.at[0, 0]


def rows_pass(kind, scale, v_rows, span, cut, pos, emb, bias, info, tokens=None, u_all=None, big=None, parts=(), puts=()):
    s0, s1 = span
    m, e = s1 - s0, emb.shape[1]
    sds = jax.ShapeDtypeStruct
    wide = kind in ("own", "side", "far")
    final = kind in ("far", "last", "whole")
    args, aliases = [pos, emb, bias, info], {}
    outs = [sds((m, e), F32)]
    sources = None
    if wide:
        sources = {"own": (0, CORE), "side": (X, X | CORE, Y, Y | CORE), "far": (X | Y, X | Y | CORE)}[kind]
        args += [h for r in sources for h in tokens[r]]
        n_loc = tokens[0][0].shape[0] + tokens[0][1].shape[0]
        outs.append(sds((8, BLK, e), BF16))
        if kind != "own":
            aliases[len(args)] = 1
            args.append(u_all)
    else:
        n_loc = BLK
        args.append(u_all)
    if final:
        if big is not None:
            aliases[len(args)] = len(outs)
            args.append(big)
        outs.append(sds((v_rows, e), F32))
    args += [a for a, _ in parts] + [a for _, a in puts]
    n_hold = max(1, len(parts) + len(puts))
    tallest = max([m] * len(parts) + [a.shape[0] for _, a in puts] + [8])
    t = STEPS[kind] * BLK
    scratch = [pltpu.VMEM((2, n_loc, e), F32)] if wide else []
    scratch += [
        pltpu.VMEM((2 if wide else 3, BLK, e), BF16), pltpu.VMEM((m, e), BF16), pltpu.VMEM((m, BLK), BF16),
        pltpu.VMEM((m, e), F32), pltpu.VMEM((n_hold, tallest, e), F32),
        DMA, DMA((3, 2)), DMA((2,)), DMA((n_hold,)), DMA((n_hold,)),
    ]
    return pl.pallas_call(
        functools.partial(rows_kernel, kind, scale, s0, m, cut, n_loc, sources, [skip for _, skip in parts], [spot for spot, _ in puts], big is not None),
        in_specs=[SMEM, ANY, VMEM, VMEM] + [ANY] * (len(args) - 4),
        out_specs=[ANY] * len(outs),
        out_shape=outs,
        scratch_shapes=scratch,
        input_output_aliases=aliases,
        compiler_params=pltpu.CompilerParams(vmem_limit_bytes=VMEM_LIMIT),
        cost_estimate=pl.CostEstimate(flops=(4 * t * m * e) // COVER, bytes_accessed=t * e * 2 + m * e * 6, transcendentals=t * m),
    )(*args)


def put_kernel(spots, pos, *refs):
    n = len(spots)
    pieces, (out_ref, hold, in_sem, out_sem) = refs[1:1 + n], refs[1 + n:]
    loads, stores = [], []
    for j, (p, (base, off)) in enumerate(zip(pieces, spots)):
        slot = hold.at[j, :p.shape[0], :]
        loads.append(pltpu.make_async_copy(p, slot, in_sem.at[j]))
        stores.append(pltpu.make_async_copy(slot, out_ref.at[pl.ds(pl.multiple_of(pos[base] + off, 8), p.shape[0]), :], out_sem.at[j]))
    for a in loads:
        a.start()
    for a, b in zip(loads, stores):
        a.wait()
        b.start()
    for b in stores:
        b.wait()


def put_rows(pos, big, puts):
    spots, pieces = [s for s, _ in puts], [a for _, a in puts]
    n, e = len(pieces), big.shape[1]
    size = sum(p.size for p in pieces)
    return pl.pallas_call(
        functools.partial(put_kernel, spots),
        in_specs=[SMEM] + [ANY] * (n + 1),
        out_specs=ANY,
        out_shape=jax.ShapeDtypeStruct(big.shape, big.dtype),
        scratch_shapes=[pltpu.VMEM((n, max(p.shape[0] for p in pieces), e), F32), DMA((n,)), DMA((n,))],
        input_output_aliases={1: 0},
        compiler_params=pltpu.CompilerParams(vmem_limit_bytes=VMEM_LIMIT),
        cost_estimate=pl.CostEstimate(flops=(size) // COVER, bytes_accessed=size * 8, transcendentals=0),
        name="put_rows",
    )(pos, big, *pieces)


def join_kernel(n_vec, idx, *refs):
    own, mine, theirs, (dw_ref, vec_ref, full, in_sem, out_sem) = refs[0], refs[1:4], refs[4:7], refs[7:]
    vp, core = idx[0], idx[1]
    half, cols = mine[0].shape
    col = lambda k: pl.ds(pl.multiple_of((vp ^ k) * cols, cols), cols)
    row = lambda c: pl.ds(pl.multiple_of(c * half, 8), half)
    loads = [pltpu.make_async_copy(own.at[:2 * half, :], full.at[:, col(0)], in_sem.at[0])]
    for k in range(3):
        loads.append(pltpu.make_async_copy(mine[k], full.at[row(core), col(k + 1)], in_sem.at[1 + k]))
        loads.append(pltpu.make_async_copy(theirs[k], full.at[row(1 - core), col(k + 1)], in_sem.at[4 + k]))
    for c in loads:
        c.start()
    for c in loads:
        c.wait()
    e = dw_ref.shape[0]
    stores = [pltpu.make_async_copy(full.at[:e, :], dw_ref, out_sem.at[0]), pltpu.make_async_copy(full.at[e:e + n_vec, :], vec_ref, out_sem.at[1])]
    for c in stores:
        c.start()
    for c in stores:
        c.wait()


def join_pass(idx, own, mine, theirs):
    half, cols = mine[0].shape
    e = 4 * cols
    return pl.pallas_call(
        functools.partial(join_kernel, 8),
        in_specs=[SMEM] + [ANY] * 7,
        out_specs=[ANY] * 2,
        out_shape=[jax.ShapeDtypeStruct((e, e), F32), jax.ShapeDtypeStruct((8, e), F32)],
        scratch_shapes=[pltpu.VMEM((2 * half, e), F32), DMA((7,)), DMA((2,))],
        compiler_params=pltpu.CompilerParams(vmem_limit_bytes=VMEM_LIMIT),
        cost_estimate=pl.CostEstimate(flops=(e * e) // COVER, bytes_accessed=e * e * 8, transcendentals=0),
        name="join",
    )(idx, own, *mine, *theirs)


def back_kernel(vp, pre_ref, norm_ref, rstd_ref, z_ref, du_ref, m1_ref, m2_ref, gain_ref, loss_ref, db_ref, dab_ref, pack_ref):
    e, cols = z_ref.shape[1], du_ref.shape[1]
    for c in range(0, cols, 128):
        cs = slice(c, c + 128)
        a, du, normed = pre_ref[:, cs], du_ref[:, cs], norm_ref[:, cs]
        cdf = 0.5 * (1.0 + lax.erf(a * (0.5 ** 0.5)))
        dg = rstd_ref[...] * (du * gain_ref[:, cs] - m1_ref[...] - normed * m2_ref[...])
        da = dg * (cdf + a * (jnp.exp(-0.5 * a * a) * 0.3989422804014327))
        dab_ref[:, cs] = da.astype(BF16).astype(F32)
        for j, x in enumerate((da, du * normed, du)):
            pack_ref[e + j:e + j + 1, cs] = jnp.sum(x, axis=0, keepdims=True)
    pack_ref[:e, :] = lax.dot_general(z_ref[...], dab_ref[...].astype(BF16), (((0,), (0,)), ((), ())), preferred_element_type=F32)
    pack_ref[e + 3:e + 4, :] = loss_ref[...]
    pack_ref[e + 4:e + 16, :] = jnp.zeros_like(pack_ref[e + 4:e + 16, :])
    pack_ref[e + 16:, :] = db_ref[...]


def back_pass(vp, pre, normed, rstd, z, du, m1, m2, gain, loss, db):
    n, cols = du.shape
    e = z.shape[1]
    n_pack = e + 16 + db.shape[0]
    block = lambda *s: pl.BlockSpec(s, lambda i, p: (0,) * len(s))
    share = lambda r: pl.BlockSpec((r, cols), lambda i, p: (0, p[0]))
    gs = pltpu.PrefetchScalarGridSpec(
        num_scalar_prefetch=1,
        grid=(1,),
        in_specs=[share(n), share(n), block(n, 128), block(n, e), block(n, cols), block(n, 128), block(n, 128), share(1), block(1, cols), block(*db.shape)],
        out_specs=[block(n, cols), block(n_pack, cols)],
    )
    return pl.pallas_call(
        back_kernel,
        grid_spec=gs,
        out_shape=[jax.ShapeDtypeStruct((n, cols), F32), jax.ShapeDtypeStruct((n_pack, cols), F32)],
        compiler_params=pltpu.CompilerParams(dimension_semantics=("arbitrary",), vmem_limit_bytes=VMEM_LIMIT),
        cost_estimate=pl.CostEstimate(flops=(2 * n * e * cols) // COVER, bytes_accessed=n * (cols * 16 + e * 2 + 1536), transcendentals=n * cols * 2),
        name="back",
    )(vp, pre, normed, rstd, z, du, m1, m2, gain, loss, db)


def spread_kernel(n_masks, vp, pos_ref, w_ref, *refs):
    pieces, (out_ref, dab, dz, obuf, in_sem, out_sem) = refs[:4], refs[4:]
    n, cols = pieces[0].shape
    loads = [pltpu.make_async_copy(p, dab.at[:, pl.ds(pl.multiple_of((vp[0] ^ k) * cols, cols), cols)], in_sem.at[k]) for k, p in enumerate(pieces)]
    for c in loads:
        c.start()
    dz[n:, :] = jnp.zeros((dz.shape[0] - n, dz.shape[1]), F32)
    n_seq, seq_len, _ = out_ref.shape
    place = lax.broadcasted_iota(I32, (seq_len, 1), 0)
    slots = pos_ref.shape[2]
    for c in loads:
        c.wait()
    stores, done = [], 0
    for b in range(n_seq):
        while done < min(n, b * n_masks + slots):
            r1 = min(n, done + 304)
            dz[done:r1, :] = dot(dab[done:r1, :].astype(BF16), w_ref[...], NT).astype(BF16).astype(F32)
            done = r1
        if b >= 4:
            stores[b - 4].wait()
        hot = jnp.where(place == pos_ref[b], 1.0, 0.0).astype(BF16)
        obuf[b % 4] = dot(hot, dz[b * n_masks:b * n_masks + slots, :].astype(BF16), NN).astype(BF16)
        c = pltpu.make_async_copy(obuf.at[b % 4], out_ref.at[b], out_sem.at[b])
        c.start()
        stores.append(c)
    for c in stores[-4:]:
        c.wait()


def spread_pass(n_masks, shape, vp, pos, w, pieces):
    n, cols = pieces[0].shape
    e = w.shape[0]
    return pl.pallas_call(
        functools.partial(spread_kernel, n_masks),
        in_specs=[SMEM, VMEM, VMEM] + [ANY] * 4,
        out_specs=ANY,
        out_shape=jax.ShapeDtypeStruct(shape, BF16),
        scratch_shapes=[pltpu.VMEM((n, 4 * cols), F32), pltpu.VMEM((n + 16, e), F32), pltpu.VMEM((4,) + shape[1:], BF16), DMA((4,)), DMA((shape[0],))],
        compiler_params=pltpu.CompilerParams(vmem_limit_bytes=VMEM_LIMIT),
        cost_estimate=pl.CostEstimate(flops=(2 * shape[0] * shape[1] * 128 * e) // COVER, bytes_accessed=shape[0] * shape[1] * e * 2, transcendentals=0),
        name="spread",
    )(vp, pos, w, *pieces)


def order_sum(xs):
    return (xs[0] + xs[1]) + (xs[2] + xs[3])


def after(x, *deps):
    return lax.optimization_barrier((x, deps))[0]


def solution(mesh):
    n_groups, n_shards = mesh.shape["dp"], mesh.shape["vp"]

    def swap(a, bit):
        return lax.ppermute(a, "dp", [(d, d ^ bit) for d in range(n_groups)])

    def swap_vp(a, bit):
        return lax.ppermute(a, "vp", [(d, d ^ bit) for d in range(n_shards)])

    def hop(a):
        return lax.ppermute(a, "dp", [(d, d ^ (Y if d & CORE else X)) for d in range(n_groups)])

    def local_step(hidden, mask_pos, labels, w_trans, b_trans, ln_gain, ln_bias, emb_table, b_vocab):
        n_rows, _, width = hidden.shape
        n_masks = mask_pos.shape[1]
        shard_rows = emb_table.shape[0]
        n_loc = n_rows * n_masks
        n_tokens = n_loc * n_groups
        slots = -(-n_masks // 16) * 16
        cut = n_loc // 32 * 16
        cols = width // n_shards
        dp, vp = lax.axis_index("dp"), lax.axis_index("vp")
        row_start = vp * shard_rows
        scale = 1.0 / n_tokens
        core, mine = dp & 1, (dp >> 1 ^ dp >> 2) & 1

        pos_pad = jnp.pad(mask_pos, ((0, 0), (0, slots - n_masks)), constant_values=-1)
        z, pre, normed, rstd, u, u_lo, u_hi = head_pass(
            n_masks, cut, hidden, jnp.broadcast_to(pos_pad[:, :, None], (n_rows, slots, 128)),
            w_trans, b_trans[None], ln_gain[None], ln_bias[None])

        x_lo, y_hi = swap(u_lo, X), swap(u_hi, Y)
        x_hi, y_lo = swap(u_hi, X), swap(u_lo, Y)
        c_lo, c_hi = swap(u_lo, CORE), swap(u_hi, CORE)

        flat_labels = labels.reshape(n_loc)
        lab_local = flat_labels - row_start
        lab_local = jnp.where((lab_local >= 0) & (lab_local < shard_rows), lab_local, -1)
        lab_local = jnp.broadcast_to(lab_local[:, None], (n_loc, 128))
        logits, stat = stats(u, emb_table, b_vocab[None], lab_local)
        all_stats = [stat] + [swap_vp(stat, b) for b in range(1, n_shards)]
        global_max = functools.reduce(jnp.maximum, [s[0] for s in all_stats])
        log_norm = global_max + jnp.log(order_sum([s[1] * jnp.exp(s[0] - global_max) for s in all_stats]))
        loss_part = jnp.sum(log_norm - order_sum([s[2] for s in all_stats]))
        lse = log_norm + jnp.log(jnp.float32(n_tokens))

        fill = (0, BLK - n_loc)
        info = jnp.stack([jnp.pad(lse, fill, constant_values=jnp.inf), jnp.pad(flat_labels.astype(F32), fill, constant_values=-1.0)])
        near, *away = [swap(info, b) for b in (CORE, X, Y, X | Y)]
        x_lo, y_hi = after((x_lo, y_hi), stat)
        d_lo, d_hi = swap(x_lo, Y), swap(y_hi, X)
        cx_lo, cy_hi = swap(x_lo, CORE), swap(y_hi, CORE)

        du_part, db_part, sums = du_pass(
            scale, n_shards, logits, emb_table, jnp.broadcast_to(lse[:, None], (n_loc, 128)), lab_local, normed, ln_gain[None])
        du_share = lax.psum_scatter(du_part.reshape(n_shards * n_loc, cols), "vp", scatter_dimension=0, tiled=True)

        half, quarter = shard_rows // 2, shard_rows // 4
        start = lambda h, c: h * half + c * quarter
        pos = jnp.stack([dp, start(mine, core), row_start + start(mine, core), start(mine, 1 - core), start(1 - mine, core), start(1 - mine, 1 - core)])
        bias_col = lax.dynamic_slice(b_vocab, (start(mine, core),), (quarter,))[:, None]
        shares = (640, 896, 960, 648)
        ends = [0]
        for w in shares[:-1]:
            ends.append(ends[-1] + max(16, quarter * w // sum(shares) // 16 * 16))
        spans = list(zip(ends, ends[1:] + [quarter]))

        def rows(kind, k, *wait, info=None, span=None, **kw):
            return rows_pass(kind, scale, shard_rows, span or spans[k], cut, after(pos, *wait), emb_table, bias_col, info, **kw)

        def send(k, chunk):
            return ((TWIN, spans[k][0]), swap(chunk, CORE)), hop(chunk)

        def forward(k, far, *wait):
            far = after(far, *wait)
            return ((FAR, spans[k][0]), far), ((FAR_TWIN, spans[k][0]), swap(far, CORE))

        tokens = {0: (u_lo, u_hi), CORE: (c_lo, c_hi), X: (x_lo, x_hi), Y: (y_lo, y_hi)}
        pair = jnp.stack([info, near])
        own0, u_all = rows("own", 0, du_part, info=pair, tokens=tokens)
        x_hi, y_lo, away = after((x_hi, y_lo, away), own0)
        away = jnp.stack(away)
        tokens[X | CORE] = cx_lo, swap(x_hi, CORE)
        tokens[Y | CORE] = swap(y_lo, CORE), cy_hi
        away_near = swap(away, CORE)
        tokens[X], tokens[Y] = (x_lo, x_hi), (y_lo, y_hi)
        own1, = rows("again", 1, own0, info=pair, u_all=u_all)
        info = jnp.concatenate([pair, jnp.stack([away, away_near], axis=1).reshape(6, 2, BLK)])
        first_two = (spans[0][0], spans[1][1])
        side, u_all = rows("side", 0, own1, info=info, span=first_two, tokens=tokens, u_all=u_all)
        d_lo, d_hi = after((d_lo, d_hi), side)
        tokens[X | Y] = d_lo, d_hi
        tokens[X | Y | CORE] = swap(d_lo, CORE), swap(d_hi, CORE)
        chunk0, u_all, big = rows("far", 0, info=info, tokens=tokens, u_all=u_all, parts=((own0, 0), (side, 0)))
        twin0, far0 = send(0, chunk0)
        chunk1, big = rows("last", 1, info=info, u_all=u_all, big=big, parts=((own1, 0), (side, spans[1][0])))
        twin1, far1 = send(1, chunk1)

        du_share = after(du_share, chunk1)
        sums = [sums] + [swap_vp(sums, b) for b in range(1, n_shards)]
        sums = order_sum(sums) / width
        m1, m2 = (jnp.broadcast_to(sums[j][:, None], (n_loc, 128)) for j in range(2))
        loss_row = jnp.pad(loss_part[None, None], ((0, 0), (0, cols - 1)))
        db_rows = -(-shard_rows // cols // 8) * 8
        db_mat = jnp.pad(db_part[0], (0, db_rows * cols - shard_rows)).reshape(db_rows, cols)
        dab, pack = back_pass(vp[None], pre, normed, rstd, z, du_share, m1, m2, ln_gain[None], loss_row, db_mat)
        back_done = dab
        pack = lax.psum(pack, "dp")
        dab = [dab] + [swap_vp(dab, b) for b in range(1, n_shards)]

        chunk2, big = rows("whole", 2, back_done, info=info, u_all=u_all, big=big, puts=[twin0])
        twin2, far2 = send(2, chunk2)
        far0, far_twin0 = forward(0, far0, chunk2)
        far1, far_twin1 = forward(1, far1, chunk2)
        pack = after(pack, chunk2)
        n_half = (width + 16) // 2
        part = lax.dynamic_slice(pack, (core * n_half, 0), (n_half, cols))
        parts = [swap_vp(part, b) for b in range(1, n_shards)]

        chunk3, big = rows("whole", 3, part, info=info, u_all=u_all, big=big, puts=[far0, twin1, far1])
        twin3, far3 = send(3, chunk3)
        far2, far_twin2 = forward(2, far2, chunk3)
        d_hidden = spread_pass(n_masks, hidden.shape, vp[None], pos_pad[:, None], w_trans, after(dab, chunk3))
        parts = after(parts, d_hidden)
        others = [swap(p, CORE) for p in parts]
        big = put_rows(pos, big, [far_twin0, far_twin1, twin2, far2, far_twin2, twin3])
        pack, parts, others = after((pack, parts, others), big)
        d_w, vec = join_pass(jnp.stack([vp, core]), pack, parts, others)
        far3 = after(far3, big)
        far3, far_twin3 = forward(3, far3)
        big = put_rows(pos, big, [far3])
        big = put_rows(pos, big, [far_twin3])

        db = pack[width + 16:].reshape(-1)[:shard_rows]
        return pack[width + 3, 0] / n_tokens, d_hidden, d_w, vec[0], vec[1], vec[2], big, db

    in_specs = (P("dp", None, None), P("dp", None), P("dp", None), P(None, None), P(None), P(None), P(None), P("vp", None), P("vp"))
    out_specs = (P(), P("dp", None, None), P(None, None), P(None), P(None), P(None), P("vp", None), P("vp"))
    return jax.shard_map(local_step, mesh=mesh, in_specs=in_specs, out_specs=out_specs, check_vma=False)
```

```python
import functools

import jax
import jax.numpy as jnp
from jax import lax
from jax.experimental import pallas as pl
from jax.experimental.pallas import tpu as pltpu
from jax.sharding import PartitionSpec as P


F32, BF16, I32 = jnp.float32, jnp.bfloat16, jnp.int32
NT = (((1,), (1,)), ((), ()))
NN = (((1,), (0,)), ((), ()))
VB = 1024
VMEM_LIMIT = 60 << 20
COVER = 100
CH = 16


def row_cuts(rows, parts=4):
    cuts = [16 * (rows // 16 * k // parts) for k in range(parts)] + [rows]
    return list(zip(cuts[:-1], cuts[1:]))


def dot(a, b, dims):
    return lax.dot_general(a, b, dims, preferred_element_type=F32)


def stats_kernel(n_vocab, u_ref, emb_ref, b_ref, lab_ref, lo_ref, hi_ref, stat_ref, m_sc, s_sc, l_sc):
    i, n_blocks = pl.program_id(0), pl.num_programs(0)
    lane = lax.broadcasted_iota(I32, (1, 128), 1)

    @pl.when(i == 0)
    def _():
        m_sc[...] = jnp.full_like(m_sc, -jnp.inf)
        s_sc[...] = jnp.zeros_like(s_sc)
        l_sc[...] = jnp.zeros_like(l_sc)

    def run(width):
        wide = -(-width // 128) * 128
        for r0, r1 in row_cuts(u_ref.shape[0]):
            tile = dot(u_ref[r0:r1, :], emb_ref[:wide, :], NT) + b_ref[:, :wide]
            if wide > width:
                tile = jnp.where(lax.broadcasted_iota(I32, (1, wide), 1) < width, tile, -jnp.inf)
            cut = lo_ref.shape[0]
            out_ref, base = (lo_ref, 0) if r0 < cut else (hi_ref, cut)
            out_ref[r0 - base:r1 - base, :wide] = tile
            for q in range(r0, r1, CH):
                rs = slice(q, min(q + CH, r1))
                parts = [out_ref[rs.start - base:rs.stop - base, k:k + 128] for k in range(0, wide, 128)]
                m_old = m_sc[rs, :]
                m_new = functools.reduce(jnp.maximum, parts, m_old)
                s_new = s_sc[rs, :] * jnp.exp(m_old - m_new)
                l_new = l_sc[rs, :]
                lab = lab_ref[rs, :] - i * VB
                for k, part in enumerate(parts):
                    s_new += jnp.exp(part - m_new)
                    l_new = jnp.where(lab == lane + k * 128, part, l_new)
                m_sc[rs, :], s_sc[rs, :], l_sc[rs, :] = m_new, s_new, l_new

    tail = n_vocab % VB
    if tail:
        pl.when(i < n_blocks - 1)(functools.partial(run, VB))
        pl.when(i == n_blocks - 1)(functools.partial(run, tail))
    else:
        run(VB)

    @pl.when(i == n_blocks - 1)
    def _():
        m_t, s_t, l_t = m_sc[...].T, s_sc[...].T, l_sc[...].T
        m_all = jnp.max(m_t, axis=0, keepdims=True)
        stat_ref[0:1, :] = m_all
        stat_ref[1:2, :] = jnp.sum(s_t * jnp.exp(m_t - m_all), axis=0, keepdims=True)
        stat_ref[2:3, :] = jnp.sum(l_t, axis=0, keepdims=True)
        stat_ref[3:8, :] = jnp.zeros_like(stat_ref[3:8, :])


def stats(u, emb, bias, lab, cut):
    t, e = u.shape
    v = emb.shape[0]
    n = pl.cdiv(v, VB)
    whole = lambda *s: pl.BlockSpec(s, lambda i: (0,) * len(s))
    return pl.pallas_call(
        functools.partial(stats_kernel, v),
        grid=(n,),
        in_specs=[whole(t, e), pl.BlockSpec((VB, e), lambda i: (i, 0)), pl.BlockSpec((1, VB), lambda i: (0, i)), whole(t, 128)],
        out_specs=[pl.BlockSpec((cut, VB), lambda i: (0, i)), pl.BlockSpec((t - cut, VB), lambda i: (0, i)), whole(8, t)],
        out_shape=[jax.ShapeDtypeStruct((cut, v), F32), jax.ShapeDtypeStruct((t - cut, v), F32), jax.ShapeDtypeStruct((8, t), F32)],
        scratch_shapes=[pltpu.VMEM((t, 128), F32)] * 3,
        compiler_params=pltpu.CompilerParams(dimension_semantics=("arbitrary",), vmem_limit_bytes=VMEM_LIMIT),
        cost_estimate=pl.CostEstimate(flops=(2 * t * v * e) // COVER, bytes_accessed=t * v * 4 + v * e * 2, transcendentals=t * v),
        name="stats",
    )(u, emb, bias, lab)


def du_kernel(n_vocab, scale, base, logits_ref, emb_ref, lse_ref, lab_ref, norm_hbm, gain_ref, out_ref, db_ref, sum_ref, du_ref, g_sc, db_sc, norm_sc, db_sc2, sem):
    i, n_blocks = pl.program_id(0), pl.num_programs(0)
    t = logits_ref.shape[0]
    lane = lax.broadcasted_iota(I32, (1, 128), 1)

    norm_copy = pltpu.make_async_copy(norm_hbm.at[base:base + t, :], norm_sc, sem)

    @pl.when(i == 0)
    def _():
        du_ref[...] = jnp.zeros_like(du_ref)

    @pl.when(i == 2)
    def _():
        norm_copy.start()

    def run(width):
        wide = -(-width // 128) * 128
        emb = emb_ref[:wide, :]
        if wide > width:
            emb = jnp.where(lax.broadcasted_iota(I32, (wide, 1), 0) < width, emb, jnp.zeros_like(emb))
        for r0, r1 in row_cuts(t, 2):
            sums = [None] * (wide // 128)
            for q in range(r0, r1, 16):
                rs = slice(q, q + 16)
                lse = lse_ref[rs, :]
                lab = lab_ref[rs, :] - i * VB
                for k in range(wide // 128):
                    c = k * 128
                    g = jnp.exp(logits_ref[rs, c:c + 128] - lse)
                    g -= jnp.where(lab == lane + c, scale, 0.0)
                    if c + 128 > width:
                        g = jnp.where(lane < width - c, g, 0.0)
                    part = g[:8] + g[8:]
                    sums[k] = part if sums[k] is None else sums[k] + part
                    g_sc[rs, c:c + 128] = g.astype(BF16)
            for k in range(wide // 128):
                cs = slice(k * 128, (k + 1) * 128)
                db_sc[:, cs] = sums[k] if r0 == 0 else db_sc[:, cs] + sums[k]
            du_ref[r0:r1, :] += dot(g_sc[r0:r1, :wide], emb, NN)
        db_ref[:, :wide] = jnp.sum(db_sc[:, :wide], axis=0, keepdims=True)

    tail = n_vocab % VB
    if tail:
        pl.when(i < n_blocks - 1)(functools.partial(run, VB))
        pl.when(i == n_blocks - 1)(functools.partial(run, tail))
    else:
        run(VB)

    @pl.when(i == n_blocks - 1)
    def _():
        norm_copy.wait()
        parts, rows, cols = out_ref.shape
        run = rows // 4 if rows % 32 == 0 else rows // 3
        for r in range(0, rows, run):
            rs = slice(r, r + run)
            total = [jnp.zeros((run, 128), F32)] * 2
            for c in range(0, parts * cols, 128):
                x = du_ref[rs, c:c + 128].astype(BF16).astype(F32)
                out_ref[c // cols, rs, c % cols:c % cols + 128] = x
                dn = x * gain_ref[:, c:c + 128]
                total = [total[0] + dn, total[1] + dn * norm_sc[rs, c:c + 128]]
            for j, x in enumerate(total):
                db_sc2[j, rs, :] = x
        for j in range(2):
            sum_ref[j:j + 1, :] = jnp.sum(db_sc2[j].T, axis=0, keepdims=True)
        sum_ref[2:, :] = jnp.zeros_like(sum_ref[2:, :])


def du_pass(scale, parts, base, logits, emb, lse, lab, normed, gain):
    t, v = logits.shape
    e = emb.shape[1]
    n = pl.cdiv(v, VB)
    whole = lambda *s: pl.BlockSpec(s, lambda i: (0,) * len(s))
    return pl.pallas_call(
        functools.partial(du_kernel, v, scale, base),
        grid=(n,),
        in_specs=[pl.BlockSpec((t, VB), lambda i: (0, i)), pl.BlockSpec((VB, e), lambda i: (i, 0)), whole(t, 128), whole(t, 128), pl.BlockSpec(memory_space=pl.ANY), whole(1, e)],
        out_specs=[whole(parts, t, e // parts), pl.BlockSpec((1, VB), lambda i: (0, i)), whole(8, t)],
        out_shape=[jax.ShapeDtypeStruct((parts, t, e // parts), F32), jax.ShapeDtypeStruct((1, v), F32), jax.ShapeDtypeStruct((8, t), F32)],
        scratch_shapes=[pltpu.VMEM((t, e), F32), pltpu.VMEM((t, VB), BF16), pltpu.VMEM((8, VB), F32), pltpu.VMEM((t, e), F32), pltpu.VMEM((2, t, 128), F32), pltpu.SemaphoreType.DMA],
        compiler_params=pltpu.CompilerParams(dimension_semantics=("arbitrary",), vmem_limit_bytes=VMEM_LIMIT),
        cost_estimate=pl.CostEstimate(flops=(2 * t * v * e) // COVER, bytes_accessed=t * v * 4 + v * e * 2, transcendentals=t * v),
        name="du_pass",
    )(logits, emb, lse, lab, normed, gain)


LN_EPS = 1e-5
CORE, X, Y = 1, 2, 4
ANY = pl.BlockSpec(memory_space=pl.ANY)
VMEM = pl.BlockSpec(memory_space=pltpu.VMEM)
SMEM = pl.BlockSpec(memory_space=pltpu.SMEM)
DMA = pltpu.SemaphoreType.DMA


def gelu_norm(a):
    cdf = 0.5 * (1.0 + lax.erf(a * (0.5 ** 0.5)))
    g = a * cdf
    centered = g - jnp.mean(g, axis=1, keepdims=True)
    rstd = lax.rsqrt(jnp.mean(centered * centered, axis=1, keepdims=True) + LN_EPS)
    return cdf, centered * rstd, rstd


def head_kernel(n_masks, cut, hid, pos_ref, w_ref, b_ref, gain_ref, bias_ref, z_out, pre_out, norm_out, rstd_out, u_out, lo_out, hi_out,
                hbuf, zf, zb, pre_v, norm_v, rstd_v, ub, uf, in_sem, out_sem):
    n_seq, seq_len = hid.shape[0], hid.shape[1]
    n_loc = n_seq * n_masks
    loads = [pltpu.make_async_copy(hid.at[b], hbuf.at[b], in_sem.at[b]) for b in range(n_seq)]
    for c in loads:
        c.start()
    lane = lax.broadcasted_iota(I32, (1, 128), 1)
    cuts = [0, cut // 32 * 16, cut, cut + (n_loc - cut) // 32 * 16, n_loc]
    done, stores = 0, []

    def send(src, dst, r0, r1, base=0):
        c = pltpu.make_async_copy(src.at[r0:r1, :], dst.at[r0 - base:r1 - base, :], out_sem.at[len(stores)])
        c.start()
        stores.append(c)

    for b in range(n_seq):
        loads[b].wait()
        hot = jnp.concatenate([jnp.where(pos_ref[b] == lane + j, 1.0, 0.0).astype(BF16) for j in range(0, seq_len, 128)], axis=1)
        zf[b * n_masks:(b + 1) * n_masks, :] = dot(hot, hbuf[b], NN)[:n_masks, :]
        while done < 4 and cuts[done + 1] <= (b + 1) * n_masks:
            r0, r1 = cuts[done], cuts[done + 1]
            z = zf[r0:r1, :].astype(BF16)
            zb[r0:r1, :] = z
            a = dot(z, w_ref[...], NN) + b_ref[...]
            pre_v[r0:r1, :] = a
            _, normed, rstd = gelu_norm(a)
            norm_v[r0:r1, :] = normed
            rstd_v[r0:r1, :] = jnp.broadcast_to(rstd, (r1 - r0, 128))
            u = (normed * gain_ref[...] + bias_ref[...]).astype(BF16)
            ub[r0:r1, :] = u
            uf[r0:r1, :] = u.astype(F32)
            done += 1
            send(uf, hi_out if r0 >= cut else lo_out, r0, r1, cut if r0 >= cut else 0)
            for src, dst in ((ub, u_out), (zb, z_out), (pre_v, pre_out), (norm_v, norm_out), (rstd_v, rstd_out)):
                send(src, dst, r0, r1)
    for c in stores:
        c.wait()


def head_pass(n_masks, cut, hidden, pos, w, b, gain, bias):
    n_seq, seq_len, e = hidden.shape
    n = n_seq * n_masks
    kinds = [((n, e), BF16), ((n, e), F32), ((n, e), F32), ((n, 128), F32), ((n, e), BF16), ((cut, e), F32), ((n - cut, e), F32)]
    return pl.pallas_call(
        functools.partial(head_kernel, n_masks, cut),
        in_specs=[ANY] + [VMEM] * 5,
        out_specs=[ANY] * len(kinds),
        out_shape=[jax.ShapeDtypeStruct(*k) for k in kinds],
        scratch_shapes=[pltpu.VMEM((n_seq, seq_len, e), BF16), pltpu.VMEM((n, e), F32)]
        + [pltpu.VMEM(*k) for k in kinds[:5]] + [pltpu.VMEM((n, e), F32), DMA((n_seq,)), DMA((24,))],
        compiler_params=pltpu.CompilerParams(vmem_limit_bytes=VMEM_LIMIT),
        cost_estimate=pl.CostEstimate(flops=(4 * n * e * e) // COVER, bytes_accessed=hidden.size * 2 + n * e * 20, transcendentals=n * e),
        name="head",
    )(hidden, pos, w, b, gain, bias)


BLK = 1280
STEPS = {"own": 2, "again": 2, "side": 4, "far": 2, "last": 2, "whole": 8}
ME, MINE, MINE_ID, TWIN, FAR, FAR_TWIN = range(6)


def rows_kernel(kind, scale, s0, m, cut, n_loc, sources, skips, spots, has_big, pos, emb_hbm, bias_ref, info_ref, *refs):
    refs = list(refs)
    take = lambda n: [refs.pop(0) for _ in range(n)]
    wide = sources is not None
    if wide:
        src = {r: take(2) for r in sources}
        if kind != "own":
            take(1)
    else:
        u_hbm, = take(1)
    if has_big:
        take(1)
    parts = take(len(skips))
    puts = take(len(spots))
    out_hbm, = take(1)
    if wide:
        u_hbm, = take(1)
    if kind in ("far", "last", "whole"):
        big_ref, = take(1)
    if wide:
        buf, = take(1)
    ring, emb_sc, g_sc, acc, hold, sem, tok_sem, back_sem, in_sem, out_sem = refs
    me = pos[ME]
    chip = lax.div(me, 2)
    n_steps = STEPS[kind]
    along_x, along_y = chip ^ 1, chip ^ 2

    def device(i):
        side = 2 * jnp.where(i < 2, jnp.minimum(along_x, along_y), jnp.maximum(along_x, along_y)) + lax.rem(i, 2)
        far = 2 * (chip ^ 3) + lax.rem(i, 2)
        if kind in ("own", "again"):
            return 2 * chip + i
        return {"side": side, "far": far, "last": far, "whole": i}[kind]

    depth = ring.shape[0]

    def fetch(i):
        slot = lax.rem(i, 2 if wide else depth)
        if not wide:
            pltpu.make_async_copy(u_hbm.at[device(i)], ring.at[slot], tok_sem.at[slot, 0]).start()
            return
        for r, (lo, hi) in src.items():
            @pl.when(device(i) ^ me == r)
            def _():
                pltpu.make_async_copy(lo, buf.at[slot, :cut, :], tok_sem.at[slot, 0]).start()
                pltpu.make_async_copy(hi, buf.at[slot, cut:, :], tok_sem.at[slot, 1]).start()

    row = lambda j, off: pl.multiple_of(pos[j] + off, 8)
    emb_copy = pltpu.make_async_copy(emb_hbm.at[pl.ds(row(MINE, s0), m), :], emb_sc, sem)
    emb_copy.start()
    fetch(0)
    loads, stores = [], []
    for j, (p, (base, off)) in enumerate(zip(puts, spots)):
        n = p.shape[0]
        loads.append(pltpu.make_async_copy(p, hold.at[j, :n, :], in_sem.at[j]))
        stores.append(pltpu.make_async_copy(hold.at[j, :n, :], big_ref.at[pl.ds(row(base, off), n), :], out_sem.at[j]))
    for j, (p, skip) in enumerate(zip(parts, skips)):
        loads.append(pltpu.make_async_copy(p.at[skip:skip + m, :], hold.at[len(puts) + j, :m, :], in_sem.at[len(puts) + j]))
    acc[...] = jnp.zeros_like(acc)
    if wide:
        for k in range(2):
            ring[k, n_loc:, :] = jnp.zeros((BLK - n_loc, ring.shape[2]), BF16)
    emb_copy.wait()
    n_cuts = max(1, round(m / 300))
    cuts = [-(-m * k // (n_cuts * 16)) * 16 for k in range(n_cuts)] + [m]
    cuts = list(zip(cuts[:-1], cuts[1:]))
    kept = lambda i: pltpu.make_async_copy(ring.at[lax.rem(i, 2)], u_hbm.at[device(i)], back_sem.at[lax.rem(i, 2)])

    @pl.loop(0, n_steps)
    def _(i):
        slot = lax.rem(i, 2 if wide else depth)
        if wide:
            any_lo, any_hi = next(iter(src.values()))
            pltpu.make_async_copy(any_lo, buf.at[slot, :cut, :], tok_sem.at[slot, 0]).wait()
            pltpu.make_async_copy(any_hi, buf.at[slot, cut:, :], tok_sem.at[slot, 1]).wait()

            @pl.when(i >= 2)
            def _():
                kept(i - 2).wait()
        else:
            pltpu.make_async_copy(u_hbm.at[device(i)], ring.at[slot], tok_sem.at[slot, 0]).wait()

        @pl.when(i + 1 < n_steps)
        def _():
            fetch(i + 1)

        @pl.when(i == 0)
        def _():
            for c in loads:
                c.start()

        for j, (a, b) in enumerate(zip(loads, stores)):
            @pl.when(i == min(2 + j, n_steps - 1))
            def _():
                a.wait()
                b.start()

        if wide:
            ring[slot, :n_loc, :] = buf[slot].astype(BF16)
            kept(i).start()
        rel = device(i) ^ me
        lse, lab = info_ref[rel, 0:1, :], info_ref[rel, 1:2, :]

        def weights(r0, r1):
            part = dot(emb_sc[r0:r1, :], ring[slot], NT)
            ids = lax.broadcasted_iota(I32, (r1 - r0, 1), 0) + (pos[MINE_ID] + (s0 + r0))
            g = jnp.exp(part + bias_ref[s0 + r0:s0 + r1, :] - lse) - jnp.where(lab == ids.astype(F32), scale, 0.0)
            g_sc[r0:r1, :] = g.astype(BF16)

        weights(*cuts[0])
        for k, (r0, r1) in enumerate(cuts):
            if k + 1 < len(cuts):
                weights(*cuts[k + 1])
            acc[r0:r1, :] += dot(g_sc[r0:r1, :], ring[slot], NN)

    for c in loads[len(puts):]:
        c.wait()
    if parts:
        acc[...] = (hold[len(puts), :m, :] + acc[...]) + hold[len(puts) + 1, :m, :]
    done = [pltpu.make_async_copy(acc, out_hbm, sem)]
    if kind in ("far", "last", "whole"):
        done.append(pltpu.make_async_copy(acc, big_ref.at[pl.ds(row(MINE, s0), m), :], emb_sem(tok_sem)))
    for c in done:
        c.start()
    if wide:
        for i in range(n_steps - 2, n_steps):
            kept(i).wait()
    for c in stores + done:
        c.wait()


def emb_sem(tok_sem):
    return tok_sem.at[0, 0]


def rows_pass(kind, scale, v_rows, span, cut, pos, emb, bias, info, tokens=None, u_all=None, big=None, parts=(), puts=()):
    s0, s1 = span
    m, e = s1 - s0, emb.shape[1]
    sds = jax.ShapeDtypeStruct
    wide = kind in ("own", "side", "far")
    final = kind in ("far", "last", "whole")
    args, aliases = [pos, emb, bias, info], {}
    outs = [sds((m, e), F32)]
    sources = None
    if wide:
        sources = {"own": (0, CORE), "side": (X, X | CORE, Y, Y | CORE), "far": (X | Y, X | Y | CORE)}[kind]
        args += [h for r in sources for h in tokens[r]]
        n_loc = tokens[0][0].shape[0] + tokens[0][1].shape[0]
        outs.append(sds((8, BLK, e), BF16))
        if kind != "own":
            aliases[len(args)] = 1
            args.append(u_all)
    else:
        n_loc = BLK
        args.append(u_all)
    if final:
        if big is not None:
            aliases[len(args)] = len(outs)
            args.append(big)
        outs.append(sds((v_rows, e), F32))
    args += [a for a, _ in parts] + [a for _, a in puts]
    n_hold = max(1, len(parts) + len(puts))
    tallest = max([m] * len(parts) + [a.shape[0] for _, a in puts] + [8])
    t = STEPS[kind] * BLK
    scratch = [pltpu.VMEM((2, n_loc, e), F32)] if wide else []
    scratch += [
        pltpu.VMEM((2 if wide else 3, BLK, e), BF16), pltpu.VMEM((m, e), BF16), pltpu.VMEM((m, BLK), BF16),
        pltpu.VMEM((m, e), F32), pltpu.VMEM((n_hold, tallest, e), F32),
        DMA, DMA((3, 2)), DMA((2,)), DMA((n_hold,)), DMA((n_hold,)),
    ]
    return pl.pallas_call(
        functools.partial(rows_kernel, kind, scale, s0, m, cut, n_loc, sources, [skip for _, skip in parts], [spot for spot, _ in puts], big is not None),
        in_specs=[SMEM, ANY, VMEM, VMEM] + [ANY] * (len(args) - 4),
        out_specs=[ANY] * len(outs),
        out_shape=outs,
        scratch_shapes=scratch,
        input_output_aliases=aliases,
        compiler_params=pltpu.CompilerParams(vmem_limit_bytes=VMEM_LIMIT),
        cost_estimate=pl.CostEstimate(flops=(4 * t * m * e) // COVER, bytes_accessed=t * e * 2 + m * e * 6, transcendentals=t * m),
    )(*args)


def put_kernel(spots, pos, *refs):
    n = len(spots)
    pieces, (out_ref, hold, in_sem, out_sem) = refs[1:1 + n], refs[1 + n:]
    loads, stores = [], []
    for j, (p, (base, off)) in enumerate(zip(pieces, spots)):
        slot = hold.at[j, :p.shape[0], :]
        loads.append(pltpu.make_async_copy(p, slot, in_sem.at[j]))
        stores.append(pltpu.make_async_copy(slot, out_ref.at[pl.ds(pl.multiple_of(pos[base] + off, 8), p.shape[0]), :], out_sem.at[j]))
    for a in loads:
        a.start()
    for a, b in zip(loads, stores):
        a.wait()
        b.start()
    for b in stores:
        b.wait()


def put_rows(pos, big, puts):
    spots, pieces = [s for s, _ in puts], [a for _, a in puts]
    n, e = len(pieces), big.shape[1]
    size = sum(p.size for p in pieces)
    return pl.pallas_call(
        functools.partial(put_kernel, spots),
        in_specs=[SMEM] + [ANY] * (n + 1),
        out_specs=ANY,
        out_shape=jax.ShapeDtypeStruct(big.shape, big.dtype),
        scratch_shapes=[pltpu.VMEM((n, max(p.shape[0] for p in pieces), e), F32), DMA((n,)), DMA((n,))],
        input_output_aliases={1: 0},
        compiler_params=pltpu.CompilerParams(vmem_limit_bytes=VMEM_LIMIT),
        cost_estimate=pl.CostEstimate(flops=(size) // COVER, bytes_accessed=size * 8, transcendentals=0),
        name="put_rows",
    )(pos, big, *pieces)


def join_kernel(n_vec, idx, *refs):
    own, mine, theirs, (dw_ref, vec_ref, full, in_sem, out_sem) = refs[0], refs[1:4], refs[4:7], refs[7:]
    vp, core = idx[0], idx[1]
    half, cols = mine[0].shape
    col = lambda k: pl.ds(pl.multiple_of((vp ^ k) * cols, cols), cols)
    row = lambda c: pl.ds(pl.multiple_of(c * half, 8), half)
    loads = [pltpu.make_async_copy(own.at[:2 * half, :], full.at[:, col(0)], in_sem.at[0])]
    for k in range(3):
        loads.append(pltpu.make_async_copy(mine[k], full.at[row(core), col(k + 1)], in_sem.at[1 + k]))
        loads.append(pltpu.make_async_copy(theirs[k], full.at[row(1 - core), col(k + 1)], in_sem.at[4 + k]))
    for c in loads:
        c.start()
    for c in loads:
        c.wait()
    e = dw_ref.shape[0]
    stores = [pltpu.make_async_copy(full.at[:e, :], dw_ref, out_sem.at[0]), pltpu.make_async_copy(full.at[e:e + n_vec, :], vec_ref, out_sem.at[1])]
    for c in stores:
        c.start()
    for c in stores:
        c.wait()


def join_pass(idx, own, mine, theirs):
    half, cols = mine[0].shape
    e = 4 * cols
    return pl.pallas_call(
        functools.partial(join_kernel, 8),
        in_specs=[SMEM] + [ANY] * 7,
        out_specs=[ANY] * 2,
        out_shape=[jax.ShapeDtypeStruct((e, e), F32), jax.ShapeDtypeStruct((8, e), F32)],
        scratch_shapes=[pltpu.VMEM((2 * half, e), F32), DMA((7,)), DMA((2,))],
        compiler_params=pltpu.CompilerParams(vmem_limit_bytes=VMEM_LIMIT),
        cost_estimate=pl.CostEstimate(flops=(e * e) // COVER, bytes_accessed=e * e * 8, transcendentals=0),
        name="join",
    )(idx, own, *mine, *theirs)


def back_kernel(base, vp, *refs):
    refs = list(refs)
    srcs = [refs.pop(0) for _ in range(7)]
    gain_ref, = [refs.pop(0)]
    extra = refs[:-10]
    dab_ref, pack_ref, pre, norm, rstd, z, m1, m2, du, sem = refs[-10:]
    n, cols = du.shape
    e = z.shape[1]
    col = pl.ds(pl.multiple_of(vp[0] * cols, cols), cols)
    rows = slice(base, base + n)
    pre_h, norm_h, rstd_h, z_h, m1_h, m2_h, du_h = srcs
    loads = [pltpu.make_async_copy(a, b, sem.at[j]) for j, (a, b) in enumerate((
        (pre_h.at[rows, col], pre), (norm_h.at[rows, col], norm), (rstd_h.at[rows, :], rstd), (m1_h.at[rows, :], m1), (m2_h.at[rows, :], m2),
        (du_h, du), (z_h.at[rows, :], z)))]
    for c in loads:
        c.start()
    for c in loads:
        c.wait()
    for j, c in enumerate(range(0, cols, 128)):
        cs = slice(c, c + 128)
        a, d, normed = pre[:, cs], du[:, cs], norm[:, cs]
        cdf = 0.5 * (1.0 + lax.erf(a * (0.5 ** 0.5)))
        dg = rstd[...] * (d * gain_ref[:, cs] - m1[...] - normed * m2[...])
        da = dg * (cdf + a * (jnp.exp(-0.5 * a * a) * 0.3989422804014327))
        dab_ref[:, cs] = da.astype(BF16).astype(F32)
        for j, x in enumerate((da, d * normed, d)):
            pack_ref[e + j:e + j + 1, cs] = jnp.sum(x, axis=0, keepdims=True)
    dw = lax.dot_general(z[...], dab_ref[...].astype(BF16), (((0,), (0,)), ((), ())), preferred_element_type=F32)
    if not extra:
        pack_ref[:e, :] = dw
        pack_ref[e + 3:, :] = jnp.zeros_like(pack_ref[e + 3:, :])
    else:
        prev, loss_ref, db_ref = extra
        pack_ref[:e, :] = prev[:e, :] + dw
        pack_ref[e:e + 3, :] += prev[e:e + 3, :]
        pack_ref[e + 3:e + 4, :] = loss_ref[...]
        pack_ref[e + 4:e + 16, :] = jnp.zeros_like(pack_ref[e + 4:e + 16, :])
        pack_ref[e + 16:, :] = db_ref[...]


def back_pass(base, vp, pre, normed, rstd, z, m1, m2, du, gain, *extra):
    n, cols = du.shape
    e = z.shape[1]
    n_pack = e + 16 + (extra[2].shape[0] if extra else 0)
    block = lambda *s: pl.BlockSpec(s, lambda i, p: (0,) * len(s))
    gs = pltpu.PrefetchScalarGridSpec(
        num_scalar_prefetch=1,
        grid=(1,),
        in_specs=[ANY] * 7 + [pl.BlockSpec((1, cols), lambda i, p: (0, p[0]))] + [block(*x.shape) for x in extra],
        out_specs=[block(n, cols), block(n_pack, cols)],
        scratch_shapes=[pltpu.VMEM((n, cols), F32)] * 2 + [pltpu.VMEM((n, 128), F32), pltpu.VMEM((n, e), BF16)] + [pltpu.VMEM((n, 128), F32)] * 2
        + [pltpu.VMEM((n, cols), F32), DMA((7,))],
    )
    return pl.pallas_call(
        functools.partial(back_kernel, base),
        grid_spec=gs,
        out_shape=[jax.ShapeDtypeStruct((n, cols), F32), jax.ShapeDtypeStruct((n_pack, cols), F32)],
        compiler_params=pltpu.CompilerParams(dimension_semantics=("arbitrary",), vmem_limit_bytes=VMEM_LIMIT),
        cost_estimate=pl.CostEstimate(flops=(2 * n * e * cols) // COVER, bytes_accessed=n * (cols * 16 + e * 2 + 1536), transcendentals=n * cols * 2),
        name="back",
    )(vp, pre, normed, rstd, z, m1, m2, du, gain, *extra)


def spread_kernel(n_masks, vp, pos_ref, w_ref, *refs):
    pieces, (out_ref, dab, dz, obuf, in_sem, out_sem) = refs[:8], refs[8:]
    cut, cols = pieces[0].shape
    n = cut + pieces[4].shape[0]
    col = lambda k: pl.ds(pl.multiple_of((vp[0] ^ k) * cols, cols), cols)
    loads = [pltpu.make_async_copy(p, dab.at[slice(0, cut) if j < 4 else slice(cut, n), col(j % 4)], in_sem.at[j]) for j, p in enumerate(pieces)]
    for c in loads:
        c.start()
    dz[n:, :] = jnp.zeros((dz.shape[0] - n, dz.shape[1]), F32)
    n_seq, seq_len, _ = out_ref.shape
    place = lax.broadcasted_iota(I32, (seq_len, 1), 0)
    slots = pos_ref.shape[2]
    for c in loads:
        c.wait()
    for r0, r1 in row_cuts(n):
        dz[r0:r1, :] = dot(dab[r0:r1, :].astype(BF16), w_ref[...], NT).astype(BF16).astype(F32)
    group = 8
    store = lambda b, j: pltpu.make_async_copy(obuf.at[j % 4], out_ref.at[b], out_sem.at[j % 4])

    @pl.loop(0, n_seq // group)
    def _(g):
        for j in range(group):
            b = g * group + j

            @pl.when(b >= 4)
            def _():
                store(b - 4, j).wait()

            hot = jnp.where(place == pos_ref[b], 1.0, 0.0).astype(BF16)
            base = pl.multiple_of(g * (group * n_masks), 8)
            low = j * n_masks // 8 * 8
            rows = dz[pl.ds(base + low, slots + 8), :][j * n_masks - low:j * n_masks - low + slots]
            obuf[j % 4] = dot(hot, rows.astype(BF16), NN).astype(BF16)
            store(b, j).start()

    for j in range(group - 4, group):
        store(n_seq - group + j, j).wait()


def spread_pass(n_masks, shape, vp, pos, w, pieces):
    cols = pieces[0].shape[1]
    n = pieces[0].shape[0] + pieces[4].shape[0]
    e = w.shape[0]
    return pl.pallas_call(
        functools.partial(spread_kernel, n_masks),
        in_specs=[SMEM, VMEM, VMEM] + [ANY] * 8,
        out_specs=ANY,
        out_shape=jax.ShapeDtypeStruct(shape, BF16),
        scratch_shapes=[pltpu.VMEM((n, 4 * cols), F32), pltpu.VMEM((n + 16, e), F32), pltpu.VMEM((4,) + shape[1:], BF16), DMA((8,)), DMA((4,))],
        compiler_params=pltpu.CompilerParams(vmem_limit_bytes=VMEM_LIMIT),
        cost_estimate=pl.CostEstimate(flops=(2 * shape[0] * shape[1] * 128 * e) // COVER, bytes_accessed=shape[0] * shape[1] * e * 2, transcendentals=0),
        name="spread",
    )(vp, pos, w, *pieces)


def order_sum(xs):
    return (xs[0] + xs[1]) + (xs[2] + xs[3])


def after(x, *deps):
    return lax.optimization_barrier((x, deps))[0]


def solution(mesh):
    n_groups, n_shards = mesh.shape["dp"], mesh.shape["vp"]

    def swap(a, bit):
        return lax.ppermute(a, "dp", [(d, d ^ bit) for d in range(n_groups)])

    def swap_vp(a, bit):
        return lax.ppermute(a, "vp", [(d, d ^ bit) for d in range(n_shards)])

    def hop(a):
        return lax.ppermute(a, "dp", [(d, d ^ (Y if d & CORE else X)) for d in range(n_groups)])

    def local_step(hidden, mask_pos, labels, w_trans, b_trans, ln_gain, ln_bias, emb_table, b_vocab):
        n_rows, _, width = hidden.shape
        n_masks = mask_pos.shape[1]
        shard_rows = emb_table.shape[0]
        n_loc = n_rows * n_masks
        n_tokens = n_loc * n_groups
        slots = -(-n_masks // 16) * 16
        cut = n_loc // 32 * 16
        cols = width // n_shards
        dp, vp = lax.axis_index("dp"), lax.axis_index("vp")
        row_start = vp * shard_rows
        scale = 1.0 / n_tokens
        core, mine = dp & 1, (dp >> 1 ^ dp >> 2) & 1

        pos_pad = jnp.pad(mask_pos, ((0, 0), (0, slots - n_masks)), constant_values=-1)
        z, pre, normed, rstd, u, u_lo, u_hi = head_pass(
            n_masks, cut, hidden, jnp.broadcast_to(pos_pad[:, :, None], (n_rows, slots, 128)),
            w_trans, b_trans[None], ln_gain[None], ln_bias[None])

        x_lo, y_hi = swap(u_lo, X), swap(u_hi, Y)
        x_hi, y_lo = swap(u_hi, X), swap(u_lo, Y)
        c_lo, c_hi = swap(u_lo, CORE), swap(u_hi, CORE)

        flat_labels = labels.reshape(n_loc)
        lab_local = flat_labels - row_start
        lab_local = jnp.where((lab_local >= 0) & (lab_local < shard_rows), lab_local, -1)
        column = lambda x: jnp.broadcast_to(x[:, None], (x.shape[0], 128))
        lab_cols = column(lab_local[:cut]), column(lab_local[cut:])
        *logits, stat = stats(u, emb_table, b_vocab[None], column(lab_local), cut)
        all_stats = [stat] + [swap_vp(stat, b) for b in range(1, n_shards)]
        global_max = functools.reduce(jnp.maximum, [s[0] for s in all_stats])
        log_norm = global_max + jnp.log(order_sum([s[1] * jnp.exp(s[0] - global_max) for s in all_stats]))
        loss_part = jnp.sum(log_norm - order_sum([s[2] for s in all_stats]))
        lse = log_norm + jnp.log(jnp.float32(n_tokens))

        fill = (0, BLK - n_loc)
        info = jnp.stack([jnp.pad(lse, fill, constant_values=jnp.inf), jnp.pad(flat_labels.astype(F32), fill, constant_values=-1.0)])
        near, *away = [swap(info, b) for b in (CORE, X, Y, X | Y)]
        x_lo, y_hi = after((x_lo, y_hi), stat)
        d_lo, d_hi = swap(x_lo, Y), swap(y_hi, X)
        cx_lo, cy_hi = swap(x_lo, CORE), swap(y_hi, CORE)

        du_shares, db_parts, sums, before = [], [], [], ()
        for j, (r0, r1) in enumerate(((0, cut), (cut, n_loc))):
            lse_col = after(column(lse[r0:r1]), *before)
            part, db, row_sums = du_pass(scale, n_shards, r0, logits[j], emb_table, lse_col, lab_cols[j], normed, ln_gain[None])
            du_shares.append(lax.psum_scatter(part.reshape(n_shards * (r1 - r0), cols), "vp", scatter_dimension=0, tiled=True))
            db_parts.append(db)
            sums.append(row_sums)
            before = (part,)
        du_part = before[0]
        sums = jnp.concatenate(sums, axis=1)
        sums = [sums] + [swap_vp(sums, b) for b in range(1, n_shards)]

        half, quarter = shard_rows // 2, shard_rows // 4
        start = lambda h, c: h * half + c * quarter
        pos = jnp.stack([dp, start(mine, core), row_start + start(mine, core), start(mine, 1 - core), start(1 - mine, core), start(1 - mine, 1 - core)])
        bias_col = lax.dynamic_slice(b_vocab, (start(mine, core),), (quarter,))[:, None]
        shares = (1280, 1088, 776)
        ends = [0]
        for w in shares[:-1]:
            ends.append(ends[-1] + max(16, quarter * w // sum(shares) // 16 * 16))
        spans = list(zip(ends, ends[1:] + [quarter]))

        def rows(kind, k, *wait, info=None, span=None, **kw):
            return rows_pass(kind, scale, shard_rows, span or spans[k], cut, after(pos, *wait), emb_table, bias_col, info, **kw)

        def send(k, chunk):
            return ((TWIN, spans[k][0]), swap(chunk, CORE)), hop(chunk)

        def forward(k, far, *wait):
            far = after(far, *wait)
            return ((FAR, spans[k][0]), far), ((FAR_TWIN, spans[k][0]), swap(far, CORE))

        tokens = {0: (u_lo, u_hi), CORE: (c_lo, c_hi), X: (x_lo, x_hi), Y: (y_lo, y_hi)}
        pair = jnp.stack([info, near])
        own, u_all = rows("own", 0, du_part, info=pair, tokens=tokens)
        x_hi, y_lo, away = after((x_hi, y_lo, away), own)
        away = jnp.stack(away)
        tokens[X | CORE] = cx_lo, swap(x_hi, CORE)
        tokens[Y | CORE] = swap(y_lo, CORE), cy_hi
        away_near = swap(away, CORE)
        tokens[X], tokens[Y] = (x_lo, x_hi), (y_lo, y_hi)
        info = jnp.concatenate([pair, jnp.stack([away, away_near], axis=1).reshape(6, 2, BLK)])

        du_a, sums = after((du_shares[0], sums), own)
        sums = order_sum(sums) / width
        m1, m2 = column(sums[0]), column(sums[1])
        dab_a, pack = back_pass(0, vp[None], pre, normed, rstd, z, m1, m2, du_a, ln_gain[None])
        dab_a = [dab_a] + [swap_vp(dab_a, b) for b in range(1, n_shards)]

        side, u_all = rows("side", 0, pack, info=info, tokens=tokens, u_all=u_all)
        d_lo, d_hi = after((d_lo, d_hi), side)
        tokens[X | Y], tokens[X | Y | CORE] = (d_lo, d_hi), (swap(d_lo, CORE), swap(d_hi, CORE))

        du_b = after(du_shares[1], side)
        loss_row = jnp.pad(loss_part[None, None], ((0, 0), (0, cols - 1)))
        db_rows = -(-shard_rows // cols // 8) * 8
        db_mat = jnp.pad((db_parts[0] + db_parts[1])[0], (0, db_rows * cols - shard_rows)).reshape(db_rows, cols)
        dab_b, pack = back_pass(cut, vp[None], pre, normed, rstd, z, m1, m2, du_b, ln_gain[None], pack, loss_row, db_mat)
        back_done = dab_b
        pack = lax.psum(pack, "dp")
        dab_b = [dab_b] + [swap_vp(dab_b, b) for b in range(1, n_shards)]

        chunk0, u_all, big = rows("far", 0, back_done, info=info, tokens=tokens, u_all=u_all, parts=((own, 0), (side, 0)))
        twin0, far0 = send(0, chunk0)
        chunk1, big = rows("whole", 1, info=info, u_all=u_all, big=big)
        twin1, far1 = send(1, chunk1)
        pack = after(pack, chunk1)
        n_half = (width + 16) // 2
        part = lax.dynamic_slice(pack, (core * n_half, 0), (n_half, cols))
        parts = [swap_vp(part, b) for b in range(1, n_shards)]

        chunk2, big = rows("whole", 2, part, info=info, u_all=u_all, big=big, puts=[twin0])
        twin2, far2 = send(2, chunk2)
        far0, far_twin0 = forward(0, far0, chunk2)
        d_hidden = spread_pass(n_masks, hidden.shape, vp[None], pos_pad[:, None], w_trans, after(dab_a + dab_b, chunk2))
        parts = after(parts, d_hidden)
        others = [swap(p, CORE) for p in parts]
        big = put_rows(pos, big, [far0, far_twin0, twin1, twin2])
        far1, far_twin1 = forward(1, far1, big)
        pack, parts, others = after((pack, parts, others), big)
        d_w, vec = join_pass(jnp.stack([vp, core]), pack, parts, others)
        big = put_rows(pos, big, [far1, far_twin1])
        far2, far_twin2 = forward(2, far2, big)
        big = put_rows(pos, big, [far2])
        big = put_rows(pos, big, [far_twin2])

        db = pack[width + 16:].reshape(-1)[:shard_rows]
        return pack[width + 3, 0] / n_tokens, d_hidden, d_w, vec[0], vec[1], vec[2], big, db

    in_specs = (P("dp", None, None), P("dp", None), P("dp", None), P(None, None), P(None), P(None), P(None), P("vp", None), P("vp"))
    out_specs = (P(), P("dp", None, None), P(None, None), P(None), P(None), P(None), P("vp", None), P("vp"))
    return jax.shard_map(local_step, mesh=mesh, in_specs=in_specs, out_specs=out_specs, check_vma=False)
```

```python
import functools

import jax
import jax.numpy as jnp
from jax import lax
from jax.experimental import pallas as pl
from jax.experimental.pallas import tpu as pltpu
from jax.sharding import PartitionSpec as P


F32, BF16, I32 = jnp.float32, jnp.bfloat16, jnp.int32
NT = (((1,), (1,)), ((), ()))
NN = (((1,), (0,)), ((), ()))
VB = 1024
VMEM_LIMIT = 60 << 20
COVER = 100
PARTS = 4
LEAST = float(jnp.finfo(jnp.float32).min)
ELSEWHERE = -(1 << 20)


def row_cuts(rows, parts=4):
    cuts = [16 * (rows // 16 * k // parts) for k in range(parts)] + [rows]
    return list(zip(cuts[:-1], cuts[1:]))


def dot(a, b, dims):
    return lax.dot_general(a, b, dims, preferred_element_type=F32)


def stats_kernel(n_vocab, u_ref, emb_ref, b_ref, lab_ref, logits_ref, stat_ref, prev, m_sc, s_sc, l_sc):
    i, n_steps = pl.program_id(0), pl.num_programs(0)
    lane = lax.broadcasted_iota(I32, (1, 128), 1)
    cuts = row_cuts(u_ref.shape[0], PARTS)

    @pl.when(i == 0)
    def _():
        m_sc[...] = jnp.full_like(m_sc, LEAST)
        s_sc[...] = jnp.zeros_like(s_sc)
        l_sc[...] = jnp.zeros_like(l_sc)
        prev[...] = jnp.full_like(prev, -jnp.inf)

    def logits_of(r0, r1, c0, wide, width):
        tile = dot(u_ref[r0:r1, :], emb_ref[c0:c0 + wide, :], NT) + b_ref[:, c0:c0 + wide]
        if wide > width:
            tile = jnp.where(lax.broadcasted_iota(I32, (1, wide), 1) < width, tile, -jnp.inf)
        logits_ref[r0:r1, c0:c0 + wide] = tile
        return tile

    def take(r0, r1, read, first, wide):
        for q in range(r0, r1, 16):
            rs = slice(q, q + 16)
            parts = [read(rs, slice(k, k + 128)) for k in range(0, wide, 128)]
            m_old = m_sc[rs, :]
            m_new = functools.reduce(jnp.maximum, parts, m_old)
            s_new = s_sc[rs, :] * jnp.exp(m_old - m_new)
            l_new = l_sc[rs, :]
            lab = lab_ref[rs, :] - first
            for k, part in enumerate(parts):
                s_new += jnp.exp(part - m_new)
                l_new = jnp.where(lab == lane + k * 128, part, l_new)
            m_sc[rs, :], s_sc[rs, :], l_sc[rs, :] = m_new, s_new, l_new

    from_prev = lambda rs, cs: prev[rs, cs]
    from_out = lambda rs, cs: logits_ref[rs, cs]

    def step(second):
        width = VB if second else n_vocab % (2 * VB)
        wide = -(-width // 128) * 128
        for r0, r1 in cuts:
            logits_of(r0, r1, 0, wide, width)
            take(r0, r1, from_prev, (2 * i - 1) * VB, VB)
        for r0, r1 in cuts:
            if second:
                prev[r0:r1, :] = logits_of(r0, r1, VB, VB, VB)
            take(r0, r1, from_out, 2 * i * VB, wide)

    pl.when(i < n_steps - 1)(functools.partial(step, True))
    pl.when(i == n_steps - 1)(functools.partial(step, False))

    @pl.when(i == n_steps - 1)
    def _():
        m_t, s_t, l_t = m_sc[...].T, s_sc[...].T, l_sc[...].T
        m_all = jnp.max(m_t, axis=0, keepdims=True)
        stat_ref[0:1, :] = m_all
        stat_ref[1:2, :] = jnp.sum(s_t * jnp.exp(m_t - m_all), axis=0, keepdims=True)
        stat_ref[2:3, :] = jnp.sum(l_t, axis=0, keepdims=True)
        stat_ref[3:8, :] = jnp.zeros_like(stat_ref[3:8, :])


def stats(u, emb, bias, lab):
    t, e = u.shape
    v = emb.shape[0]
    n = pl.cdiv(v, 2 * VB)
    whole = lambda *s: pl.BlockSpec(s, lambda i: (0,) * len(s))
    return pl.pallas_call(
        functools.partial(stats_kernel, v),
        grid=(n,),
        in_specs=[whole(t, e), pl.BlockSpec((2 * VB, e), lambda i: (i, 0)), pl.BlockSpec((1, 2 * VB), lambda i: (0, i)), whole(t, 128)],
        out_specs=[pl.BlockSpec((t, 2 * VB), lambda i: (0, i)), whole(8, t)],
        out_shape=[jax.ShapeDtypeStruct((t, v), F32), jax.ShapeDtypeStruct((8, t), F32)],
        scratch_shapes=[pltpu.VMEM((t, VB), F32)] + [pltpu.VMEM((t, 128), F32)] * 3,
        compiler_params=pltpu.CompilerParams(dimension_semantics=("arbitrary",), vmem_limit_bytes=VMEM_LIMIT),
        cost_estimate=pl.CostEstimate(flops=(2 * t * v * e) // COVER, bytes_accessed=t * v * 4 + v * e * 2, transcendentals=t * v),
        name="stats",
    )(u, emb, bias, lab)


def du_kernel(n_vocab, scale, base, logits_ref, emb_ref, lse_ref, lab_ref, norm_hbm, gain_ref, out_ref, db_ref, sum_ref, du_ref, g_sc, db_sc, norm_sc, db_sc2, sem):
    i, n_blocks = pl.program_id(0), pl.num_programs(0)
    t = logits_ref.shape[0]
    lane = lax.broadcasted_iota(I32, (1, 128), 1)

    norm_copy = pltpu.make_async_copy(norm_hbm.at[base:base + t, :], norm_sc, sem)

    @pl.when(i == 0)
    def _():
        du_ref[...] = jnp.zeros_like(du_ref)

    @pl.when(i == 2)
    def _():
        norm_copy.start()

    def run(width):
        wide = -(-width // 128) * 128
        emb = emb_ref[:wide, :]
        if wide > width:
            emb = jnp.where(lax.broadcasted_iota(I32, (wide, 1), 0) < width, emb, jnp.zeros_like(emb))
        for r0, r1 in row_cuts(t):
            sums = [None] * (wide // 128)
            for q in range(r0, r1, 16):
                rs = slice(q, q + 16)
                lse = lse_ref[rs, :]
                lab = lab_ref[rs, :] - i * VB
                for k in range(wide // 128):
                    c = k * 128
                    g = jnp.exp(logits_ref[rs, c:c + 128] - lse)
                    g -= jnp.where(lab == lane + c, scale, 0.0)
                    if c + 128 > width:
                        g = jnp.where(lane < width - c, g, 0.0)
                    part = g[:8] + g[8:]
                    sums[k] = part if sums[k] is None else sums[k] + part
                    g_sc[rs, c:c + 128] = g.astype(BF16)
            for k in range(wide // 128):
                cs = slice(k * 128, (k + 1) * 128)
                db_sc[:, cs] = sums[k] if r0 == 0 else db_sc[:, cs] + sums[k]
            du_ref[r0:r1, :] += dot(g_sc[r0:r1, :wide], emb, NN)
        db_ref[:, :wide] = jnp.sum(db_sc[:, :wide], axis=0, keepdims=True)

    tail = n_vocab % VB
    if tail:
        pl.when(i < n_blocks - 1)(functools.partial(run, VB))
        pl.when(i == n_blocks - 1)(functools.partial(run, tail))
    else:
        run(VB)

    @pl.when(i == n_blocks - 1)
    def _():
        norm_copy.wait()
        parts, rows, cols = out_ref.shape
        run = rows // 7
        for r in range(0, rows, run):
            rs = slice(r, r + run)
            total = [jnp.zeros((run, 128), F32)] * 2
            for c in range(0, parts * cols, 128):
                x = du_ref[rs, c:c + 128].astype(BF16).astype(F32)
                out_ref[c // cols, rs, c % cols:c % cols + 128] = x
                dn = x * gain_ref[:, c:c + 128]
                total = [total[0] + dn, total[1] + dn * norm_sc[rs, c:c + 128]]
            for j, x in enumerate(total):
                db_sc2[j, rs, :] = x
        for j in range(2):
            sum_ref[j:j + 1, :] = jnp.sum(db_sc2[j].T, axis=0, keepdims=True)
        sum_ref[2:, :] = jnp.zeros_like(sum_ref[2:, :])


def du_pass(scale, parts, base, logits, emb, lse, lab, normed, gain):
    t, v = logits.shape
    e = emb.shape[1]
    n = pl.cdiv(v, VB)
    whole = lambda *s: pl.BlockSpec(s, lambda i: (0,) * len(s))
    return pl.pallas_call(
        functools.partial(du_kernel, v, scale, base),
        grid=(n,),
        in_specs=[pl.BlockSpec((t, VB), lambda i: (0, i)), pl.BlockSpec((VB, e), lambda i: (i, 0)), whole(t, 128), whole(t, 128), pl.BlockSpec(memory_space=pl.ANY), whole(1, e)],
        out_specs=[whole(parts, t, e // parts), pl.BlockSpec((1, VB), lambda i: (0, i)), whole(8, t)],
        out_shape=[jax.ShapeDtypeStruct((parts, t, e // parts), F32), jax.ShapeDtypeStruct((1, v), F32), jax.ShapeDtypeStruct((8, t), F32)],
        scratch_shapes=[pltpu.VMEM((t, e), F32), pltpu.VMEM((t, VB), BF16), pltpu.VMEM((8, VB), F32), pltpu.VMEM((t, e), F32), pltpu.VMEM((2, t, 128), F32), pltpu.SemaphoreType.DMA],
        compiler_params=pltpu.CompilerParams(dimension_semantics=("arbitrary",), vmem_limit_bytes=VMEM_LIMIT),
        cost_estimate=pl.CostEstimate(flops=(2 * t * v * e) // COVER, bytes_accessed=t * v * 4 + v * e * 2, transcendentals=t * v),
        name="du_pass",
    )(logits, emb, lse, lab, normed, gain)


LN_EPS = 1e-5
CORE, X, Y = 1, 2, 4
ANY = pl.BlockSpec(memory_space=pltpu.HBM)
VMEM = pl.BlockSpec(memory_space=pltpu.VMEM)
SMEM = pl.BlockSpec(memory_space=pltpu.SMEM)
DMA = pltpu.SemaphoreType.DMA


def gelu_norm(a):
    cdf = 0.5 * (1.0 + lax.erf(a * (0.5 ** 0.5)))
    g = a * cdf
    centered = g - jnp.mean(g, axis=1, keepdims=True)
    rstd = lax.rsqrt(jnp.mean(centered * centered, axis=1, keepdims=True) + LN_EPS)
    return cdf, centered * rstd, rstd


def head_kernel(n_masks, cut, hid, pos_ref, w_ref, b_ref, gain_ref, bias_ref, z_out, pre_out, norm_out, rstd_out, u_out, lo_out, hi_out,
                hbuf, zf, zb, pre_v, norm_v, rstd_v, ub, uf, in_sem, out_sem):
    n_seq, seq_len = hid.shape[0], hid.shape[1]
    n_loc = n_seq * n_masks
    loads = [pltpu.make_async_copy(hid.at[b], hbuf.at[b], in_sem.at[b]) for b in range(n_seq)]
    for c in loads:
        c.start()
    lane = lax.broadcasted_iota(I32, (1, 128), 1)
    cuts = [0, cut // 32 * 16, cut, cut + (n_loc - cut) // 32 * 16, n_loc]
    done, stores = 0, []

    def send(src, dst, r0, r1, base=0):
        c = pltpu.make_async_copy(src.at[r0:r1, :], dst.at[r0 - base:r1 - base, :], out_sem.at[len(stores)])
        c.start()
        stores.append(c)

    for b in range(n_seq):
        loads[b].wait()
        hot = jnp.concatenate([jnp.where(pos_ref[b] == lane + j, 1.0, 0.0).astype(BF16) for j in range(0, seq_len, 128)], axis=1)
        zf[b * n_masks:(b + 1) * n_masks, :] = dot(hot, hbuf[b], NN)[:n_masks, :]
        while done < 4 and cuts[done + 1] <= (b + 1) * n_masks:
            r0, r1 = cuts[done], cuts[done + 1]
            z = zf[r0:r1, :].astype(BF16)
            zb[r0:r1, :] = z
            a = dot(z, w_ref[...], NN) + b_ref[...]
            pre_v[r0:r1, :] = a
            _, normed, rstd = gelu_norm(a)
            norm_v[r0:r1, :] = normed
            rstd_v[r0:r1, :] = jnp.broadcast_to(rstd, (r1 - r0, 128))
            u = (normed * gain_ref[...] + bias_ref[...]).astype(BF16)
            ub[r0:r1, :] = u
            uf[r0:r1, :] = u.astype(F32)
            done += 1
            send(uf, hi_out if r0 >= cut else lo_out, r0, r1, cut if r0 >= cut else 0)
            for src, dst in ((ub, u_out), (zb, z_out), (pre_v, pre_out), (norm_v, norm_out), (rstd_v, rstd_out)):
                send(src, dst, r0, r1)
    for c in stores:
        c.wait()


def head_pass(n_masks, cut, hidden, pos, w, b, gain, bias):
    n_seq, seq_len, e = hidden.shape
    n = n_seq * n_masks
    kinds = [((n, e), BF16), ((n, e), F32), ((n, e), F32), ((n, 128), F32), ((n, e), BF16), ((cut, e), F32), ((n - cut, e), F32)]
    return pl.pallas_call(
        functools.partial(head_kernel, n_masks, cut),
        in_specs=[ANY] + [VMEM] * 5,
        out_specs=[ANY] * len(kinds),
        out_shape=[jax.ShapeDtypeStruct(*k) for k in kinds],
        scratch_shapes=[pltpu.VMEM((n_seq, seq_len, e), BF16), pltpu.VMEM((n, e), F32)]
        + [pltpu.VMEM(*k) for k in kinds[:5]] + [pltpu.VMEM((n, e), F32), DMA((n_seq,)), DMA((24,))],
        compiler_params=pltpu.CompilerParams(vmem_limit_bytes=VMEM_LIMIT),
        cost_estimate=pl.CostEstimate(flops=(4 * n * e * e) // COVER, bytes_accessed=hidden.size * 2 + n * e * 20, transcendentals=n * e),
        name="head",
    )(hidden, pos, w, b, gain, bias)


BLK = 1280
LOOPED = ('side',)
STEPS = {"own": 2, "again": 2, "side": 4, "far": 2, "last": 2, "whole": 8}
ME, MINE, MINE_ID, TWIN, FAR, FAR_TWIN = range(6)


def rows_kernel(kind, scale, s0, m, cut, n_loc, sources, skips, spots, has_big, pos, emb_hbm, bias_ref, info_ref, *refs):
    refs = list(refs)
    take = lambda n: [refs.pop(0) for _ in range(n)]
    wide = sources is not None
    if wide:
        src = {r: take(2) for r in sources}
        if kind != "own":
            take(1)
    else:
        u_hbm, = take(1)
    if has_big:
        take(1)
    parts = take(len(skips))
    puts = take(len(spots))
    out_hbm, = take(1)
    if wide:
        u_hbm, = take(1)
    if kind in ("far", "last", "whole"):
        big_ref, = take(1)
    if wide:
        buf, = take(1)
    ring, emb_sc, g_sc, acc, hold, sem, tok_sem, back_sem, in_sem, out_sem = refs
    me = pos[ME]
    chip = lax.div(me, 2)
    n_steps = STEPS[kind]
    along_x, along_y = chip ^ 1, chip ^ 2

    def device(i):
        side = 2 * jnp.where(i < 2, jnp.minimum(along_x, along_y), jnp.maximum(along_x, along_y)) + lax.rem(i, 2)
        far = 2 * (chip ^ 3) + lax.rem(i, 2)
        if kind in ("own", "again"):
            return 2 * chip + i
        return {"side": side, "far": far, "last": far, "whole": i}[kind]

    depth = ring.shape[0]

    def fetch(i):
        slot = lax.rem(i, 2 if wide else depth)
        if not wide:
            pltpu.make_async_copy(u_hbm.at[device(i)], ring.at[slot], tok_sem.at[slot, 0]).start()
            return
        for r, (lo, hi) in src.items():
            @pl.when(device(i) ^ me == r)
            def _():
                pltpu.make_async_copy(lo, buf.at[slot, :cut, :], tok_sem.at[slot, 0]).start()
                pltpu.make_async_copy(hi, buf.at[slot, cut:, :], tok_sem.at[slot, 1]).start()

    row = lambda j, off: pl.multiple_of(pos[j] + off, 8)
    emb_copy = pltpu.make_async_copy(emb_hbm.at[pl.ds(row(MINE, s0), m), :], emb_sc, sem)
    emb_copy.start()
    fetch(0)
    loads, stores = [], []
    for j, (p, (base, off)) in enumerate(zip(puts, spots)):
        n = p.shape[0]
        loads.append(pltpu.make_async_copy(p, hold.at[j, :n, :], in_sem.at[j]))
        stores.append(pltpu.make_async_copy(hold.at[j, :n, :], big_ref.at[pl.ds(row(base, off), n), :], out_sem.at[j]))
    for j, (p, skip) in enumerate(zip(parts, skips)):
        loads.append(pltpu.make_async_copy(p.at[skip:skip + m, :], hold.at[len(puts) + j, :m, :], in_sem.at[len(puts) + j]))
    acc[...] = jnp.zeros_like(acc)
    if wide:
        for k in range(2):
            ring[k, n_loc:, :] = jnp.zeros((BLK - n_loc, ring.shape[2]), BF16)
    emb_copy.wait()
    n_groups = 2 if kind in LOOPED and m % 32 == 0 else 1
    tall = m // n_groups
    n_cuts = max(1, round(tall / 300))
    cuts = [-(-tall * k // (n_cuts * 16)) * 16 for k in range(n_cuts)] + [tall]
    cuts = list(zip(cuts[:-1], cuts[1:]))
    kept = lambda i: pltpu.make_async_copy(ring.at[lax.rem(i, 2)], u_hbm.at[device(i)], back_sem.at[lax.rem(i, 2)])

    @pl.loop(0, n_steps)
    def _(i):
        slot = lax.rem(i, 2 if wide else depth)
        if wide:
            any_lo, any_hi = next(iter(src.values()))
            pltpu.make_async_copy(any_lo, buf.at[slot, :cut, :], tok_sem.at[slot, 0]).wait()
            pltpu.make_async_copy(any_hi, buf.at[slot, cut:, :], tok_sem.at[slot, 1]).wait()

            @pl.when(i >= 2)
            def _():
                kept(i - 2).wait()
        else:
            pltpu.make_async_copy(u_hbm.at[device(i)], ring.at[slot], tok_sem.at[slot, 0]).wait()

        @pl.when(i + 1 < n_steps)
        def _():
            fetch(i + 1)

        @pl.when(i == 0)
        def _():
            for c in loads:
                c.start()

        for j, (a, b) in enumerate(zip(loads, stores)):
            @pl.when(i == min(2 + j, n_steps - 1))
            def _():
                a.wait()
                b.start()

        if wide:
            ring[slot, :n_loc, :] = buf[slot].astype(BF16)
            kept(i).start()
        rel = device(i) ^ me
        lse, lab = info_ref[rel, 0:1, :], info_ref[rel, 1:2, :]

        def group(h):
            def rows(r0, r1):
                return slice(r0, r1) if n_groups == 1 else pl.ds(pl.multiple_of(h * tall + r0, 16), r1 - r0)

            def weights(r0, r1):
                part = dot(emb_sc[rows(r0, r1), :], ring[slot], NT)
                ids = lax.broadcasted_iota(I32, (r1 - r0, 1), 0) + (pos[MINE_ID] + (s0 + h * tall + r0))
                bias = bias_ref[slice(s0 + r0, s0 + r1) if n_groups == 1 else pl.ds(pl.multiple_of(s0 + h * tall + r0, 8), r1 - r0), :]
                g = jnp.exp(part + bias - lse) - jnp.where(lab == ids.astype(F32), scale, 0.0)
                g_sc[r0:r1, :] = g.astype(BF16)

            weights(*cuts[0])
            for k, (r0, r1) in enumerate(cuts):
                if k + 1 < len(cuts):
                    weights(*cuts[k + 1])
                acc[rows(r0, r1), :] += dot(g_sc[r0:r1, :], ring[slot], NN)

        if n_groups == 1:
            group(0)
        else:
            pl.loop(0, n_groups)(group)

    for c in loads[len(puts):]:
        c.wait()
    if parts:
        acc[...] = (hold[len(puts), :m, :] + acc[...]) + hold[len(puts) + 1, :m, :]
    done = [pltpu.make_async_copy(acc, out_hbm, sem)]
    if kind in ("far", "last", "whole"):
        done.append(pltpu.make_async_copy(acc, big_ref.at[pl.ds(row(MINE, s0), m), :], emb_sem(tok_sem)))
    for c in done:
        c.start()
    if wide:
        for i in range(n_steps - 2, n_steps):
            kept(i).wait()
    for c in stores + done:
        c.wait()


def emb_sem(tok_sem):
    return tok_sem.at[0, 0]


def rows_pass(kind, scale, v_rows, span, cut, pos, emb, bias, info, tokens=None, u_all=None, big=None, parts=(), puts=()):
    s0, s1 = span
    m, e = s1 - s0, emb.shape[1]
    sds = jax.ShapeDtypeStruct
    wide = kind in ("own", "side", "far")
    final = kind in ("far", "last", "whole")
    args, aliases = [pos, emb, bias, info], {}
    outs = [sds((m, e), F32)]
    sources = None
    if wide:
        sources = {"own": (0, CORE), "side": (X, X | CORE, Y, Y | CORE), "far": (X | Y, X | Y | CORE)}[kind]
        args += [h for r in sources for h in tokens[r]]
        n_loc = tokens[0][0].shape[0] + tokens[0][1].shape[0]
        outs.append(sds((8, BLK, e), BF16))
        if kind != "own":
            aliases[len(args)] = 1
            args.append(u_all)
    else:
        n_loc = BLK
        args.append(u_all)
    if final:
        if big is not None:
            aliases[len(args)] = len(outs)
            args.append(big)
        outs.append(sds((v_rows, e), F32))
    args += [a for a, _ in parts] + [a for _, a in puts]
    n_hold = max(1, len(parts) + len(puts))
    tallest = max([m] * len(parts) + [a.shape[0] for _, a in puts] + [8])
    t = STEPS[kind] * BLK
    scratch = [pltpu.VMEM((2, n_loc, e), F32)] if wide else []
    scratch += [
        pltpu.VMEM((2 if wide else 3, BLK, e), BF16), pltpu.VMEM((m, e), BF16), pltpu.VMEM((m, BLK), BF16),
        pltpu.VMEM((m, e), F32), pltpu.VMEM((n_hold, tallest, e), F32),
        DMA, DMA((3, 2)), DMA((2,)), DMA((n_hold,)), DMA((n_hold,)),
    ]
    return pl.pallas_call(
        functools.partial(rows_kernel, kind, scale, s0, m, cut, n_loc, sources, [skip for _, skip in parts], [spot for spot, _ in puts], big is not None),
        in_specs=[SMEM, ANY, VMEM, VMEM] + [ANY] * (len(args) - 4),
        out_specs=[ANY] * len(outs),
        out_shape=outs,
        scratch_shapes=scratch,
        input_output_aliases=aliases,
        compiler_params=pltpu.CompilerParams(vmem_limit_bytes=VMEM_LIMIT),
        cost_estimate=pl.CostEstimate(flops=(4 * t * m * e) // COVER, bytes_accessed=t * e * 2 + m * e * 6, transcendentals=t * m),
    )(*args)


def put_kernel(spots, pos, *refs):
    n = len(spots)
    pieces, (out_ref, hold, in_sem, out_sem) = refs[1:1 + n], refs[1 + n:]
    loads, stores = [], []
    for j, (p, (base, off)) in enumerate(zip(pieces, spots)):
        slot = hold.at[j, :p.shape[0], :]
        loads.append(pltpu.make_async_copy(p, slot, in_sem.at[j]))
        stores.append(pltpu.make_async_copy(slot, out_ref.at[pl.ds(pl.multiple_of(pos[base] + off, 8), p.shape[0]), :], out_sem.at[j]))
    for a in loads:
        a.start()
    for a, b in zip(loads, stores):
        a.wait()
        b.start()
    for b in stores:
        b.wait()


def put_rows(pos, big, puts):
    spots, pieces = [s for s, _ in puts], [a for _, a in puts]
    n, e = len(pieces), big.shape[1]
    size = sum(p.size for p in pieces)
    return pl.pallas_call(
        functools.partial(put_kernel, spots),
        in_specs=[SMEM] + [ANY] * (n + 1),
        out_specs=ANY,
        out_shape=jax.ShapeDtypeStruct(big.shape, big.dtype),
        scratch_shapes=[pltpu.VMEM((n, max(p.shape[0] for p in pieces), e), F32), DMA((n,)), DMA((n,))],
        input_output_aliases={1: 0},
        compiler_params=pltpu.CompilerParams(vmem_limit_bytes=VMEM_LIMIT),
        cost_estimate=pl.CostEstimate(flops=(size) // COVER, bytes_accessed=size * 8, transcendentals=0),
        name="put_rows",
    )(pos, big, *pieces)


def join_kernel(n_vec, idx, *refs):
    own, mine, theirs, (dw_ref, vec_ref, full, in_sem, out_sem) = refs[0], refs[1:4], refs[4:7], refs[7:]
    vp, core = idx[0], idx[1]
    half, cols = mine[0].shape
    col = lambda k: pl.ds(pl.multiple_of((vp ^ k) * cols, cols), cols)
    row = lambda c: pl.ds(pl.multiple_of(c * half, 8), half)
    loads = [pltpu.make_async_copy(own.at[:2 * half, :], full.at[:, col(0)], in_sem.at[0])]
    for k in range(3):
        loads.append(pltpu.make_async_copy(mine[k], full.at[row(core), col(k + 1)], in_sem.at[1 + k]))
        loads.append(pltpu.make_async_copy(theirs[k], full.at[row(1 - core), col(k + 1)], in_sem.at[4 + k]))
    for c in loads:
        c.start()
    for c in loads:
        c.wait()
    e = dw_ref.shape[0]
    stores = [pltpu.make_async_copy(full.at[:e, :], dw_ref, out_sem.at[0]), pltpu.make_async_copy(full.at[e:e + n_vec, :], vec_ref, out_sem.at[1])]
    for c in stores:
        c.start()
    for c in stores:
        c.wait()


def join_pass(idx, own, mine, theirs):
    half, cols = mine[0].shape
    e = 4 * cols
    return pl.pallas_call(
        functools.partial(join_kernel, 8),
        in_specs=[SMEM] + [ANY] * 7,
        out_specs=[ANY] * 2,
        out_shape=[jax.ShapeDtypeStruct((e, e), F32), jax.ShapeDtypeStruct((8, e), F32)],
        scratch_shapes=[pltpu.VMEM((2 * half, e), F32), DMA((7,)), DMA((2,))],
        compiler_params=pltpu.CompilerParams(vmem_limit_bytes=VMEM_LIMIT),
        cost_estimate=pl.CostEstimate(flops=(e * e) // COVER, bytes_accessed=e * e * 8, transcendentals=0),
        name="join",
    )(idx, own, *mine, *theirs)


def back_kernel(base, vp, *refs):
    refs = list(refs)
    srcs = [refs.pop(0) for _ in range(7)]
    gain_ref, = [refs.pop(0)]
    extra = refs[:-10]
    dab_ref, pack_ref, pre, norm, rstd, z, m1, m2, du, sem = refs[-10:]
    n, cols = du.shape
    e = z.shape[1]
    col = pl.ds(pl.multiple_of(vp[0] * cols, cols), cols)
    rows = slice(base, base + n)
    pre_h, norm_h, rstd_h, z_h, m1_h, m2_h, du_h = srcs
    loads = [pltpu.make_async_copy(a, b, sem.at[j]) for j, (a, b) in enumerate((
        (pre_h.at[rows, col], pre), (norm_h.at[rows, col], norm), (rstd_h.at[rows, :], rstd), (m1_h.at[rows, :], m1), (m2_h.at[rows, :], m2),
        (du_h, du), (z_h.at[rows, :], z)))]
    for c in loads:
        c.start()
    for c in loads:
        c.wait()
    for j, c in enumerate(range(0, cols, 128)):
        cs = slice(c, c + 128)
        a, d, normed = pre[:, cs], du[:, cs], norm[:, cs]
        cdf = 0.5 * (1.0 + lax.erf(a * (0.5 ** 0.5)))
        dg = rstd[...] * (d * gain_ref[:, cs] - m1[...] - normed * m2[...])
        da = dg * (cdf + a * (jnp.exp(-0.5 * a * a) * 0.3989422804014327))
        dab_ref[:, cs] = da.astype(BF16).astype(F32)
        for j, x in enumerate((da, d * normed, d)):
            pack_ref[e + j:e + j + 1, cs] = jnp.sum(x, axis=0, keepdims=True)
    loss_ref, db_ref = extra
    pack_ref[:e, :] = lax.dot_general(z[...], dab_ref[...].astype(BF16), (((0,), (0,)), ((), ())), preferred_element_type=F32)
    pack_ref[e + 3:e + 4, :] = loss_ref[...]
    pack_ref[e + 4:e + 16, :] = jnp.zeros_like(pack_ref[e + 4:e + 16, :])
    pack_ref[e + 16:, :] = db_ref[...]


def back_pass(base, vp, pre, normed, rstd, z, m1, m2, du, gain, *extra):
    n, cols = du.shape
    e = z.shape[1]
    n_pack = e + 16 + extra[1].shape[0]
    block = lambda *s: pl.BlockSpec(s, lambda i, p: (0,) * len(s))
    gs = pltpu.PrefetchScalarGridSpec(
        num_scalar_prefetch=1,
        grid=(1,),
        in_specs=[ANY] * 7 + [pl.BlockSpec((1, cols), lambda i, p: (0, p[0]))] + [block(*x.shape) for x in extra],
        out_specs=[block(n, cols), block(n_pack, cols)],
        scratch_shapes=[pltpu.VMEM((n, cols), F32)] * 2 + [pltpu.VMEM((n, 128), F32), pltpu.VMEM((n, e), BF16)] + [pltpu.VMEM((n, 128), F32)] * 2
        + [pltpu.VMEM((n, cols), F32), DMA((7,))],
    )
    return pl.pallas_call(
        functools.partial(back_kernel, base),
        grid_spec=gs,
        out_shape=[jax.ShapeDtypeStruct((n, cols), F32), jax.ShapeDtypeStruct((n_pack, cols), F32)],
        compiler_params=pltpu.CompilerParams(dimension_semantics=("arbitrary",), vmem_limit_bytes=VMEM_LIMIT),
        cost_estimate=pl.CostEstimate(flops=(2 * n * e * cols) // COVER, bytes_accessed=n * (cols * 16 + e * 2 + 1536), transcendentals=n * cols * 2),
        name="back",
    )(vp, pre, normed, rstd, z, m1, m2, du, gain, *extra)


def spread_kernel(n_masks, vp, pos_ref, w_ref, *refs):
    pieces, (out_ref, dab, dz, obuf, in_sem, out_sem) = refs[:4], refs[4:]
    n, cols = pieces[0].shape
    col = lambda k: pl.ds(pl.multiple_of((vp[0] ^ k) * cols, cols), cols)
    loads = [pltpu.make_async_copy(p, dab.at[:, col(j)], in_sem.at[j]) for j, p in enumerate(pieces)]
    for c in loads:
        c.start()
    dz[n:, :] = jnp.zeros((dz.shape[0] - n, dz.shape[1]), F32)
    n_seq, seq_len, _ = out_ref.shape
    place = lax.broadcasted_iota(I32, (seq_len, 1), 0)
    slots = pos_ref.shape[2]
    for c in loads:
        c.wait()
    for r0, r1 in row_cuts(n):
        dz[r0:r1, :] = dot(dab[r0:r1, :].astype(BF16), w_ref[...], NT).astype(BF16).astype(F32)
    group = 8
    store = lambda b, j: pltpu.make_async_copy(obuf.at[j % 4], out_ref.at[b], out_sem.at[j % 4])

    @pl.loop(0, n_seq // group)
    def _(g):
        for j in range(group):
            b = g * group + j

            @pl.when(b >= 4)
            def _():
                store(b - 4, j).wait()

            hot = jnp.where(place == pos_ref[b], 1.0, 0.0).astype(BF16)
            base = pl.multiple_of(g * (group * n_masks), 8)
            low = j * n_masks // 8 * 8
            rows = dz[pl.ds(base + low, slots + 8), :][j * n_masks - low:j * n_masks - low + slots]
            obuf[j % 4] = dot(hot, rows.astype(BF16), NN).astype(BF16)
            store(b, j).start()

    for j in range(group - 4, group):
        store(n_seq - group + j, j).wait()


def spread_pass(n_masks, shape, vp, pos, w, pieces):
    n, cols = pieces[0].shape
    e = w.shape[0]
    return pl.pallas_call(
        functools.partial(spread_kernel, n_masks),
        in_specs=[SMEM, VMEM, VMEM] + [ANY] * 4,
        out_specs=ANY,
        out_shape=jax.ShapeDtypeStruct(shape, BF16),
        scratch_shapes=[pltpu.VMEM((n, 4 * cols), F32), pltpu.VMEM((n + 16, e), F32), pltpu.VMEM((4,) + shape[1:], BF16), DMA((4,)), DMA((4,))],
        compiler_params=pltpu.CompilerParams(vmem_limit_bytes=VMEM_LIMIT),
        cost_estimate=pl.CostEstimate(flops=(2 * shape[0] * shape[1] * 128 * e) // COVER, bytes_accessed=shape[0] * shape[1] * e * 2, transcendentals=0),
        name="spread",
    )(vp, pos, w, *pieces)


def order_sum(xs):
    return (xs[0] + xs[1]) + (xs[2] + xs[3])


def after(x, *deps):
    return lax.optimization_barrier((x, deps))[0]


def solution(mesh):
    n_groups, n_shards = mesh.shape["dp"], mesh.shape["vp"]

    def swap(a, bit):
        return lax.ppermute(a, "dp", [(d, d ^ bit) for d in range(n_groups)])

    def swap_vp(a, bit):
        return lax.ppermute(a, "vp", [(d, d ^ bit) for d in range(n_shards)])

    def hop(a):
        return lax.ppermute(a, "dp", [(d, d ^ (Y if d & CORE else X)) for d in range(n_groups)])

    def local_step(hidden, mask_pos, labels, w_trans, b_trans, ln_gain, ln_bias, emb_table, b_vocab):
        n_rows, _, width = hidden.shape
        n_masks = mask_pos.shape[1]
        shard_rows = emb_table.shape[0]
        n_loc = n_rows * n_masks
        n_tokens = n_loc * n_groups
        slots = -(-n_masks // 16) * 16
        cut = n_loc // 32 * 16
        cols = width // n_shards
        dp, vp = lax.axis_index("dp"), lax.axis_index("vp")
        row_start = vp * shard_rows
        scale = 1.0 / n_tokens
        core, mine = dp & 1, (dp >> 1 ^ dp >> 2) & 1

        pos_pad = jnp.pad(mask_pos, ((0, 0), (0, slots - n_masks)), constant_values=-1)
        z, pre, normed, rstd, u, u_lo, u_hi = head_pass(
            n_masks, cut, hidden, jnp.broadcast_to(pos_pad[:, :, None], (n_rows, slots, 128)),
            w_trans, b_trans[None], ln_gain[None], ln_bias[None])

        x_lo, y_hi = swap(u_lo, X), swap(u_hi, Y)
        x_hi, y_lo = swap(u_hi, X), swap(u_lo, Y)
        c_lo, c_hi = swap(u_lo, CORE), swap(u_hi, CORE)

        flat_labels = labels.reshape(n_loc)
        lab_local = flat_labels - row_start
        lab_local = jnp.where((lab_local >= 0) & (lab_local < shard_rows), lab_local, ELSEWHERE)
        column = lambda x: jnp.broadcast_to(x[:, None], (x.shape[0], 128))
        lab_col = column(lab_local)
        logits, stat = stats(u, emb_table, b_vocab[None], lab_col)
        all_stats = [stat] + [swap_vp(stat, b) for b in range(1, n_shards)]
        global_max = functools.reduce(jnp.maximum, [s[0] for s in all_stats])
        log_norm = global_max + jnp.log(order_sum([s[1] * jnp.exp(s[0] - global_max) for s in all_stats]))
        loss_part = jnp.sum(log_norm - order_sum([s[2] for s in all_stats]))
        lse = log_norm + jnp.log(jnp.float32(n_tokens))

        fill = (0, BLK - n_loc)
        info = jnp.stack([jnp.pad(lse, fill, constant_values=jnp.inf), jnp.pad(flat_labels.astype(F32), fill, constant_values=-1.0)])
        near, *away = [swap(info, b) for b in (CORE, X, Y, X | Y)]
        x_lo, y_hi = after((x_lo, y_hi), stat)
        d_lo, d_hi = swap(x_lo, Y), swap(y_hi, X)
        cx_lo, cy_hi = swap(x_lo, CORE), swap(y_hi, CORE)

        du_part, db_part, sums = du_pass(scale, n_shards, 0, logits, emb_table, column(lse), lab_col, normed, ln_gain[None])
        du_share = lax.psum_scatter(du_part.reshape(n_shards * n_loc, cols), "vp", scatter_dimension=0, tiled=True)
        sums = [sums] + [swap_vp(sums, b) for b in range(1, n_shards)]

        half, quarter = shard_rows // 2, shard_rows // 4
        start = lambda h, c: h * half + c * quarter
        pos = jnp.stack([dp, start(mine, core), row_start + start(mine, core), start(mine, 1 - core), start(1 - mine, core), start(1 - mine, 1 - core)])
        bias_col = lax.dynamic_slice(b_vocab, (start(mine, core),), (quarter,))[:, None]
        shares = (1280, 1216, 648)
        ends = [0]
        for w in shares[:-1]:
            ends.append(ends[-1] + max(16, quarter * w // sum(shares) // 16 * 16))
        spans = list(zip(ends, ends[1:] + [quarter]))

        def rows(kind, k, *wait, info=None, span=None, **kw):
            return rows_pass(kind, scale, shard_rows, span or spans[k], cut, after(pos, *wait), emb_table, bias_col, info, **kw)

        def send(k, chunk):
            return ((TWIN, spans[k][0]), swap(chunk, CORE)), hop(chunk)

        def forward(k, far, *wait):
            far = after(far, *wait)
            return ((FAR, spans[k][0]), far), ((FAR_TWIN, spans[k][0]), swap(far, CORE))

        tokens = {0: (u_lo, u_hi), CORE: (c_lo, c_hi), X: (x_lo, x_hi), Y: (y_lo, y_hi)}
        pair = jnp.stack([info, near])
        own, u_all = rows("own", 0, du_part, info=pair, tokens=tokens)
        x_hi, y_lo, away = after((x_hi, y_lo, away), own)
        away = jnp.stack(away)
        tokens[X | CORE] = cx_lo, swap(x_hi, CORE)
        tokens[Y | CORE] = swap(y_lo, CORE), cy_hi
        away_near = swap(away, CORE)
        tokens[X], tokens[Y] = (x_lo, x_hi), (y_lo, y_hi)
        info = jnp.concatenate([pair, jnp.stack([away, away_near], axis=1).reshape(6, 2, BLK)])

        sums = order_sum(after(sums, own)) / width
        m1, m2 = column(sums[0]), column(sums[1])
        side, u_all = rows("side", 0, m2, info=info, tokens=tokens, u_all=u_all)
        d_lo, d_hi = after((d_lo, d_hi), side)
        tokens[X | Y], tokens[X | Y | CORE] = (d_lo, d_hi), (swap(d_lo, CORE), swap(d_hi, CORE))
        chunk0, u_all, big = rows("far", 0, info=info, tokens=tokens, u_all=u_all, parts=((own, 0), (side, 0)))
        twin0, far0 = send(0, chunk0)

        du_share = after(du_share, chunk0)
        loss_row = jnp.pad(loss_part[None, None], ((0, 0), (0, cols - 1)))
        db_rows = -(-shard_rows // cols // 8) * 8
        db_mat = jnp.pad(db_part[0], (0, db_rows * cols - shard_rows)).reshape(db_rows, cols)
        dab, pack = back_pass(0, vp[None], pre, normed, rstd, z, m1, m2, du_share, ln_gain[None], loss_row, db_mat)
        back_done = dab
        pack = lax.psum(pack, "dp")
        dab = [dab] + [swap_vp(dab, b) for b in range(1, n_shards)]

        chunk1, big = rows("whole", 1, back_done, info=info, u_all=u_all, big=big)
        twin1, far1 = send(1, chunk1)
        pack = after(pack, chunk1)
        n_half = (width + 16) // 2
        part = lax.dynamic_slice(pack, (core * n_half, 0), (n_half, cols))
        parts = [swap_vp(part, b) for b in range(1, n_shards)]
        far0, far_twin0 = forward(0, far0, chunk1)

        chunk2, big = rows("whole", 2, part, info=info, u_all=u_all, big=big, puts=[twin0, far0])
        twin2, far2 = send(2, chunk2)
        far1, far_twin1 = forward(1, far1, chunk2)
        d_hidden = spread_pass(n_masks, hidden.shape, vp[None], pos_pad[:, None], w_trans, after(dab, chunk2))
        big = put_rows(after(pos, d_hidden), big, [far_twin0, twin1, far1, twin2, far_twin1])
        far2, far_twin2 = forward(2, far2, big)
        big = put_rows(pos, big, [far2])
        big = put_rows(pos, big, [far_twin2])
        parts = after(parts, far2)
        others = [swap(p, CORE) for p in parts]
        d_w, vec = join_pass(jnp.stack([vp, core]), pack, parts, others)

        db = pack[width + 16:].reshape(-1)[:shard_rows]
        return pack[width + 3, 0] / n_tokens, d_hidden, d_w, vec[0], vec[1], vec[2], big, db

    in_specs = (P("dp", None, None), P("dp", None), P("dp", None), P(None, None), P(None), P(None), P(None), P("vp", None), P("vp"))
    out_specs = (P(), P("dp", None, None), P(None, None), P(None), P(None), P(None), P("vp", None), P("vp"))
    return jax.shard_map(local_step, mesh=mesh, in_specs=in_specs, out_specs=out_specs, check_vma=False)
```

```python
import functools

import jax
import jax.numpy as jnp
from jax import lax
from jax.experimental import pallas as pl
from jax.experimental.pallas import tpu as pltpu
from jax.sharding import PartitionSpec as P


F32, BF16, I32 = jnp.float32, jnp.bfloat16, jnp.int32
NT = (((1,), (1,)), ((), ()))
NN = (((1,), (0,)), ((), ()))
VB = 1024
VMEM_LIMIT = 60 << 20
COVER = 100
PARTS = 4
LEAST = float(jnp.finfo(jnp.float32).min)
ELSEWHERE = -(1 << 20)


def row_cuts(rows, parts=4):
    cuts = [16 * (rows // 16 * k // parts) for k in range(parts)] + [rows]
    return list(zip(cuts[:-1], cuts[1:]))


def dot(a, b, dims):
    return lax.dot_general(a, b, dims, preferred_element_type=F32)


def stats_kernel(n_vocab, u_ref, emb_ref, b_ref, lab_ref, logits_ref, stat_ref, prev, m_sc, s_sc, l_sc):
    i, n_steps = pl.program_id(0), pl.num_programs(0)
    lane = lax.broadcasted_iota(I32, (1, 128), 1)
    cuts = row_cuts(u_ref.shape[0], PARTS)

    @pl.when(i == 0)
    def _():
        m_sc[...] = jnp.full_like(m_sc, LEAST)
        s_sc[...] = jnp.zeros_like(s_sc)
        l_sc[...] = jnp.zeros_like(l_sc)
        prev[...] = jnp.full_like(prev, -jnp.inf)

    def logits_of(r0, r1, c0, wide, width):
        tile = dot(u_ref[r0:r1, :], emb_ref[c0:c0 + wide, :], NT) + b_ref[:, c0:c0 + wide]
        if wide > width:
            tile = jnp.where(lax.broadcasted_iota(I32, (1, wide), 1) < width, tile, -jnp.inf)
        logits_ref[r0:r1, c0:c0 + wide] = tile
        return tile

    def take(r0, r1, read, first, wide):
        for q in range(r0, r1, 16):
            rs = slice(q, q + 16)
            parts = [read(rs, slice(k, k + 128)) for k in range(0, wide, 128)]
            m_old = m_sc[rs, :]
            m_new = functools.reduce(jnp.maximum, parts, m_old)
            s_new = s_sc[rs, :] * jnp.exp(m_old - m_new)
            l_new = l_sc[rs, :]
            lab = lab_ref[rs, :] - first
            for k, part in enumerate(parts):
                s_new += jnp.exp(part - m_new)
                l_new = jnp.where(lab == lane + k * 128, part, l_new)
            m_sc[rs, :], s_sc[rs, :], l_sc[rs, :] = m_new, s_new, l_new

    from_prev = lambda rs, cs: prev[rs, cs]
    from_out = lambda rs, cs: logits_ref[rs, cs]

    def step(second):
        width = VB if second else n_vocab % (2 * VB)
        wide = -(-width // 128) * 128
        for r0, r1 in cuts:
            logits_of(r0, r1, 0, wide, width)
            take(r0, r1, from_prev, (2 * i - 1) * VB, VB)
        for r0, r1 in cuts:
            if second:
                prev[r0:r1, :] = logits_of(r0, r1, VB, VB, VB)
            take(r0, r1, from_out, 2 * i * VB, wide)

    pl.when(i < n_steps - 1)(functools.partial(step, True))
    pl.when(i == n_steps - 1)(functools.partial(step, False))

    @pl.when(i == n_steps - 1)
    def _():
        m_t, s_t, l_t = m_sc[...].T, s_sc[...].T, l_sc[...].T
        m_all = jnp.max(m_t, axis=0, keepdims=True)
        stat_ref[0:1, :] = m_all
        stat_ref[1:2, :] = jnp.sum(s_t * jnp.exp(m_t - m_all), axis=0, keepdims=True)
        stat_ref[2:3, :] = jnp.sum(l_t, axis=0, keepdims=True)
        stat_ref[3:8, :] = jnp.zeros_like(stat_ref[3:8, :])


def stats(u, emb, bias, lab):
    t, e = u.shape
    v = emb.shape[0]
    n = pl.cdiv(v, 2 * VB)
    whole = lambda *s: pl.BlockSpec(s, lambda i: (0,) * len(s))
    return pl.pallas_call(
        functools.partial(stats_kernel, v),
        grid=(n,),
        in_specs=[whole(t, e), pl.BlockSpec((2 * VB, e), lambda i: (i, 0)), pl.BlockSpec((1, 2 * VB), lambda i: (0, i)), whole(t, 128)],
        out_specs=[pl.BlockSpec((t, 2 * VB), lambda i: (0, i)), whole(8, t)],
        out_shape=[jax.ShapeDtypeStruct((t, v), F32), jax.ShapeDtypeStruct((8, t), F32)],
        scratch_shapes=[pltpu.VMEM((t, VB), F32)] + [pltpu.VMEM((t, 128), F32)] * 3,
        compiler_params=pltpu.CompilerParams(dimension_semantics=("arbitrary",), vmem_limit_bytes=VMEM_LIMIT),
        cost_estimate=pl.CostEstimate(flops=(2 * t * v * e) // COVER, bytes_accessed=t * v * 4 + v * e * 2, transcendentals=t * v),
        name="stats",
    )(u, emb, bias, lab)


def du_kernel(n_vocab, scale, base, logits_ref, emb_ref, lse_ref, lab_ref, norm_hbm, gain_ref, out_ref, db_ref, sum_ref, du_ref, g_sc, db_sc, norm_sc, db_sc2, sem):
    i, n_blocks = pl.program_id(0), pl.num_programs(0)
    t = logits_ref.shape[0]
    lane = lax.broadcasted_iota(I32, (1, 128), 1)

    norm_copy = pltpu.make_async_copy(norm_hbm.at[base:base + t, :], norm_sc, sem)

    @pl.when(i == 0)
    def _():
        du_ref[...] = jnp.zeros_like(du_ref)

    @pl.when(i == 2)
    def _():
        norm_copy.start()

    def run(width):
        wide = -(-width // 128) * 128
        emb = emb_ref[:wide, :]
        if wide > width:
            emb = jnp.where(lax.broadcasted_iota(I32, (wide, 1), 0) < width, emb, jnp.zeros_like(emb))
        for r0, r1 in row_cuts(t):
            sums = [None] * (wide // 128)
            for q in range(r0, r1, 16):
                rs = slice(q, q + 16)
                lse = lse_ref[rs, :]
                lab = lab_ref[rs, :] - i * VB
                for k in range(wide // 128):
                    c = k * 128
                    g = jnp.exp(logits_ref[rs, c:c + 128] - lse)
                    g -= jnp.where(lab == lane + c, scale, 0.0)
                    if c + 128 > width:
                        g = jnp.where(lane < width - c, g, 0.0)
                    part = g[:8] + g[8:]
                    sums[k] = part if sums[k] is None else sums[k] + part
                    g_sc[rs, c:c + 128] = g.astype(BF16)
            for k in range(wide // 128):
                cs = slice(k * 128, (k + 1) * 128)
                db_sc[:, cs] = sums[k] if r0 == 0 else db_sc[:, cs] + sums[k]
            du_ref[r0:r1, :] += dot(g_sc[r0:r1, :wide], emb, NN)
        db_ref[:, :wide] = jnp.sum(db_sc[:, :wide], axis=0, keepdims=True)

    tail = n_vocab % VB
    if tail:
        pl.when(i < n_blocks - 1)(functools.partial(run, VB))
        pl.when(i == n_blocks - 1)(functools.partial(run, tail))
    else:
        run(VB)

    @pl.when(i == n_blocks - 1)
    def _():
        norm_copy.wait()
        parts, rows, cols = out_ref.shape
        run = rows // 7
        for r in range(0, rows, run):
            rs = slice(r, r + run)
            total = [jnp.zeros((run, 128), F32)] * 2
            for c in range(0, parts * cols, 128):
                x = du_ref[rs, c:c + 128].astype(BF16).astype(F32)
                out_ref[c // cols, rs, c % cols:c % cols + 128] = x
                dn = x * gain_ref[:, c:c + 128]
                total = [total[0] + dn, total[1] + dn * norm_sc[rs, c:c + 128]]
            for j, x in enumerate(total):
                db_sc2[j, rs, :] = x
        for j in range(2):
            sum_ref[j:j + 1, :] = jnp.sum(db_sc2[j].T, axis=0, keepdims=True)
        sum_ref[2:, :] = jnp.zeros_like(sum_ref[2:, :])


def du_pass(scale, parts, base, logits, emb, lse, lab, normed, gain):
    t, v = logits.shape
    e = emb.shape[1]
    n = pl.cdiv(v, VB)
    whole = lambda *s: pl.BlockSpec(s, lambda i: (0,) * len(s))
    return pl.pallas_call(
        functools.partial(du_kernel, v, scale, base),
        grid=(n,),
        in_specs=[pl.BlockSpec((t, VB), lambda i: (0, i)), pl.BlockSpec((VB, e), lambda i: (i, 0)), whole(t, 128), whole(t, 128), pl.BlockSpec(memory_space=pl.ANY), whole(1, e)],
        out_specs=[whole(parts, t, e // parts), pl.BlockSpec((1, VB), lambda i: (0, i)), whole(8, t)],
        out_shape=[jax.ShapeDtypeStruct((parts, t, e // parts), F32), jax.ShapeDtypeStruct((1, v), F32), jax.ShapeDtypeStruct((8, t), F32)],
        scratch_shapes=[pltpu.VMEM((t, e), F32), pltpu.VMEM((t, VB), BF16), pltpu.VMEM((8, VB), F32), pltpu.VMEM((t, e), F32), pltpu.VMEM((2, t, 128), F32), pltpu.SemaphoreType.DMA],
        compiler_params=pltpu.CompilerParams(dimension_semantics=("arbitrary",), vmem_limit_bytes=VMEM_LIMIT),
        cost_estimate=pl.CostEstimate(flops=(2 * t * v * e) // COVER, bytes_accessed=t * v * 4 + v * e * 2, transcendentals=t * v),
        name="du_pass",
    )(logits, emb, lse, lab, normed, gain)


LN_EPS = 1e-5
CORE, X, Y = 1, 2, 4
ANY = pl.BlockSpec(memory_space=pltpu.HBM)
VMEM = pl.BlockSpec(memory_space=pltpu.VMEM)
SMEM = pl.BlockSpec(memory_space=pltpu.SMEM)
DMA = pltpu.SemaphoreType.DMA


def gelu_norm(a):
    cdf = 0.5 * (1.0 + lax.erf(a * (0.5 ** 0.5)))
    g = a * cdf
    centered = g - jnp.mean(g, axis=1, keepdims=True)
    rstd = lax.rsqrt(jnp.mean(centered * centered, axis=1, keepdims=True) + LN_EPS)
    return cdf, centered * rstd, rstd


def head_kernel(n_masks, cut, hid, pos_ref, w_ref, b_ref, gain_ref, bias_ref, z_out, pre_out, norm_out, rstd_out, u_out, lo_out, hi_out,
                hbuf, zf, zb, pre_v, norm_v, rstd_v, ub, uf, in_sem, out_sem):
    n_seq, seq_len = hid.shape[0], hid.shape[1]
    n_loc = n_seq * n_masks
    loads = [pltpu.make_async_copy(hid.at[b], hbuf.at[b], in_sem.at[b]) for b in range(n_seq)]
    for c in loads:
        c.start()
    lane = lax.broadcasted_iota(I32, (1, 128), 1)
    cuts = [0, cut // 32 * 16, cut, cut + (n_loc - cut) // 32 * 16, n_loc]
    done, stores = 0, []

    def send(src, dst, r0, r1, base=0):
        c = pltpu.make_async_copy(src.at[r0:r1, :], dst.at[r0 - base:r1 - base, :], out_sem.at[len(stores)])
        c.start()
        stores.append(c)

    for b in range(n_seq):
        loads[b].wait()
        hot = jnp.concatenate([jnp.where(pos_ref[b] == lane + j, 1.0, 0.0).astype(BF16) for j in range(0, seq_len, 128)], axis=1)
        zf[b * n_masks:(b + 1) * n_masks, :] = dot(hot, hbuf[b], NN)[:n_masks, :]
        while done < 4 and cuts[done + 1] <= (b + 1) * n_masks:
            r0, r1 = cuts[done], cuts[done + 1]
            z = zf[r0:r1, :].astype(BF16)
            zb[r0:r1, :] = z
            a = dot(z, w_ref[...], NN) + b_ref[...]
            pre_v[r0:r1, :] = a
            _, normed, rstd = gelu_norm(a)
            norm_v[r0:r1, :] = normed
            rstd_v[r0:r1, :] = jnp.broadcast_to(rstd, (r1 - r0, 128))
            u = (normed * gain_ref[...] + bias_ref[...]).astype(BF16)
            ub[r0:r1, :] = u
            uf[r0:r1, :] = u.astype(F32)
            done += 1
            send(uf, hi_out if r0 >= cut else lo_out, r0, r1, cut if r0 >= cut else 0)
            for src, dst in ((ub, u_out), (zb, z_out), (pre_v, pre_out), (norm_v, norm_out), (rstd_v, rstd_out)):
                send(src, dst, r0, r1)
    for c in stores:
        c.wait()


def head_pass(n_masks, cut, hidden, pos, w, b, gain, bias):
    n_seq, seq_len, e = hidden.shape
    n = n_seq * n_masks
    kinds = [((n, e), BF16), ((n, e), F32), ((n, e), F32), ((n, 128), F32), ((n, e), BF16), ((cut, e), F32), ((n - cut, e), F32)]
    return pl.pallas_call(
        functools.partial(head_kernel, n_masks, cut),
        in_specs=[ANY] + [VMEM] * 5,
        out_specs=[ANY] * len(kinds),
        out_shape=[jax.ShapeDtypeStruct(*k) for k in kinds],
        scratch_shapes=[pltpu.VMEM((n_seq, seq_len, e), BF16), pltpu.VMEM((n, e), F32)]
        + [pltpu.VMEM(*k) for k in kinds[:5]] + [pltpu.VMEM((n, e), F32), DMA((n_seq,)), DMA((24,))],
        compiler_params=pltpu.CompilerParams(vmem_limit_bytes=VMEM_LIMIT),
        cost_estimate=pl.CostEstimate(flops=(4 * n * e * e) // COVER, bytes_accessed=hidden.size * 2 + n * e * 20, transcendentals=n * e),
        name="head",
    )(hidden, pos, w, b, gain, bias)


BLK = 1280
LOOPED = ('side',)
STEPS = {"own": 2, "again": 2, "side": 4, "far": 2, "last": 2, "whole": 8}
ME, MINE, MINE_ID, TWIN, FAR, FAR_TWIN = range(6)


def rows_kernel(kind, scale, s0, m, cut, n_loc, sources, skips, spots, has_big, pos, emb_hbm, bias_ref, info_ref, *refs):
    refs = list(refs)
    take = lambda n: [refs.pop(0) for _ in range(n)]
    wide = sources is not None
    if wide:
        src = {r: take(2) for r in sources}
        if kind != "own":
            take(1)
    else:
        u_hbm, = take(1)
    if has_big:
        take(1)
    parts = take(len(skips))
    puts = take(len(spots))
    out_hbm, = take(1)
    if wide:
        u_hbm, = take(1)
    if kind in ("far", "last", "whole"):
        big_ref, = take(1)
    if wide:
        buf, = take(1)
    ring, emb_sc, g_sc, acc, hold, sem, tok_sem, back_sem, in_sem, out_sem = refs
    me = pos[ME]
    chip = lax.div(me, 2)
    n_steps = STEPS[kind]
    along_x, along_y = chip ^ 1, chip ^ 2

    def device(i):
        side = 2 * jnp.where(i < 2, jnp.minimum(along_x, along_y), jnp.maximum(along_x, along_y)) + lax.rem(i, 2)
        far = 2 * (chip ^ 3) + lax.rem(i, 2)
        if kind in ("own", "again"):
            return 2 * chip + i
        return {"side": side, "far": far, "last": far, "whole": i}[kind]

    depth = ring.shape[0]

    def fetch(i):
        slot = lax.rem(i, 2 if wide else depth)
        if not wide:
            pltpu.make_async_copy(u_hbm.at[device(i)], ring.at[slot], tok_sem.at[slot, 0]).start()
            return
        for r, (lo, hi) in src.items():
            @pl.when(device(i) ^ me == r)
            def _():
                pltpu.make_async_copy(lo, buf.at[slot, :cut, :], tok_sem.at[slot, 0]).start()
                pltpu.make_async_copy(hi, buf.at[slot, cut:, :], tok_sem.at[slot, 1]).start()

    row = lambda j, off: pl.multiple_of(pos[j] + off, 8)
    emb_copy = pltpu.make_async_copy(emb_hbm.at[pl.ds(row(MINE, s0), m), :], emb_sc, sem)
    emb_copy.start()
    fetch(0)
    loads, stores = [], []
    for j, (p, (base, off)) in enumerate(zip(puts, spots)):
        n = p.shape[0]
        loads.append(pltpu.make_async_copy(p, hold.at[j, :n, :], in_sem.at[j]))
        stores.append(pltpu.make_async_copy(hold.at[j, :n, :], big_ref.at[pl.ds(row(base, off), n), :], out_sem.at[j]))
    for j, (p, skip) in enumerate(zip(parts, skips)):
        loads.append(pltpu.make_async_copy(p.at[skip:skip + m, :], hold.at[len(puts) + j, :m, :], in_sem.at[len(puts) + j]))
    acc[...] = jnp.zeros_like(acc)
    if wide:
        for k in range(2):
            ring[k, n_loc:, :] = jnp.zeros((BLK - n_loc, ring.shape[2]), BF16)
    emb_copy.wait()
    n_groups = 2 if kind in LOOPED and m % 32 == 0 else 1
    tall = m // n_groups
    n_cuts = max(1, round(tall / 300))
    cuts = [-(-tall * k // (n_cuts * 16)) * 16 for k in range(n_cuts)] + [tall]
    cuts = list(zip(cuts[:-1], cuts[1:]))
    kept = lambda i: pltpu.make_async_copy(ring.at[lax.rem(i, 2)], u_hbm.at[device(i)], back_sem.at[lax.rem(i, 2)])

    @pl.loop(0, n_steps)
    def _(i):
        slot = lax.rem(i, 2 if wide else depth)
        if wide:
            any_lo, any_hi = next(iter(src.values()))
            pltpu.make_async_copy(any_lo, buf.at[slot, :cut, :], tok_sem.at[slot, 0]).wait()
            pltpu.make_async_copy(any_hi, buf.at[slot, cut:, :], tok_sem.at[slot, 1]).wait()

            @pl.when(i >= 2)
            def _():
                kept(i - 2).wait()
        else:
            pltpu.make_async_copy(u_hbm.at[device(i)], ring.at[slot], tok_sem.at[slot, 0]).wait()

        @pl.when(i + 1 < n_steps)
        def _():
            fetch(i + 1)

        @pl.when(i == 0)
        def _():
            for c in loads:
                c.start()

        for j, (a, b) in enumerate(zip(loads, stores)):
            @pl.when(i == min(2 + j, n_steps - 1))
            def _():
                a.wait()
                b.start()

        if wide:
            ring[slot, :n_loc, :] = buf[slot].astype(BF16)
            kept(i).start()
        rel = device(i) ^ me
        lse, lab = info_ref[rel, 0:1, :], info_ref[rel, 1:2, :]

        def group(h):
            def rows(r0, r1):
                return slice(r0, r1) if n_groups == 1 else pl.ds(pl.multiple_of(h * tall + r0, 16), r1 - r0)

            def weights(r0, r1):
                part = dot(emb_sc[rows(r0, r1), :], ring[slot], NT)
                ids = lax.broadcasted_iota(I32, (r1 - r0, 1), 0) + (pos[MINE_ID] + (s0 + h * tall + r0))
                bias = bias_ref[slice(s0 + r0, s0 + r1) if n_groups == 1 else pl.ds(pl.multiple_of(s0 + h * tall + r0, 8), r1 - r0), :]
                g = jnp.exp(part + bias - lse) - jnp.where(lab == ids.astype(F32), scale, 0.0)
                g_sc[r0:r1, :] = g.astype(BF16)

            weights(*cuts[0])
            for k, (r0, r1) in enumerate(cuts):
                if k + 1 < len(cuts):
                    weights(*cuts[k + 1])
                acc[rows(r0, r1), :] += dot(g_sc[r0:r1, :], ring[slot], NN)

        if n_groups == 1:
            group(0)
        else:
            pl.loop(0, n_groups)(group)

    for c in loads[len(puts):]:
        c.wait()
    if parts:
        acc[...] = (hold[len(puts), :m, :] + acc[...]) + hold[len(puts) + 1, :m, :]
    done = [pltpu.make_async_copy(acc, out_hbm, sem)]
    if kind in ("far", "last", "whole"):
        done.append(pltpu.make_async_copy(acc, big_ref.at[pl.ds(row(MINE, s0), m), :], emb_sem(tok_sem)))
    for c in done:
        c.start()
    if wide:
        for i in range(n_steps - 2, n_steps):
            kept(i).wait()
    for c in stores + done:
        c.wait()


def emb_sem(tok_sem):
    return tok_sem.at[0, 0]


def rows_pass(kind, scale, v_rows, span, cut, pos, emb, bias, info, tokens=None, u_all=None, big=None, parts=(), puts=()):
    s0, s1 = span
    m, e = s1 - s0, emb.shape[1]
    sds = jax.ShapeDtypeStruct
    wide = kind in ("own", "side", "far")
    final = kind in ("far", "last", "whole")
    args, aliases = [pos, emb, bias, info], {}
    outs = [sds((m, e), F32)]
    sources = None
    if wide:
        sources = {"own": (0, CORE), "side": (X, X | CORE, Y, Y | CORE), "far": (X | Y, X | Y | CORE)}[kind]
        args += [h for r in sources for h in tokens[r]]
        n_loc = tokens[0][0].shape[0] + tokens[0][1].shape[0]
        outs.append(sds((8, BLK, e), BF16))
        if kind != "own":
            aliases[len(args)] = 1
            args.append(u_all)
    else:
        n_loc = BLK
        args.append(u_all)
    if final:
        if big is not None:
            aliases[len(args)] = len(outs)
            args.append(big)
        outs.append(sds((v_rows, e), F32))
    args += [a for a, _ in parts] + [a for _, a in puts]
    n_hold = max(1, len(parts) + len(puts))
    tallest = max([m] * len(parts) + [a.shape[0] for _, a in puts] + [8])
    t = STEPS[kind] * BLK
    scratch = [pltpu.VMEM((2, n_loc, e), F32)] if wide else []
    scratch += [
        pltpu.VMEM((2 if wide else 3, BLK, e), BF16), pltpu.VMEM((m, e), BF16), pltpu.VMEM((m, BLK), BF16),
        pltpu.VMEM((m, e), F32), pltpu.VMEM((n_hold, tallest, e), F32),
        DMA, DMA((3, 2)), DMA((2,)), DMA((n_hold,)), DMA((n_hold,)),
    ]
    return pl.pallas_call(
        functools.partial(rows_kernel, kind, scale, s0, m, cut, n_loc, sources, [skip for _, skip in parts], [spot for spot, _ in puts], big is not None),
        in_specs=[SMEM, ANY, VMEM, VMEM] + [ANY] * (len(args) - 4),
        out_specs=[ANY] * len(outs),
        out_shape=outs,
        scratch_shapes=scratch,
        input_output_aliases=aliases,
        compiler_params=pltpu.CompilerParams(vmem_limit_bytes=VMEM_LIMIT),
        cost_estimate=pl.CostEstimate(flops=(4 * t * m * e) // COVER, bytes_accessed=t * e * 2 + m * e * 6, transcendentals=t * m),
    )(*args)


def put_kernel(spots, pos, *refs):
    n = len(spots)
    pieces, (out_ref, hold, in_sem, out_sem) = refs[1:1 + n], refs[1 + n:]
    loads, stores = [], []
    for j, (p, (base, off)) in enumerate(zip(pieces, spots)):
        slot = hold.at[j, :p.shape[0], :]
        loads.append(pltpu.make_async_copy(p, slot, in_sem.at[j]))
        stores.append(pltpu.make_async_copy(slot, out_ref.at[pl.ds(pl.multiple_of(pos[base] + off, 8), p.shape[0]), :], out_sem.at[j]))
    for a in loads:
        a.start()
    for a, b in zip(loads, stores):
        a.wait()
        b.start()
    for b in stores:
        b.wait()


def put_rows(pos, big, puts):
    spots, pieces = [s for s, _ in puts], [a for _, a in puts]
    n, e = len(pieces), big.shape[1]
    size = sum(p.size for p in pieces)
    return pl.pallas_call(
        functools.partial(put_kernel, spots),
        in_specs=[SMEM] + [ANY] * (n + 1),
        out_specs=ANY,
        out_shape=jax.ShapeDtypeStruct(big.shape, big.dtype),
        scratch_shapes=[pltpu.VMEM((n, max(p.shape[0] for p in pieces), e), F32), DMA((n,)), DMA((n,))],
        input_output_aliases={1: 0},
        compiler_params=pltpu.CompilerParams(vmem_limit_bytes=VMEM_LIMIT),
        cost_estimate=pl.CostEstimate(flops=(size) // COVER, bytes_accessed=size * 8, transcendentals=0),
        name="put_rows",
    )(pos, big, *pieces)


def join_kernel(n_vec, idx, *refs):
    own, mine, theirs, (dw_ref, vec_ref, full, in_sem, out_sem) = refs[0], refs[1:4], refs[4:7], refs[7:]
    vp, core = idx[0], idx[1]
    half, cols = mine[0].shape
    col = lambda k: pl.ds(pl.multiple_of((vp ^ k) * cols, cols), cols)
    row = lambda c: pl.ds(pl.multiple_of(c * half, 8), half)
    loads = [pltpu.make_async_copy(own.at[:2 * half, :], full.at[:, col(0)], in_sem.at[0])]
    for k in range(3):
        loads.append(pltpu.make_async_copy(mine[k], full.at[row(core), col(k + 1)], in_sem.at[1 + k]))
        loads.append(pltpu.make_async_copy(theirs[k], full.at[row(1 - core), col(k + 1)], in_sem.at[4 + k]))
    for c in loads:
        c.start()
    for c in loads:
        c.wait()
    e = dw_ref.shape[0]
    stores = [pltpu.make_async_copy(full.at[:e, :], dw_ref, out_sem.at[0]), pltpu.make_async_copy(full.at[e:e + n_vec, :], vec_ref, out_sem.at[1])]
    for c in stores:
        c.start()
    for c in stores:
        c.wait()


def join_pass(idx, own, mine, theirs):
    half, cols = mine[0].shape
    e = 4 * cols
    return pl.pallas_call(
        functools.partial(join_kernel, 8),
        in_specs=[SMEM] + [ANY] * 7,
        out_specs=[ANY] * 2,
        out_shape=[jax.ShapeDtypeStruct((e, e), F32), jax.ShapeDtypeStruct((8, e), F32)],
        scratch_shapes=[pltpu.VMEM((2 * half, e), F32), DMA((7,)), DMA((2,))],
        compiler_params=pltpu.CompilerParams(vmem_limit_bytes=VMEM_LIMIT),
        cost_estimate=pl.CostEstimate(flops=(e * e) // COVER, bytes_accessed=e * e * 8, transcendentals=0),
        name="join",
    )(idx, own, *mine, *theirs)


def back_kernel(base, vp, *refs):
    refs = list(refs)
    srcs = [refs.pop(0) for _ in range(7)]
    gain_ref, = [refs.pop(0)]
    extra = refs[:-10]
    dab_ref, pack_ref, pre, norm, rstd, z, m1, m2, du, sem = refs[-10:]
    n, cols = du.shape
    e = z.shape[1]
    col = pl.ds(pl.multiple_of(vp[0] * cols, cols), cols)
    rows = slice(base, base + n)
    pre_h, norm_h, rstd_h, z_h, m1_h, m2_h, du_h = srcs
    loads = [pltpu.make_async_copy(a, b, sem.at[j]) for j, (a, b) in enumerate((
        (pre_h.at[rows, col], pre), (norm_h.at[rows, col], norm), (rstd_h.at[rows, :], rstd), (m1_h.at[rows, :], m1), (m2_h.at[rows, :], m2),
        (du_h, du), (z_h.at[rows, :], z)))]
    for c in loads:
        c.start()
    for c in loads:
        c.wait()
    for j, c in enumerate(range(0, cols, 128)):
        cs = slice(c, c + 128)
        a, d, normed = pre[:, cs], du[:, cs], norm[:, cs]
        cdf = 0.5 * (1.0 + lax.erf(a * (0.5 ** 0.5)))
        dg = rstd[...] * (d * gain_ref[:, cs] - m1[...] - normed * m2[...])
        da = dg * (cdf + a * (jnp.exp(-0.5 * a * a) * 0.3989422804014327))
        dab_ref[:, cs] = da.astype(BF16).astype(F32)
        for j, x in enumerate((da, d * normed, d)):
            pack_ref[e + j:e + j + 1, cs] = jnp.sum(x, axis=0, keepdims=True)
    loss_ref, db_ref = extra
    pack_ref[:e, :] = lax.dot_general(z[...], dab_ref[...].astype(BF16), (((0,), (0,)), ((), ())), preferred_element_type=F32)
    pack_ref[e + 3:e + 4, :] = loss_ref[...]
    pack_ref[e + 4:e + 16, :] = jnp.zeros_like(pack_ref[e + 4:e + 16, :])
    pack_ref[e + 16:, :] = db_ref[...]


def back_pass(base, vp, pre, normed, rstd, z, m1, m2, du, gain, *extra):
    n, cols = du.shape
    e = z.shape[1]
    n_pack = e + 16 + extra[1].shape[0]
    block = lambda *s: pl.BlockSpec(s, lambda i, p: (0,) * len(s))
    gs = pltpu.PrefetchScalarGridSpec(
        num_scalar_prefetch=1,
        grid=(1,),
        in_specs=[ANY] * 7 + [pl.BlockSpec((1, cols), lambda i, p: (0, p[0]))] + [block(*x.shape) for x in extra],
        out_specs=[block(n, cols), block(n_pack, cols)],
        scratch_shapes=[pltpu.VMEM((n, cols), F32)] * 2 + [pltpu.VMEM((n, 128), F32), pltpu.VMEM((n, e), BF16)] + [pltpu.VMEM((n, 128), F32)] * 2
        + [pltpu.VMEM((n, cols), F32), DMA((7,))],
    )
    return pl.pallas_call(
        functools.partial(back_kernel, base),
        grid_spec=gs,
        out_shape=[jax.ShapeDtypeStruct((n, cols), F32), jax.ShapeDtypeStruct((n_pack, cols), F32)],
        compiler_params=pltpu.CompilerParams(dimension_semantics=("arbitrary",), vmem_limit_bytes=VMEM_LIMIT),
        cost_estimate=pl.CostEstimate(flops=(2 * n * e * cols) // COVER, bytes_accessed=n * (cols * 16 + e * 2 + 1536), transcendentals=n * cols * 2),
        name="back",
    )(vp, pre, normed, rstd, z, m1, m2, du, gain, *extra)


def spread_kernel(n_masks, vp, pos_ref, w_ref, *refs):
    pieces, (out_ref, dab, dz, obuf, in_sem, out_sem) = refs[:4], refs[4:]
    n, cols = pieces[0].shape
    col = lambda k: pl.ds(pl.multiple_of((vp[0] ^ k) * cols, cols), cols)
    loads = [pltpu.make_async_copy(p, dab.at[:, col(j)], in_sem.at[j]) for j, p in enumerate(pieces)]
    for c in loads:
        c.start()
    dz[n:, :] = jnp.zeros((dz.shape[0] - n, dz.shape[1]), F32)
    n_seq, seq_len, _ = out_ref.shape
    place = lax.broadcasted_iota(I32, (seq_len, 1), 0)
    slots = pos_ref.shape[2]
    for c in loads:
        c.wait()
    for r0, r1 in row_cuts(n):
        dz[r0:r1, :] = dot(dab[r0:r1, :].astype(BF16), w_ref[...], NT).astype(BF16).astype(F32)
    group = 8
    store = lambda b, j: pltpu.make_async_copy(obuf.at[j % 4], out_ref.at[b], out_sem.at[j % 4])

    @pl.loop(0, n_seq // group)
    def _(g):
        for j in range(group):
            b = g * group + j

            @pl.when(b >= 4)
            def _():
                store(b - 4, j).wait()

            hot = jnp.where(place == pos_ref[b], 1.0, 0.0).astype(BF16)
            base = pl.multiple_of(g * (group * n_masks), 8)
            low = j * n_masks // 8 * 8
            rows = dz[pl.ds(base + low, slots + 8), :][j * n_masks - low:j * n_masks - low + slots]
            obuf[j % 4] = dot(hot, rows.astype(BF16), NN).astype(BF16)
            store(b, j).start()

    for j in range(group - 4, group):
        store(n_seq - group + j, j).wait()


def spread_pass(n_masks, shape, vp, pos, w, pieces):
    n, cols = pieces[0].shape
    e = w.shape[0]
    return pl.pallas_call(
        functools.partial(spread_kernel, n_masks),
        in_specs=[SMEM, VMEM, VMEM] + [ANY] * 4,
        out_specs=ANY,
        out_shape=jax.ShapeDtypeStruct(shape, BF16),
        scratch_shapes=[pltpu.VMEM((n, 4 * cols), F32), pltpu.VMEM((n + 16, e), F32), pltpu.VMEM((4,) + shape[1:], BF16), DMA((4,)), DMA((4,))],
        compiler_params=pltpu.CompilerParams(vmem_limit_bytes=VMEM_LIMIT),
        cost_estimate=pl.CostEstimate(flops=(2 * shape[0] * shape[1] * 128 * e) // COVER, bytes_accessed=shape[0] * shape[1] * e * 2, transcendentals=0),
        name="spread",
    )(vp, pos, w, *pieces)


def order_sum(xs):
    return (xs[0] + xs[1]) + (xs[2] + xs[3])


def after(x, *deps):
    return lax.optimization_barrier((x, deps))[0]


def solution(mesh):
    n_groups, n_shards = mesh.shape["dp"], mesh.shape["vp"]

    def swap(a, bit):
        return lax.ppermute(a, "dp", [(d, d ^ bit) for d in range(n_groups)])

    def swap_vp(a, bit):
        return lax.ppermute(a, "vp", [(d, d ^ bit) for d in range(n_shards)])

    def hop(a):
        return lax.ppermute(a, "dp", [(d, d ^ (Y if d & CORE else X)) for d in range(n_groups)])

    def local_step(hidden, mask_pos, labels, w_trans, b_trans, ln_gain, ln_bias, emb_table, b_vocab):
        n_rows, _, width = hidden.shape
        n_masks = mask_pos.shape[1]
        shard_rows = emb_table.shape[0]
        n_loc = n_rows * n_masks
        n_tokens = n_loc * n_groups
        slots = -(-n_masks // 16) * 16
        cut = n_loc // 32 * 16
        cols = width // n_shards
        dp, vp = lax.axis_index("dp"), lax.axis_index("vp")
        row_start = vp * shard_rows
        scale = 1.0 / n_tokens
        core, mine = dp & 1, (dp >> 1 ^ dp >> 2) & 1

        pos_pad = jnp.pad(mask_pos, ((0, 0), (0, slots - n_masks)), constant_values=-1)
        z, pre, normed, rstd, u, u_lo, u_hi = head_pass(
            n_masks, cut, hidden, jnp.broadcast_to(pos_pad[:, :, None], (n_rows, slots, 128)),
            w_trans, b_trans[None], ln_gain[None], ln_bias[None])

        x_lo, y_hi = swap(u_lo, X), swap(u_hi, Y)
        x_hi, y_lo = swap(u_hi, X), swap(u_lo, Y)
        c_lo, c_hi = swap(u_lo, CORE), swap(u_hi, CORE)

        flat_labels = labels.reshape(n_loc)
        lab_local = flat_labels - row_start
        lab_local = jnp.where((lab_local >= 0) & (lab_local < shard_rows), lab_local, ELSEWHERE)
        column = lambda x: jnp.broadcast_to(x[:, None], (x.shape[0], 128))
        lab_col = column(lab_local)
        logits, stat = stats(u, emb_table, b_vocab[None], lab_col)
        all_stats = [stat] + [swap_vp(stat, b) for b in range(1, n_shards)]
        global_max = functools.reduce(jnp.maximum, [s[0] for s in all_stats])
        log_norm = global_max + jnp.log(order_sum([s[1] * jnp.exp(s[0] - global_max) for s in all_stats]))
        loss_part = jnp.sum(log_norm - order_sum([s[2] for s in all_stats]))
        lse = log_norm + jnp.log(jnp.float32(n_tokens))

        du_part, db_part, sums = du_pass(scale, n_shards, 0, logits, emb_table, column(lse), lab_col, normed, ln_gain[None])
        du_share = lax.psum_scatter(du_part.reshape(n_shards * n_loc, cols), "vp", scatter_dimension=0, tiled=True)
        lse = after(lse, du_part)
        fill = (0, BLK - n_loc)
        info = jnp.stack([jnp.pad(lse, fill, constant_values=jnp.inf), jnp.pad(flat_labels.astype(F32), fill, constant_values=-1.0)])
        near, *away = [swap(info, b) for b in (CORE, X, Y, X | Y)]
        x_lo, y_hi = after((x_lo, y_hi), du_part)
        d_lo, d_hi = swap(x_lo, Y), swap(y_hi, X)
        cx_lo, cy_hi = swap(x_lo, CORE), swap(y_hi, CORE)

        sums = [sums] + [swap_vp(sums, b) for b in range(1, n_shards)]

        half, quarter = shard_rows // 2, shard_rows // 4
        start = lambda h, c: h * half + c * quarter
        pos = jnp.stack([dp, start(mine, core), row_start + start(mine, core), start(mine, 1 - core), start(1 - mine, core), start(1 - mine, 1 - core)])
        bias_col = lax.dynamic_slice(b_vocab, (start(mine, core),), (quarter,))[:, None]
        shares = (1280, 1088, 776)
        ends = [0]
        for w in shares[:-1]:
            ends.append(ends[-1] + max(16, quarter * w // sum(shares) // 16 * 16))
        spans = list(zip(ends, ends[1:] + [quarter]))

        def rows(kind, k, *wait, info=None, span=None, **kw):
            return rows_pass(kind, scale, shard_rows, span or spans[k], cut, after(pos, *wait), emb_table, bias_col, info, **kw)

        def send(k, chunk):
            return ((TWIN, spans[k][0]), swap(chunk, CORE)), hop(chunk)

        def forward(k, far, *wait):
            far = after(far, *wait)
            return ((FAR, spans[k][0]), far), ((FAR_TWIN, spans[k][0]), swap(far, CORE))

        tokens = {0: (u_lo, u_hi), CORE: (c_lo, c_hi), X: (x_lo, x_hi), Y: (y_lo, y_hi)}
        pair = jnp.stack([info, near])
        own, u_all = rows("own", 0, du_part, info=pair, tokens=tokens)
        x_hi, y_lo, away = after((x_hi, y_lo, away), own)
        away = jnp.stack(away)
        tokens[X | CORE] = cx_lo, swap(x_hi, CORE)
        tokens[Y | CORE] = swap(y_lo, CORE), cy_hi
        away_near = swap(away, CORE)
        tokens[X], tokens[Y] = (x_lo, x_hi), (y_lo, y_hi)
        info = jnp.concatenate([pair, jnp.stack([away, away_near], axis=1).reshape(6, 2, BLK)])

        sums = order_sum(after(sums, own)) / width
        m1, m2 = column(sums[0]), column(sums[1])
        side, u_all = rows("side", 0, m2, info=info, tokens=tokens, u_all=u_all)
        d_lo, d_hi = after((d_lo, d_hi), side)
        tokens[X | Y], tokens[X | Y | CORE] = (d_lo, d_hi), (swap(d_lo, CORE), swap(d_hi, CORE))
        du_share = after(du_share, side)
        loss_row = jnp.pad(loss_part[None, None], ((0, 0), (0, cols - 1)))
        db_rows = -(-shard_rows // cols // 8) * 8
        db_mat = jnp.pad(db_part[0], (0, db_rows * cols - shard_rows)).reshape(db_rows, cols)
        dab, pack = back_pass(0, vp[None], pre, normed, rstd, z, m1, m2, du_share, ln_gain[None], loss_row, db_mat)
        back_done = dab
        pack = lax.psum(pack, "dp")
        dab = [dab] + [swap_vp(dab, b) for b in range(1, n_shards)]

        chunk0, u_all, big = rows("far", 0, back_done, info=info, tokens=tokens, u_all=u_all, parts=((own, 0), (side, 0)))
        twin0, far0 = send(0, chunk0)
        chunk1, big = rows("whole", 1, info=info, u_all=u_all, big=big)
        twin1, far1 = send(1, chunk1)
        pack = after(pack, chunk1)
        n_half = (width + 16) // 2
        part = lax.dynamic_slice(pack, (core * n_half, 0), (n_half, cols))
        parts = [swap_vp(part, b) for b in range(1, n_shards)]
        far0, far_twin0 = forward(0, far0, chunk1)

        chunk2, big = rows("whole", 2, part, info=info, u_all=u_all, big=big, puts=[twin0, far0])
        twin2, far2 = send(2, chunk2)
        d_hidden = spread_pass(n_masks, hidden.shape, vp[None], pos_pad[:, None], w_trans, after(dab, chunk2))
        far1, far_twin1 = forward(1, far1, d_hidden)
        big = put_rows(pos, big, [far_twin0, twin1, far1, twin2])
        parts = after(parts, big)
        others = [swap(p, CORE) for p in parts]
        big = put_rows(pos, big, [far_twin1])
        pack, parts, others = after((pack, parts, others), big)
        d_w, vec = join_pass(jnp.stack([vp, core]), pack, parts, others)
        db = pack[width + 16:].reshape(-1)[:shard_rows]
        loss = pack[width + 3, 0] / n_tokens
        grads = vec[0], vec[1], vec[2]
        far2, far_twin2 = forward(2, far2, big, d_w, db, loss, *grads)
        big = put_rows(pos, big, [far2])
        big = put_rows(pos, big, [far_twin2])

        return loss, d_hidden, d_w, *grads, big, db

    in_specs = (P("dp", None, None), P("dp", None), P("dp", None), P(None, None), P(None), P(None), P(None), P("vp", None), P("vp"))
    out_specs = (P(), P("dp", None, None), P(None, None), P(None), P(None), P(None), P("vp", None), P("vp"))
    return jax.shard_map(local_step, mesh=mesh, in_specs=in_specs, out_specs=out_specs, check_vma=False)
```

```python
import functools

import jax
import jax.numpy as jnp
from jax import lax
from jax.experimental import pallas as pl
from jax.experimental.pallas import tpu as pltpu
from jax.sharding import PartitionSpec as P


F32, BF16, I32 = jnp.float32, jnp.bfloat16, jnp.int32
NT = (((1,), (1,)), ((), ()))
NN = (((1,), (0,)), ((), ()))
VB = 1024
VMEM_LIMIT = 60 << 20
COVER = 100
PARTS = 4
LEAST = float(jnp.finfo(jnp.float32).min)
ELSEWHERE = -(1 << 20)


def row_cuts(rows, parts=4):
    cuts = [16 * (rows // 16 * k // parts) for k in range(parts)] + [rows]
    return list(zip(cuts[:-1], cuts[1:]))


def dot(a, b, dims):
    return lax.dot_general(a, b, dims, preferred_element_type=F32)


def stats_kernel(n_vocab, u_ref, emb_ref, b_ref, lab_ref, logits_ref, stat_ref, prev, m_sc, s_sc, l_sc):
    i, n_steps = pl.program_id(0), pl.num_programs(0)
    lane = lax.broadcasted_iota(I32, (1, 128), 1)
    cuts = row_cuts(u_ref.shape[0], PARTS)

    @pl.when(i == 0)
    def _():
        m_sc[...] = jnp.full_like(m_sc, LEAST)
        s_sc[...] = jnp.zeros_like(s_sc)
        l_sc[...] = jnp.zeros_like(l_sc)
        prev[...] = jnp.full_like(prev, -jnp.inf)

    def logits_of(r0, r1, c0, wide, width):
        tile = dot(u_ref[r0:r1, :], emb_ref[c0:c0 + wide, :], NT) + b_ref[:, c0:c0 + wide]
        if wide > width:
            tile = jnp.where(lax.broadcasted_iota(I32, (1, wide), 1) < width, tile, -jnp.inf)
        logits_ref[r0:r1, c0:c0 + wide] = tile
        return tile

    def take(r0, r1, read, first, wide):
        for q in range(r0, r1, 16):
            rs = slice(q, q + 16)
            parts = [read(rs, slice(k, k + 128)) for k in range(0, wide, 128)]
            m_old = m_sc[rs, :]
            m_new = functools.reduce(jnp.maximum, parts, m_old)
            s_new = s_sc[rs, :] * jnp.exp(m_old - m_new)
            l_new = l_sc[rs, :]
            lab = lab_ref[rs, :] - first
            for k, part in enumerate(parts):
                s_new += jnp.exp(part - m_new)
                l_new = jnp.where(lab == lane + k * 128, part, l_new)
            m_sc[rs, :], s_sc[rs, :], l_sc[rs, :] = m_new, s_new, l_new

    from_prev = lambda rs, cs: prev[rs, cs]
    from_out = lambda rs, cs: logits_ref[rs, cs]

    def step(second):
        width = VB if second else n_vocab % (2 * VB)
        wide = -(-width // 128) * 128
        for r0, r1 in cuts:
            logits_of(r0, r1, 0, wide, width)
            take(r0, r1, from_prev, (2 * i - 1) * VB, VB)
        for r0, r1 in cuts:
            if second:
                prev[r0:r1, :] = logits_of(r0, r1, VB, VB, VB)
            take(r0, r1, from_out, 2 * i * VB, wide)

    pl.when(i < n_steps - 1)(functools.partial(step, True))
    pl.when(i == n_steps - 1)(functools.partial(step, False))

    @pl.when(i == n_steps - 1)
    def _():
        m_t, s_t, l_t = m_sc[...].T, s_sc[...].T, l_sc[...].T
        m_all = jnp.max(m_t, axis=0, keepdims=True)
        stat_ref[0:1, :] = m_all
        stat_ref[1:2, :] = jnp.sum(s_t * jnp.exp(m_t - m_all), axis=0, keepdims=True)
        stat_ref[2:3, :] = jnp.sum(l_t, axis=0, keepdims=True)
        stat_ref[3:8, :] = jnp.zeros_like(stat_ref[3:8, :])


def stats(u, emb, bias, lab):
    t, e = u.shape
    v = emb.shape[0]
    n = pl.cdiv(v, 2 * VB)
    whole = lambda *s: pl.BlockSpec(s, lambda i: (0,) * len(s))
    return pl.pallas_call(
        functools.partial(stats_kernel, v),
        grid=(n,),
        in_specs=[whole(t, e), pl.BlockSpec((2 * VB, e), lambda i: (i, 0)), pl.BlockSpec((1, 2 * VB), lambda i: (0, i)), whole(t, 128)],
        out_specs=[pl.BlockSpec((t, 2 * VB), lambda i: (0, i)), whole(8, t)],
        out_shape=[jax.ShapeDtypeStruct((t, v), F32), jax.ShapeDtypeStruct((8, t), F32)],
        scratch_shapes=[pltpu.VMEM((t, VB), F32)] + [pltpu.VMEM((t, 128), F32)] * 3,
        compiler_params=pltpu.CompilerParams(dimension_semantics=("arbitrary",), vmem_limit_bytes=VMEM_LIMIT),
        cost_estimate=pl.CostEstimate(flops=(2 * t * v * e) // COVER, bytes_accessed=t * v * 4 + v * e * 2, transcendentals=t * v),
        name="stats",
    )(u, emb, bias, lab)


def du_kernel(n_vocab, scale, base, logits_ref, emb_ref, lse_ref, lab_ref, norm_hbm, gain_ref, out_ref, db_ref, sum_ref, du_ref, g_sc, db_sc, norm_sc, db_sc2, sem):
    i, n_blocks = pl.program_id(0), pl.num_programs(0)
    t = logits_ref.shape[0]
    lane = lax.broadcasted_iota(I32, (1, 128), 1)

    norm_copy = pltpu.make_async_copy(norm_hbm.at[base:base + t, :], norm_sc, sem)

    @pl.when(i == 0)
    def _():
        du_ref[...] = jnp.zeros_like(du_ref)

    @pl.when(i == 2)
    def _():
        norm_copy.start()

    def run(width):
        wide = -(-width // 128) * 128
        emb = emb_ref[:wide, :]
        if wide > width:
            emb = jnp.where(lax.broadcasted_iota(I32, (wide, 1), 0) < width, emb, jnp.zeros_like(emb))
        for r0, r1 in row_cuts(t):
            sums = [None] * (wide // 128)
            for q in range(r0, r1, 16):
                rs = slice(q, q + 16)
                lse = lse_ref[rs, :]
                lab = lab_ref[rs, :] - i * VB
                for k in range(wide // 128):
                    c = k * 128
                    g = jnp.exp(logits_ref[rs, c:c + 128] - lse)
                    g -= jnp.where(lab == lane + c, scale, 0.0)
                    if c + 128 > width:
                        g = jnp.where(lane < width - c, g, 0.0)
                    part = g[:8] + g[8:]
                    sums[k] = part if sums[k] is None else sums[k] + part
                    g_sc[rs, c:c + 128] = g.astype(BF16)
            for k in range(wide // 128):
                cs = slice(k * 128, (k + 1) * 128)
                db_sc[:, cs] = sums[k] if r0 == 0 else db_sc[:, cs] + sums[k]
            du_ref[r0:r1, :] += dot(g_sc[r0:r1, :wide], emb, NN)
        db_ref[:, :wide] = jnp.sum(db_sc[:, :wide], axis=0, keepdims=True)

    tail = n_vocab % VB
    if tail:
        pl.when(i < n_blocks - 1)(functools.partial(run, VB))
        pl.when(i == n_blocks - 1)(functools.partial(run, tail))
    else:
        run(VB)

    @pl.when(i == n_blocks - 1)
    def _():
        norm_copy.wait()
        parts, rows, cols = out_ref.shape
        run = rows // 7
        for r in range(0, rows, run):
            rs = slice(r, r + run)
            total = [jnp.zeros((run, 128), F32)] * 2
            for c in range(0, parts * cols, 128):
                x = du_ref[rs, c:c + 128].astype(BF16).astype(F32)
                out_ref[c // cols, rs, c % cols:c % cols + 128] = x
                dn = x * gain_ref[:, c:c + 128]
                total = [total[0] + dn, total[1] + dn * norm_sc[rs, c:c + 128]]
            for j, x in enumerate(total):
                db_sc2[j, rs, :] = x
        for j in range(2):
            sum_ref[j:j + 1, :] = jnp.sum(db_sc2[j].T, axis=0, keepdims=True)
        sum_ref[2:, :] = jnp.zeros_like(sum_ref[2:, :])


def du_pass(scale, parts, base, logits, emb, lse, lab, normed, gain):
    t, v = logits.shape
    e = emb.shape[1]
    n = pl.cdiv(v, VB)
    whole = lambda *s: pl.BlockSpec(s, lambda i: (0,) * len(s))
    return pl.pallas_call(
        functools.partial(du_kernel, v, scale, base),
        grid=(n,),
        in_specs=[pl.BlockSpec((t, VB), lambda i: (0, i)), pl.BlockSpec((VB, e), lambda i: (i, 0)), whole(t, 128), whole(t, 128), pl.BlockSpec(memory_space=pl.ANY), whole(1, e)],
        out_specs=[whole(parts, t, e // parts), pl.BlockSpec((1, VB), lambda i: (0, i)), whole(8, t)],
        out_shape=[jax.ShapeDtypeStruct((parts, t, e // parts), F32), jax.ShapeDtypeStruct((1, v), F32), jax.ShapeDtypeStruct((8, t), F32)],
        scratch_shapes=[pltpu.VMEM((t, e), F32), pltpu.VMEM((t, VB), BF16), pltpu.VMEM((8, VB), F32), pltpu.VMEM((t, e), F32), pltpu.VMEM((2, t, 128), F32), pltpu.SemaphoreType.DMA],
        compiler_params=pltpu.CompilerParams(dimension_semantics=("arbitrary",), vmem_limit_bytes=VMEM_LIMIT),
        cost_estimate=pl.CostEstimate(flops=(2 * t * v * e) // COVER, bytes_accessed=t * v * 4 + v * e * 2, transcendentals=t * v),
        name="du_pass",
    )(logits, emb, lse, lab, normed, gain)


LN_EPS = 1e-5
CORE, X, Y = 1, 2, 4
ANY = pl.BlockSpec(memory_space=pltpu.HBM)
VMEM = pl.BlockSpec(memory_space=pltpu.VMEM)
SMEM = pl.BlockSpec(memory_space=pltpu.SMEM)
DMA = pltpu.SemaphoreType.DMA


def gelu_norm(a):
    cdf = 0.5 * (1.0 + lax.erf(a * (0.5 ** 0.5)))
    g = a * cdf
    centered = g - jnp.mean(g, axis=1, keepdims=True)
    rstd = lax.rsqrt(jnp.mean(centered * centered, axis=1, keepdims=True) + LN_EPS)
    return cdf, centered * rstd, rstd


def head_kernel(n_masks, cut, hid, pos_ref, w_ref, b_ref, gain_ref, bias_ref, z_out, pre_out, norm_out, rstd_out, u_out, lo_out, hi_out,
                hbuf, zf, zb, pre_v, norm_v, rstd_v, ub, uf, in_sem, out_sem):
    n_seq, seq_len = hid.shape[0], hid.shape[1]
    n_loc = n_seq * n_masks
    loads = [pltpu.make_async_copy(hid.at[b], hbuf.at[b], in_sem.at[b]) for b in range(n_seq)]
    for c in loads:
        c.start()
    lane = lax.broadcasted_iota(I32, (1, 128), 1)
    cuts = [0, cut // 32 * 16, cut, cut + (n_loc - cut) // 32 * 16, n_loc]
    done, stores = 0, []

    def send(src, dst, r0, r1, base=0):
        c = pltpu.make_async_copy(src.at[r0:r1, :], dst.at[r0 - base:r1 - base, :], out_sem.at[len(stores)])
        c.start()
        stores.append(c)

    for b in range(n_seq):
        loads[b].wait()
        hot = jnp.concatenate([jnp.where(pos_ref[b] == lane + j, 1.0, 0.0).astype(BF16) for j in range(0, seq_len, 128)], axis=1)
        zf[b * n_masks:(b + 1) * n_masks, :] = dot(hot, hbuf[b], NN)[:n_masks, :]
        while done < 4 and cuts[done + 1] <= (b + 1) * n_masks:
            r0, r1 = cuts[done], cuts[done + 1]
            z = zf[r0:r1, :].astype(BF16)
            zb[r0:r1, :] = z
            a = dot(z, w_ref[...], NN) + b_ref[...]
            pre_v[r0:r1, :] = a
            _, normed, rstd = gelu_norm(a)
            norm_v[r0:r1, :] = normed
            rstd_v[r0:r1, :] = jnp.broadcast_to(rstd, (r1 - r0, 128))
            u = (normed * gain_ref[...] + bias_ref[...]).astype(BF16)
            ub[r0:r1, :] = u
            uf[r0:r1, :] = u.astype(F32)
            done += 1
            send(uf, hi_out if r0 >= cut else lo_out, r0, r1, cut if r0 >= cut else 0)
            for src, dst in ((ub, u_out), (zb, z_out), (pre_v, pre_out), (norm_v, norm_out), (rstd_v, rstd_out)):
                send(src, dst, r0, r1)
    for c in stores:
        c.wait()


def head_pass(n_masks, cut, hidden, pos, w, b, gain, bias):
    n_seq, seq_len, e = hidden.shape
    n = n_seq * n_masks
    kinds = [((n, e), BF16), ((n, e), F32), ((n, e), F32), ((n, 128), F32), ((n, e), BF16), ((cut, e), F32), ((n - cut, e), F32)]
    return pl.pallas_call(
        functools.partial(head_kernel, n_masks, cut),
        in_specs=[ANY] + [VMEM] * 5,
        out_specs=[ANY] * len(kinds),
        out_shape=[jax.ShapeDtypeStruct(*k) for k in kinds],
        scratch_shapes=[pltpu.VMEM((n_seq, seq_len, e), BF16), pltpu.VMEM((n, e), F32)]
        + [pltpu.VMEM(*k) for k in kinds[:5]] + [pltpu.VMEM((n, e), F32), DMA((n_seq,)), DMA((24,))],
        compiler_params=pltpu.CompilerParams(vmem_limit_bytes=VMEM_LIMIT),
        cost_estimate=pl.CostEstimate(flops=(4 * n * e * e) // COVER, bytes_accessed=hidden.size * 2 + n * e * 20, transcendentals=n * e),
        name="head",
    )(hidden, pos, w, b, gain, bias)


BLK = 1280
LOOPED = ('side',)
STEPS = {"own": 2, "again": 2, "side": 4, "far": 2, "last": 2, "whole": 8}
ME, MINE, MINE_ID, TWIN, FAR, FAR_TWIN = range(6)


def rows_kernel(kind, scale, s0, m, cut, n_loc, sources, skips, spots, has_big, pos, emb_hbm, bias_ref, info_ref, *refs):
    refs = list(refs)
    take = lambda n: [refs.pop(0) for _ in range(n)]
    wide = sources is not None
    if wide:
        src = {r: take(2) for r in sources}
        if kind != "own":
            take(1)
    else:
        u_hbm, = take(1)
    if has_big:
        take(1)
    parts = take(len(skips))
    puts = take(len(spots))
    out_hbm, = take(1)
    if wide:
        u_hbm, = take(1)
    if kind in ("far", "last", "whole"):
        big_ref, = take(1)
    if wide:
        buf, = take(1)
    ring, emb_sc, g_sc, acc, hold, sem, tok_sem, back_sem, in_sem, out_sem = refs
    me = pos[ME]
    chip = lax.div(me, 2)
    n_steps = STEPS[kind]
    along_x, along_y = chip ^ 1, chip ^ 2

    def device(i):
        side = 2 * jnp.where(i < 2, jnp.minimum(along_x, along_y), jnp.maximum(along_x, along_y)) + lax.rem(i, 2)
        far = 2 * (chip ^ 3) + lax.rem(i, 2)
        if kind in ("own", "again"):
            return 2 * chip + i
        return {"side": side, "far": far, "last": far, "whole": i}[kind]

    depth = ring.shape[0]

    def fetch(i):
        slot = lax.rem(i, 2 if wide else depth)
        if not wide:
            pltpu.make_async_copy(u_hbm.at[device(i)], ring.at[slot], tok_sem.at[slot, 0]).start()
            return
        for r, (lo, hi) in src.items():
            @pl.when(device(i) ^ me == r)
            def _():
                pltpu.make_async_copy(lo, buf.at[slot, :cut, :], tok_sem.at[slot, 0]).start()
                pltpu.make_async_copy(hi, buf.at[slot, cut:, :], tok_sem.at[slot, 1]).start()

    row = lambda j, off: pl.multiple_of(pos[j] + off, 8)
    emb_copy = pltpu.make_async_copy(emb_hbm.at[pl.ds(row(MINE, s0), m), :], emb_sc, sem)
    emb_copy.start()
    fetch(0)
    loads, stores = [], []
    for j, (p, (base, off)) in enumerate(zip(puts, spots)):
        n = p.shape[0]
        loads.append(pltpu.make_async_copy(p, hold.at[j, :n, :], in_sem.at[j]))
        stores.append(pltpu.make_async_copy(hold.at[j, :n, :], big_ref.at[pl.ds(row(base, off), n), :], out_sem.at[j]))
    for j, (p, skip) in enumerate(zip(parts, skips)):
        loads.append(pltpu.make_async_copy(p.at[skip:skip + m, :], hold.at[len(puts) + j, :m, :], in_sem.at[len(puts) + j]))
    acc[...] = jnp.zeros_like(acc)
    if wide:
        for k in range(2):
            ring[k, n_loc:, :] = jnp.zeros((BLK - n_loc, ring.shape[2]), BF16)
    emb_copy.wait()
    n_groups = 2 if kind in LOOPED and m % 32 == 0 else 1
    tall = m // n_groups
    n_cuts = max(1, round(tall / 300))
    cuts = [-(-tall * k // (n_cuts * 16)) * 16 for k in range(n_cuts)] + [tall]
    cuts = list(zip(cuts[:-1], cuts[1:]))
    kept = lambda i: pltpu.make_async_copy(ring.at[lax.rem(i, 2)], u_hbm.at[device(i)], back_sem.at[lax.rem(i, 2)])

    @pl.loop(0, n_steps)
    def _(i):
        slot = lax.rem(i, 2 if wide else depth)
        if wide:
            any_lo, any_hi = next(iter(src.values()))
            pltpu.make_async_copy(any_lo, buf.at[slot, :cut, :], tok_sem.at[slot, 0]).wait()
            pltpu.make_async_copy(any_hi, buf.at[slot, cut:, :], tok_sem.at[slot, 1]).wait()

            @pl.when(i >= 2)
            def _():
                kept(i - 2).wait()
        else:
            pltpu.make_async_copy(u_hbm.at[device(i)], ring.at[slot], tok_sem.at[slot, 0]).wait()

        @pl.when(i + 1 < n_steps)
        def _():
            fetch(i + 1)

        @pl.when(i == 0)
        def _():
            for c in loads:
                c.start()

        for j, (a, b) in enumerate(zip(loads, stores)):
            @pl.when(i == min(2 + j, n_steps - 1))
            def _():
                a.wait()
                b.start()

        if wide:
            ring[slot, :n_loc, :] = buf[slot].astype(BF16)
            kept(i).start()
        rel = device(i) ^ me
        lse, lab = info_ref[rel, 0:1, :], info_ref[rel, 1:2, :]

        def group(h):
            def rows(r0, r1):
                return slice(r0, r1) if n_groups == 1 else pl.ds(pl.multiple_of(h * tall + r0, 16), r1 - r0)

            def weights(r0, r1):
                part = dot(emb_sc[rows(r0, r1), :], ring[slot], NT)
                ids = lax.broadcasted_iota(I32, (r1 - r0, 1), 0) + (pos[MINE_ID] + (s0 + h * tall + r0))
                bias = bias_ref[slice(s0 + r0, s0 + r1) if n_groups == 1 else pl.ds(pl.multiple_of(s0 + h * tall + r0, 8), r1 - r0), :]
                g = jnp.exp(part + bias - lse) - jnp.where(lab == ids.astype(F32), scale, 0.0)
                g_sc[r0:r1, :] = g.astype(BF16)

            weights(*cuts[0])
            for k, (r0, r1) in enumerate(cuts):
                if k + 1 < len(cuts):
                    weights(*cuts[k + 1])
                acc[rows(r0, r1), :] += dot(g_sc[r0:r1, :], ring[slot], NN)

        if n_groups == 1:
            group(0)
        else:
            pl.loop(0, n_groups)(group)

    for c in loads[len(puts):]:
        c.wait()
    if parts:
        acc[...] = (hold[len(puts), :m, :] + acc[...]) + hold[len(puts) + 1, :m, :]
    done = [pltpu.make_async_copy(acc, out_hbm, sem)]
    if kind in ("far", "last", "whole"):
        done.append(pltpu.make_async_copy(acc, big_ref.at[pl.ds(row(MINE, s0), m), :], emb_sem(tok_sem)))
    for c in done:
        c.start()
    if wide:
        for i in range(n_steps - 2, n_steps):
            kept(i).wait()
    for c in stores + done:
        c.wait()


def emb_sem(tok_sem):
    return tok_sem.at[0, 0]


def rows_pass(kind, scale, v_rows, span, cut, pos, emb, bias, info, tokens=None, u_all=None, big=None, parts=(), puts=()):
    s0, s1 = span
    m, e = s1 - s0, emb.shape[1]
    sds = jax.ShapeDtypeStruct
    wide = kind in ("own", "side", "far")
    final = kind in ("far", "last", "whole")
    args, aliases = [pos, emb, bias, info], {}
    outs = [sds((m, e), F32)]
    sources = None
    if wide:
        sources = {"own": (0, CORE), "side": (X, X | CORE, Y, Y | CORE), "far": (X | Y, X | Y | CORE)}[kind]
        args += [h for r in sources for h in tokens[r]]
        n_loc = tokens[0][0].shape[0] + tokens[0][1].shape[0]
        outs.append(sds((8, BLK, e), BF16))
        if kind != "own":
            aliases[len(args)] = 1
            args.append(u_all)
    else:
        n_loc = BLK
        args.append(u_all)
    if final:
        if big is not None:
            aliases[len(args)] = len(outs)
            args.append(big)
        outs.append(sds((v_rows, e), F32))
    args += [a for a, _ in parts] + [a for _, a in puts]
    n_hold = max(1, len(parts) + len(puts))
    tallest = max([m] * len(parts) + [a.shape[0] for _, a in puts] + [8])
    t = STEPS[kind] * BLK
    scratch = [pltpu.VMEM((2, n_loc, e), F32)] if wide else []
    scratch += [
        pltpu.VMEM((2 if wide else 3, BLK, e), BF16), pltpu.VMEM((m, e), BF16), pltpu.VMEM((m, BLK), BF16),
        pltpu.VMEM((m, e), F32), pltpu.VMEM((n_hold, tallest, e), F32),
        DMA, DMA((3, 2)), DMA((2,)), DMA((n_hold,)), DMA((n_hold,)),
    ]
    return pl.pallas_call(
        functools.partial(rows_kernel, kind, scale, s0, m, cut, n_loc, sources, [skip for _, skip in parts], [spot for spot, _ in puts], big is not None),
        in_specs=[SMEM, ANY, VMEM, VMEM] + [ANY] * (len(args) - 4),
        out_specs=[ANY] * len(outs),
        out_shape=outs,
        scratch_shapes=scratch,
        input_output_aliases=aliases,
        compiler_params=pltpu.CompilerParams(vmem_limit_bytes=VMEM_LIMIT),
        cost_estimate=pl.CostEstimate(flops=(4 * t * m * e) // COVER, bytes_accessed=t * e * 2 + m * e * 6, transcendentals=t * m),
    )(*args)


def put_kernel(spots, pos, *refs):
    n = len(spots)
    pieces, (out_ref, hold, in_sem, out_sem) = refs[1:1 + n], refs[1 + n:]
    loads, stores = [], []
    for j, (p, (base, off)) in enumerate(zip(pieces, spots)):
        slot = hold.at[j, :p.shape[0], :]
        loads.append(pltpu.make_async_copy(p, slot, in_sem.at[j]))
        stores.append(pltpu.make_async_copy(slot, out_ref.at[pl.ds(pl.multiple_of(pos[base] + off, 8), p.shape[0]), :], out_sem.at[j]))
    for a in loads:
        a.start()
    for a, b in zip(loads, stores):
        a.wait()
        b.start()
    for b in stores:
        b.wait()


def put_rows(pos, big, puts):
    spots, pieces = [s for s, _ in puts], [a for _, a in puts]
    n, e = len(pieces), big.shape[1]
    size = sum(p.size for p in pieces)
    return pl.pallas_call(
        functools.partial(put_kernel, spots),
        in_specs=[SMEM] + [ANY] * (n + 1),
        out_specs=ANY,
        out_shape=jax.ShapeDtypeStruct(big.shape, big.dtype),
        scratch_shapes=[pltpu.VMEM((n, max(p.shape[0] for p in pieces), e), F32), DMA((n,)), DMA((n,))],
        input_output_aliases={1: 0},
        compiler_params=pltpu.CompilerParams(vmem_limit_bytes=VMEM_LIMIT),
        cost_estimate=pl.CostEstimate(flops=(size) // COVER, bytes_accessed=size * 8, transcendentals=0),
        name="put_rows",
    )(pos, big, *pieces)


def join_kernel(n_vec, idx, *refs):
    own, mine, theirs, (dw_ref, vec_ref, full, in_sem, out_sem) = refs[0], refs[1:4], refs[4:7], refs[7:]
    vp, core = idx[0], idx[1]
    half, cols = mine[0].shape
    col = lambda k: pl.ds(pl.multiple_of((vp ^ k) * cols, cols), cols)
    row = lambda c: pl.ds(pl.multiple_of(c * half, 8), half)
    loads = [pltpu.make_async_copy(own.at[:2 * half, :], full.at[:, col(0)], in_sem.at[0])]
    for k in range(3):
        loads.append(pltpu.make_async_copy(mine[k], full.at[row(core), col(k + 1)], in_sem.at[1 + k]))
        loads.append(pltpu.make_async_copy(theirs[k], full.at[row(1 - core), col(k + 1)], in_sem.at[4 + k]))
    for c in loads:
        c.start()
    for c in loads:
        c.wait()
    e = dw_ref.shape[0]
    stores = [pltpu.make_async_copy(full.at[:e, :], dw_ref, out_sem.at[0]), pltpu.make_async_copy(full.at[e:e + n_vec, :], vec_ref, out_sem.at[1])]
    for c in stores:
        c.start()
    for c in stores:
        c.wait()


def join_pass(idx, own, mine, theirs):
    half, cols = mine[0].shape
    e = 4 * cols
    return pl.pallas_call(
        functools.partial(join_kernel, 8),
        in_specs=[SMEM] + [ANY] * 7,
        out_specs=[ANY] * 2,
        out_shape=[jax.ShapeDtypeStruct((e, e), F32), jax.ShapeDtypeStruct((8, e), F32)],
        scratch_shapes=[pltpu.VMEM((2 * half, e), F32), DMA((7,)), DMA((2,))],
        compiler_params=pltpu.CompilerParams(vmem_limit_bytes=VMEM_LIMIT),
        cost_estimate=pl.CostEstimate(flops=(e * e) // COVER, bytes_accessed=e * e * 8, transcendentals=0),
        name="join",
    )(idx, own, *mine, *theirs)


def back_kernel(base, vp, *refs):
    refs = list(refs)
    srcs = [refs.pop(0) for _ in range(7)]
    gain_ref, = [refs.pop(0)]
    extra = refs[:-10]
    dab_ref, pack_ref, pre, norm, rstd, z, m1, m2, du, sem = refs[-10:]
    n, cols = du.shape
    e = z.shape[1]
    col = pl.ds(pl.multiple_of(vp[0] * cols, cols), cols)
    rows = slice(base, base + n)
    pre_h, norm_h, rstd_h, z_h, m1_h, m2_h, du_h = srcs
    loads = [pltpu.make_async_copy(a, b, sem.at[j]) for j, (a, b) in enumerate((
        (pre_h.at[rows, col], pre), (norm_h.at[rows, col], norm), (rstd_h.at[rows, :], rstd), (m1_h.at[rows, :], m1), (m2_h.at[rows, :], m2),
        (du_h, du), (z_h.at[rows, :], z)))]
    for c in loads:
        c.start()
    for c in loads:
        c.wait()
    for j, c in enumerate(range(0, cols, 128)):
        cs = slice(c, c + 128)
        a, d, normed = pre[:, cs], du[:, cs], norm[:, cs]
        cdf = 0.5 * (1.0 + lax.erf(a * (0.5 ** 0.5)))
        dg = rstd[...] * (d * gain_ref[:, cs] - m1[...] - normed * m2[...])
        da = dg * (cdf + a * (jnp.exp(-0.5 * a * a) * 0.3989422804014327))
        dab_ref[:, cs] = da.astype(BF16).astype(F32)
        for j, x in enumerate((da, d * normed, d)):
            pack_ref[e + j:e + j + 1, cs] = jnp.sum(x, axis=0, keepdims=True)
    loss_ref, db_ref = extra
    pack_ref[:e, :] = lax.dot_general(z[...], dab_ref[...].astype(BF16), (((0,), (0,)), ((), ())), preferred_element_type=F32)
    pack_ref[e + 3:e + 4, :] = loss_ref[...]
    pack_ref[e + 4:e + 16, :] = jnp.zeros_like(pack_ref[e + 4:e + 16, :])
    pack_ref[e + 16:, :] = db_ref[...]


def back_pass(base, vp, pre, normed, rstd, z, m1, m2, du, gain, *extra):
    n, cols = du.shape
    e = z.shape[1]
    n_pack = e + 16 + extra[1].shape[0]
    block = lambda *s: pl.BlockSpec(s, lambda i, p: (0,) * len(s))
    gs = pltpu.PrefetchScalarGridSpec(
        num_scalar_prefetch=1,
        grid=(1,),
        in_specs=[ANY] * 7 + [pl.BlockSpec((1, cols), lambda i, p: (0, p[0]))] + [block(*x.shape) for x in extra],
        out_specs=[block(n, cols), block(n_pack, cols)],
        scratch_shapes=[pltpu.VMEM((n, cols), F32)] * 2 + [pltpu.VMEM((n, 128), F32), pltpu.VMEM((n, e), BF16)] + [pltpu.VMEM((n, 128), F32)] * 2
        + [pltpu.VMEM((n, cols), F32), DMA((7,))],
    )
    return pl.pallas_call(
        functools.partial(back_kernel, base),
        grid_spec=gs,
        out_shape=[jax.ShapeDtypeStruct((n, cols), F32), jax.ShapeDtypeStruct((n_pack, cols), F32)],
        compiler_params=pltpu.CompilerParams(dimension_semantics=("arbitrary",), vmem_limit_bytes=VMEM_LIMIT),
        cost_estimate=pl.CostEstimate(flops=(2 * n * e * cols) // COVER, bytes_accessed=n * (cols * 16 + e * 2 + 1536), transcendentals=n * cols * 2),
        name="back",
    )(vp, pre, normed, rstd, z, m1, m2, du, gain, *extra)


def spread_kernel(n_masks, vp, pos_ref, w_ref, *refs):
    pieces, (out_ref, dab, dz, obuf, in_sem, out_sem) = refs[:4], refs[4:]
    n, cols = pieces[0].shape
    col = lambda k: pl.ds(pl.multiple_of((vp[0] ^ k) * cols, cols), cols)
    loads = [pltpu.make_async_copy(p, dab.at[:, col(j)], in_sem.at[j]) for j, p in enumerate(pieces)]
    for c in loads:
        c.start()
    dz[n:, :] = jnp.zeros((dz.shape[0] - n, dz.shape[1]), F32)
    n_seq, seq_len, _ = out_ref.shape
    place = lax.broadcasted_iota(I32, (seq_len, 1), 0)
    slots = pos_ref.shape[2]
    for c in loads:
        c.wait()
    for r0, r1 in row_cuts(n):
        dz[r0:r1, :] = dot(dab[r0:r1, :].astype(BF16), w_ref[...], NT).astype(BF16).astype(F32)
    group = 8
    store = lambda b, j: pltpu.make_async_copy(obuf.at[j % 4], out_ref.at[b], out_sem.at[j % 4])

    @pl.loop(0, n_seq // group)
    def _(g):
        for j in range(group):
            b = g * group + j

            @pl.when(b >= 4)
            def _():
                store(b - 4, j).wait()

            hot = jnp.where(place == pos_ref[b], 1.0, 0.0).astype(BF16)
            base = pl.multiple_of(g * (group * n_masks), 8)
            low = j * n_masks // 8 * 8
            rows = dz[pl.ds(base + low, slots + 8), :][j * n_masks - low:j * n_masks - low + slots]
            obuf[j % 4] = dot(hot, rows.astype(BF16), NN).astype(BF16)
            store(b, j).start()

    for j in range(group - 4, group):
        store(n_seq - group + j, j).wait()


def spread_pass(n_masks, shape, vp, pos, w, pieces):
    n, cols = pieces[0].shape
    e = w.shape[0]
    return pl.pallas_call(
        functools.partial(spread_kernel, n_masks),
        in_specs=[SMEM, VMEM, VMEM] + [ANY] * 4,
        out_specs=ANY,
        out_shape=jax.ShapeDtypeStruct(shape, BF16),
        scratch_shapes=[pltpu.VMEM((n, 4 * cols), F32), pltpu.VMEM((n + 16, e), F32), pltpu.VMEM((4,) + shape[1:], BF16), DMA((4,)), DMA((4,))],
        compiler_params=pltpu.CompilerParams(vmem_limit_bytes=VMEM_LIMIT),
        cost_estimate=pl.CostEstimate(flops=(2 * shape[0] * shape[1] * 128 * e) // COVER, bytes_accessed=shape[0] * shape[1] * e * 2, transcendentals=0),
        name="spread",
    )(vp, pos, w, *pieces)


def order_sum(xs):
    return (xs[0] + xs[1]) + (xs[2] + xs[3])


def after(x, *deps):
    return lax.optimization_barrier((x, deps))[0]


def solution(mesh):
    n_groups, n_shards = mesh.shape["dp"], mesh.shape["vp"]

    def swap(a, bit):
        return lax.ppermute(a, "dp", [(d, d ^ bit) for d in range(n_groups)])

    def swap_vp(a, bit):
        return lax.ppermute(a, "vp", [(d, d ^ bit) for d in range(n_shards)])

    def hop(a):
        return lax.ppermute(a, "dp", [(d, d ^ (Y if d & CORE else X)) for d in range(n_groups)])

    def local_step(hidden, mask_pos, labels, w_trans, b_trans, ln_gain, ln_bias, emb_table, b_vocab):
        n_rows, _, width = hidden.shape
        n_masks = mask_pos.shape[1]
        shard_rows = emb_table.shape[0]
        n_loc = n_rows * n_masks
        n_tokens = n_loc * n_groups
        slots = -(-n_masks // 16) * 16
        cut = n_loc // 32 * 16
        cols = width // n_shards
        dp, vp = lax.axis_index("dp"), lax.axis_index("vp")
        row_start = vp * shard_rows
        scale = 1.0 / n_tokens
        core, mine = dp & 1, (dp >> 1 ^ dp >> 2) & 1

        pos_pad = jnp.pad(mask_pos, ((0, 0), (0, slots - n_masks)), constant_values=-1)
        z, pre, normed, rstd, u, u_lo, u_hi = head_pass(
            n_masks, cut, hidden, jnp.broadcast_to(pos_pad[:, :, None], (n_rows, slots, 128)),
            w_trans, b_trans[None], ln_gain[None], ln_bias[None])

        x_lo, y_hi = swap(u_lo, X), swap(u_hi, Y)
        x_hi, y_lo = swap(u_hi, X), swap(u_lo, Y)
        c_lo, c_hi = swap(u_lo, CORE), swap(u_hi, CORE)

        flat_labels = labels.reshape(n_loc)
        lab_local = flat_labels - row_start
        lab_local = jnp.where((lab_local >= 0) & (lab_local < shard_rows), lab_local, ELSEWHERE)
        column = lambda x: jnp.broadcast_to(x[:, None], (x.shape[0], 128))
        lab_col = column(lab_local)
        logits, stat = stats(u, emb_table, b_vocab[None], lab_col)
        all_stats = [stat] + [swap_vp(stat, b) for b in range(1, n_shards)]
        global_max = functools.reduce(jnp.maximum, [s[0] for s in all_stats])
        log_norm = global_max + jnp.log(order_sum([s[1] * jnp.exp(s[0] - global_max) for s in all_stats]))
        loss_part = jnp.sum(log_norm - order_sum([s[2] for s in all_stats]))
        lse = log_norm + jnp.log(jnp.float32(n_tokens))

        du_part, db_part, sums = du_pass(scale, n_shards, 0, logits, emb_table, column(lse), lab_col, normed, ln_gain[None])
        du_share = lax.psum_scatter(du_part.reshape(n_shards * n_loc, cols), "vp", scatter_dimension=0, tiled=True)
        lse = after(lse, du_part)
        fill = (0, BLK - n_loc)
        info = jnp.stack([jnp.pad(lse, fill, constant_values=jnp.inf), jnp.pad(flat_labels.astype(F32), fill, constant_values=-1.0)])
        near, *away = [swap(info, b) for b in (CORE, X, Y, X | Y)]
        x_lo, y_hi = after((x_lo, y_hi), du_part)
        d_lo, d_hi = swap(x_lo, Y), swap(y_hi, X)
        cx_lo, cy_hi = swap(x_lo, CORE), swap(y_hi, CORE)

        half, quarter = shard_rows // 2, shard_rows // 4
        start = lambda h, c: h * half + c * quarter
        pos = jnp.stack([dp, start(mine, core), row_start + start(mine, core), start(mine, 1 - core), start(1 - mine, core), start(1 - mine, 1 - core)])
        bias_col = lax.dynamic_slice(b_vocab, (start(mine, core),), (quarter,))[:, None]
        shares = (1088, 1088, 968)
        ends = [0]
        for w in shares[:-1]:
            ends.append(ends[-1] + max(16, quarter * w // sum(shares) // 16 * 16))
        spans = list(zip(ends, ends[1:] + [quarter]))

        def rows(kind, k, *wait, info=None, span=None, **kw):
            return rows_pass(kind, scale, shard_rows, span or spans[k], cut, after(pos, *wait), emb_table, bias_col, info, **kw)

        def send(k, chunk):
            return ((TWIN, spans[k][0]), swap(chunk, CORE)), hop(chunk)

        def forward(k, far, *wait):
            far = after(far, *wait)
            return ((FAR, spans[k][0]), far), ((FAR_TWIN, spans[k][0]), swap(far, CORE))

        tokens = {0: (u_lo, u_hi), CORE: (c_lo, c_hi), X: (x_lo, x_hi), Y: (y_lo, y_hi)}
        pair = jnp.stack([info, near])
        own, u_all = rows("own", 0, du_part, info=pair, tokens=tokens)
        x_hi, y_lo, away = after((x_hi, y_lo, away), own)
        away = jnp.stack(away)
        tokens[X | CORE] = cx_lo, swap(x_hi, CORE)
        tokens[Y | CORE] = swap(y_lo, CORE), cy_hi
        away_near = swap(away, CORE)
        tokens[X], tokens[Y] = (x_lo, x_hi), (y_lo, y_hi)
        info = jnp.concatenate([pair, jnp.stack([away, away_near], axis=1).reshape(6, 2, BLK)])

        sums = after(sums, own)
        sums = [sums] + [swap_vp(sums, b) for b in range(1, n_shards)]
        side, u_all = rows("side", 0, info=info, tokens=tokens, u_all=u_all)
        d_lo, d_hi = after((d_lo, d_hi), side)
        tokens[X | Y], tokens[X | Y | CORE] = (d_lo, d_hi), (swap(d_lo, CORE), swap(d_hi, CORE))
        sums = order_sum(after(sums, side)) / width
        m1, m2 = column(sums[0]), column(sums[1])
        chunk0, u_all, big = rows("far", 0, m1, m2, info=info, tokens=tokens, u_all=u_all, parts=((own, 0), (side, 0)))
        twin0, far0 = send(0, chunk0)

        du_share = after(du_share, chunk0)
        loss_row = jnp.pad(loss_part[None, None], ((0, 0), (0, cols - 1)))
        db_rows = -(-shard_rows // cols // 8) * 8
        db_mat = jnp.pad(db_part[0], (0, db_rows * cols - shard_rows)).reshape(db_rows, cols)
        dab, pack = back_pass(0, vp[None], pre, normed, rstd, z, m1, m2, du_share, ln_gain[None], loss_row, db_mat)
        back_done = dab
        pack = lax.psum(pack, "dp")
        dab = [dab] + [swap_vp(dab, b) for b in range(1, n_shards)]

        chunk1, big = rows("whole", 1, back_done, info=info, u_all=u_all, big=big, puts=[twin0])
        twin1, far1 = send(1, chunk1)
        pack = after(pack, chunk1)
        n_half = (width + 16) // 2
        part = lax.dynamic_slice(pack, (core * n_half, 0), (n_half, cols))
        parts = [swap_vp(part, b) for b in range(1, n_shards)]
        far0, far_twin0 = forward(0, far0, chunk1)

        chunk2, big = rows("whole", 2, part, info=info, u_all=u_all, big=big, puts=[far0, far_twin0])
        twin2, far2 = send(2, chunk2)
        big = put_rows(pos, big, [twin1, ((FAR, spans[1][0]), far1)])
        far1, far_twin1 = forward(1, far1, big)
        d_hidden = spread_pass(n_masks, hidden.shape, vp[None], pos_pad[:, None], w_trans, after(dab, big))
        parts = after(parts, d_hidden)
        others = [swap(p, CORE) for p in parts]
        big = put_rows(after(pos, d_hidden), big, [far_twin1, twin2])
        pack, parts, others = after((pack, parts, others), big)
        d_w, vec = join_pass(jnp.stack([vp, core]), pack, parts, others)
        db = pack[width + 16:].reshape(-1)[:shard_rows]
        loss = pack[width + 3, 0] / n_tokens
        grads = vec[0], vec[1], vec[2]
        far2, far_twin2 = forward(2, far2, big, d_w, db, loss, *grads)
        big = put_rows(pos, big, [far2])
        big = put_rows(pos, big, [far_twin2])

        return loss, d_hidden, d_w, *grads, big, db

    in_specs = (P("dp", None, None), P("dp", None), P("dp", None), P(None, None), P(None), P(None), P(None), P("vp", None), P("vp"))
    out_specs = (P(), P("dp", None, None), P(None, None), P(None), P(None), P(None), P("vp", None), P("vp"))
    return jax.shard_map(local_step, mesh=mesh, in_specs=in_specs, out_specs=out_specs, check_vma=False)
```

```python
import functools

import jax
import jax.numpy as jnp
from jax import lax
from jax.experimental import pallas as pl
from jax.experimental.pallas import tpu as pltpu
from jax.sharding import PartitionSpec as P


F32, BF16, I32 = jnp.float32, jnp.bfloat16, jnp.int32
NT = (((1,), (1,)), ((), ()))
NN = (((1,), (0,)), ((), ()))
VB = 1024
VMEM_LIMIT = 60 << 20
COVER = 100
PARTS = 4
LEAST = float(jnp.finfo(jnp.float32).min)
ELSEWHERE = -(1 << 20)


def row_cuts(rows, parts=4):
    cuts = [16 * (rows // 16 * k // parts) for k in range(parts)] + [rows]
    return list(zip(cuts[:-1], cuts[1:]))


def dot(a, b, dims):
    return lax.dot_general(a, b, dims, preferred_element_type=F32)


def stats_kernel(n_vocab, u_ref, emb_ref, b_ref, lab_ref, logits_ref, stat_ref, prev, m_sc, s_sc, l_sc):
    i, n_steps = pl.program_id(0), pl.num_programs(0)
    lane = lax.broadcasted_iota(I32, (1, 128), 1)
    cuts = row_cuts(u_ref.shape[0], PARTS)

    @pl.when(i == 0)
    def _():
        m_sc[...] = jnp.full_like(m_sc, LEAST)
        s_sc[...] = jnp.zeros_like(s_sc)
        l_sc[...] = jnp.zeros_like(l_sc)
        prev[...] = jnp.full_like(prev, -jnp.inf)

    def logits_of(r0, r1, c0, wide, width):
        tile = dot(u_ref[r0:r1, :], emb_ref[c0:c0 + wide, :], NT) + b_ref[:, c0:c0 + wide]
        if wide > width:
            tile = jnp.where(lax.broadcasted_iota(I32, (1, wide), 1) < width, tile, -jnp.inf)
        logits_ref[r0:r1, c0:c0 + wide] = tile
        return tile

    def take(r0, r1, read, first, wide):
        for q in range(r0, r1, 16):
            rs = slice(q, q + 16)
            parts = [read(rs, slice(k, k + 128)) for k in range(0, wide, 128)]
            m_old = m_sc[rs, :]
            m_new = functools.reduce(jnp.maximum, parts, m_old)
            s_new = s_sc[rs, :] * jnp.exp(m_old - m_new)
            l_new = l_sc[rs, :]
            lab = lab_ref[rs, :] - first
            for k, part in enumerate(parts):
                s_new += jnp.exp(part - m_new)
                l_new = jnp.where(lab == lane + k * 128, part, l_new)
            m_sc[rs, :], s_sc[rs, :], l_sc[rs, :] = m_new, s_new, l_new

    from_prev = lambda rs, cs: prev[rs, cs]
    from_out = lambda rs, cs: logits_ref[rs, cs]

    def step(second):
        width = VB if second else n_vocab % (2 * VB)
        wide = -(-width // 128) * 128
        for r0, r1 in cuts:
            logits_of(r0, r1, 0, wide, width)
            take(r0, r1, from_prev, (2 * i - 1) * VB, VB)
        for r0, r1 in cuts:
            if second:
                prev[r0:r1, :] = logits_of(r0, r1, VB, VB, VB)
            take(r0, r1, from_out, 2 * i * VB, wide)

    pl.when(i < n_steps - 1)(functools.partial(step, True))
    pl.when(i == n_steps - 1)(functools.partial(step, False))

    @pl.when(i == n_steps - 1)
    def _():
        m_t, s_t, l_t = m_sc[...].T, s_sc[...].T, l_sc[...].T
        m_all = jnp.max(m_t, axis=0, keepdims=True)
        stat_ref[0:1, :] = m_all
        stat_ref[1:2, :] = jnp.sum(s_t * jnp.exp(m_t - m_all), axis=0, keepdims=True)
        stat_ref[2:3, :] = jnp.sum(l_t, axis=0, keepdims=True)
        stat_ref[3:8, :] = jnp.zeros_like(stat_ref[3:8, :])


def stats(u, emb, bias, lab):
    t, e = u.shape
    v = emb.shape[0]
    n = pl.cdiv(v, 2 * VB)
    whole = lambda *s: pl.BlockSpec(s, lambda i: (0,) * len(s))
    return pl.pallas_call(
        functools.partial(stats_kernel, v),
        grid=(n,),
        in_specs=[whole(t, e), pl.BlockSpec((2 * VB, e), lambda i: (i, 0)), pl.BlockSpec((1, 2 * VB), lambda i: (0, i)), whole(t, 128)],
        out_specs=[pl.BlockSpec((t, 2 * VB), lambda i: (0, i)), whole(8, t)],
        out_shape=[jax.ShapeDtypeStruct((t, v), F32), jax.ShapeDtypeStruct((8, t), F32)],
        scratch_shapes=[pltpu.VMEM((t, VB), F32)] + [pltpu.VMEM((t, 128), F32)] * 3,
        compiler_params=pltpu.CompilerParams(dimension_semantics=("arbitrary",), vmem_limit_bytes=VMEM_LIMIT),
        cost_estimate=pl.CostEstimate(flops=(2 * t * v * e) // COVER, bytes_accessed=t * v * 4 + v * e * 2, transcendentals=t * v),
        name="stats",
    )(u, emb, bias, lab)


def du_kernel(n_vocab, scale, base, logits_ref, emb_ref, lse_ref, lab_ref, norm_hbm, gain_ref, out_ref, db_ref, sum_ref, du_ref, g_sc, db_sc, norm_sc, db_sc2, sem):
    i, n_blocks = pl.program_id(0), pl.num_programs(0)
    t = logits_ref.shape[0]
    lane = lax.broadcasted_iota(I32, (1, 128), 1)

    norm_copy = pltpu.make_async_copy(norm_hbm.at[base:base + t, :], norm_sc, sem)

    @pl.when(i == 0)
    def _():
        du_ref[...] = jnp.zeros_like(du_ref)

    @pl.when(i == 2)
    def _():
        norm_copy.start()

    def run(width):
        wide = -(-width // 128) * 128
        emb = emb_ref[:wide, :]
        if wide > width:
            emb = jnp.where(lax.broadcasted_iota(I32, (wide, 1), 0) < width, emb, jnp.zeros_like(emb))
        for r0, r1 in row_cuts(t):
            sums = [None] * (wide // 128)
            for q in range(r0, r1, 16):
                rs = slice(q, q + 16)
                lse = lse_ref[rs, :]
                lab = lab_ref[rs, :] - i * VB
                for k in range(wide // 128):
                    c = k * 128
                    g = jnp.exp(logits_ref[rs, c:c + 128] - lse)
                    g -= jnp.where(lab == lane + c, scale, 0.0)
                    if c + 128 > width:
                        g = jnp.where(lane < width - c, g, 0.0)
                    part = g[:8] + g[8:]
                    sums[k] = part if sums[k] is None else sums[k] + part
                    g_sc[rs, c:c + 128] = g.astype(BF16)
            for k in range(wide // 128):
                cs = slice(k * 128, (k + 1) * 128)
                db_sc[:, cs] = sums[k] if r0 == 0 else db_sc[:, cs] + sums[k]
            du_ref[r0:r1, :] += dot(g_sc[r0:r1, :wide], emb, NN)
        db_ref[:, :wide] = jnp.sum(db_sc[:, :wide], axis=0, keepdims=True)

    tail = n_vocab % VB
    if tail:
        pl.when(i < n_blocks - 1)(functools.partial(run, VB))
        pl.when(i == n_blocks - 1)(functools.partial(run, tail))
    else:
        run(VB)

    @pl.when(i == n_blocks - 1)
    def _():
        norm_copy.wait()
        parts, rows, cols = out_ref.shape
        run = rows // 7
        for r in range(0, rows, run):
            rs = slice(r, r + run)
            total = [jnp.zeros((run, 128), F32)] * 2
            for c in range(0, parts * cols, 128):
                x = du_ref[rs, c:c + 128].astype(BF16).astype(F32)
                out_ref[c // cols, rs, c % cols:c % cols + 128] = x
                dn = x * gain_ref[:, c:c + 128]
                total = [total[0] + dn, total[1] + dn * norm_sc[rs, c:c + 128]]
            for j, x in enumerate(total):
                db_sc2[j, rs, :] = x
        for j in range(2):
            sum_ref[j:j + 1, :] = jnp.sum(db_sc2[j].T, axis=0, keepdims=True)
        sum_ref[2:, :] = jnp.zeros_like(sum_ref[2:, :])


def du_pass(scale, parts, base, logits, emb, lse, lab, normed, gain):
    t, v = logits.shape
    e = emb.shape[1]
    n = pl.cdiv(v, VB)
    whole = lambda *s: pl.BlockSpec(s, lambda i: (0,) * len(s))
    return pl.pallas_call(
        functools.partial(du_kernel, v, scale, base),
        grid=(n,),
        in_specs=[pl.BlockSpec((t, VB), lambda i: (0, i)), pl.BlockSpec((VB, e), lambda i: (i, 0)), whole(t, 128), whole(t, 128), pl.BlockSpec(memory_space=pl.ANY), whole(1, e)],
        out_specs=[whole(parts, t, e // parts), pl.BlockSpec((1, VB), lambda i: (0, i)), whole(8, t)],
        out_shape=[jax.ShapeDtypeStruct((parts, t, e // parts), F32), jax.ShapeDtypeStruct((1, v), F32), jax.ShapeDtypeStruct((8, t), F32)],
        scratch_shapes=[pltpu.VMEM((t, e), F32), pltpu.VMEM((t, VB), BF16), pltpu.VMEM((8, VB), F32), pltpu.VMEM((t, e), F32), pltpu.VMEM((2, t, 128), F32), pltpu.SemaphoreType.DMA],
        compiler_params=pltpu.CompilerParams(dimension_semantics=("arbitrary",), vmem_limit_bytes=VMEM_LIMIT),
        cost_estimate=pl.CostEstimate(flops=(2 * t * v * e) // COVER, bytes_accessed=t * v * 4 + v * e * 2, transcendentals=t * v),
        name="du_pass",
    )(logits, emb, lse, lab, normed, gain)


LN_EPS = 1e-5
CORE, X, Y = 1, 2, 4
ANY = pl.BlockSpec(memory_space=pltpu.HBM)
VMEM = pl.BlockSpec(memory_space=pltpu.VMEM)
SMEM = pl.BlockSpec(memory_space=pltpu.SMEM)
DMA = pltpu.SemaphoreType.DMA


def gelu_norm(a):
    cdf = 0.5 * (1.0 + lax.erf(a * (0.5 ** 0.5)))
    g = a * cdf
    centered = g - jnp.mean(g, axis=1, keepdims=True)
    rstd = lax.rsqrt(jnp.mean(centered * centered, axis=1, keepdims=True) + LN_EPS)
    return cdf, centered * rstd, rstd


def head_kernel(n_masks, cut, hid, pos_ref, w_ref, b_ref, gain_ref, bias_ref, z_out, pre_out, norm_out, rstd_out, u_out, lo_out, hi_out,
                hbuf, zf, zb, pre_v, norm_v, rstd_v, ub, uf, in_sem, out_sem):
    n_seq, seq_len = hid.shape[0], hid.shape[1]
    n_loc = n_seq * n_masks
    loads = [pltpu.make_async_copy(hid.at[b], hbuf.at[b], in_sem.at[b]) for b in range(n_seq)]
    for c in loads:
        c.start()
    lane = lax.broadcasted_iota(I32, (1, 128), 1)
    cuts = [0, cut // 32 * 16, cut, cut + (n_loc - cut) // 32 * 16, n_loc]
    done, stores = 0, []

    def send(src, dst, r0, r1, base=0):
        c = pltpu.make_async_copy(src.at[r0:r1, :], dst.at[r0 - base:r1 - base, :], out_sem.at[len(stores)])
        c.start()
        stores.append(c)

    for b in range(n_seq):
        loads[b].wait()
        hot = jnp.concatenate([jnp.where(pos_ref[b] == lane + j, 1.0, 0.0).astype(BF16) for j in range(0, seq_len, 128)], axis=1)
        zf[b * n_masks:(b + 1) * n_masks, :] = dot(hot, hbuf[b], NN)[:n_masks, :]
        while done < 4 and cuts[done + 1] <= (b + 1) * n_masks:
            r0, r1 = cuts[done], cuts[done + 1]
            z = zf[r0:r1, :].astype(BF16)
            zb[r0:r1, :] = z
            a = dot(z, w_ref[...], NN) + b_ref[...]
            pre_v[r0:r1, :] = a
            _, normed, rstd = gelu_norm(a)
            norm_v[r0:r1, :] = normed
            rstd_v[r0:r1, :] = jnp.broadcast_to(rstd, (r1 - r0, 128))
            u = (normed * gain_ref[...] + bias_ref[...]).astype(BF16)
            ub[r0:r1, :] = u
            uf[r0:r1, :] = u.astype(F32)
            done += 1
            send(uf, hi_out if r0 >= cut else lo_out, r0, r1, cut if r0 >= cut else 0)
            for src, dst in ((ub, u_out), (zb, z_out), (pre_v, pre_out), (norm_v, norm_out), (rstd_v, rstd_out)):
                send(src, dst, r0, r1)
    for c in stores:
        c.wait()


def head_pass(n_masks, cut, hidden, pos, w, b, gain, bias):
    n_seq, seq_len, e = hidden.shape
    n = n_seq * n_masks
    kinds = [((n, e), BF16), ((n, e), F32), ((n, e), F32), ((n, 128), F32), ((n, e), BF16), ((cut, e), F32), ((n - cut, e), F32)]
    return pl.pallas_call(
        functools.partial(head_kernel, n_masks, cut),
        in_specs=[ANY] + [VMEM] * 5,
        out_specs=[ANY] * len(kinds),
        out_shape=[jax.ShapeDtypeStruct(*k) for k in kinds],
        scratch_shapes=[pltpu.VMEM((n_seq, seq_len, e), BF16), pltpu.VMEM((n, e), F32)]
        + [pltpu.VMEM(*k) for k in kinds[:5]] + [pltpu.VMEM((n, e), F32), DMA((n_seq,)), DMA((24,))],
        compiler_params=pltpu.CompilerParams(vmem_limit_bytes=VMEM_LIMIT),
        cost_estimate=pl.CostEstimate(flops=(4 * n * e * e) // COVER, bytes_accessed=hidden.size * 2 + n * e * 20, transcendentals=n * e),
        name="head",
    )(hidden, pos, w, b, gain, bias)


BLK = 1280
LOOPED = ('side',)
STEPS = {"own": 2, "again": 2, "side": 4, "far": 2, "last": 2, "whole": 8}
ME, MINE, MINE_ID, TWIN, FAR, FAR_TWIN = range(6)


def rows_kernel(kind, scale, s0, m, cut, n_loc, sources, skips, spots, has_big, pos, emb_hbm, bias_ref, info_ref, *refs):
    refs = list(refs)
    take = lambda n: [refs.pop(0) for _ in range(n)]
    wide = sources is not None
    if wide:
        src = {r: take(2) for r in sources}
        if kind != "own":
            take(1)
    else:
        u_hbm, = take(1)
    if has_big:
        take(1)
    parts = take(len(skips))
    puts = take(len(spots))
    out_hbm, = take(1)
    if wide:
        u_hbm, = take(1)
    if kind in ("far", "last", "whole"):
        big_ref, = take(1)
    if wide:
        buf, = take(1)
    ring, emb_sc, g_sc, acc, hold, sem, tok_sem, back_sem, in_sem, out_sem = refs
    me = pos[ME]
    chip = lax.div(me, 2)
    n_steps = STEPS[kind]
    along_x, along_y = chip ^ 1, chip ^ 2

    def device(i):
        side = 2 * jnp.where(i < 2, jnp.minimum(along_x, along_y), jnp.maximum(along_x, along_y)) + lax.rem(i, 2)
        far = 2 * (chip ^ 3) + lax.rem(i, 2)
        if kind in ("own", "again"):
            return 2 * chip + i
        return {"side": side, "far": far, "last": far, "whole": i}[kind]

    depth = ring.shape[0]

    def fetch(i):
        slot = lax.rem(i, 2 if wide else depth)
        if not wide:
            pltpu.make_async_copy(u_hbm.at[device(i)], ring.at[slot], tok_sem.at[slot, 0]).start()
            return
        for r, (lo, hi) in src.items():
            @pl.when(device(i) ^ me == r)
            def _():
                pltpu.make_async_copy(lo, buf.at[slot, :cut, :], tok_sem.at[slot, 0]).start()
                pltpu.make_async_copy(hi, buf.at[slot, cut:, :], tok_sem.at[slot, 1]).start()

    row = lambda j, off: pl.multiple_of(pos[j] + off, 8)
    emb_copy = pltpu.make_async_copy(emb_hbm.at[pl.ds(row(MINE, s0), m), :], emb_sc, sem)
    emb_copy.start()
    fetch(0)
    loads, stores = [], []
    for j, (p, (base, off)) in enumerate(zip(puts, spots)):
        n = p.shape[0]
        loads.append(pltpu.make_async_copy(p, hold.at[j, :n, :], in_sem.at[j]))
        stores.append(pltpu.make_async_copy(hold.at[j, :n, :], big_ref.at[pl.ds(row(base, off), n), :], out_sem.at[j]))
    for j, (p, skip) in enumerate(zip(parts, skips)):
        loads.append(pltpu.make_async_copy(p.at[skip:skip + m, :], hold.at[len(puts) + j, :m, :], in_sem.at[len(puts) + j]))
    acc[...] = jnp.zeros_like(acc)
    if wide:
        for k in range(2):
            ring[k, n_loc:, :] = jnp.zeros((BLK - n_loc, ring.shape[2]), BF16)
    emb_copy.wait()
    n_groups = 2 if kind in LOOPED and m % 32 == 0 else 1
    tall = m // n_groups
    n_cuts = max(1, round(tall / 300))
    cuts = [-(-tall * k // (n_cuts * 16)) * 16 for k in range(n_cuts)] + [tall]
    cuts = list(zip(cuts[:-1], cuts[1:]))
    kept = lambda i: pltpu.make_async_copy(ring.at[lax.rem(i, 2)], u_hbm.at[device(i)], back_sem.at[lax.rem(i, 2)])

    @pl.loop(0, n_steps)
    def _(i):
        slot = lax.rem(i, 2 if wide else depth)
        if wide:
            any_lo, any_hi = next(iter(src.values()))
            pltpu.make_async_copy(any_lo, buf.at[slot, :cut, :], tok_sem.at[slot, 0]).wait()
            pltpu.make_async_copy(any_hi, buf.at[slot, cut:, :], tok_sem.at[slot, 1]).wait()

            @pl.when(i >= 2)
            def _():
                kept(i - 2).wait()
        else:
            pltpu.make_async_copy(u_hbm.at[device(i)], ring.at[slot], tok_sem.at[slot, 0]).wait()

        @pl.when(i + 1 < n_steps)
        def _():
            fetch(i + 1)

        @pl.when(i == 0)
        def _():
            for c in loads:
                c.start()

        for j, (a, b) in enumerate(zip(loads, stores)):
            @pl.when(i == min(2 + j, n_steps - 1))
            def _():
                a.wait()
                b.start()

        if wide:
            ring[slot, :n_loc, :] = buf[slot].astype(BF16)
            kept(i).start()
        rel = device(i) ^ me
        lse, lab = info_ref[rel, 0:1, :], info_ref[rel, 1:2, :]

        def group(h):
            def rows(r0, r1):
                return slice(r0, r1) if n_groups == 1 else pl.ds(pl.multiple_of(h * tall + r0, 16), r1 - r0)

            def weights(r0, r1):
                part = dot(emb_sc[rows(r0, r1), :], ring[slot], NT)
                ids = lax.broadcasted_iota(I32, (r1 - r0, 1), 0) + (pos[MINE_ID] + (s0 + h * tall + r0))
                bias = bias_ref[slice(s0 + r0, s0 + r1) if n_groups == 1 else pl.ds(pl.multiple_of(s0 + h * tall + r0, 8), r1 - r0), :]
                g = jnp.exp(part + bias - lse) - jnp.where(lab == ids.astype(F32), scale, 0.0)
                g_sc[r0:r1, :] = g.astype(BF16)

            weights(*cuts[0])
            for k, (r0, r1) in enumerate(cuts):
                if k + 1 < len(cuts):
                    weights(*cuts[k + 1])
                acc[rows(r0, r1), :] += dot(g_sc[r0:r1, :], ring[slot], NN)

        if n_groups == 1:
            group(0)
        else:
            pl.loop(0, n_groups)(group)

    for c in loads[len(puts):]:
        c.wait()
    if parts:
        acc[...] = (hold[len(puts), :m, :] + acc[...]) + hold[len(puts) + 1, :m, :]
    done = [pltpu.make_async_copy(acc, out_hbm, sem)]
    if kind in ("far", "last", "whole"):
        done.append(pltpu.make_async_copy(acc, big_ref.at[pl.ds(row(MINE, s0), m), :], emb_sem(tok_sem)))
    for c in done:
        c.start()
    if wide:
        for i in range(n_steps - 2, n_steps):
            kept(i).wait()
    for c in stores + done:
        c.wait()


def emb_sem(tok_sem):
    return tok_sem.at[0, 0]


def rows_pass(kind, scale, v_rows, span, cut, pos, emb, bias, info, tokens=None, u_all=None, big=None, parts=(), puts=()):
    s0, s1 = span
    m, e = s1 - s0, emb.shape[1]
    sds = jax.ShapeDtypeStruct
    wide = kind in ("own", "side", "far")
    final = kind in ("far", "last", "whole")
    args, aliases = [pos, emb, bias, info], {}
    outs = [sds((m, e), F32)]
    sources = None
    if wide:
        sources = {"own": (0, CORE), "side": (X, X | CORE, Y, Y | CORE), "far": (X | Y, X | Y | CORE)}[kind]
        args += [h for r in sources for h in tokens[r]]
        n_loc = tokens[0][0].shape[0] + tokens[0][1].shape[0]
        outs.append(sds((8, BLK, e), BF16))
        if kind != "own":
            aliases[len(args)] = 1
            args.append(u_all)
    else:
        n_loc = BLK
        args.append(u_all)
    if final:
        if big is not None:
            aliases[len(args)] = len(outs)
            args.append(big)
        outs.append(sds((v_rows, e), F32))
    args += [a for a, _ in parts] + [a for _, a in puts]
    n_hold = max(1, len(parts) + len(puts))
    tallest = max([m] * len(parts) + [a.shape[0] for _, a in puts] + [8])
    t = STEPS[kind] * BLK
    scratch = [pltpu.VMEM((2, n_loc, e), F32)] if wide else []
    scratch += [
        pltpu.VMEM((2 if wide else 3, BLK, e), BF16), pltpu.VMEM((m, e), BF16), pltpu.VMEM((m, BLK), BF16),
        pltpu.VMEM((m, e), F32), pltpu.VMEM((n_hold, tallest, e), F32),
        DMA, DMA((3, 2)), DMA((2,)), DMA((n_hold,)), DMA((n_hold,)),
    ]
    return pl.pallas_call(
        functools.partial(rows_kernel, kind, scale, s0, m, cut, n_loc, sources, [skip for _, skip in parts], [spot for spot, _ in puts], big is not None),
        in_specs=[SMEM, ANY, VMEM, VMEM] + [ANY] * (len(args) - 4),
        out_specs=[ANY] * len(outs),
        out_shape=outs,
        scratch_shapes=scratch,
        input_output_aliases=aliases,
        compiler_params=pltpu.CompilerParams(vmem_limit_bytes=VMEM_LIMIT),
        cost_estimate=pl.CostEstimate(flops=(4 * t * m * e) // COVER, bytes_accessed=t * e * 2 + m * e * 6, transcendentals=t * m),
    )(*args)


def put_kernel(spots, pos, *refs):
    n = len(spots)
    pieces, (out_ref, hold, in_sem, out_sem) = refs[1:1 + n], refs[1 + n:]
    loads, stores = [], []
    for j, (p, (base, off)) in enumerate(zip(pieces, spots)):
        slot = hold.at[j, :p.shape[0], :]
        loads.append(pltpu.make_async_copy(p, slot, in_sem.at[j]))
        stores.append(pltpu.make_async_copy(slot, out_ref.at[pl.ds(pl.multiple_of(pos[base] + off, 8), p.shape[0]), :], out_sem.at[j]))
    for a in loads:
        a.start()
    for a, b in zip(loads, stores):
        a.wait()
        b.start()
    for b in stores:
        b.wait()


def put_rows(pos, big, puts):
    spots, pieces = [s for s, _ in puts], [a for _, a in puts]
    n, e = len(pieces), big.shape[1]
    size = sum(p.size for p in pieces)
    return pl.pallas_call(
        functools.partial(put_kernel, spots),
        in_specs=[SMEM] + [ANY] * (n + 1),
        out_specs=ANY,
        out_shape=jax.ShapeDtypeStruct(big.shape, big.dtype),
        scratch_shapes=[pltpu.VMEM((n, max(p.shape[0] for p in pieces), e), F32), DMA((n,)), DMA((n,))],
        input_output_aliases={1: 0},
        compiler_params=pltpu.CompilerParams(vmem_limit_bytes=VMEM_LIMIT),
        cost_estimate=pl.CostEstimate(flops=(size) // COVER, bytes_accessed=size * 8, transcendentals=0),
        name="put_rows",
    )(pos, big, *pieces)


def join_kernel(n_vec, idx, *refs):
    own, mine, theirs, (dw_ref, vec_ref, full, in_sem, out_sem) = refs[0], refs[1:4], refs[4:7], refs[7:]
    vp, core = idx[0], idx[1]
    half, cols = mine[0].shape
    col = lambda k: pl.ds(pl.multiple_of((vp ^ k) * cols, cols), cols)
    row = lambda c: pl.ds(pl.multiple_of(c * half, 8), half)
    loads = [pltpu.make_async_copy(own.at[:2 * half, :], full.at[:, col(0)], in_sem.at[0])]
    for k in range(3):
        loads.append(pltpu.make_async_copy(mine[k], full.at[row(core), col(k + 1)], in_sem.at[1 + k]))
        loads.append(pltpu.make_async_copy(theirs[k], full.at[row(1 - core), col(k + 1)], in_sem.at[4 + k]))
    for c in loads:
        c.start()
    for c in loads:
        c.wait()
    e = dw_ref.shape[0]
    stores = [pltpu.make_async_copy(full.at[:e, :], dw_ref, out_sem.at[0]), pltpu.make_async_copy(full.at[e:e + n_vec, :], vec_ref, out_sem.at[1])]
    for c in stores:
        c.start()
    for c in stores:
        c.wait()


def join_pass(idx, own, mine, theirs):
    half, cols = mine[0].shape
    e = 4 * cols
    return pl.pallas_call(
        functools.partial(join_kernel, 8),
        in_specs=[SMEM] + [ANY] * 7,
        out_specs=[ANY] * 2,
        out_shape=[jax.ShapeDtypeStruct((e, e), F32), jax.ShapeDtypeStruct((8, e), F32)],
        scratch_shapes=[pltpu.VMEM((2 * half, e), F32), DMA((7,)), DMA((2,))],
        compiler_params=pltpu.CompilerParams(vmem_limit_bytes=VMEM_LIMIT),
        cost_estimate=pl.CostEstimate(flops=(e * e) // COVER, bytes_accessed=e * e * 8, transcendentals=0),
        name="join",
    )(idx, own, *mine, *theirs)


def back_kernel(base, vp, *refs):
    refs = list(refs)
    srcs = [refs.pop(0) for _ in range(7)]
    gain_ref, = [refs.pop(0)]
    extra = refs[:-10]
    dab_ref, pack_ref, pre, norm, rstd, z, m1, m2, du, sem = refs[-10:]
    n, cols = du.shape
    e = z.shape[1]
    col = pl.ds(pl.multiple_of(vp[0] * cols, cols), cols)
    rows = slice(base, base + n)
    pre_h, norm_h, rstd_h, z_h, m1_h, m2_h, du_h = srcs
    loads = [pltpu.make_async_copy(a, b, sem.at[j]) for j, (a, b) in enumerate((
        (pre_h.at[rows, col], pre), (norm_h.at[rows, col], norm), (rstd_h.at[rows, :], rstd), (m1_h.at[rows, :], m1), (m2_h.at[rows, :], m2),
        (du_h, du), (z_h.at[rows, :], z)))]
    for c in loads:
        c.start()
    for c in loads:
        c.wait()
    for j, c in enumerate(range(0, cols, 128)):
        cs = slice(c, c + 128)
        a, d, normed = pre[:, cs], du[:, cs], norm[:, cs]
        cdf = 0.5 * (1.0 + lax.erf(a * (0.5 ** 0.5)))
        dg = rstd[...] * (d * gain_ref[:, cs] - m1[...] - normed * m2[...])
        da = dg * (cdf + a * (jnp.exp(-0.5 * a * a) * 0.3989422804014327))
        dab_ref[:, cs] = da.astype(BF16).astype(F32)
        for j, x in enumerate((da, d * normed, d)):
            pack_ref[e + j:e + j + 1, cs] = jnp.sum(x, axis=0, keepdims=True)
    loss_ref, db_ref = extra
    pack_ref[:e, :] = lax.dot_general(z[...], dab_ref[...].astype(BF16), (((0,), (0,)), ((), ())), preferred_element_type=F32)
    pack_ref[e + 3:e + 4, :] = loss_ref[...]
    pack_ref[e + 4:e + 16, :] = jnp.zeros_like(pack_ref[e + 4:e + 16, :])
    pack_ref[e + 16:, :] = db_ref[...]


def back_pass(base, vp, pre, normed, rstd, z, m1, m2, du, gain, *extra):
    n, cols = du.shape
    e = z.shape[1]
    n_pack = e + 16 + extra[1].shape[0]
    block = lambda *s: pl.BlockSpec(s, lambda i, p: (0,) * len(s))
    gs = pltpu.PrefetchScalarGridSpec(
        num_scalar_prefetch=1,
        grid=(1,),
        in_specs=[ANY] * 7 + [pl.BlockSpec((1, cols), lambda i, p: (0, p[0]))] + [block(*x.shape) for x in extra],
        out_specs=[block(n, cols), block(n_pack, cols)],
        scratch_shapes=[pltpu.VMEM((n, cols), F32)] * 2 + [pltpu.VMEM((n, 128), F32), pltpu.VMEM((n, e), BF16)] + [pltpu.VMEM((n, 128), F32)] * 2
        + [pltpu.VMEM((n, cols), F32), DMA((7,))],
    )
    return pl.pallas_call(
        functools.partial(back_kernel, base),
        grid_spec=gs,
        out_shape=[jax.ShapeDtypeStruct((n, cols), F32), jax.ShapeDtypeStruct((n_pack, cols), F32)],
        compiler_params=pltpu.CompilerParams(dimension_semantics=("arbitrary",), vmem_limit_bytes=VMEM_LIMIT),
        cost_estimate=pl.CostEstimate(flops=(2 * n * e * cols) // COVER, bytes_accessed=n * (cols * 16 + e * 2 + 1536), transcendentals=n * cols * 2),
        name="back",
    )(vp, pre, normed, rstd, z, m1, m2, du, gain, *extra)


def spread_kernel(n_masks, vp, pos_ref, w_ref, *refs):
    pieces, (out_ref, dab, dz, obuf, in_sem, out_sem) = refs[:4], refs[4:]
    n, cols = pieces[0].shape
    col = lambda k: pl.ds(pl.multiple_of((vp[0] ^ k) * cols, cols), cols)
    loads = [pltpu.make_async_copy(p, dab.at[:, col(j)], in_sem.at[j]) for j, p in enumerate(pieces)]
    for c in loads:
        c.start()
    dz[n:, :] = jnp.zeros((dz.shape[0] - n, dz.shape[1]), F32)
    n_seq, seq_len, _ = out_ref.shape
    place = lax.broadcasted_iota(I32, (seq_len, 1), 0)
    slots = pos_ref.shape[2]
    for c in loads:
        c.wait()
    for r0, r1 in row_cuts(n):
        dz[r0:r1, :] = dot(dab[r0:r1, :].astype(BF16), w_ref[...], NT).astype(BF16).astype(F32)
    group = 8
    store = lambda b, j: pltpu.make_async_copy(obuf.at[j % 4], out_ref.at[b], out_sem.at[j % 4])

    @pl.loop(0, n_seq // group)
    def _(g):
        for j in range(group):
            b = g * group + j

            @pl.when(b >= 4)
            def _():
                store(b - 4, j).wait()

            hot = jnp.where(place == pos_ref[b], 1.0, 0.0).astype(BF16)
            base = pl.multiple_of(g * (group * n_masks), 8)
            low = j * n_masks // 8 * 8
            rows = dz[pl.ds(base + low, slots + 8), :][j * n_masks - low:j * n_masks - low + slots]
            obuf[j % 4] = dot(hot, rows.astype(BF16), NN).astype(BF16)
            store(b, j).start()

    for j in range(group - 4, group):
        store(n_seq - group + j, j).wait()


def spread_pass(n_masks, shape, vp, pos, w, pieces):
    n, cols = pieces[0].shape
    e = w.shape[0]
    return pl.pallas_call(
        functools.partial(spread_kernel, n_masks),
        in_specs=[SMEM, VMEM, VMEM] + [ANY] * 4,
        out_specs=ANY,
        out_shape=jax.ShapeDtypeStruct(shape, BF16),
        scratch_shapes=[pltpu.VMEM((n, 4 * cols), F32), pltpu.VMEM((n + 16, e), F32), pltpu.VMEM((4,) + shape[1:], BF16), DMA((4,)), DMA((4,))],
        compiler_params=pltpu.CompilerParams(vmem_limit_bytes=VMEM_LIMIT),
        cost_estimate=pl.CostEstimate(flops=(2 * shape[0] * shape[1] * 128 * e) // COVER, bytes_accessed=shape[0] * shape[1] * e * 2, transcendentals=0),
        name="spread",
    )(vp, pos, w, *pieces)


def order_sum(xs):
    return (xs[0] + xs[1]) + (xs[2] + xs[3])


def after(x, *deps):
    return lax.optimization_barrier((x, deps))[0]


def solution(mesh):
    n_groups, n_shards = mesh.shape["dp"], mesh.shape["vp"]

    def swap(a, bit):
        return lax.ppermute(a, "dp", [(d, d ^ bit) for d in range(n_groups)])

    def swap_vp(a, bit):
        return lax.ppermute(a, "vp", [(d, d ^ bit) for d in range(n_shards)])

    def hop(a):
        return lax.ppermute(a, "dp", [(d, d ^ (Y if d & CORE else X)) for d in range(n_groups)])

    def local_step(hidden, mask_pos, labels, w_trans, b_trans, ln_gain, ln_bias, emb_table, b_vocab):
        n_rows, _, width = hidden.shape
        n_masks = mask_pos.shape[1]
        shard_rows = emb_table.shape[0]
        n_loc = n_rows * n_masks
        n_tokens = n_loc * n_groups
        slots = -(-n_masks // 16) * 16
        cut = n_loc // 32 * 16
        cols = width // n_shards
        dp, vp = lax.axis_index("dp"), lax.axis_index("vp")
        row_start = vp * shard_rows
        scale = 1.0 / n_tokens
        core, mine = dp & 1, (dp >> 1 ^ dp >> 2) & 1

        pos_pad = jnp.pad(mask_pos, ((0, 0), (0, slots - n_masks)), constant_values=-1)
        z, pre, normed, rstd, u, u_lo, u_hi = head_pass(
            n_masks, cut, hidden, jnp.broadcast_to(pos_pad[:, :, None], (n_rows, slots, 128)),
            w_trans, b_trans[None], ln_gain[None], ln_bias[None])

        x_lo, y_hi = swap(u_lo, X), swap(u_hi, Y)
        x_hi, y_lo = swap(u_hi, X), swap(u_lo, Y)
        c_lo, c_hi = swap(u_lo, CORE), swap(u_hi, CORE)

        flat_labels = labels.reshape(n_loc)
        lab_local = flat_labels - row_start
        lab_local = jnp.where((lab_local >= 0) & (lab_local < shard_rows), lab_local, ELSEWHERE)
        column = lambda x: jnp.broadcast_to(x[:, None], (x.shape[0], 128))
        lab_col = column(lab_local)
        logits, stat = stats(u, emb_table, b_vocab[None], lab_col)
        all_stats = [stat] + [swap_vp(stat, b) for b in range(1, n_shards)]
        global_max = functools.reduce(jnp.maximum, [s[0] for s in all_stats])
        log_norm = global_max + jnp.log(order_sum([s[1] * jnp.exp(s[0] - global_max) for s in all_stats]))
        loss_part = jnp.sum(log_norm - order_sum([s[2] for s in all_stats]))
        lse = log_norm + jnp.log(jnp.float32(n_tokens))

        du_part, db_part, sums = du_pass(scale, n_shards, 0, logits, emb_table, column(lse), lab_col, normed, ln_gain[None])
        du_share = lax.psum_scatter(du_part.reshape(n_shards * n_loc, cols), "vp", scatter_dimension=0, tiled=True)
        lse = after(lse, du_part)
        fill = (0, BLK - n_loc)
        info = jnp.stack([jnp.pad(lse, fill, constant_values=jnp.inf), jnp.pad(flat_labels.astype(F32), fill, constant_values=-1.0)])
        near, *away = [swap(info, b) for b in (CORE, X, Y, X | Y)]
        x_lo, y_hi = after((x_lo, y_hi), du_part)
        d_lo, d_hi = swap(x_lo, Y), swap(y_hi, X)
        cx_lo, cy_hi = swap(x_lo, CORE), swap(y_hi, CORE)

        half, quarter = shard_rows // 2, shard_rows // 4
        start = lambda h, c: h * half + c * quarter
        pos = jnp.stack([dp, start(mine, core), row_start + start(mine, core), start(mine, 1 - core), start(1 - mine, core), start(1 - mine, 1 - core)])
        bias_col = lax.dynamic_slice(b_vocab, (start(mine, core),), (quarter,))[:, None]
        shares = (1088, 960, 640, 456)
        ends = [0]
        for w in shares[:-1]:
            ends.append(ends[-1] + max(16, quarter * w // sum(shares) // 16 * 16))
        spans = list(zip(ends, ends[1:] + [quarter]))

        def rows(kind, k, *wait, info=None, span=None, **kw):
            return rows_pass(kind, scale, shard_rows, span or spans[k], cut, after(pos, *wait), emb_table, bias_col, info, **kw)

        def send(k, chunk):
            return ((TWIN, spans[k][0]), swap(chunk, CORE)), hop(chunk)

        def forward(k, far, *wait):
            far = after(far, *wait)
            return ((FAR, spans[k][0]), far), ((FAR_TWIN, spans[k][0]), swap(far, CORE))

        tokens = {0: (u_lo, u_hi), CORE: (c_lo, c_hi), X: (x_lo, x_hi), Y: (y_lo, y_hi)}
        pair = jnp.stack([info, near])
        own, u_all = rows("own", 0, du_part, info=pair, tokens=tokens)
        x_hi, y_lo, away = after((x_hi, y_lo, away), own)
        away = jnp.stack(away)
        tokens[X | CORE] = cx_lo, swap(x_hi, CORE)
        tokens[Y | CORE] = swap(y_lo, CORE), cy_hi
        away_near = swap(away, CORE)
        tokens[X], tokens[Y] = (x_lo, x_hi), (y_lo, y_hi)
        info = jnp.concatenate([pair, jnp.stack([away, away_near], axis=1).reshape(6, 2, BLK)])

        sums = after(sums, own)
        sums = [sums] + [swap_vp(sums, b) for b in range(1, n_shards)]
        side, u_all = rows("side", 0, info=info, tokens=tokens, u_all=u_all)
        d_lo, d_hi = after((d_lo, d_hi), side)
        tokens[X | Y], tokens[X | Y | CORE] = (d_lo, d_hi), (swap(d_lo, CORE), swap(d_hi, CORE))
        sums = order_sum(after(sums, side)) / width
        m1, m2 = column(sums[0]), column(sums[1])
        chunk0, u_all, big = rows("far", 0, m1, m2, info=info, tokens=tokens, u_all=u_all, parts=((own, 0), (side, 0)))
        twin0, far0 = send(0, chunk0)

        du_share = after(du_share, chunk0)
        loss_row = jnp.pad(loss_part[None, None], ((0, 0), (0, cols - 1)))
        db_rows = -(-shard_rows // cols // 8) * 8
        db_mat = jnp.pad(db_part[0], (0, db_rows * cols - shard_rows)).reshape(db_rows, cols)
        dab, pack = back_pass(0, vp[None], pre, normed, rstd, z, m1, m2, du_share, ln_gain[None], loss_row, db_mat)
        back_done = dab
        pack = lax.psum(pack, "dp")
        dab_1, dab_2 = swap_vp(dab, 1), swap_vp(dab, 2)

        chunk1, big = rows("whole", 1, back_done, info=info, u_all=u_all, big=big, puts=[twin0])
        twin1, far1 = send(1, chunk1)
        pack = after(pack, chunk1)
        n_half = (width + 16) // 2
        part = lax.dynamic_slice(pack, (core * n_half, 0), (n_half, cols))
        parts = [swap_vp(part, b) for b in range(1, n_shards)]
        far0, far_twin0 = forward(0, far0, chunk1)
        dab_2 = after(dab_2, chunk1)
        dab_3 = swap_vp(dab_2, 1)

        chunk2, big = rows("whole", 2, part, info=info, u_all=u_all, big=big, puts=[far0, far_twin0])
        twin2, far2 = send(2, chunk2)
        far1, far_twin1 = forward(1, far1, chunk2)
        chunk3, big = rows("whole", 3, info=info, u_all=u_all, big=big, puts=[twin1, far1])
        twin3, far3 = send(3, chunk3)
        far2, far_twin2 = forward(2, far2, chunk3)
        d_hidden = spread_pass(n_masks, hidden.shape, vp[None], pos_pad[:, None], w_trans, after([dab, dab_1, dab_2, dab_3], chunk3))
        parts = after(parts, d_hidden)
        others = [swap(p, CORE) for p in parts]
        big = put_rows(after(pos, d_hidden), big, [far_twin1, twin2, far2, far_twin2, twin3])
        pack, parts, others = after((pack, parts, others), big)
        d_w, vec = join_pass(jnp.stack([vp, core]), pack, parts, others)
        db = pack[width + 16:].reshape(-1)[:shard_rows]
        loss = pack[width + 3, 0] / n_tokens
        grads = vec[0], vec[1], vec[2]
        far3, far_twin3 = forward(3, far3, big, d_w, db, loss, *grads)
        big = put_rows(pos, big, [far3])
        big = put_rows(pos, big, [far_twin3])

        return loss, d_hidden, d_w, *grads, big, db

    in_specs = (P("dp", None, None), P("dp", None), P("dp", None), P(None, None), P(None), P(None), P(None), P("vp", None), P("vp"))
    out_specs = (P(), P("dp", None, None), P(None, None), P(None), P(None), P(None), P("vp", None), P("vp"))
    return jax.shard_map(local_step, mesh=mesh, in_specs=in_specs, out_specs=out_specs, check_vma=False)
```

```python
import functools

import jax
import jax.numpy as jnp
from jax import lax
from jax.experimental import pallas as pl
from jax.experimental.pallas import tpu as pltpu
from jax.sharding import PartitionSpec as P


F32, BF16, I32 = jnp.float32, jnp.bfloat16, jnp.int32
NT = (((1,), (1,)), ((), ()))
NN = (((1,), (0,)), ((), ()))
VB = 1024
VMEM_LIMIT = 67_000_000
COVER = 100
PARTS = 4
LEAST = float(jnp.finfo(jnp.float32).min)
ELSEWHERE = -(1 << 20)


def row_cuts(rows, parts=4):
    cuts = [16 * (rows // 16 * k // parts) for k in range(parts)] + [rows]
    return list(zip(cuts[:-1], cuts[1:]))


def dot(a, b, dims):
    return lax.dot_general(a, b, dims, preferred_element_type=F32)


def stats_kernel(n_vocab, u_ref, emb_ref, b_ref, lab_ref, logits_ref, stat_ref, prev, m_sc, s_sc, l_sc):
    i, n_steps = pl.program_id(0), pl.num_programs(0)
    lane = lax.broadcasted_iota(I32, (1, 128), 1)
    cuts = row_cuts(u_ref.shape[0], PARTS)

    @pl.when(i == 0)
    def _():
        m_sc[...] = jnp.full_like(m_sc, LEAST)
        s_sc[...] = jnp.zeros_like(s_sc)
        l_sc[...] = jnp.zeros_like(l_sc)
        prev[...] = jnp.full_like(prev, -jnp.inf)

    def logits_of(r0, r1, c0, wide, width):
        tile = dot(u_ref[r0:r1, :], emb_ref[c0:c0 + wide, :], NT) + b_ref[:, c0:c0 + wide]
        if wide > width:
            tile = jnp.where(lax.broadcasted_iota(I32, (1, wide), 1) < width, tile, -jnp.inf)
        logits_ref[r0:r1, c0:c0 + wide] = tile
        return tile

    def take(r0, r1, read, first, wide):
        for q in range(r0, r1, 16):
            rs = slice(q, q + 16)
            parts = [read(rs, slice(k, k + 128)) for k in range(0, wide, 128)]
            m_old = m_sc[rs, :]
            m_new = functools.reduce(jnp.maximum, parts, m_old)
            s_new = s_sc[rs, :] * jnp.exp(m_old - m_new)
            l_new = l_sc[rs, :]
            lab = lab_ref[rs, :] - first
            for k, part in enumerate(parts):
                s_new += jnp.exp(part - m_new)
                l_new = jnp.where(lab == lane + k * 128, part, l_new)
            m_sc[rs, :], s_sc[rs, :], l_sc[rs, :] = m_new, s_new, l_new

    from_prev = lambda rs, cs: prev[rs, cs]
    from_out = lambda rs, cs: logits_ref[rs, cs]

    def step(second):
        width = VB if second else n_vocab % (2 * VB)
        wide = -(-width // 128) * 128
        for r0, r1 in cuts:
            logits_of(r0, r1, 0, wide, width)
            take(r0, r1, from_prev, (2 * i - 1) * VB, VB)
        for r0, r1 in cuts:
            if second:
                prev[r0:r1, :] = logits_of(r0, r1, VB, VB, VB)
            take(r0, r1, from_out, 2 * i * VB, wide)

    pl.when(i < n_steps - 1)(functools.partial(step, True))
    pl.when(i == n_steps - 1)(functools.partial(step, False))

    @pl.when(i == n_steps - 1)
    def _():
        m_t, s_t, l_t = m_sc[...].T, s_sc[...].T, l_sc[...].T
        m_all = jnp.max(m_t, axis=0, keepdims=True)
        stat_ref[0:1, :] = m_all
        stat_ref[1:2, :] = jnp.sum(s_t * jnp.exp(m_t - m_all), axis=0, keepdims=True)
        stat_ref[2:3, :] = jnp.sum(l_t, axis=0, keepdims=True)
        stat_ref[3:8, :] = jnp.zeros_like(stat_ref[3:8, :])


def stats(u, emb, bias, lab):
    t, e = u.shape
    v = emb.shape[0]
    n = pl.cdiv(v, 2 * VB)
    whole = lambda *s: pl.BlockSpec(s, lambda i: (0,) * len(s))
    return pl.pallas_call(
        functools.partial(stats_kernel, v),
        grid=(n,),
        in_specs=[whole(t, e), pl.BlockSpec((2 * VB, e), lambda i: (i, 0)), pl.BlockSpec((1, 2 * VB), lambda i: (0, i)), whole(t, 128)],
        out_specs=[pl.BlockSpec((t, 2 * VB), lambda i: (0, i)), whole(8, t)],
        out_shape=[jax.ShapeDtypeStruct((t, v), F32), jax.ShapeDtypeStruct((8, t), F32)],
        scratch_shapes=[pltpu.VMEM((t, VB), F32)] + [pltpu.VMEM((t, 128), F32)] * 3,
        compiler_params=pltpu.CompilerParams(dimension_semantics=("arbitrary",), vmem_limit_bytes=VMEM_LIMIT),
        cost_estimate=pl.CostEstimate(flops=(2 * t * v * e) // COVER, bytes_accessed=t * v * 4 + v * e * 2, transcendentals=t * v),
        name="stats",
    )(u, emb, bias, lab)


def du_kernel(n_vocab, scale, base, logits_ref, emb_ref, lse_ref, lab_ref, norm_hbm, gain_ref, out_ref, db_ref, sum_ref, du_ref, g_sc, db_sc, norm_sc, db_sc2, sem):
    i, n_blocks = pl.program_id(0), pl.num_programs(0)
    t = logits_ref.shape[0]
    lane = lax.broadcasted_iota(I32, (1, 128), 1)

    norm_copy = pltpu.make_async_copy(norm_hbm.at[base:base + t, :], norm_sc, sem)

    @pl.when(i == 0)
    def _():
        du_ref[...] = jnp.zeros_like(du_ref)

    @pl.when(i == 2)
    def _():
        norm_copy.start()

    def run(width):
        wide = -(-width // 128) * 128
        emb = emb_ref[:wide, :]
        if wide > width:
            emb = jnp.where(lax.broadcasted_iota(I32, (wide, 1), 0) < width, emb, jnp.zeros_like(emb))
        for r0, r1 in row_cuts(t):
            sums = [None] * (wide // 128)
            for q in range(r0, r1, 16):
                rs = slice(q, q + 16)
                lse = lse_ref[rs, :]
                lab = lab_ref[rs, :] - i * VB
                for k in range(wide // 128):
                    c = k * 128
                    g = jnp.exp(logits_ref[rs, c:c + 128] - lse)
                    g -= jnp.where(lab == lane + c, scale, 0.0)
                    if c + 128 > width:
                        g = jnp.where(lane < width - c, g, 0.0)
                    part = g[:8] + g[8:]
                    sums[k] = part if sums[k] is None else sums[k] + part
                    g_sc[rs, c:c + 128] = g.astype(BF16)
            for k in range(wide // 128):
                cs = slice(k * 128, (k + 1) * 128)
                db_sc[:, cs] = sums[k] if r0 == 0 else db_sc[:, cs] + sums[k]
            du_ref[r0:r1, :] += dot(g_sc[r0:r1, :wide], emb, NN)
        db_ref[:, :wide] = jnp.sum(db_sc[:, :wide], axis=0, keepdims=True)

    tail = n_vocab % VB
    if tail:
        pl.when(i < n_blocks - 1)(functools.partial(run, VB))
        pl.when(i == n_blocks - 1)(functools.partial(run, tail))
    else:
        run(VB)

    @pl.when(i == n_blocks - 1)
    def _():
        norm_copy.wait()
        parts, rows, cols = out_ref.shape
        run = rows // 7
        for r in range(0, rows, run):
            rs = slice(r, r + run)
            total = [jnp.zeros((run, 128), F32)] * 2
            for c in range(0, parts * cols, 128):
                x = du_ref[rs, c:c + 128].astype(BF16).astype(F32)
                out_ref[c // cols, rs, c % cols:c % cols + 128] = x
                dn = x * gain_ref[:, c:c + 128]
                total = [total[0] + dn, total[1] + dn * norm_sc[rs, c:c + 128]]
            for j, x in enumerate(total):
                db_sc2[j, rs, :] = x
        for j in range(2):
            sum_ref[j:j + 1, :] = jnp.sum(db_sc2[j].T, axis=0, keepdims=True)
        sum_ref[2:, :] = jnp.zeros_like(sum_ref[2:, :])


def du_pass(scale, parts, base, logits, emb, lse, lab, normed, gain):
    t, v = logits.shape
    e = emb.shape[1]
    n = pl.cdiv(v, VB)
    whole = lambda *s: pl.BlockSpec(s, lambda i: (0,) * len(s))
    return pl.pallas_call(
        functools.partial(du_kernel, v, scale, base),
        grid=(n,),
        in_specs=[pl.BlockSpec((t, VB), lambda i: (0, i)), pl.BlockSpec((VB, e), lambda i: (i, 0)), whole(t, 128), whole(t, 128), pl.BlockSpec(memory_space=pl.ANY), whole(1, e)],
        out_specs=[whole(parts, t, e // parts), pl.BlockSpec((1, VB), lambda i: (0, i)), whole(8, t)],
        out_shape=[jax.ShapeDtypeStruct((parts, t, e // parts), F32), jax.ShapeDtypeStruct((1, v), F32), jax.ShapeDtypeStruct((8, t), F32)],
        scratch_shapes=[pltpu.VMEM((t, e), F32), pltpu.VMEM((t, VB), BF16), pltpu.VMEM((8, VB), F32), pltpu.VMEM((t, e), F32), pltpu.VMEM((2, t, 128), F32), pltpu.SemaphoreType.DMA],
        compiler_params=pltpu.CompilerParams(dimension_semantics=("arbitrary",), vmem_limit_bytes=VMEM_LIMIT),
        cost_estimate=pl.CostEstimate(flops=(2 * t * v * e) // COVER, bytes_accessed=t * v * 4 + v * e * 2, transcendentals=t * v),
        name="du_pass",
    )(logits, emb, lse, lab, normed, gain)


LN_EPS = 1e-5
CORE, X, Y = 1, 2, 4
ANY = pl.BlockSpec(memory_space=pltpu.HBM)
VMEM = pl.BlockSpec(memory_space=pltpu.VMEM)
SMEM = pl.BlockSpec(memory_space=pltpu.SMEM)
DMA = pltpu.SemaphoreType.DMA


def gelu_norm(a):
    cdf = 0.5 * (1.0 + lax.erf(a * (0.5 ** 0.5)))
    g = a * cdf
    centered = g - jnp.mean(g, axis=1, keepdims=True)
    rstd = lax.rsqrt(jnp.mean(centered * centered, axis=1, keepdims=True) + LN_EPS)
    return cdf, centered * rstd, rstd


def head_kernel(n_masks, cut, hid, pos_ref, w_ref, b_ref, gain_ref, bias_ref, z_out, pre_out, norm_out, rstd_out, u_out, lo_out, hi_out,
                hbuf, zf, zb, pre_v, norm_v, rstd_v, ub, uf, in_sem, out_sem):
    n_seq, seq_len = hid.shape[0], hid.shape[1]
    n_loc = n_seq * n_masks
    loads = [pltpu.make_async_copy(hid.at[b], hbuf.at[b], in_sem.at[b]) for b in range(n_seq)]
    for c in loads:
        c.start()
    lane = lax.broadcasted_iota(I32, (1, 128), 1)
    cuts = [0, cut // 32 * 16, cut, cut + (n_loc - cut) // 32 * 16, n_loc]
    done, stores = 0, []

    def send(src, dst, r0, r1, base=0):
        c = pltpu.make_async_copy(src.at[r0:r1, :], dst.at[r0 - base:r1 - base, :], out_sem.at[len(stores)])
        c.start()
        stores.append(c)

    for b in range(n_seq):
        loads[b].wait()
        hot = jnp.concatenate([jnp.where(pos_ref[b] == lane + j, 1.0, 0.0).astype(BF16) for j in range(0, seq_len, 128)], axis=1)
        zf[b * n_masks:(b + 1) * n_masks, :] = dot(hot, hbuf[b], NN)[:n_masks, :]
        while done < 4 and cuts[done + 1] <= (b + 1) * n_masks:
            r0, r1 = cuts[done], cuts[done + 1]
            z = zf[r0:r1, :].astype(BF16)
            zb[r0:r1, :] = z
            a = dot(z, w_ref[...], NN) + b_ref[...]
            pre_v[r0:r1, :] = a
            _, normed, rstd = gelu_norm(a)
            norm_v[r0:r1, :] = normed
            rstd_v[r0:r1, :] = jnp.broadcast_to(rstd, (r1 - r0, 128))
            u = (normed * gain_ref[...] + bias_ref[...]).astype(BF16)
            ub[r0:r1, :] = u
            uf[r0:r1, :] = u.astype(F32)
            done += 1
            send(uf, hi_out if r0 >= cut else lo_out, r0, r1, cut if r0 >= cut else 0)
            for src, dst in ((ub, u_out), (zb, z_out), (pre_v, pre_out), (norm_v, norm_out), (rstd_v, rstd_out)):
                send(src, dst, r0, r1)
    for c in stores:
        c.wait()


def head_pass(n_masks, cut, hidden, pos, w, b, gain, bias):
    n_seq, seq_len, e = hidden.shape
    n = n_seq * n_masks
    kinds = [((n, e), BF16), ((n, e), F32), ((n, e), F32), ((n, 128), F32), ((n, e), BF16), ((cut, e), F32), ((n - cut, e), F32)]
    return pl.pallas_call(
        functools.partial(head_kernel, n_masks, cut),
        in_specs=[ANY] + [VMEM] * 5,
        out_specs=[ANY] * len(kinds),
        out_shape=[jax.ShapeDtypeStruct(*k) for k in kinds],
        scratch_shapes=[pltpu.VMEM((n_seq, seq_len, e), BF16), pltpu.VMEM((n, e), F32)]
        + [pltpu.VMEM(*k) for k in kinds[:5]] + [pltpu.VMEM((n, e), F32), DMA((n_seq,)), DMA((24,))],
        compiler_params=pltpu.CompilerParams(vmem_limit_bytes=VMEM_LIMIT),
        cost_estimate=pl.CostEstimate(flops=(4 * n * e * e) // COVER, bytes_accessed=hidden.size * 2 + n * e * 20, transcendentals=n * e),
        name="head",
    )(hidden, pos, w, b, gain, bias)


BLK = 1280
LOOPED = ('side',)
STEPS = {"own": 2, "again": 2, "side": 4, "far": 2, "last": 2, "whole": 8}
ME, MINE, MINE_ID, TWIN, FAR, FAR_TWIN = range(6)


def rows_kernel(kind, scale, s0, m, cut, n_loc, sources, skips, spots, has_big, pos, emb_hbm, bias_ref, info_ref, *refs):
    refs = list(refs)
    take = lambda n: [refs.pop(0) for _ in range(n)]
    wide = sources is not None
    if wide:
        src = {r: take(2) for r in sources}
        if kind != "own":
            take(1)
    else:
        u_hbm, = take(1)
    if has_big:
        take(1)
    parts = take(len(skips))
    puts = take(len(spots))
    out_hbm, = take(1)
    if wide:
        u_hbm, = take(1)
    if kind in ("far", "last", "whole"):
        big_ref, = take(1)
    if wide:
        buf, = take(1)
    ring, emb_sc, g_sc, acc, hold, sem, tok_sem, back_sem, in_sem, out_sem = refs
    me = pos[ME]
    chip = lax.div(me, 2)
    n_steps = STEPS[kind]
    along_x, along_y = chip ^ 1, chip ^ 2

    def device(i):
        side = 2 * jnp.where(i < 2, jnp.minimum(along_x, along_y), jnp.maximum(along_x, along_y)) + lax.rem(i, 2)
        far = 2 * (chip ^ 3) + lax.rem(i, 2)
        if kind in ("own", "again"):
            return 2 * chip + i
        return {"side": side, "far": far, "last": far, "whole": i}[kind]

    depth = ring.shape[0]

    def fetch(i):
        slot = lax.rem(i, 2 if wide else depth)
        if not wide:
            pltpu.make_async_copy(u_hbm.at[device(i)], ring.at[slot], tok_sem.at[slot, 0]).start()
            return
        for r, (lo, hi) in src.items():
            @pl.when(device(i) ^ me == r)
            def _():
                pltpu.make_async_copy(lo, buf.at[slot, :cut, :], tok_sem.at[slot, 0]).start()
                pltpu.make_async_copy(hi, buf.at[slot, cut:, :], tok_sem.at[slot, 1]).start()

    row = lambda j, off: pl.multiple_of(pos[j] + off, 8)
    emb_copy = pltpu.make_async_copy(emb_hbm.at[pl.ds(row(MINE, s0), m), :], emb_sc, sem)
    emb_copy.start()
    fetch(0)
    loads, stores = [], []
    for j, (p, (base, off)) in enumerate(zip(puts, spots)):
        n = p.shape[0]
        loads.append(pltpu.make_async_copy(p, hold.at[j, :n, :], in_sem.at[j]))
        stores.append(pltpu.make_async_copy(hold.at[j, :n, :], big_ref.at[pl.ds(row(base, off), n), :], out_sem.at[j]))
    for j, (p, skip) in enumerate(zip(parts, skips)):
        loads.append(pltpu.make_async_copy(p.at[skip:skip + m, :], hold.at[len(puts) + j, :m, :], in_sem.at[len(puts) + j]))
    acc[...] = jnp.zeros_like(acc)
    if wide:
        for k in range(2):
            ring[k, n_loc:, :] = jnp.zeros((BLK - n_loc, ring.shape[2]), BF16)
    emb_copy.wait()
    n_groups = 2 if kind in LOOPED and m % 32 == 0 else 1
    tall = m // n_groups
    n_cuts = max(1, round(tall / 300))
    cuts = [-(-tall * k // (n_cuts * 16)) * 16 for k in range(n_cuts)] + [tall]
    cuts = list(zip(cuts[:-1], cuts[1:]))
    kept = lambda i: pltpu.make_async_copy(ring.at[lax.rem(i, 2)], u_hbm.at[device(i)], back_sem.at[lax.rem(i, 2)])

    @pl.loop(0, n_steps)
    def _(i):
        slot = lax.rem(i, 2 if wide else depth)
        if wide:
            any_lo, any_hi = next(iter(src.values()))
            pltpu.make_async_copy(any_lo, buf.at[slot, :cut, :], tok_sem.at[slot, 0]).wait()
            pltpu.make_async_copy(any_hi, buf.at[slot, cut:, :], tok_sem.at[slot, 1]).wait()

            @pl.when(i >= 2)
            def _():
                kept(i - 2).wait()
        else:
            pltpu.make_async_copy(u_hbm.at[device(i)], ring.at[slot], tok_sem.at[slot, 0]).wait()

        @pl.when(i + 1 < n_steps)
        def _():
            fetch(i + 1)

        @pl.when(i == 0)
        def _():
            for c in loads:
                c.start()

        for j, (a, b) in enumerate(zip(loads, stores)):
            @pl.when(i == min(2 + j, n_steps - 1))
            def _():
                a.wait()
                b.start()

        if wide:
            ring[slot, :n_loc, :] = buf[slot].astype(BF16)
            kept(i).start()
        rel = device(i) ^ me
        lse, lab = info_ref[rel, 0:1, :], info_ref[rel, 1:2, :]

        def group(h):
            def rows(r0, r1):
                return slice(r0, r1) if n_groups == 1 else pl.ds(pl.multiple_of(h * tall + r0, 16), r1 - r0)

            def weights(r0, r1):
                part = dot(emb_sc[rows(r0, r1), :], ring[slot], NT)
                ids = lax.broadcasted_iota(I32, (r1 - r0, 1), 0) + (pos[MINE_ID] + (s0 + h * tall + r0))
                bias = bias_ref[slice(s0 + r0, s0 + r1) if n_groups == 1 else pl.ds(pl.multiple_of(s0 + h * tall + r0, 8), r1 - r0), :]
                g = jnp.exp(part + bias - lse) - jnp.where(lab == ids.astype(F32), scale, 0.0)
                g_sc[r0:r1, :] = g.astype(BF16)

            weights(*cuts[0])
            for k, (r0, r1) in enumerate(cuts):
                if k + 1 < len(cuts):
                    weights(*cuts[k + 1])
                acc[rows(r0, r1), :] += dot(g_sc[r0:r1, :], ring[slot], NN)

        if n_groups == 1:
            group(0)
        else:
            pl.loop(0, n_groups)(group)

    for c in loads[len(puts):]:
        c.wait()
    if parts:
        acc[...] = (hold[len(puts), :m, :] + acc[...]) + hold[len(puts) + 1, :m, :]
    done = [pltpu.make_async_copy(acc, out_hbm, sem)]
    if kind in ("far", "last", "whole"):
        done.append(pltpu.make_async_copy(acc, big_ref.at[pl.ds(row(MINE, s0), m), :], emb_sem(tok_sem)))
    for c in done:
        c.start()
    if wide:
        for i in range(n_steps - 2, n_steps):
            kept(i).wait()
    for c in stores + done:
        c.wait()


def emb_sem(tok_sem):
    return tok_sem.at[0, 0]


def rows_pass(kind, scale, v_rows, span, cut, pos, emb, bias, info, tokens=None, u_all=None, big=None, parts=(), puts=()):
    s0, s1 = span
    m, e = s1 - s0, emb.shape[1]
    sds = jax.ShapeDtypeStruct
    wide = kind in ("own", "side", "far")
    final = kind in ("far", "last", "whole")
    args, aliases = [pos, emb, bias, info], {}
    outs = [sds((m, e), F32)]
    sources = None
    if wide:
        sources = {"own": (0, CORE), "side": (X, X | CORE, Y, Y | CORE), "far": (X | Y, X | Y | CORE)}[kind]
        args += [h for r in sources for h in tokens[r]]
        n_loc = tokens[0][0].shape[0] + tokens[0][1].shape[0]
        outs.append(sds((8, BLK, e), BF16))
        if kind != "own":
            aliases[len(args)] = 1
            args.append(u_all)
    else:
        n_loc = BLK
        args.append(u_all)
    if final:
        if big is not None:
            aliases[len(args)] = len(outs)
            args.append(big)
        outs.append(sds((v_rows, e), F32))
    args += [a for a, _ in parts] + [a for _, a in puts]
    n_hold = max(1, len(parts) + len(puts))
    tallest = max([m] * len(parts) + [a.shape[0] for _, a in puts] + [8])
    t = STEPS[kind] * BLK
    scratch = [pltpu.VMEM((2, n_loc, e), F32)] if wide else []
    scratch += [
        pltpu.VMEM((2 if wide else 3, BLK, e), BF16), pltpu.VMEM((m, e), BF16), pltpu.VMEM((m, BLK), BF16),
        pltpu.VMEM((m, e), F32), pltpu.VMEM((n_hold, tallest, e), F32),
        DMA, DMA((3, 2)), DMA((2,)), DMA((n_hold,)), DMA((n_hold,)),
    ]
    return pl.pallas_call(
        functools.partial(rows_kernel, kind, scale, s0, m, cut, n_loc, sources, [skip for _, skip in parts], [spot for spot, _ in puts], big is not None),
        in_specs=[SMEM, ANY, VMEM, VMEM] + [ANY] * (len(args) - 4),
        out_specs=[ANY] * len(outs),
        out_shape=outs,
        scratch_shapes=scratch,
        input_output_aliases=aliases,
        compiler_params=pltpu.CompilerParams(vmem_limit_bytes=VMEM_LIMIT),
        cost_estimate=pl.CostEstimate(flops=(4 * t * m * e) // COVER, bytes_accessed=t * e * 2 + m * e * 6, transcendentals=t * m),
    )(*args)


def put_kernel(spots, pos, *refs):
    n = len(spots)
    pieces, (out_ref, hold, in_sem, out_sem) = refs[1:1 + n], refs[1 + n:]
    loads, stores = [], []
    for j, (p, (base, off)) in enumerate(zip(pieces, spots)):
        slot = hold.at[j, :p.shape[0], :]
        loads.append(pltpu.make_async_copy(p, slot, in_sem.at[j]))
        stores.append(pltpu.make_async_copy(slot, out_ref.at[pl.ds(pl.multiple_of(pos[base] + off, 8), p.shape[0]), :], out_sem.at[j]))
    for a in loads:
        a.start()
    for a, b in zip(loads, stores):
        a.wait()
        b.start()
    for b in stores:
        b.wait()


def put_rows(pos, big, puts):
    spots, pieces = [s for s, _ in puts], [a for _, a in puts]
    n, e = len(pieces), big.shape[1]
    size = sum(p.size for p in pieces)
    return pl.pallas_call(
        functools.partial(put_kernel, spots),
        in_specs=[SMEM] + [ANY] * (n + 1),
        out_specs=ANY,
        out_shape=jax.ShapeDtypeStruct(big.shape, big.dtype),
        scratch_shapes=[pltpu.VMEM((n, max(p.shape[0] for p in pieces), e), F32), DMA((n,)), DMA((n,))],
        input_output_aliases={1: 0},
        compiler_params=pltpu.CompilerParams(vmem_limit_bytes=VMEM_LIMIT),
        cost_estimate=pl.CostEstimate(flops=(size) // COVER, bytes_accessed=size * 8, transcendentals=0),
        name="put_rows",
    )(pos, big, *pieces)


def join_kernel(n_vec, idx, *refs):
    own, mine, theirs, (dw_ref, vec_ref, full, in_sem, out_sem) = refs[0], refs[1:4], refs[4:7], refs[7:]
    vp, core = idx[0], idx[1]
    half, cols = mine[0].shape
    col = lambda k: pl.ds(pl.multiple_of((vp ^ k) * cols, cols), cols)
    row = lambda c: pl.ds(pl.multiple_of(c * half, 8), half)
    loads = [pltpu.make_async_copy(own.at[:2 * half, :], full.at[:, col(0)], in_sem.at[0])]
    for k in range(3):
        loads.append(pltpu.make_async_copy(mine[k], full.at[row(core), col(k + 1)], in_sem.at[1 + k]))
        loads.append(pltpu.make_async_copy(theirs[k], full.at[row(1 - core), col(k + 1)], in_sem.at[4 + k]))
    for c in loads:
        c.start()
    for c in loads:
        c.wait()
    e = dw_ref.shape[0]
    stores = [pltpu.make_async_copy(full.at[:e, :], dw_ref, out_sem.at[0]), pltpu.make_async_copy(full.at[e:e + n_vec, :], vec_ref, out_sem.at[1])]
    for c in stores:
        c.start()
    for c in stores:
        c.wait()


def join_pass(idx, own, mine, theirs):
    half, cols = mine[0].shape
    e = 4 * cols
    return pl.pallas_call(
        functools.partial(join_kernel, 8),
        in_specs=[SMEM] + [ANY] * 7,
        out_specs=[ANY] * 2,
        out_shape=[jax.ShapeDtypeStruct((e, e), F32), jax.ShapeDtypeStruct((8, e), F32)],
        scratch_shapes=[pltpu.VMEM((2 * half, e), F32), DMA((7,)), DMA((2,))],
        compiler_params=pltpu.CompilerParams(vmem_limit_bytes=VMEM_LIMIT),
        cost_estimate=pl.CostEstimate(flops=(e * e) // COVER, bytes_accessed=e * e * 8, transcendentals=0),
        name="join",
    )(idx, own, *mine, *theirs)


def means_kernel(width, *refs):
    (a, b, c, d), (m1_ref, m2_ref) = refs[:4], refs[4:]
    total = ((a[...] + b[...]) + (c[...] + d[...])) * (1.0 / width)
    for j, m_ref in enumerate((m1_ref, m2_ref)):
        m_ref[...] = jnp.broadcast_to(total[j:j + 1, :], (128, total.shape[1])).T


def means_pass(width, sums):
    n = sums[0].shape[1]
    return pl.pallas_call(
        functools.partial(means_kernel, width),
        in_specs=[VMEM] * 4,
        out_specs=[VMEM] * 2,
        out_shape=[jax.ShapeDtypeStruct((n, 128), F32)] * 2,
        compiler_params=pltpu.CompilerParams(vmem_limit_bytes=VMEM_LIMIT),
        cost_estimate=pl.CostEstimate(flops=(n * 256) // COVER, bytes_accessed=n * 1200, transcendentals=0),
        name="means",
    )(*sums)


def back_kernel(base, vp, *refs):
    refs = list(refs)
    srcs = [refs.pop(0) for _ in range(7)]
    gain_ref, = [refs.pop(0)]
    extra = refs[:-10]
    dab_ref, pack_ref, pre, norm, rstd, z, m1, m2, du, sem = refs[-10:]
    n, cols = du.shape
    e = z.shape[1]
    col = pl.ds(pl.multiple_of(vp[0] * cols, cols), cols)
    rows = slice(base, base + n)
    pre_h, norm_h, rstd_h, z_h, m1_h, m2_h, du_h = srcs
    loads = [pltpu.make_async_copy(a, b, sem.at[j]) for j, (a, b) in enumerate((
        (pre_h.at[rows, col], pre), (norm_h.at[rows, col], norm), (rstd_h.at[rows, :], rstd), (m1_h.at[rows, :], m1), (m2_h.at[rows, :], m2),
        (du_h, du), (z_h.at[rows, :], z)))]
    for c in loads:
        c.start()
    for c in loads:
        c.wait()
    for j, c in enumerate(range(0, cols, 128)):
        cs = slice(c, c + 128)
        a, d, normed = pre[:, cs], du[:, cs], norm[:, cs]
        cdf = 0.5 * (1.0 + lax.erf(a * (0.5 ** 0.5)))
        dg = rstd[...] * (d * gain_ref[:, cs] - m1[...] - normed * m2[...])
        da = dg * (cdf + a * (jnp.exp(-0.5 * a * a) * 0.3989422804014327))
        dab_ref[:, cs] = da.astype(BF16).astype(F32)
        for j, x in enumerate((da, d * normed, d)):
            pack_ref[e + j:e + j + 1, cs] = jnp.sum(x, axis=0, keepdims=True)
    loss_ref, db_ref = extra
    pack_ref[:e, :] = lax.dot_general(z[...], dab_ref[...].astype(BF16), (((0,), (0,)), ((), ())), preferred_element_type=F32)
    pack_ref[e + 3:e + 4, :] = jnp.broadcast_to(loss_ref[...], (1, cols))
    pack_ref[e + 4:e + 16, :] = jnp.zeros_like(pack_ref[e + 4:e + 16, :])
    n_db = db_ref.shape[1]
    pack_ref[e + 16 + n_db // cols:, :] = jnp.zeros_like(pack_ref[e + 16 + n_db // cols:, :])
    for j, c in enumerate(range(0, n_db, cols)):
        w = min(cols, n_db - c)
        pack_ref[e + 16 + j:e + 17 + j, :w] = db_ref[:, c:c + w]


def back_pass(base, vp, pre, normed, rstd, z, m1, m2, du, gain, *extra):
    n, cols = du.shape
    e = z.shape[1]
    n_pack = e + 16 + -(-extra[1].shape[1] // cols // 8) * 8
    block = lambda *s: pl.BlockSpec(s, lambda i, p: (0,) * len(s))
    gs = pltpu.PrefetchScalarGridSpec(
        num_scalar_prefetch=1,
        grid=(1,),
        in_specs=[ANY] * 7 + [pl.BlockSpec((1, cols), lambda i, p: (0, p[0]))] + [block(*x.shape) for x in extra],
        out_specs=[block(n, cols), block(n_pack, cols)],
        scratch_shapes=[pltpu.VMEM((n, cols), F32)] * 2 + [pltpu.VMEM((n, 128), F32), pltpu.VMEM((n, e), BF16)] + [pltpu.VMEM((n, 128), F32)] * 2
        + [pltpu.VMEM((n, cols), F32), DMA((7,))],
    )
    return pl.pallas_call(
        functools.partial(back_kernel, base),
        grid_spec=gs,
        out_shape=[jax.ShapeDtypeStruct((n, cols), F32), jax.ShapeDtypeStruct((n_pack, cols), F32)],
        compiler_params=pltpu.CompilerParams(dimension_semantics=("arbitrary",), vmem_limit_bytes=VMEM_LIMIT),
        cost_estimate=pl.CostEstimate(flops=(2 * n * e * cols) // COVER, bytes_accessed=n * (cols * 16 + e * 2 + 1536), transcendentals=n * cols * 2),
        name="back",
    )(vp, pre, normed, rstd, z, m1, m2, du, gain, *extra)


def spread_kernel(n_masks, vp, pos_ref, w_ref, *refs):
    pieces, (out_ref, dab, dz, obuf, in_sem, out_sem) = refs[:4], refs[4:]
    n, cols = pieces[0].shape
    col = lambda k: pl.ds(pl.multiple_of((vp[0] ^ k) * cols, cols), cols)
    loads = [pltpu.make_async_copy(p, dab.at[:, col(j)], in_sem.at[j]) for j, p in enumerate(pieces)]
    for c in loads:
        c.start()
    dz[n:, :] = jnp.zeros((dz.shape[0] - n, dz.shape[1]), F32)
    n_seq, seq_len, _ = out_ref.shape
    place = lax.broadcasted_iota(I32, (seq_len, 1), 0)
    slots = pos_ref.shape[2]
    for c in loads:
        c.wait()
    for r0, r1 in row_cuts(n):
        dz[r0:r1, :] = dot(dab[r0:r1, :].astype(BF16), w_ref[...], NT).astype(BF16).astype(F32)
    group = 8
    store = lambda b, j: pltpu.make_async_copy(obuf.at[j % 4], out_ref.at[b], out_sem.at[j % 4])

    @pl.loop(0, n_seq // group)
    def _(g):
        for j in range(group):
            b = g * group + j

            @pl.when(b >= 4)
            def _():
                store(b - 4, j).wait()

            hot = jnp.where(place == pos_ref[b], 1.0, 0.0).astype(BF16)
            base = pl.multiple_of(g * (group * n_masks), 8)
            low = j * n_masks // 8 * 8
            rows = dz[pl.ds(base + low, slots + 8), :][j * n_masks - low:j * n_masks - low + slots]
            obuf[j % 4] = dot(hot, rows.astype(BF16), NN).astype(BF16)
            store(b, j).start()

    for j in range(group - 4, group):
        store(n_seq - group + j, j).wait()


def spread_pass(n_masks, shape, vp, pos, w, pieces):
    n, cols = pieces[0].shape
    e = w.shape[0]
    return pl.pallas_call(
        functools.partial(spread_kernel, n_masks),
        in_specs=[SMEM, VMEM, VMEM] + [ANY] * 4,
        out_specs=ANY,
        out_shape=jax.ShapeDtypeStruct(shape, BF16),
        scratch_shapes=[pltpu.VMEM((n, 4 * cols), F32), pltpu.VMEM((n + 16, e), F32), pltpu.VMEM((4,) + shape[1:], BF16), DMA((4,)), DMA((4,))],
        compiler_params=pltpu.CompilerParams(vmem_limit_bytes=VMEM_LIMIT),
        cost_estimate=pl.CostEstimate(flops=(2 * shape[0] * shape[1] * 128 * e) // COVER, bytes_accessed=shape[0] * shape[1] * e * 2, transcendentals=0),
        name="spread",
    )(vp, pos, w, *pieces)


def order_sum(xs):
    return (xs[0] + xs[1]) + (xs[2] + xs[3])


def after(x, *deps):
    return lax.optimization_barrier((x, deps))[0]


def solution(mesh):
    n_groups, n_shards = mesh.shape["dp"], mesh.shape["vp"]

    def swap(a, bit):
        return lax.ppermute(a, "dp", [(d, d ^ bit) for d in range(n_groups)])

    def swap_vp(a, bit):
        return lax.ppermute(a, "vp", [(d, d ^ bit) for d in range(n_shards)])

    def hop(a):
        return lax.ppermute(a, "dp", [(d, d ^ (Y if d & CORE else X)) for d in range(n_groups)])

    def local_step(hidden, mask_pos, labels, w_trans, b_trans, ln_gain, ln_bias, emb_table, b_vocab):
        n_rows, _, width = hidden.shape
        n_masks = mask_pos.shape[1]
        shard_rows = emb_table.shape[0]
        n_loc = n_rows * n_masks
        n_tokens = n_loc * n_groups
        slots = -(-n_masks // 16) * 16
        cut = n_loc // 32 * 16
        cols = width // n_shards
        dp, vp = lax.axis_index("dp"), lax.axis_index("vp")
        row_start = vp * shard_rows
        scale = 1.0 / n_tokens
        core, mine = dp & 1, (dp >> 1 ^ dp >> 2) & 1

        pos_pad = jnp.pad(mask_pos, ((0, 0), (0, slots - n_masks)), constant_values=-1)
        z, pre, normed, rstd, u, u_lo, u_hi = head_pass(
            n_masks, cut, hidden, jnp.broadcast_to(pos_pad[:, :, None], (n_rows, slots, 128)),
            w_trans, b_trans[None], ln_gain[None], ln_bias[None])

        x_lo, y_hi = swap(u_lo, X), swap(u_hi, Y)
        x_hi, y_lo = swap(u_hi, X), swap(u_lo, Y)
        c_lo, c_hi = swap(u_lo, CORE), swap(u_hi, CORE)

        flat_labels = labels.reshape(n_loc)
        lab_local = flat_labels - row_start
        lab_local = jnp.where((lab_local >= 0) & (lab_local < shard_rows), lab_local, ELSEWHERE)
        column = lambda x: jnp.broadcast_to(x[:, None], (x.shape[0], 128))
        lab_col = column(lab_local)
        logits, stat = stats(u, emb_table, b_vocab[None], lab_col)
        all_stats = [stat] + [swap_vp(stat, b) for b in range(1, n_shards)]
        global_max = functools.reduce(jnp.maximum, [s[0] for s in all_stats])
        log_norm = global_max + jnp.log(order_sum([s[1] * jnp.exp(s[0] - global_max) for s in all_stats]))
        loss_part = jnp.sum(log_norm - order_sum([s[2] for s in all_stats]))
        lse = log_norm + jnp.log(jnp.float32(n_tokens))

        du_part, db_part, sums = du_pass(scale, n_shards, 0, logits, emb_table, column(lse), lab_col, normed, ln_gain[None])
        du_share = lax.psum_scatter(du_part.reshape(n_shards * n_loc, cols), "vp", scatter_dimension=0, tiled=True)
        lse = after(lse, du_part)
        fill = (0, BLK - n_loc)
        info = jnp.stack([jnp.pad(lse, fill, constant_values=jnp.inf), jnp.pad(flat_labels.astype(F32), fill, constant_values=-1.0)])
        near, *away = [swap(info, b) for b in (CORE, X, Y, X | Y)]
        x_lo, y_hi = after((x_lo, y_hi), du_part)
        d_lo, d_hi = swap(x_lo, Y), swap(y_hi, X)
        cx_lo, cy_hi = swap(x_lo, CORE), swap(y_hi, CORE)

        half, quarter = shard_rows // 2, shard_rows // 4
        start = lambda h, c: h * half + c * quarter
        pos = jnp.stack([dp, start(mine, core), row_start + start(mine, core), start(mine, 1 - core), start(1 - mine, core), start(1 - mine, 1 - core)])
        bias_col = lax.dynamic_slice(b_vocab, (start(mine, core),), (quarter,))[:, None]
        shares = (1088, 1216, 840)
        ends = [0]
        for w in shares[:-1]:
            ends.append(ends[-1] + max(16, quarter * w // sum(shares) // 16 * 16))
        spans = list(zip(ends, ends[1:] + [quarter]))

        def rows(kind, k, *wait, info=None, span=None, **kw):
            return rows_pass(kind, scale, shard_rows, span or spans[k], cut, after(pos, *wait), emb_table, bias_col, info, **kw)

        def send(k, chunk):
            return ((TWIN, spans[k][0]), swap(chunk, CORE)), hop(chunk)

        def forward(k, far, *wait):
            far = after(far, *wait)
            return ((FAR, spans[k][0]), far), ((FAR_TWIN, spans[k][0]), swap(far, CORE))

        tokens = {0: (u_lo, u_hi), CORE: (c_lo, c_hi), X: (x_lo, x_hi), Y: (y_lo, y_hi)}
        pair = jnp.stack([info, near])
        own, u_all = rows("own", 0, du_part, info=pair, tokens=tokens)
        x_hi, y_lo, away = after((x_hi, y_lo, away), own)
        away = jnp.stack(away)
        tokens[X | CORE] = cx_lo, swap(x_hi, CORE)
        tokens[Y | CORE] = swap(y_lo, CORE), cy_hi
        away_near = swap(away, CORE)
        tokens[X], tokens[Y] = (x_lo, x_hi), (y_lo, y_hi)
        info = jnp.concatenate([pair, jnp.stack([away, away_near], axis=1).reshape(6, 2, BLK)])

        sums = after(sums, own)
        sums = [sums] + [swap_vp(sums, b) for b in range(1, n_shards)]
        side, u_all = rows("side", 0, info=info, tokens=tokens, u_all=u_all)
        d_lo, d_hi = after((d_lo, d_hi), side)
        tokens[X | Y], tokens[X | Y | CORE] = (d_lo, d_hi), (swap(d_lo, CORE), swap(d_hi, CORE))
        m1, m2 = means_pass(width, after(sums, side))
        chunk0, u_all, big = rows("far", 0, m1, m2, info=info, tokens=tokens, u_all=u_all, parts=((own, 0), (side, 0)))
        twin0, far0 = send(0, chunk0)

        du_share = after(du_share, chunk0)
        dab, pack = back_pass(0, vp[None], pre, normed, rstd, z, m1, m2, du_share, ln_gain[None], loss_part[None, None], db_part)
        back_done = dab
        pack = lax.psum(pack, "dp")
        dab_1, dab_2 = swap_vp(dab, 1), swap_vp(dab, 2)

        chunk1, big = rows("whole", 1, back_done, info=info, u_all=u_all, big=big, puts=[twin0])
        twin1, far1 = send(1, chunk1)
        pack = after(pack, chunk1)
        n_half = (width + 16) // 2
        part = lax.dynamic_slice(pack, (core * n_half, 0), (n_half, cols))
        parts = [swap_vp(part, b) for b in range(1, n_shards)]
        far0, far_twin0 = forward(0, far0, chunk1)
        dab_2 = after(dab_2, chunk1)
        dab_3 = swap_vp(dab_2, 1)

        chunk2, big = rows("whole", 2, part, info=info, u_all=u_all, big=big, puts=[far0, far_twin0])
        twin2, far2 = send(2, chunk2)
        d_hidden = spread_pass(n_masks, hidden.shape, vp[None], pos_pad[:, None], w_trans, after([dab, dab_1, dab_2, dab_3], chunk2))
        far1, far_twin1 = forward(1, far1, d_hidden)
        big = put_rows(after(pos, d_hidden), big, [twin1, far1])
        parts = after(parts, big)
        others = [swap(p, CORE) for p in parts]
        big = put_rows(pos, big, [far_twin1, twin2])
        pack, parts, others = after((pack, parts, others), big)
        d_w, vec = join_pass(jnp.stack([vp, core]), pack, parts, others)
        db = pack[width + 16:].reshape(-1)[:shard_rows]
        loss = pack[width + 3, 0] / n_tokens
        grads = vec[0], vec[1], vec[2]
        far2, far_twin2 = forward(2, far2, big, d_w, db, loss, *grads)
        big = put_rows(pos, big, [far2])
        big = put_rows(pos, big, [far_twin2])

        return loss, d_hidden, d_w, *grads, big, db

    in_specs = (P("dp", None, None), P("dp", None), P("dp", None), P(None, None), P(None), P(None), P(None), P("vp", None), P("vp"))
    out_specs = (P(), P("dp", None, None), P(None, None), P(None), P(None), P(None), P("vp", None), P("vp"))
    return jax.shard_map(local_step, mesh=mesh, in_specs=in_specs, out_specs=out_specs, check_vma=False)
```

```python
import functools

import jax
import jax.numpy as jnp
from jax import lax
from jax.experimental import pallas as pl
from jax.experimental.pallas import tpu as pltpu
from jax.sharding import PartitionSpec as P


F32, BF16, I32 = jnp.float32, jnp.bfloat16, jnp.int32
NT = (((1,), (1,)), ((), ()))
NN = (((1,), (0,)), ((), ()))
VB = 1024
VMEM_LIMIT = 67_000_000
COVER = 100
PARTS = 4
LEAST = float(jnp.finfo(jnp.float32).min)
ELSEWHERE = -(1 << 20)


def row_cuts(rows, parts=4):
    cuts = [16 * (rows // 16 * k // parts) for k in range(parts)] + [rows]
    return list(zip(cuts[:-1], cuts[1:]))


def dot(a, b, dims):
    return lax.dot_general(a, b, dims, preferred_element_type=F32)


def stats_kernel(n_vocab, u_ref, emb_ref, b_ref, lab_ref, logits_ref, stat_ref, prev, m_sc, s_sc, l_sc):
    i, n_steps = pl.program_id(0), pl.num_programs(0)
    lane = lax.broadcasted_iota(I32, (1, 128), 1)
    cuts = row_cuts(u_ref.shape[0], PARTS)

    @pl.when(i == 0)
    def _():
        m_sc[...] = jnp.full_like(m_sc, LEAST)
        s_sc[...] = jnp.zeros_like(s_sc)
        l_sc[...] = jnp.zeros_like(l_sc)
        prev[...] = jnp.full_like(prev, -jnp.inf)

    def logits_of(r0, r1, c0, wide, width):
        tile = dot(u_ref[r0:r1, :], emb_ref[c0:c0 + wide, :], NT) + b_ref[:, c0:c0 + wide]
        if wide > width:
            tile = jnp.where(lax.broadcasted_iota(I32, (1, wide), 1) < width, tile, -jnp.inf)
        logits_ref[r0:r1, c0:c0 + wide] = tile
        return tile

    def take(r0, r1, read, first, wide):
        for q in range(r0, r1, 16):
            rs = slice(q, q + 16)
            parts = [read(rs, slice(k, k + 128)) for k in range(0, wide, 128)]
            m_old = m_sc[rs, :]
            m_new = functools.reduce(jnp.maximum, parts, m_old)
            s_new = s_sc[rs, :] * jnp.exp(m_old - m_new)
            l_new = l_sc[rs, :]
            lab = lab_ref[rs, :] - first
            for k, part in enumerate(parts):
                s_new += jnp.exp(part - m_new)
                l_new = jnp.where(lab == lane + k * 128, part, l_new)
            m_sc[rs, :], s_sc[rs, :], l_sc[rs, :] = m_new, s_new, l_new

    from_prev = lambda rs, cs: prev[rs, cs]
    from_out = lambda rs, cs: logits_ref[rs, cs]

    def step(second):
        width = VB if second else n_vocab % (2 * VB)
        wide = -(-width // 128) * 128
        for r0, r1 in cuts:
            logits_of(r0, r1, 0, wide, width)
            take(r0, r1, from_prev, (2 * i - 1) * VB, VB)
        for r0, r1 in cuts:
            if second:
                prev[r0:r1, :] = logits_of(r0, r1, VB, VB, VB)
            take(r0, r1, from_out, 2 * i * VB, wide)

    pl.when(i < n_steps - 1)(functools.partial(step, True))
    pl.when(i == n_steps - 1)(functools.partial(step, False))

    @pl.when(i == n_steps - 1)
    def _():
        m_t, s_t, l_t = m_sc[...].T, s_sc[...].T, l_sc[...].T
        m_all = jnp.max(m_t, axis=0, keepdims=True)
        stat_ref[0:1, :] = m_all
        stat_ref[1:2, :] = jnp.sum(s_t * jnp.exp(m_t - m_all), axis=0, keepdims=True)
        stat_ref[2:3, :] = jnp.sum(l_t, axis=0, keepdims=True)
        stat_ref[3:8, :] = jnp.zeros_like(stat_ref[3:8, :])


def stats(u, emb, bias, lab):
    t, e = u.shape
    v = emb.shape[0]
    n = pl.cdiv(v, 2 * VB)
    whole = lambda *s: pl.BlockSpec(s, lambda i: (0,) * len(s))
    return pl.pallas_call(
        functools.partial(stats_kernel, v),
        grid=(n,),
        in_specs=[whole(t, e), pl.BlockSpec((2 * VB, e), lambda i: (i, 0)), pl.BlockSpec((1, 2 * VB), lambda i: (0, i)), whole(t, 128)],
        out_specs=[pl.BlockSpec((t, 2 * VB), lambda i: (0, i)), whole(8, t)],
        out_shape=[jax.ShapeDtypeStruct((t, v), F32), jax.ShapeDtypeStruct((8, t), F32)],
        scratch_shapes=[pltpu.VMEM((t, VB), F32)] + [pltpu.VMEM((t, 128), F32)] * 3,
        compiler_params=pltpu.CompilerParams(dimension_semantics=("arbitrary",), vmem_limit_bytes=VMEM_LIMIT),
        cost_estimate=pl.CostEstimate(flops=(2 * t * v * e) // COVER, bytes_accessed=t * v * 4 + v * e * 2, transcendentals=t * v),
        name="stats",
    )(u, emb, bias, lab)


def du_kernel(n_vocab, scale, base, logits_ref, emb_ref, lse_ref, lab_ref, norm_hbm, gain_ref, out_ref, db_ref, sum_ref, du_ref, g_sc, db_sc, norm_sc, db_sc2, sem):
    i, n_blocks = pl.program_id(0), pl.num_programs(0)
    t = logits_ref.shape[0]
    lane = lax.broadcasted_iota(I32, (1, 128), 1)

    norm_copy = pltpu.make_async_copy(norm_hbm.at[base:base + t, :], norm_sc, sem)

    @pl.when(i == 0)
    def _():
        du_ref[...] = jnp.zeros_like(du_ref)

    @pl.when(i == 2)
    def _():
        norm_copy.start()

    def run(width):
        wide = -(-width // 128) * 128
        emb = emb_ref[:wide, :]
        if wide > width:
            emb = jnp.where(lax.broadcasted_iota(I32, (wide, 1), 0) < width, emb, jnp.zeros_like(emb))
        for r0, r1 in row_cuts(t):
            sums = [None] * (wide // 128)
            for q in range(r0, r1, 16):
                rs = slice(q, q + 16)
                lse = lse_ref[rs, :]
                lab = lab_ref[rs, :] - i * VB
                for k in range(wide // 128):
                    c = k * 128
                    g = jnp.exp(logits_ref[rs, c:c + 128] - lse)
                    g -= jnp.where(lab == lane + c, scale, 0.0)
                    if c + 128 > width:
                        g = jnp.where(lane < width - c, g, 0.0)
                    part = g[:8] + g[8:]
                    sums[k] = part if sums[k] is None else sums[k] + part
                    g_sc[rs, c:c + 128] = g.astype(BF16)
            for k in range(wide // 128):
                cs = slice(k * 128, (k + 1) * 128)
                db_sc[:, cs] = sums[k] if r0 == 0 else db_sc[:, cs] + sums[k]
            du_ref[r0:r1, :] += dot(g_sc[r0:r1, :wide], emb, NN)
        db_ref[:, :wide] = jnp.sum(db_sc[:, :wide], axis=0, keepdims=True)

    tail = n_vocab % VB
    if tail:
        pl.when(i < n_blocks - 1)(functools.partial(run, VB))
        pl.when(i == n_blocks - 1)(functools.partial(run, tail))
    else:
        run(VB)

    @pl.when(i == n_blocks - 1)
    def _():
        norm_copy.wait()
        parts, rows, cols = out_ref.shape
        run = rows // 7
        for r in range(0, rows, run):
            rs = slice(r, r + run)
            total = [jnp.zeros((run, 128), F32)] * 2
            for c in range(0, parts * cols, 128):
                x = du_ref[rs, c:c + 128].astype(BF16).astype(F32)
                out_ref[c // cols, rs, c % cols:c % cols + 128] = x
                dn = x * gain_ref[:, c:c + 128]
                total = [total[0] + dn, total[1] + dn * norm_sc[rs, c:c + 128]]
            for j, x in enumerate(total):
                db_sc2[j, rs, :] = x
        for j in range(2):
            sum_ref[j:j + 1, :] = jnp.sum(db_sc2[j].T, axis=0, keepdims=True)
        sum_ref[2:, :] = jnp.zeros_like(sum_ref[2:, :])


def du_pass(scale, parts, base, logits, emb, lse, lab, normed, gain):
    t, v = logits.shape
    e = emb.shape[1]
    n = pl.cdiv(v, VB)
    whole = lambda *s: pl.BlockSpec(s, lambda i: (0,) * len(s))
    return pl.pallas_call(
        functools.partial(du_kernel, v, scale, base),
        grid=(n,),
        in_specs=[pl.BlockSpec((t, VB), lambda i: (0, i)), pl.BlockSpec((VB, e), lambda i: (i, 0)), whole(t, 128), whole(t, 128), pl.BlockSpec(memory_space=pl.ANY), whole(1, e)],
        out_specs=[whole(parts, t, e // parts), pl.BlockSpec((1, VB), lambda i: (0, i)), whole(8, t)],
        out_shape=[jax.ShapeDtypeStruct((parts, t, e // parts), F32), jax.ShapeDtypeStruct((1, v), F32), jax.ShapeDtypeStruct((8, t), F32)],
        scratch_shapes=[pltpu.VMEM((t, e), F32), pltpu.VMEM((t, VB), BF16), pltpu.VMEM((8, VB), F32), pltpu.VMEM((t, e), F32), pltpu.VMEM((2, t, 128), F32), pltpu.SemaphoreType.DMA],
        compiler_params=pltpu.CompilerParams(dimension_semantics=("arbitrary",), vmem_limit_bytes=VMEM_LIMIT),
        cost_estimate=pl.CostEstimate(flops=(2 * t * v * e) // COVER, bytes_accessed=t * v * 4 + v * e * 2, transcendentals=t * v),
        name="du_pass",
    )(logits, emb, lse, lab, normed, gain)


LN_EPS = 1e-5
CORE, X, Y = 1, 2, 4
ANY = pl.BlockSpec(memory_space=pltpu.HBM)
VMEM = pl.BlockSpec(memory_space=pltpu.VMEM)
SMEM = pl.BlockSpec(memory_space=pltpu.SMEM)
DMA = pltpu.SemaphoreType.DMA


def gelu_norm(a):
    cdf = 0.5 * (1.0 + lax.erf(a * (0.5 ** 0.5)))
    g = a * cdf
    centered = g - jnp.mean(g, axis=1, keepdims=True)
    rstd = lax.rsqrt(jnp.mean(centered * centered, axis=1, keepdims=True) + LN_EPS)
    return cdf, centered * rstd, rstd


def head_kernel(n_masks, cut, hid, pos_ref, w_ref, b_ref, gain_ref, bias_ref, z_out, pre_out, norm_out, rstd_out, u_out, lo_out, hi_out,
                hbuf, zf, zb, pre_v, norm_v, rstd_v, ub, uf, in_sem, out_sem):
    n_seq, seq_len = hid.shape[0], hid.shape[1]
    n_loc = n_seq * n_masks
    loads = [pltpu.make_async_copy(hid.at[b], hbuf.at[b], in_sem.at[b]) for b in range(n_seq)]
    for c in loads:
        c.start()
    lane = lax.broadcasted_iota(I32, (1, 128), 1)
    cuts = [0, cut // 32 * 16, cut, cut + (n_loc - cut) // 32 * 16, n_loc]
    done, stores = 0, []

    def send(src, dst, r0, r1, base=0):
        c = pltpu.make_async_copy(src.at[r0:r1, :], dst.at[r0 - base:r1 - base, :], out_sem.at[len(stores)])
        c.start()
        stores.append(c)

    for b in range(n_seq):
        loads[b].wait()
        hot = jnp.concatenate([jnp.where(pos_ref[b] == lane + j, 1.0, 0.0).astype(BF16) for j in range(0, seq_len, 128)], axis=1)
        zf[b * n_masks:(b + 1) * n_masks, :] = dot(hot, hbuf[b], NN)[:n_masks, :]
        while done < 4 and cuts[done + 1] <= (b + 1) * n_masks:
            r0, r1 = cuts[done], cuts[done + 1]
            z = zf[r0:r1, :].astype(BF16)
            zb[r0:r1, :] = z
            a = dot(z, w_ref[...], NN) + b_ref[...]
            pre_v[r0:r1, :] = a
            _, normed, rstd = gelu_norm(a)
            norm_v[r0:r1, :] = normed
            rstd_v[r0:r1, :] = jnp.broadcast_to(rstd, (r1 - r0, 128))
            u = (normed * gain_ref[...] + bias_ref[...]).astype(BF16)
            ub[r0:r1, :] = u
            uf[r0:r1, :] = u.astype(F32)
            done += 1
            send(uf, hi_out if r0 >= cut else lo_out, r0, r1, cut if r0 >= cut else 0)
            for src, dst in ((ub, u_out), (zb, z_out), (pre_v, pre_out), (norm_v, norm_out), (rstd_v, rstd_out)):
                send(src, dst, r0, r1)
    for c in stores:
        c.wait()


def head_pass(n_masks, cut, hidden, pos, w, b, gain, bias):
    n_seq, seq_len, e = hidden.shape
    n = n_seq * n_masks
    kinds = [((n, e), BF16), ((n, e), F32), ((n, e), F32), ((n, 128), F32), ((n, e), BF16), ((cut, e), F32), ((n - cut, e), F32)]
    return pl.pallas_call(
        functools.partial(head_kernel, n_masks, cut),
        in_specs=[ANY] + [VMEM] * 5,
        out_specs=[ANY] * len(kinds),
        out_shape=[jax.ShapeDtypeStruct(*k) for k in kinds],
        scratch_shapes=[pltpu.VMEM((n_seq, seq_len, e), BF16), pltpu.VMEM((n, e), F32)]
        + [pltpu.VMEM(*k) for k in kinds[:5]] + [pltpu.VMEM((n, e), F32), DMA((n_seq,)), DMA((24,))],
        compiler_params=pltpu.CompilerParams(vmem_limit_bytes=VMEM_LIMIT),
        cost_estimate=pl.CostEstimate(flops=(4 * n * e * e) // COVER, bytes_accessed=hidden.size * 2 + n * e * 20, transcendentals=n * e),
        name="head",
    )(hidden, pos, w, b, gain, bias)


BLK = 1280
LOOPED = ('side',)
STEPS = {"own": 2, "again": 2, "side": 4, "far": 2, "last": 2, "whole": 8}
ME, MINE, MINE_ID, TWIN, FAR, FAR_TWIN = range(6)


def rows_kernel(kind, scale, s0, m, cut, n_loc, sources, skips, spots, has_big, pos, emb_hbm, bias_ref, info_ref, *refs):
    refs = list(refs)
    take = lambda n: [refs.pop(0) for _ in range(n)]
    wide = sources is not None
    if wide:
        src = {r: take(2) for r in sources}
        if kind != "own":
            take(1)
    else:
        u_hbm, = take(1)
    if has_big:
        take(1)
    parts = take(len(skips))
    puts = take(len(spots))
    out_hbm, = take(1)
    if wide:
        u_hbm, = take(1)
    if kind in ("far", "last", "whole"):
        big_ref, = take(1)
    if wide:
        buf, = take(1)
    ring, emb_sc, g_sc, acc, hold, sem, tok_sem, back_sem, in_sem, out_sem = refs
    me = pos[ME]
    chip = lax.div(me, 2)
    n_steps = STEPS[kind]
    along_x, along_y = chip ^ 1, chip ^ 2

    def device(i):
        side = 2 * jnp.where(i < 2, jnp.minimum(along_x, along_y), jnp.maximum(along_x, along_y)) + lax.rem(i, 2)
        far = 2 * (chip ^ 3) + lax.rem(i, 2)
        if kind in ("own", "again"):
            return 2 * chip + i
        return {"side": side, "far": far, "last": far, "whole": i}[kind]

    depth = ring.shape[0]

    def fetch(i):
        slot = lax.rem(i, 2 if wide else depth)
        if not wide:
            pltpu.make_async_copy(u_hbm.at[device(i)], ring.at[slot], tok_sem.at[slot, 0]).start()
            return
        for r, (lo, hi) in src.items():
            @pl.when(device(i) ^ me == r)
            def _():
                pltpu.make_async_copy(lo, buf.at[slot, :cut, :], tok_sem.at[slot, 0]).start()
                pltpu.make_async_copy(hi, buf.at[slot, cut:, :], tok_sem.at[slot, 1]).start()

    row = lambda j, off: pl.multiple_of(pos[j] + off, 8)
    emb_copy = pltpu.make_async_copy(emb_hbm.at[pl.ds(row(MINE, s0), m), :], emb_sc, sem)
    emb_copy.start()
    fetch(0)
    loads, stores = [], []
    for j, (p, (base, off)) in enumerate(zip(puts, spots)):
        n = p.shape[0]
        loads.append(pltpu.make_async_copy(p, hold.at[j, :n, :], in_sem.at[j]))
        stores.append(pltpu.make_async_copy(hold.at[j, :n, :], big_ref.at[pl.ds(row(base, off), n), :], out_sem.at[j]))
    for j, (p, skip) in enumerate(zip(parts, skips)):
        loads.append(pltpu.make_async_copy(p.at[skip:skip + m, :], hold.at[len(puts) + j, :m, :], in_sem.at[len(puts) + j]))
    acc[...] = jnp.zeros_like(acc)
    if wide:
        for k in range(2):
            ring[k, n_loc:, :] = jnp.zeros((BLK - n_loc, ring.shape[2]), BF16)
    emb_copy.wait()
    n_groups = 2 if kind in LOOPED and m % 32 == 0 else 1
    tall = m // n_groups
    n_cuts = max(1, round(tall / 300))
    cuts = [-(-tall * k // (n_cuts * 16)) * 16 for k in range(n_cuts)] + [tall]
    cuts = list(zip(cuts[:-1], cuts[1:]))
    kept = lambda i: pltpu.make_async_copy(ring.at[lax.rem(i, 2)], u_hbm.at[device(i)], back_sem.at[lax.rem(i, 2)])

    @pl.loop(0, n_steps)
    def _(i):
        slot = lax.rem(i, 2 if wide else depth)
        if wide:
            any_lo, any_hi = next(iter(src.values()))
            pltpu.make_async_copy(any_lo, buf.at[slot, :cut, :], tok_sem.at[slot, 0]).wait()
            pltpu.make_async_copy(any_hi, buf.at[slot, cut:, :], tok_sem.at[slot, 1]).wait()

            @pl.when(i >= 2)
            def _():
                kept(i - 2).wait()
        else:
            pltpu.make_async_copy(u_hbm.at[device(i)], ring.at[slot], tok_sem.at[slot, 0]).wait()

        @pl.when(i + 1 < n_steps)
        def _():
            fetch(i + 1)

        @pl.when(i == 0)
        def _():
            for c in loads:
                c.start()

        for j, (a, b) in enumerate(zip(loads, stores)):
            @pl.when(i == min(2 + j, n_steps - 1))
            def _():
                a.wait()
                b.start()

        if wide:
            ring[slot, :n_loc, :] = buf[slot].astype(BF16)
            kept(i).start()
        rel = device(i) ^ me
        lse, lab = info_ref[rel, 0:1, :], info_ref[rel, 1:2, :]

        def group(h):
            def rows(r0, r1):
                return slice(r0, r1) if n_groups == 1 else pl.ds(pl.multiple_of(h * tall + r0, 16), r1 - r0)

            def weights(r0, r1):
                part = dot(emb_sc[rows(r0, r1), :], ring[slot], NT)
                ids = lax.broadcasted_iota(I32, (r1 - r0, 1), 0) + (pos[MINE_ID] + (s0 + h * tall + r0))
                bias = bias_ref[slice(s0 + r0, s0 + r1) if n_groups == 1 else pl.ds(pl.multiple_of(s0 + h * tall + r0, 8), r1 - r0), :]
                g = jnp.exp(part + bias - lse) - jnp.where(lab == ids.astype(F32), scale, 0.0)
                g_sc[r0:r1, :] = g.astype(BF16)

            weights(*cuts[0])
            for k, (r0, r1) in enumerate(cuts):
                if k + 1 < len(cuts):
                    weights(*cuts[k + 1])
                acc[rows(r0, r1), :] += dot(g_sc[r0:r1, :], ring[slot], NN)

        if n_groups == 1:
            group(0)
        else:
            pl.loop(0, n_groups)(group)

    for c in loads[len(puts):]:
        c.wait()
    if parts:
        acc[...] = (hold[len(puts), :m, :] + acc[...]) + hold[len(puts) + 1, :m, :]
    done = [pltpu.make_async_copy(acc, out_hbm, sem)]
    if kind in ("far", "last", "whole"):
        done.append(pltpu.make_async_copy(acc, big_ref.at[pl.ds(row(MINE, s0), m), :], emb_sem(tok_sem)))
    for c in done:
        c.start()
    if wide:
        for i in range(n_steps - 2, n_steps):
            kept(i).wait()
    for c in stores + done:
        c.wait()


def emb_sem(tok_sem):
    return tok_sem.at[0, 0]


def rows_pass(kind, scale, v_rows, span, cut, pos, emb, bias, info, tokens=None, u_all=None, big=None, parts=(), puts=()):
    s0, s1 = span
    m, e = s1 - s0, emb.shape[1]
    sds = jax.ShapeDtypeStruct
    wide = kind in ("own", "side", "far")
    final = kind in ("far", "last", "whole")
    args, aliases = [pos, emb, bias, info], {}
    outs = [sds((m, e), F32)]
    sources = None
    if wide:
        sources = {"own": (0, CORE), "side": (X, X | CORE, Y, Y | CORE), "far": (X | Y, X | Y | CORE)}[kind]
        args += [h for r in sources for h in tokens[r]]
        n_loc = tokens[0][0].shape[0] + tokens[0][1].shape[0]
        outs.append(sds((8, BLK, e), BF16))
        if kind != "own":
            aliases[len(args)] = 1
            args.append(u_all)
    else:
        n_loc = BLK
        args.append(u_all)
    if final:
        if big is not None:
            aliases[len(args)] = len(outs)
            args.append(big)
        outs.append(sds((v_rows, e), F32))
    args += [a for a, _ in parts] + [a for _, a in puts]
    n_hold = max(1, len(parts) + len(puts))
    tallest = max([m] * len(parts) + [a.shape[0] for _, a in puts] + [8])
    t = STEPS[kind] * BLK
    scratch = [pltpu.VMEM((2, n_loc, e), F32)] if wide else []
    scratch += [
        pltpu.VMEM((2 if wide else 3, BLK, e), BF16), pltpu.VMEM((m, e), BF16), pltpu.VMEM((m, BLK), BF16),
        pltpu.VMEM((m, e), F32), pltpu.VMEM((n_hold, tallest, e), F32),
        DMA, DMA((3, 2)), DMA((2,)), DMA((n_hold,)), DMA((n_hold,)),
    ]
    return pl.pallas_call(
        functools.partial(rows_kernel, kind, scale, s0, m, cut, n_loc, sources, [skip for _, skip in parts], [spot for spot, _ in puts], big is not None),
        in_specs=[SMEM, ANY, VMEM, VMEM] + [ANY] * (len(args) - 4),
        out_specs=[ANY] * len(outs),
        out_shape=outs,
        scratch_shapes=scratch,
        input_output_aliases=aliases,
        compiler_params=pltpu.CompilerParams(vmem_limit_bytes=VMEM_LIMIT),
        cost_estimate=pl.CostEstimate(flops=(4 * t * m * e) // COVER, bytes_accessed=t * e * 2 + m * e * 6, transcendentals=t * m),
    )(*args)


def put_kernel(spots, pos, *refs):
    n = len(spots)
    pieces, (out_ref, hold, in_sem, out_sem) = refs[1:1 + n], refs[1 + n:]
    loads, stores = [], []
    for j, (p, (base, off)) in enumerate(zip(pieces, spots)):
        slot = hold.at[j, :p.shape[0], :]
        loads.append(pltpu.make_async_copy(p, slot, in_sem.at[j]))
        stores.append(pltpu.make_async_copy(slot, out_ref.at[pl.ds(pl.multiple_of(pos[base] + off, 8), p.shape[0]), :], out_sem.at[j]))
    for a in loads:
        a.start()
    for a, b in zip(loads, stores):
        a.wait()
        b.start()
    for b in stores:
        b.wait()


def put_rows(pos, big, puts):
    spots, pieces = [s for s, _ in puts], [a for _, a in puts]
    n, e = len(pieces), big.shape[1]
    size = sum(p.size for p in pieces)
    return pl.pallas_call(
        functools.partial(put_kernel, spots),
        in_specs=[SMEM] + [ANY] * (n + 1),
        out_specs=ANY,
        out_shape=jax.ShapeDtypeStruct(big.shape, big.dtype),
        scratch_shapes=[pltpu.VMEM((n, max(p.shape[0] for p in pieces), e), F32), DMA((n,)), DMA((n,))],
        input_output_aliases={1: 0},
        compiler_params=pltpu.CompilerParams(vmem_limit_bytes=VMEM_LIMIT),
        cost_estimate=pl.CostEstimate(flops=(size) // COVER, bytes_accessed=size * 8, transcendentals=0),
        name="put_rows",
    )(pos, big, *pieces)


def join_kernel(n_vec, idx, *refs):
    own, mine, theirs, (dw_ref, vec_ref, full, in_sem, out_sem) = refs[0], refs[1:4], refs[4:7], refs[7:]
    vp, core = idx[0], idx[1]
    half, cols = mine[0].shape
    col = lambda k: pl.ds(pl.multiple_of((vp ^ k) * cols, cols), cols)
    row = lambda c: pl.ds(pl.multiple_of(c * half, 8), half)
    loads = [pltpu.make_async_copy(own.at[:2 * half, :], full.at[:, col(0)], in_sem.at[0])]
    for k in range(3):
        loads.append(pltpu.make_async_copy(mine[k], full.at[row(core), col(k + 1)], in_sem.at[1 + k]))
        loads.append(pltpu.make_async_copy(theirs[k], full.at[row(1 - core), col(k + 1)], in_sem.at[4 + k]))
    for c in loads:
        c.start()
    for c in loads:
        c.wait()
    e = dw_ref.shape[0]
    stores = [pltpu.make_async_copy(full.at[:e, :], dw_ref, out_sem.at[0]), pltpu.make_async_copy(full.at[e:e + n_vec, :], vec_ref, out_sem.at[1])]
    for c in stores:
        c.start()
    for c in stores:
        c.wait()


def join_pass(idx, own, mine, theirs):
    half, cols = mine[0].shape
    e = 4 * cols
    return pl.pallas_call(
        functools.partial(join_kernel, 8),
        in_specs=[SMEM] + [ANY] * 7,
        out_specs=[ANY] * 2,
        out_shape=[jax.ShapeDtypeStruct((e, e), F32), jax.ShapeDtypeStruct((8, e), F32)],
        scratch_shapes=[pltpu.VMEM((2 * half, e), F32), DMA((7,)), DMA((2,))],
        compiler_params=pltpu.CompilerParams(vmem_limit_bytes=VMEM_LIMIT),
        cost_estimate=pl.CostEstimate(flops=(e * e) // COVER, bytes_accessed=e * e * 8, transcendentals=0),
        name="join",
    )(idx, own, *mine, *theirs)


def means_kernel(width, *refs):
    (a, b, c, d), (m1_ref, m2_ref) = refs[:4], refs[4:]
    total = ((a[...] + b[...]) + (c[...] + d[...])) * (1.0 / width)
    for j, m_ref in enumerate((m1_ref, m2_ref)):
        m_ref[...] = jnp.broadcast_to(total[j:j + 1, :], (128, total.shape[1])).T


def means_pass(width, sums):
    n = sums[0].shape[1]
    return pl.pallas_call(
        functools.partial(means_kernel, width),
        in_specs=[VMEM] * 4,
        out_specs=[VMEM] * 2,
        out_shape=[jax.ShapeDtypeStruct((n, 128), F32)] * 2,
        compiler_params=pltpu.CompilerParams(vmem_limit_bytes=VMEM_LIMIT),
        cost_estimate=pl.CostEstimate(flops=(n * 256) // COVER, bytes_accessed=n * 1200, transcendentals=0),
        name="means",
    )(*sums)


def back_kernel(base, vp, *refs):
    refs = list(refs)
    srcs = [refs.pop(0) for _ in range(7)]
    gain_ref, = [refs.pop(0)]
    extra = refs[:-10]
    dab_ref, pack_ref, pre, norm, rstd, z, m1, m2, du, sem = refs[-10:]
    n, cols = du.shape
    e = z.shape[1]
    col = pl.ds(pl.multiple_of(vp[0] * cols, cols), cols)
    rows = slice(base, base + n)
    pre_h, norm_h, rstd_h, z_h, m1_h, m2_h, du_h = srcs
    loads = [pltpu.make_async_copy(a, b, sem.at[j]) for j, (a, b) in enumerate((
        (pre_h.at[rows, col], pre), (norm_h.at[rows, col], norm), (rstd_h.at[rows, :], rstd), (m1_h.at[rows, :], m1), (m2_h.at[rows, :], m2),
        (du_h, du), (z_h.at[rows, :], z)))]
    for c in loads:
        c.start()
    for c in loads:
        c.wait()
    for j, c in enumerate(range(0, cols, 128)):
        cs = slice(c, c + 128)
        a, d, normed = pre[:, cs], du[:, cs], norm[:, cs]
        cdf = 0.5 * (1.0 + lax.erf(a * (0.5 ** 0.5)))
        dg = rstd[...] * (d * gain_ref[:, cs] - m1[...] - normed * m2[...])
        da = dg * (cdf + a * (jnp.exp(-0.5 * a * a) * 0.3989422804014327))
        dab_ref[:, cs] = da.astype(BF16).astype(F32)
        for j, x in enumerate((da, d * normed, d)):
            pack_ref[e + j:e + j + 1, cs] = jnp.sum(x, axis=0, keepdims=True)
    loss_ref, db_ref = extra
    pack_ref[:e, :] = lax.dot_general(z[...], dab_ref[...].astype(BF16), (((0,), (0,)), ((), ())), preferred_element_type=F32)
    pack_ref[e + 3:e + 4, :] = jnp.broadcast_to(loss_ref[...], (1, cols))
    pack_ref[e + 4:e + 16, :] = jnp.zeros_like(pack_ref[e + 4:e + 16, :])
    n_db = db_ref.shape[1]
    pack_ref[e + 16 + n_db // cols:, :] = jnp.zeros_like(pack_ref[e + 16 + n_db // cols:, :])
    for j, c in enumerate(range(0, n_db, cols)):
        w = min(cols, n_db - c)
        pack_ref[e + 16 + j:e + 17 + j, :w] = db_ref[:, c:c + w]


def back_pass(base, vp, pre, normed, rstd, z, m1, m2, du, gain, *extra):
    n, cols = du.shape
    e = z.shape[1]
    n_pack = e + 16 + -(-extra[1].shape[1] // cols // 8) * 8
    block = lambda *s: pl.BlockSpec(s, lambda i, p: (0,) * len(s))
    gs = pltpu.PrefetchScalarGridSpec(
        num_scalar_prefetch=1,
        grid=(1,),
        in_specs=[ANY] * 7 + [pl.BlockSpec((1, cols), lambda i, p: (0, p[0]))] + [block(*x.shape) for x in extra],
        out_specs=[block(n, cols), block(n_pack, cols)],
        scratch_shapes=[pltpu.VMEM((n, cols), F32)] * 2 + [pltpu.VMEM((n, 128), F32), pltpu.VMEM((n, e), BF16)] + [pltpu.VMEM((n, 128), F32)] * 2
        + [pltpu.VMEM((n, cols), F32), DMA((7,))],
    )
    return pl.pallas_call(
        functools.partial(back_kernel, base),
        grid_spec=gs,
        out_shape=[jax.ShapeDtypeStruct((n, cols), F32), jax.ShapeDtypeStruct((n_pack, cols), F32)],
        compiler_params=pltpu.CompilerParams(dimension_semantics=("arbitrary",), vmem_limit_bytes=VMEM_LIMIT),
        cost_estimate=pl.CostEstimate(flops=(2 * n * e * cols) // COVER, bytes_accessed=n * (cols * 16 + e * 2 + 1536), transcendentals=n * cols * 2),
        name="back",
    )(vp, pre, normed, rstd, z, m1, m2, du, gain, *extra)


def spread_kernel(n_masks, vp, pos_ref, w_ref, *refs):
    pieces, (out_ref, dab, dz, obuf, in_sem, out_sem) = refs[:4], refs[4:]
    n, cols = pieces[0].shape
    col = lambda k: pl.ds(pl.multiple_of((vp[0] ^ k) * cols, cols), cols)
    loads = [pltpu.make_async_copy(p, dab.at[:, col(j)], in_sem.at[j]) for j, p in enumerate(pieces)]
    for c in loads:
        c.start()
    dz[n:, :] = jnp.zeros((dz.shape[0] - n, dz.shape[1]), F32)
    n_seq, seq_len, _ = out_ref.shape
    place = lax.broadcasted_iota(I32, (seq_len, 1), 0)
    slots = pos_ref.shape[2]
    for c in loads:
        c.wait()
    for r0, r1 in row_cuts(n):
        dz[r0:r1, :] = dot(dab[r0:r1, :].astype(BF16), w_ref[...], NT).astype(BF16).astype(F32)
    group = 8
    store = lambda b, j: pltpu.make_async_copy(obuf.at[j % 4], out_ref.at[b], out_sem.at[j % 4])

    @pl.loop(0, n_seq // group)
    def _(g):
        for j in range(group):
            b = g * group + j

            @pl.when(b >= 4)
            def _():
                store(b - 4, j).wait()

            hot = jnp.where(place == pos_ref[b], 1.0, 0.0).astype(BF16)
            base = pl.multiple_of(g * (group * n_masks), 8)
            low = j * n_masks // 8 * 8
            rows = dz[pl.ds(base + low, slots + 8), :][j * n_masks - low:j * n_masks - low + slots]
            obuf[j % 4] = dot(hot, rows.astype(BF16), NN).astype(BF16)
            store(b, j).start()

    for j in range(group - 4, group):
        store(n_seq - group + j, j).wait()


def spread_pass(n_masks, shape, vp, pos, w, pieces):
    n, cols = pieces[0].shape
    e = w.shape[0]
    return pl.pallas_call(
        functools.partial(spread_kernel, n_masks),
        in_specs=[SMEM, VMEM, VMEM] + [ANY] * 4,
        out_specs=ANY,
        out_shape=jax.ShapeDtypeStruct(shape, BF16),
        scratch_shapes=[pltpu.VMEM((n, 4 * cols), F32), pltpu.VMEM((n + 16, e), F32), pltpu.VMEM((4,) + shape[1:], BF16), DMA((4,)), DMA((4,))],
        compiler_params=pltpu.CompilerParams(vmem_limit_bytes=VMEM_LIMIT),
        cost_estimate=pl.CostEstimate(flops=(2 * shape[0] * shape[1] * 128 * e) // COVER, bytes_accessed=shape[0] * shape[1] * e * 2, transcendentals=0),
        name="spread",
    )(vp, pos, w, *pieces)


def order_sum(xs):
    return (xs[0] + xs[1]) + (xs[2] + xs[3])


def after(x, *deps):
    return lax.optimization_barrier((x, deps))[0]


def solution(mesh):
    n_groups, n_shards = mesh.shape["dp"], mesh.shape["vp"]

    def swap(a, bit):
        return lax.ppermute(a, "dp", [(d, d ^ bit) for d in range(n_groups)])

    def swap_vp(a, bit):
        return lax.ppermute(a, "vp", [(d, d ^ bit) for d in range(n_shards)])

    def hop(a):
        return lax.ppermute(a, "dp", [(d, d ^ (Y if d & CORE else X)) for d in range(n_groups)])

    def local_step(hidden, mask_pos, labels, w_trans, b_trans, ln_gain, ln_bias, emb_table, b_vocab):
        n_rows, _, width = hidden.shape
        n_masks = mask_pos.shape[1]
        shard_rows = emb_table.shape[0]
        n_loc = n_rows * n_masks
        n_tokens = n_loc * n_groups
        slots = -(-n_masks // 16) * 16
        cut = n_loc // 32 * 16
        cols = width // n_shards
        dp, vp = lax.axis_index("dp"), lax.axis_index("vp")
        row_start = vp * shard_rows
        scale = 1.0 / n_tokens
        core, mine = dp & 1, (dp >> 1 ^ dp >> 2) & 1

        pos_pad = jnp.pad(mask_pos, ((0, 0), (0, slots - n_masks)), constant_values=-1)
        z, pre, normed, rstd, u, u_lo, u_hi = head_pass(
            n_masks, cut, hidden, jnp.broadcast_to(pos_pad[:, :, None], (n_rows, slots, 128)),
            w_trans, b_trans[None], ln_gain[None], ln_bias[None])

        x_lo, y_hi = swap(u_lo, X), swap(u_hi, Y)
        x_hi, y_lo = swap(u_hi, X), swap(u_lo, Y)
        c_lo, c_hi = swap(u_lo, CORE), swap(u_hi, CORE)

        flat_labels = labels.reshape(n_loc)
        lab_local = flat_labels - row_start
        lab_local = jnp.where((lab_local >= 0) & (lab_local < shard_rows), lab_local, ELSEWHERE)
        column = lambda x: jnp.broadcast_to(x[:, None], (x.shape[0], 128))
        lab_col = column(lab_local)
        logits, stat = stats(u, emb_table, b_vocab[None], lab_col)
        all_stats = [stat] + [swap_vp(stat, b) for b in range(1, n_shards)]
        global_max = functools.reduce(jnp.maximum, [s[0] for s in all_stats])
        log_norm = global_max + jnp.log(order_sum([s[1] * jnp.exp(s[0] - global_max) for s in all_stats]))
        loss_part = jnp.sum(log_norm - order_sum([s[2] for s in all_stats]))
        lse = log_norm + jnp.log(jnp.float32(n_tokens))

        du_part, db_part, sums = du_pass(scale, n_shards, 0, logits, emb_table, column(lse), lab_col, normed, ln_gain[None])
        du_share = lax.psum_scatter(du_part.reshape(n_shards * n_loc, cols), "vp", scatter_dimension=0, tiled=True)
        lse = after(lse, du_part)
        fill = (0, BLK - n_loc)
        info = jnp.stack([jnp.pad(lse, fill, constant_values=jnp.inf), jnp.pad(flat_labels.astype(F32), fill, constant_values=-1.0)])
        near, *away = [swap(info, b) for b in (CORE, X, Y, X | Y)]
        x_lo, y_hi = after((x_lo, y_hi), du_part)
        d_lo, d_hi = swap(x_lo, Y), swap(y_hi, X)
        cx_lo, cy_hi = swap(x_lo, CORE), swap(y_hi, CORE)

        half, quarter = shard_rows // 2, shard_rows // 4
        start = lambda h, c: h * half + c * quarter
        pos = jnp.stack([dp, start(mine, core), row_start + start(mine, core), start(mine, 1 - core), start(1 - mine, core), start(1 - mine, 1 - core)])
        bias_col = lax.dynamic_slice(b_vocab, (start(mine, core),), (quarter,))[:, None]
        shares = (1088, 1280, 776)
        ends = [0]
        for w in shares[:-1]:
            ends.append(ends[-1] + max(16, quarter * w // sum(shares) // 16 * 16))
        spans = list(zip(ends, ends[1:] + [quarter]))

        def rows(kind, k, *wait, info=None, span=None, **kw):
            return rows_pass(kind, scale, shard_rows, span or spans[k], cut, after(pos, *wait), emb_table, bias_col, info, **kw)

        def send(k, chunk):
            return ((TWIN, spans[k][0]), swap(chunk, CORE)), hop(chunk)

        def forward(k, far, *wait):
            far = after(far, *wait)
            return ((FAR, spans[k][0]), far), ((FAR_TWIN, spans[k][0]), swap(far, CORE))

        tokens = {0: (u_lo, u_hi), CORE: (c_lo, c_hi), X: (x_lo, x_hi), Y: (y_lo, y_hi)}
        pair = jnp.stack([info, near])
        own, u_all = rows("own", 0, du_part, info=pair, tokens=tokens)
        x_hi, y_lo, away = after((x_hi, y_lo, away), own)
        away = jnp.stack(away)
        tokens[X | CORE] = cx_lo, swap(x_hi, CORE)
        tokens[Y | CORE] = swap(y_lo, CORE), cy_hi
        away_near = swap(away, CORE)
        tokens[X], tokens[Y] = (x_lo, x_hi), (y_lo, y_hi)
        info = jnp.concatenate([pair, jnp.stack([away, away_near], axis=1).reshape(6, 2, BLK)])

        sums = after(sums, own)
        sums = [sums] + [swap_vp(sums, b) for b in range(1, n_shards)]
        side, u_all = rows("side", 0, info=info, tokens=tokens, u_all=u_all)
        d_lo, d_hi = after((d_lo, d_hi), side)
        tokens[X | Y], tokens[X | Y | CORE] = (d_lo, d_hi), (swap(d_lo, CORE), swap(d_hi, CORE))
        m1, m2 = means_pass(width, after(sums, side))
        chunk0, u_all, big = rows("far", 0, m1, m2, info=info, tokens=tokens, u_all=u_all, parts=((own, 0), (side, 0)))
        twin0, far0 = send(0, chunk0)

        du_share = after(du_share, chunk0)
        dab, pack = back_pass(0, vp[None], pre, normed, rstd, z, m1, m2, du_share, ln_gain[None], loss_part[None, None], db_part)
        back_done = dab
        pack = lax.psum(pack, "dp")
        dab_1, dab_2 = swap_vp(dab, 1), swap_vp(dab, 2)

        chunk1, big = rows("whole", 1, back_done, info=info, u_all=u_all, big=big, puts=[twin0])
        twin1, far1 = send(1, chunk1)
        pack = after(pack, chunk1)
        n_half = (width + 16) // 2
        part = lax.dynamic_slice(pack, (core * n_half, 0), (n_half, cols))
        parts = [swap_vp(part, b) for b in range(1, n_shards)]
        far0, far_twin0 = forward(0, far0, chunk1)
        dab_2 = after(dab_2, chunk1)
        dab_3 = swap_vp(dab_2, 1)

        chunk2, big = rows("whole", 2, part, info=info, u_all=u_all, big=big, puts=[far0])
        twin2, far2 = send(2, chunk2)
        d_hidden = spread_pass(n_masks, hidden.shape, vp[None], pos_pad[:, None], w_trans, after([dab, dab_1, dab_2, dab_3], chunk2))
        far1, far_twin1 = forward(1, far1, d_hidden)
        big = put_rows(after(pos, d_hidden), big, [far_twin0, twin1, far1])
        parts = after(parts, big)
        others = [swap(p, CORE) for p in parts]
        big = put_rows(pos, big, [far_twin1, twin2])
        pack, parts, others = after((pack, parts, others), big)
        d_w, vec = join_pass(jnp.stack([vp, core]), pack, parts, others)
        db = pack[width + 16:].reshape(-1)[:shard_rows]
        loss = pack[width + 3, 0] / n_tokens
        grads = vec[0], vec[1], vec[2]
        far2, far_twin2 = forward(2, far2, big, d_w, db, loss, *grads)
        big = put_rows(pos, big, [far2])
        big = put_rows(pos, big, [far_twin2])

        return loss, d_hidden, d_w, *grads, big, db

    in_specs = (P("dp", None, None), P("dp", None), P("dp", None), P(None, None), P(None), P(None), P(None), P("vp", None), P("vp"))
    out_specs = (P(), P("dp", None, None), P(None, None), P(None), P(None), P(None), P("vp", None), P("vp"))
    return jax.shard_map(local_step, mesh=mesh, in_specs=in_specs, out_specs=out_specs, check_vma=False)
```
